32 devices in a mesh: rep: 1 (over z), kv: 32 (over y, x, core).
Axes of the slice: x: 4, y: 4, z: 1, core: 2. Of those that a mesh axis runs over, the one named last changes fastest.
The devices are a block of a 4x4x8 slice.
Arguments:
- embeds: bfloat16 [2, 2048, 2048], P(None, ('rep', 'kv'))
- w_query: bfloat16 [2, 2048, 2048], replicated
- w_key: bfloat16 [2, 2048, 256], replicated
- w_value: bfloat16 [2, 2048, 256], replicated
- w_out: bfloat16 [2, 2048, 2048], replicated
- w_up: bfloat16 [2, 2048, 11008], replicated
- w_down: bfloat16 [2, 11008, 2048], replicated
- k_pool: bfloat16 [6144, 2, 32, 2, 128], P(('rep', 'kv'))
- v_pool: bfloat16 [6144, 2, 32, 2, 128], P(('rep', 'kv'))
- new_table: int32 [2048, 2], P('rep')
- seq_lens: int32 [2048], P('rep')
- mig_src: int32 [64], P('rep')
- mig_dst: int32 [64], P('rep')
Outputs:
- output 1: bfloat16 [2, 2048, 2048], P(None, ('rep', 'kv'))
- output 2: bfloat16 [6144, 2, 32, 2, 128], P(('rep', 'kv'))
- output 3: bfloat16 [6144, 2, 32, 2, 128], P(('rep', 'kv'))
All inputs are finite; a program needn't handle non-finite values.
Results may differ from the reference program's by a relative error of at most 0.0164352.
Values are sent between devices in bfloat16 or wider.
A program may use at most 768 MiB of HBM per device.

```python
import jax
import jax.numpy as jnp
from jax import lax

D = 2048
HEADS = 16
KV_HEADS = 2
HEAD = 128
FF = 11008
PAGE = 32
LAYERS = 2
GROUP = 32
SEQ_DEV = 64
PAGES_SEQ = 2
MIG = 64
BATCH = GROUP * SEQ_DEV
SLOTS = PAGES_SEQ * SEQ_DEV + MIG


def draw_layout(layout_key):
    key_hot, key_shift, key_perm, key_rank, key_len = jax.random.split(layout_key, 5)
    hot_dev = jax.random.randint(key_hot, (), 0, GROUP)
    alt_dev = (hot_dev + GROUP // 2) % GROUP
    dev_shift = jax.random.randint(key_shift, (), 0, GROUP)
    slot_perm = jax.vmap(lambda sub_key: jax.random.permutation(sub_key, SLOTS))(jax.random.split(key_perm, GROUP))
    seq_ids = jnp.arange(BATCH)[:, None]
    page_ids = jnp.arange(PAGES_SEQ)[None, :]
    home_dev = seq_ids // SEQ_DEV
    base_dev = (home_dev + page_ids + dev_shift) % GROUP
    base_local = slot_perm[base_dev, page_ids * SEQ_DEV + seq_ids % SEQ_DEV]
    new_table = (base_dev * SLOTS + base_local).astype(jnp.int32)
    eligible = (base_dev != hot_dev) & (base_dev != alt_dev)
    is_last = jnp.broadcast_to(page_ids == PAGES_SEQ - 1, (BATCH, PAGES_SEQ))
    total_pages = BATCH * PAGES_SEQ
    rank_ids = jax.random.permutation(key_rank, total_pages).reshape(BATCH, PAGES_SEQ)
    priority = jnp.where(eligible, jnp.where(is_last, 0, total_pages), 2 * total_pages) + rank_ids
    chosen = jnp.argsort(priority.reshape(-1))[:MIG]
    entry_ids = jnp.arange(MIG)
    src_dev = jnp.where(entry_ids % 8 == 7, alt_dev, hot_dev)
    src_local = slot_perm[src_dev, PAGES_SEQ * SEQ_DEV + entry_ids]
    mig_src = (src_dev * SLOTS + src_local).astype(jnp.int32)
    mig_dst = new_table.reshape(-1)[chosen]
    len_offsets = jax.random.randint(key_len, (BATCH,), 0, PAGE - 1)
    len_offsets = len_offsets.at[0].set(PAGE - 2).at[1].set(0)
    seq_lens = ((PAGES_SEQ - 1) * PAGE + len_offsets).astype(jnp.int32)
    return new_table, seq_lens, mig_src, mig_dst


def setup_inputs(seed: int = 0, part: int = 0) -> dict:
    base_key = jax.random.key(seed)
    part_key = jax.random.fold_in(base_key, part)
    w_keys = jax.random.split(base_key, 6)
    p_keys = jax.random.split(part_key, 5)
    new_table, seq_lens, mig_src, mig_dst = draw_layout(p_keys[0])
    embeds = jax.random.normal(p_keys[1], (2, BATCH, D), jnp.float32).astype(jnp.bfloat16)
    out_scale = (PAGES_SEQ / (HEADS * HEAD)) ** 0.5
    w_query = (jax.random.normal(w_keys[0], (LAYERS, D, HEADS * HEAD), jnp.float32) * 0.5 * D ** -0.5).astype(jnp.bfloat16)
    w_key = (jax.random.normal(w_keys[1], (LAYERS, D, KV_HEADS * HEAD), jnp.float32) * D ** -0.5).astype(jnp.bfloat16)
    w_value = (jax.random.normal(w_keys[2], (LAYERS, D, KV_HEADS * HEAD), jnp.float32) * D ** -0.5).astype(jnp.bfloat16)
    w_out = (jax.random.normal(w_keys[3], (LAYERS, HEADS * HEAD, D), jnp.float32) * out_scale).astype(jnp.bfloat16)
    w_up = (jax.random.normal(w_keys[4], (LAYERS, D, FF), jnp.float32) * D ** -0.5).astype(jnp.bfloat16)
    w_down = (jax.random.normal(w_keys[5], (LAYERS, FF, D), jnp.float32) * FF ** -0.5).astype(jnp.bfloat16)
    pool_shape = (GROUP * SLOTS, LAYERS, PAGE, KV_HEADS, HEAD)
    k_pool = jax.random.normal(p_keys[2], pool_shape, jnp.float32).astype(jnp.bfloat16)
    slot_mean = jax.random.normal(p_keys[3], (GROUP * SLOTS, LAYERS, 1, KV_HEADS, HEAD), jnp.float32)
    v_pool = (0.5 * jax.random.normal(p_keys[4], pool_shape, jnp.float32) + slot_mean).astype(jnp.bfloat16)
    return {'embeds': embeds, 'w_query': w_query, 'w_key': w_key, 'w_value': w_value, 'w_out': w_out, 'w_up': w_up, 'w_down': w_down, 'k_pool': k_pool, 'v_pool': v_pool, 'new_table': new_table, 'seq_lens': seq_lens, 'mig_src': mig_src, 'mig_dst': mig_dst}


def attend_all(queries, k_layer, v_layer, new_table, seq_lens, step_idx):
    group_heads = HEADS // KV_HEADS
    positions = jnp.arange(PAGES_SEQ)[:, None] * PAGE + jnp.arange(PAGE)[None, :]

    def one_seq(args):
        q_row, row_slots, seq_len = args
        keys_f = k_layer[row_slots].astype(jnp.float32)
        vals_f = v_layer[row_slots].astype(jnp.float32)
        q_grp = q_row.astype(jnp.float32).reshape(KV_HEADS, group_heads, HEAD)
        scores = jnp.einsum('kgd,pikd->kgpi', q_grp, keys_f) * HEAD ** -0.5
        scores = jnp.where(positions <= seq_len + step_idx, scores, -jnp.inf)
        flat_scores = scores.reshape(KV_HEADS, group_heads, PAGES_SEQ * PAGE)
        probs_f = jax.nn.softmax(flat_scores, axis=-1).reshape(scores.shape)
        attn_f = jnp.einsum('kgpi,pikd->kgd', probs_f, vals_f)
        return attn_f.reshape(HEADS * HEAD).astype(jnp.bfloat16)

    return lax.map(one_seq, (queries, new_table, seq_lens))


def reference(embeds, w_query, w_key, w_value, w_out, w_up, w_down, k_pool, v_pool, new_table, seq_lens, mig_src, mig_dst):
    k_pool = k_pool.at[mig_dst].set(k_pool[mig_src]).at[mig_src].set(0)
    v_pool = v_pool.at[mig_dst].set(v_pool[mig_src]).at[mig_src].set(0)
    batch_rows = embeds.shape[1]
    step_outs = []
    for step_idx in range(2):
        hidden = embeds[step_idx]
        positions = seq_lens + step_idx
        slot_ids = jnp.take_along_axis(new_table, (positions // PAGE)[:, None], axis=1)[:, 0]
        offsets = positions % PAGE
        for layer_idx in range(LAYERS):
            queries = jnp.dot(hidden, w_query[layer_idx], preferred_element_type=jnp.float32).astype(jnp.bfloat16)
            new_keys = jnp.dot(hidden, w_key[layer_idx], preferred_element_type=jnp.float32).astype(jnp.bfloat16).reshape(batch_rows, KV_HEADS, HEAD)
            new_vals = jnp.dot(hidden, w_value[layer_idx], preferred_element_type=jnp.float32).astype(jnp.bfloat16).reshape(batch_rows, KV_HEADS, HEAD)
            k_pool = k_pool.at[slot_ids, layer_idx, offsets].set(new_keys)
            v_pool = v_pool.at[slot_ids, layer_idx, offsets].set(new_vals)
            attn_out = attend_all(queries.reshape(batch_rows, HEADS, HEAD), k_pool[:, layer_idx], v_pool[:, layer_idx], new_table, seq_lens, step_idx)
            hidden = (hidden.astype(jnp.float32) + jnp.dot(attn_out, w_out[layer_idx], preferred_element_type=jnp.float32)).astype(jnp.bfloat16)
            up_proj = jnp.dot(hidden, w_up[layer_idx], preferred_element_type=jnp.float32).astype(jnp.bfloat16)
            act_vals = jax.nn.gelu(up_proj.astype(jnp.float32), approximate=True).astype(jnp.bfloat16)
            hidden = (hidden.astype(jnp.float32) + jnp.dot(act_vals, w_down[layer_idx], preferred_element_type=jnp.float32)).astype(jnp.bfloat16)
        step_outs.append(hidden)
    return jnp.stack(step_outs), k_pool, v_pool
```

```python
import functools

import jax
import jax.numpy as jnp
from jax import lax
from jax.experimental import pallas as pl
from jax.experimental.pallas import tpu as pltpu
from jax.sharding import PartitionSpec as P

ANY = pl.BlockSpec(memory_space=pl.ANY)
SMEM = pl.BlockSpec(memory_space=pltpu.SMEM)
VMEM = pl.BlockSpec(memory_space=pltpu.VMEM)
CHUNK = 256
UNROLL = 8


def gather_pages_kernel(idx_ref, k_hbm, v_hbm, k_out, v_out, sem):
    rows = k_out.shape[0]

    def copies(i):
        slot = jnp.maximum(idx_ref[i], 0)
        return (pltpu.make_async_copy(k_hbm.at[slot], k_out.at[i], sem), pltpu.make_async_copy(v_hbm.at[slot], v_out.at[i], sem))

    @pl.loop(0, rows)
    def _(i):
        @pl.when(idx_ref[i] >= 0)
        def _():
            for copy in copies(i):
                copy.start()

        @pl.when(idx_ref[i] < 0)
        def _():
            k_out[i] = jnp.zeros(k_out.shape[1:], k_out.dtype)
            v_out[i] = jnp.zeros(v_out.shape[1:], v_out.dtype)

    @pl.loop(0, rows)
    def _(i):
        @pl.when(idx_ref[i] >= 0)
        def _():
            for copy in copies(i):
                copy.wait()


def gather_pages(idx, k_pool, v_pool):
    shape = jax.ShapeDtypeStruct((idx.shape[0],) + k_pool.shape[1:], k_pool.dtype)
    return pl.pallas_call(
        gather_pages_kernel,
        out_shape=[shape, shape],
        in_specs=[SMEM, ANY, ANY],
        out_specs=[VMEM, VMEM],
        scratch_shapes=[pltpu.SemaphoreType.DMA],
        compiler_params=pltpu.CompilerParams(vmem_limit_bytes=32 << 20),
        name="gather_pages",
    )(idx, k_pool, v_pool)


def migrate_kernel(dst_ref, src_ref, k_hbm, v_hbm, mk_hbm, mv_hbm, k_out, v_out, k_buf, v_buf, sem, fix_sem):
    slots = k_buf.shape[0]
    entries = dst_ref.shape[0]
    parts = 4
    size = slots // parts
    pairs = ((k_hbm, k_buf, k_out), (v_hbm, v_buf, v_out))

    def load(part, p):
        src, buf, _ = pairs[p]
        return pltpu.make_async_copy(src.at[pl.ds(part * size, size)], buf.at[pl.ds(part * size, size)], sem.at[p, part])

    def store(part, p):
        _, buf, dst = pairs[p]
        return pltpu.make_async_copy(buf.at[pl.ds(part * size, size)], dst.at[pl.ds(part * size, size)], sem.at[p, part])

    for part in range(parts):
        for p in range(2):
            load(part, p).start()
    for part in range(parts):
        for p in range(2):
            load(part, p).wait()

    def fixes(e):
        slot = jnp.maximum(dst_ref[e], 0)
        return (pltpu.make_async_copy(mk_hbm.at[e], k_buf.at[slot], fix_sem), pltpu.make_async_copy(mv_hbm.at[e], v_buf.at[slot], fix_sem))

    @pl.loop(0, entries)
    def _(e):
        @pl.when(dst_ref[e] >= 0)
        def _():
            for copy in fixes(e):
                copy.start()

        @pl.when(src_ref[e] >= 0)
        def _():
            slot = jnp.maximum(src_ref[e], 0)
            k_buf[slot] = jnp.zeros(k_buf.shape[1:], k_buf.dtype)
            v_buf[slot] = jnp.zeros(v_buf.shape[1:], v_buf.dtype)

    @pl.loop(0, entries)
    def _(e):
        @pl.when(dst_ref[e] >= 0)
        def _():
            for copy in fixes(e):
                copy.wait()

    for part in range(parts):
        for p in range(2):
            store(part, p).start()
    for part in range(parts):
        for p in range(2):
            store(part, p).wait()


def migrate(dst_local, src_local, k_pool, v_pool, mig_k, mig_v):
    shape = jax.ShapeDtypeStruct(k_pool.shape, k_pool.dtype)
    return pl.pallas_call(
        migrate_kernel,
        out_shape=[shape, shape],
        in_specs=[SMEM, SMEM, ANY, ANY, ANY, ANY],
        out_specs=[ANY, ANY],
        scratch_shapes=[
            pltpu.VMEM(k_pool.shape, k_pool.dtype),
            pltpu.VMEM(k_pool.shape, k_pool.dtype),
            pltpu.SemaphoreType.DMA((2, 4)),
            pltpu.SemaphoreType.DMA,
        ],
        compiler_params=pltpu.CompilerParams(vmem_limit_bytes=32 << 20),
        name="migrate",
    )(dst_local, src_local, k_pool, v_pool, mig_k, mig_v)


def decode_kernel(dims, sc_ref, x_ref, p0k_hbm, p0v_hbm, wq, wk, wv, wo, wu, wd, k_in, v_in, y_ref, k_out, v_out,
                  col_buf, row_buf, p0k, p0v, p1k, p1v, q_s, kn_s, vn_s, o_s, att, act, acc, col_sem, row_sem, page_sem, out_sem):
    rows, layers, heads, kv_heads, head_dim, page, width, ff, stride = dims
    tokens = 2 * rows
    n_col, n_row = col_buf.shape[0], row_buf.shape[0]
    n_q, n_o, n_u = heads * head_dim // CHUNK, width // CHUNK, ff // CHUNK
    col_layer = n_q + 2 + n_o + n_u
    col_total, row_total = layers * col_layer, layers * n_u
    group_heads = heads // kv_heads
    f32, bf16 = jnp.float32, jnp.bfloat16

    def col_start(g):
        @pl.when(g < col_total)
        def _():
            layer, pos = g // col_layer, g % col_layer
            slot = g % n_col

            def go(src, c):
                start = pl.multiple_of(c * CHUNK, CHUNK)
                pltpu.make_async_copy(src.at[layer, :, pl.ds(start, CHUNK)], col_buf.at[slot], col_sem.at[slot]).start()

            @pl.when(pos < n_q)
            def _():
                go(wq, pos)

            @pl.when(pos == n_q)
            def _():
                go(wk, 0)

            @pl.when(pos == n_q + 1)
            def _():
                go(wv, 0)

            @pl.when((pos >= n_q + 2) & (pos < n_q + 2 + n_o))
            def _():
                go(wo, pos - (n_q + 2))

            @pl.when(pos >= n_q + 2 + n_o)
            def _():
                go(wu, pos - (n_q + 2 + n_o))

    def row_start(g):
        @pl.when(g < row_total)
        def _():
            layer, pos = g // n_u, g % n_u
            slot = g % n_row
            start = pl.multiple_of(pos * CHUNK, CHUNK)
            pltpu.make_async_copy(wd.at[layer, pl.ds(start, CHUNK), :], row_buf.at[slot], row_sem.at[slot]).start()

    def col_take(g):
        slot = g % n_col
        pltpu.make_async_copy(wk.at[0], col_buf.at[slot], col_sem.at[slot]).wait()

        @pl.when(g > 0)
        def _():
            col_start(g + n_col - 1)

        return slot

    def row_take(g):
        slot = g % n_row
        pltpu.make_async_copy(wd.at[0, pl.ds(0, CHUNK), :], row_buf.at[slot], row_sem.at[slot]).wait()

        @pl.when(g > 0)
        def _():
            row_start(g + n_row - 1)

        return slot

    @pl.loop(0, n_q + 2)
    def _(g):
        col_start(g)

    page_copies = ((p0k_hbm, p0k), (p0v_hbm, p0v))
    for p, (src, dst) in enumerate(page_copies):
        pltpu.make_async_copy(src, dst, page_sem.at[p]).start()

    def own_pages(i):
        slot = sc_ref[0, i]
        return (pltpu.make_async_copy(k_in.at[slot], p1k.at[i], page_sem.at[2]), pltpu.make_async_copy(v_in.at[slot], p1v.at[i], page_sem.at[3]))

    @pl.loop(0, rows)
    def _(i):
        for copy in own_pages(i):
            copy.start()

    @pl.loop(n_q + 2, n_col)
    def _(g):
        col_start(g)

    @pl.loop(0, n_row)
    def _(g):
        row_start(g)

    y_ref[...] = x_ref[...]

    col_pos = lax.broadcasted_iota(jnp.int32, (2 * heads, 2 * page * kv_heads), 1)
    row_pos = lax.broadcasted_iota(jnp.int32, (2 * heads, 2 * page * kv_heads), 0)
    same_head = (col_pos % kv_heads) == (row_pos % heads) // group_heads
    limit = jnp.where(same_head, col_pos // kv_heads - row_pos // heads, 4 * page)
    page_iota = lax.broadcasted_iota(jnp.int32, (page * kv_heads, head_dim), 0)
    page_pos, page_head = page_iota // kv_heads, page_iota % kv_heads

    @pl.loop(0, layers)
    def _(layer):
        col0 = layer * col_layer

        @pl.loop(0, n_q + 2)
        def _(j):
            slot = col_take(col0 + j)
            out = jnp.dot(y_ref[...], col_buf[slot], preferred_element_type=f32).astype(bf16).astype(f32)

            def put(dst, first):
                for h in range(CHUNK // head_dim):
                    at = pl.multiple_of((first + h) * stride, 8)
                    dst[pl.ds(at, tokens), :] = out[:, h * head_dim:(h + 1) * head_dim]

            @pl.when(j < n_q)
            def _():
                put(q_s, j * (CHUNK // head_dim))

            @pl.when(j == n_q)
            def _():
                put(kn_s, 0)

            @pl.when(j == n_q + 1)
            def _():
                put(vn_s, 0)

        @pl.when(layer == 0)
        def _():
            for p, (src, dst) in enumerate(page_copies):
                pltpu.make_async_copy(src, dst, page_sem.at[p]).wait()

            @pl.loop(0, rows)
            def _(i):
                for copy in own_pages(i):
                    copy.wait()

        def attend(i):
            n = sc_ref[1, i]

            def updated(page_ref, new_ref):
                val = page_ref[i, layer].astype(f32)
                for t in range(2):
                    parts = [new_ref[pl.ds(g * stride + t * rows + i, 1), :] for g in range(kv_heads)]
                    new = parts[0]
                    for g in range(1, kv_heads):
                        new = jnp.where(page_head == g, parts[g], new)
                    val = jnp.where(page_pos == n - page + t, new, val)
                val = val.astype(bf16)
                page_ref[i, layer] = val
                return val

            keys = jnp.concatenate([p0k[i, layer], updated(p1k, kn_s)], axis=0)
            vals = jnp.concatenate([p0v[i, layer], updated(p1v, vn_s)], axis=0)
            qs = jnp.concatenate([q_s[pl.ds(t * rows + i, heads, stride=stride), :] for t in range(2)], axis=0)
            scores = lax.dot_general(qs.astype(bf16), keys, (((1,), (1,)), ((), ())), preferred_element_type=f32) * head_dim ** -0.5
            scores = jnp.where(limit <= n, scores, -jnp.inf)
            probs = jnp.exp(scores - jnp.max(scores, axis=1, keepdims=True))
            total = jnp.sum(probs, axis=1, keepdims=True)
            out = jnp.dot(probs.astype(bf16), vals, preferred_element_type=f32) / total
            for t in range(2):
                o_s[pl.ds(t * rows + i, heads, stride=stride), :] = out[t * heads:(t + 1) * heads]

        unroll = min(UNROLL, rows)

        @pl.loop(0, rows // unroll)
        def _(block):
            for u in range(unroll):
                attend(block * unroll + u)

        for h in range(heads):
            att[:, h * head_dim:(h + 1) * head_dim] = o_s[h * stride:h * stride + tokens, :].astype(bf16)

        @pl.loop(0, rows)
        def _(i):
            @pl.when(sc_ref[2, i] > 0)
            def _():
                slot = sc_ref[0, i]
                pltpu.make_async_copy(p1k.at[i, layer], k_out.at[slot, layer], out_sem).start()
                pltpu.make_async_copy(p1v.at[i, layer], v_out.at[slot, layer], out_sem).start()

        @pl.loop(0, n_o)
        def _(j):
            slot = col_take(col0 + n_q + 2 + j)
            at = pl.ds(pl.multiple_of(j * CHUNK, CHUNK), CHUNK)
            out = jnp.dot(att[...], col_buf[slot], preferred_element_type=f32)
            y_ref[:, at] = (y_ref[:, at].astype(f32) + out).astype(bf16)

        @pl.loop(0, n_u)
        def _(j):
            slot = col_take(col0 + n_q + 2 + n_o + j)
            at = pl.ds(pl.multiple_of(j * CHUNK, CHUNK), CHUNK)
            up = jnp.dot(y_ref[...], col_buf[slot], preferred_element_type=f32).astype(bf16)
            act[:, at] = jax.nn.gelu(up.astype(f32), approximate=True).astype(bf16)

        acc[...] = y_ref[...].astype(f32)

        @pl.loop(0, n_u)
        def _(j):
            slot = row_take(layer * n_u + j)
            at = pl.ds(pl.multiple_of(j * CHUNK, CHUNK), CHUNK)
            acc[...] += jnp.dot(act[:, at], row_buf[slot], preferred_element_type=f32)

        y_ref[...] = acc[...].astype(bf16)

    @pl.loop(0, rows)
    def _(i):
        @pl.when(sc_ref[2, i] > 0)
        def _():
            slot = sc_ref[0, i]
            pltpu.make_async_copy(p1k.at[i], k_out.at[slot], out_sem).wait()
            pltpu.make_async_copy(p1v.at[i], v_out.at[slot], out_sem).wait()


def decode(scalars, x, p0k, p0v, weights, k_pool, v_pool, page):
    w_query, w_key, w_value, w_out, w_up, w_down = weights
    layers, width, q_width = w_query.shape
    ff = w_up.shape[2]
    rows = x.shape[0] // 2
    page_rows, head_dim = k_pool.shape[2:]
    kv_heads = w_key.shape[2] // head_dim
    heads = q_width // head_dim
    tokens = 2 * rows
    stride = tokens + 8
    dims = (rows, layers, heads, kv_heads, head_dim, page, width, ff, stride)
    f32, bf16 = jnp.float32, jnp.bfloat16
    n_col = n_row = 12
    pool_shape = jax.ShapeDtypeStruct(k_pool.shape, k_pool.dtype)
    page_buf = pltpu.VMEM((rows, layers, page_rows, head_dim), bf16)
    weight_bytes = 2 * sum(w.size for w in weights)
    return pl.pallas_call(
        functools.partial(decode_kernel, dims),
        out_shape=[jax.ShapeDtypeStruct(x.shape, x.dtype), pool_shape, pool_shape],
        in_specs=[SMEM, VMEM] + [ANY] * 10,
        out_specs=[VMEM, ANY, ANY],
        input_output_aliases={10: 1, 11: 2},
        scratch_shapes=[
            pltpu.VMEM((n_col, width, CHUNK), bf16),
            pltpu.VMEM((n_row, CHUNK, width), bf16),
            page_buf, page_buf, page_buf, page_buf,
            pltpu.VMEM((heads * stride, head_dim), f32),
            pltpu.VMEM((kv_heads * stride, head_dim), f32),
            pltpu.VMEM((kv_heads * stride, head_dim), f32),
            pltpu.VMEM((heads * stride, head_dim), f32),
            pltpu.VMEM((tokens, q_width), bf16),
            pltpu.VMEM((tokens, ff), bf16),
            pltpu.VMEM((tokens, width), f32),
            pltpu.SemaphoreType.DMA((n_col,)),
            pltpu.SemaphoreType.DMA((n_row,)),
            pltpu.SemaphoreType.DMA((4,)),
            pltpu.SemaphoreType.DMA,
        ],
        compiler_params=pltpu.CompilerParams(vmem_limit_bytes=62 << 20),
        cost_estimate=pl.CostEstimate(flops=weight_bytes * tokens, bytes_accessed=weight_bytes, transcendentals=0),
        name="decode",
    )(scalars, x, p0k, p0v, *weights, k_pool, v_pool)


def rotate(arrays, shift, group_size):
    def branch(r):
        perm = [(i, (i + r) % group_size) for i in range(group_size)]
        return lambda args: tuple(lax.ppermute(a, 'kv', perm) for a in args) if r else args
    return lax.switch(shift, [branch(r) for r in range(group_size)], tuple(arrays))


def solution(mesh):
    group_size = mesh.shape['kv']
    pool_spec = P(('rep', 'kv'))
    tok_spec = P(None, ('rep', 'kv'), None)

    def device_fn(embeds, w_query, w_key, w_value, w_out, w_up, w_down, k_pool5, v_pool5, new_table, seq_lens, mig_src, mig_dst):
        me = lax.axis_index('kv')
        slots, layers, page, kv_heads, head_dim = k_pool5.shape
        rows, width = embeds.shape[1:]
        weights = (w_query, w_key, w_value, w_out, w_up, w_down)
        k_pool = k_pool5.reshape(slots, layers, page * kv_heads, head_dim)
        v_pool = v_pool5.reshape(slots, layers, page * kv_heads, head_dim)

        def local(ids):
            loc = ids - me * slots
            return jnp.where((loc >= 0) & (loc < slots), loc, -1)

        first_new, last_new = new_table[:, 0], new_table[:, 1]
        moved = first_new[None, :] == mig_dst[:, None]
        first_old = jnp.where(jnp.any(moved, axis=0), jnp.sum(jnp.where(moved, mig_src[:, None], 0), axis=0), first_new)
        home = jnp.arange(first_new.shape[0], dtype=jnp.int32) // rows
        worker = last_new // slots
        shift_of = (worker - home + group_size) % group_size
        first_dev = first_old // slots
        first_shift = (worker - first_dev + group_size) % group_size
        shift_ids = jnp.arange(group_size, dtype=jnp.int32)
        wanted = jnp.any(shift_of[None, :] == shift_ids[:, None], axis=1)

        mig_k, mig_v = gather_pages(local(mig_src), k_pool, v_pool)
        mig_k, mig_v = lax.psum((mig_k, mig_v), 'kv')

        def take(vec, dev):
            return lax.dynamic_slice(vec, (dev * rows,), (rows,))

        def first_pages(shift, shift2, got_k, got_v):
            dest = (me + shift2) % group_size
            src_home = (dest - shift + group_size) % group_size
            slot = jnp.clip(take(first_old, src_home) - me * slots, 0, slots - 1)
            pk, pv = gather_pages(slot, k_pool, v_pool)
            pk, pv = rotate((pk, pv), shift2, group_size)
            if got_k is None:
                return pk, pv
            mine = (take(first_shift, (me - shift + group_size) % group_size) == shift2)[:, None, None, None]
            return jnp.where(mine, pk, got_k), jnp.where(mine, pv, got_v)

        def one_round(shift, y, k_new, v_new):
            src_home = (me - shift + group_size) % group_size
            in_round = shift_of == shift
            wanted2 = jnp.any(in_round[None, :] & (first_shift[None, :] == shift_ids[:, None]), axis=1)
            (x,) = rotate((embeds.reshape(2 * rows, width),), shift, group_size)
            first2 = jnp.argmax(wanted2).astype(jnp.int32)
            pk, pv = first_pages(shift, first2, None, None)

            def more(state):
                left, pk, pv = state
                shift2 = jnp.argmax(left).astype(jnp.int32)
                pk, pv = first_pages(shift, shift2, pk, pv)
                return left & (shift_ids != shift2), pk, pv

            _, pk, pv = lax.while_loop(lambda state: jnp.any(state[0]), more, (wanted2 & (shift_ids != first2), pk, pv))
            valid = take(shift_of, src_home) == shift
            slot = jnp.clip(take(last_new, src_home) - me * slots, 0, slots - 1)
            scalars = jnp.stack([slot, take(seq_lens, src_home), valid.astype(jnp.int32)])
            out, k_new, v_new = decode(scalars, x, pk, pv, weights, k_new, v_new, page)
            (back,) = rotate((out,), (group_size - shift) % group_size, group_size)
            back = back.reshape(2, rows, width)
            if y is not None:
                mine = (take(shift_of, me) == shift)[None, :, None]
                back = jnp.where(mine, back, y)
            return back, k_new, v_new

        k_new, v_new = migrate(local(mig_dst), local(mig_src), k_pool, v_pool, mig_k, mig_v)
        first = jnp.argmax(wanted).astype(jnp.int32)
        y, k_new, v_new = one_round(first, None, k_new, v_new)

        def more_rounds(state):
            left, y, k_new, v_new = state
            shift = jnp.argmax(left).astype(jnp.int32)
            y, k_new, v_new = one_round(shift, y, k_new, v_new)
            return left & (shift_ids != shift), y, k_new, v_new

        _, y, k_new, v_new = lax.while_loop(lambda state: jnp.any(state[0]), more_rounds, (wanted & (shift_ids != first), y, k_new, v_new))
        return y, k_new.reshape(k_pool5.shape), v_new.reshape(v_pool5.shape)

    return jax.shard_map(device_fn, mesh=mesh, in_specs=(tok_spec, P(), P(), P(), P(), P(), P(), pool_spec, pool_spec, P('rep', None), P('rep'), P('rep'), P('rep')), out_specs=(tok_spec, pool_spec, pool_spec), check_vma=False)
```

```python
import functools
import math

import jax
import jax.numpy as jnp
from jax import lax
from jax.experimental import pallas as pl
from jax.experimental.pallas import tpu as pltpu
from jax.sharding import PartitionSpec as P

ANY = pl.BlockSpec(memory_space=pl.ANY)
SMEM = pl.BlockSpec(memory_space=pltpu.SMEM)
VMEM = pl.BlockSpec(memory_space=pltpu.VMEM)
CHUNK = 256
UNROLL = 8


def gather_pages_kernel(idx_ref, k_hbm, v_hbm, k_out, v_out, sem):
    rows = k_out.shape[0]

    @pl.loop(0, rows)
    def _(i):
        pltpu.make_async_copy(k_hbm.at[idx_ref[i]], k_out.at[i], sem).start()
        pltpu.make_async_copy(v_hbm.at[idx_ref[i]], v_out.at[i], sem).start()

    pltpu.make_async_copy(k_hbm.at[pl.ds(0, rows)], k_out, sem).wait()
    pltpu.make_async_copy(v_hbm.at[pl.ds(0, rows)], v_out, sem).wait()


def gather_pages(idx, k_pool, v_pool):
    shape = jax.ShapeDtypeStruct((idx.shape[0],) + k_pool.shape[1:], k_pool.dtype)
    return pl.pallas_call(
        gather_pages_kernel,
        out_shape=[shape, shape],
        in_specs=[SMEM, ANY, ANY],
        out_specs=[VMEM, VMEM],
        scratch_shapes=[pltpu.SemaphoreType.DMA],
        compiler_params=pltpu.CompilerParams(vmem_limit_bytes=60 << 20),
        name="gather_pages",
    )(idx, k_pool, v_pool)


def gather_migrated_kernel(idx_ref, k_hbm, v_hbm, out, sem):
    layers, units = out.shape[:2]
    entries = units // 2

    def copies(e):
        slot = jnp.maximum(idx_ref[e], 0)
        return [pltpu.make_async_copy(src.at[slot, l], out.at[l, p * entries + e], sem) for l in range(layers) for p, src in enumerate((k_hbm, v_hbm))]

    @pl.loop(0, entries)
    def _(e):
        @pl.when(idx_ref[e] >= 0)
        def _():
            for copy in copies(e):
                copy.start()

        @pl.when(idx_ref[e] < 0)
        def _():
            for l in range(layers):
                for p in range(2):
                    out[l, p * entries + e] = jnp.zeros(out.shape[2:], out.dtype)

    @pl.loop(0, entries)
    def _(e):
        @pl.when(idx_ref[e] >= 0)
        def _():
            for copy in copies(e):
                copy.wait()


def gather_migrated(idx, k_pool, v_pool):
    layers, page_rows, head_dim = k_pool.shape[1:]
    return pl.pallas_call(
        gather_migrated_kernel,
        out_shape=jax.ShapeDtypeStruct((layers, 2 * idx.shape[0], page_rows, head_dim), k_pool.dtype),
        in_specs=[SMEM, ANY, ANY],
        out_specs=VMEM,
        scratch_shapes=[pltpu.SemaphoreType.DMA],
        compiler_params=pltpu.CompilerParams(vmem_limit_bytes=60 << 20),
        name="gather_migrated",
    )(idx, k_pool, v_pool)


def share_kernel(side, in_hbm, out, work, core_buf, ring_buf, load_sem, send_sem, recv_sem):
    layers, units = out.shape[:2]
    half = units // 2
    stream = half // 4
    me = lax.axis_index('kv')
    core, x, y = me % 2, me // 2 % side, me // (2 * side)

    def pairings(pos, stride):
        return (((pos + 1) // 2 % 2, me + (1 - 2 * (pos % 2)) * stride), (pos // 2, me + (side - 1 - 2 * pos) * stride))

    x_pairs, y_pairs = pairings(x, 2), pairings(y, 2 * side)
    orders = [x_pairs + y_pairs, x_pairs[::-1] + y_pairs[::-1], y_pairs + x_pairs, y_pairs[::-1] + x_pairs[::-1]]
    partner = me + 1 - 2 * core
    barrier = pltpu.get_barrier_semaphore()

    def send(src, dst, step, lane, dev):
        copy = pltpu.make_async_remote_copy(src, dst, send_sem.at[step, lane], recv_sem.at[step, lane], device_id={'kv': dev})
        copy.start()
        return copy

    def add(dst_at, buf, src_at, count):
        @pl.loop(0, count)
        def _(u):
            for l in range(layers):
                work[l, dst_at + u] = work[l, dst_at + u] + buf[l, src_at + u]

    def part(ref, at, count):
        return ref.at[:, pl.ds(at, count)]

    base, other = core * half, (1 - core) * half
    loads = [pltpu.make_async_copy(part(in_hbm, at, half), part(work, at, half), load_sem.at[i]) for i, at in enumerate((other, base))]
    for load in loads:
        load.start()
    peers = [partner] + [dev for _, dev in x_pairs + y_pairs]
    for dev in peers:
        pl.semaphore_signal(barrier, inc=1, device_id={'kv': dev})
    pl.semaphore_wait(barrier, len(peers))
    loads[0].wait()
    copy = send(part(work, other, half), core_buf, 0, 0, partner)
    loads[1].wait()
    copy.wait()
    add(base, core_buf, 0, half)

    held = [base + k * stream for k in range(4)]
    size = stream
    path = []
    for step in range(4):
        size = size // 2
        copies = []
        for k in range(4):
            bit, dev = orders[k][step]
            copies.append(send(part(work, held[k] + (1 - bit) * size, size), part(ring_buf, k * stream + stream - 2 * size, size), 1 + step, k, dev))
        for k in range(4):
            bit, _ = orders[k][step]
            copies[k].wait()
            held[k] = held[k] + bit * size
            add(held[k], ring_buf, k * stream + stream - 2 * size, size)
        path.append(list(held))

    for k in range(4):
        for l in range(layers):
            for u in range(size):
                out[l, held[k] + u] = work[l, held[k] + u]

    for step in range(3, -1, -1):
        copies = []
        for k in range(4):
            _, dev = orders[k][step]
            at = part(out, path[step][k], size)
            copies.append(send(at, at, 8 - step, k, dev))
        for k in range(4):
            copies[k].wait()
        size = 2 * size

    at = part(out, base, half)
    send(at, at, 9, 0, partner).wait()


def share(mig, side):
    layers, units = mig.shape[:2]
    return pl.pallas_call(
        functools.partial(share_kernel, side),
        out_shape=jax.ShapeDtypeStruct(mig.shape, mig.dtype),
        in_specs=[ANY],
        out_specs=VMEM,
        scratch_shapes=[
            pltpu.VMEM(mig.shape, mig.dtype),
            pltpu.VMEM((layers, units // 2) + mig.shape[2:], mig.dtype),
            pltpu.VMEM((layers, units // 2) + mig.shape[2:], mig.dtype),
            pltpu.SemaphoreType.DMA((2,)),
            pltpu.SemaphoreType.DMA((10, 4)),
            pltpu.SemaphoreType.DMA((10, 4)),
        ],
        compiler_params=pltpu.CompilerParams(collective_id=0, has_side_effects=True, vmem_limit_bytes=60 << 20),
        name="share",
    )(mig)


def migrate_kernel(dst_ref, src_ref, k_hbm, v_hbm, mig_hbm, k_out, v_out, k_buf, v_buf, sem, fix_sem):
    slots = k_buf.shape[0]
    entries = dst_ref.shape[0]
    parts = 4
    size = slots // parts
    pairs = ((k_hbm, k_buf, k_out), (v_hbm, v_buf, v_out))

    def load(part, p):
        src, buf, _ = pairs[p]
        return pltpu.make_async_copy(src.at[pl.ds(part * size, size)], buf.at[pl.ds(part * size, size)], sem.at[p, part])

    def store(part, p):
        _, buf, dst = pairs[p]
        return pltpu.make_async_copy(buf.at[pl.ds(part * size, size)], dst.at[pl.ds(part * size, size)], sem.at[p, part])

    for part in range(parts):
        for p in range(2):
            load(part, p).start()
    for part in range(parts):
        for p in range(2):
            load(part, p).wait()

    def fixes(e):
        slot = jnp.maximum(dst_ref[e], 0)
        return [pltpu.make_async_copy(mig_hbm.at[l, p * entries + e], buf.at[slot, l], fix_sem) for l in range(mig_hbm.shape[0]) for p, buf in enumerate((k_buf, v_buf))]

    @pl.loop(0, entries)
    def _(e):
        @pl.when(dst_ref[e] >= 0)
        def _():
            for copy in fixes(e):
                copy.start()

        @pl.when(src_ref[e] >= 0)
        def _():
            slot = jnp.maximum(src_ref[e], 0)
            k_buf[slot] = jnp.zeros(k_buf.shape[1:], k_buf.dtype)
            v_buf[slot] = jnp.zeros(v_buf.shape[1:], v_buf.dtype)

    @pl.loop(0, entries)
    def _(e):
        @pl.when(dst_ref[e] >= 0)
        def _():
            for copy in fixes(e):
                copy.wait()

    for part in range(parts):
        for p in range(2):
            store(part, p).start()
    for part in range(parts):
        for p in range(2):
            store(part, p).wait()


def migrate(dst_local, src_local, k_pool, v_pool, mig):
    shape = jax.ShapeDtypeStruct(k_pool.shape, k_pool.dtype)
    return pl.pallas_call(
        migrate_kernel,
        out_shape=[shape, shape],
        in_specs=[SMEM, SMEM, ANY, ANY, ANY],
        out_specs=[ANY, ANY],
        scratch_shapes=[
            pltpu.VMEM(k_pool.shape, k_pool.dtype),
            pltpu.VMEM(k_pool.shape, k_pool.dtype),
            pltpu.SemaphoreType.DMA((2, 4)),
            pltpu.SemaphoreType.DMA,
        ],
        compiler_params=pltpu.CompilerParams(vmem_limit_bytes=60 << 20),
        name="migrate",
    )(dst_local, src_local, k_pool, v_pool, mig)


def decode_kernel(dims, sc_ref, x_ref, p0k_hbm, p0v_hbm, wq, wk, wv, wo, wu, wd, k_in, v_in, y_ref, k_out, v_out,
                  col_buf, row_buf, p0k, p0v, p1k, p1v, q_s, kn_s, vn_s, o_s, att, act, acc, col_sem, row_sem, page_sem, out_sem):
    rows, layers, heads, kv_heads, head_dim, page, width, ff, stride = dims
    tokens = 2 * rows
    n_col, n_row = col_buf.shape[0], row_buf.shape[0]
    n_q, n_o, n_u = heads * head_dim // CHUNK, width // CHUNK, ff // CHUNK
    col_layer = n_q + 2 + n_o + n_u
    col_total, row_total = layers * col_layer, layers * n_u
    group_heads = heads // kv_heads
    f32, bf16 = jnp.float32, jnp.bfloat16

    def layer_of(g, per_layer):
        return sum((g >= per_layer * l).astype(jnp.int32) for l in range(1, layers))

    def col_start(g):
        @pl.when(g < col_total)
        def _():
            layer = layer_of(g, col_layer)
            pos = g - layer * col_layer
            slot = g % n_col

            def go(src, c):
                start = pl.multiple_of(c * CHUNK, CHUNK)
                pltpu.make_async_copy(src.at[layer, :, pl.ds(start, CHUNK)], col_buf.at[slot], col_sem.at[slot]).start()

            @pl.when(pos < n_q)
            def _():
                go(wq, pos)

            @pl.when(pos == n_q)
            def _():
                go(wk, 0)

            @pl.when(pos == n_q + 1)
            def _():
                go(wv, 0)

            @pl.when((pos >= n_q + 2) & (pos < n_q + 2 + n_o))
            def _():
                go(wo, pos - (n_q + 2))

            @pl.when(pos >= n_q + 2 + n_o)
            def _():
                go(wu, pos - (n_q + 2 + n_o))

    def row_start(g):
        @pl.when(g < row_total)
        def _():
            layer = layer_of(g, n_u)
            slot = g % n_row
            start = pl.multiple_of((g - layer * n_u) * CHUNK, CHUNK)
            pltpu.make_async_copy(wd.at[layer, pl.ds(start, CHUNK), :], row_buf.at[slot], row_sem.at[slot]).start()

    def with_cols(g, count, body):
        slots = [(g + u) % n_col for u in range(count)]
        for slot in slots:
            pltpu.make_async_copy(wk.at[0], col_buf.at[slot], col_sem.at[slot]).wait()
        body([col_buf.at[slot] for slot in slots])
        for u in range(count):
            col_start(g + u + n_col)

    def with_rows(g, count, body):
        slots = [(g + u) % n_row for u in range(count)]
        for slot in slots:
            pltpu.make_async_copy(wd.at[0, pl.ds(0, CHUNK), :], row_buf.at[slot], row_sem.at[slot]).wait()
        body([row_buf.at[slot] for slot in slots])
        for u in range(count):
            row_start(g + u + n_row)

    @pl.loop(0, n_q + 2)
    def _(g):
        col_start(g)

    page_copies = ((p0k_hbm, p0k), (p0v_hbm, p0v))
    for p, (src, dst) in enumerate(page_copies):
        pltpu.make_async_copy(src, dst, page_sem.at[p]).start()

    def own_pages(i):
        slot = sc_ref[0, i]
        return (pltpu.make_async_copy(k_in.at[slot], p1k.at[i], page_sem.at[2]), pltpu.make_async_copy(v_in.at[slot], p1v.at[i], page_sem.at[3]))

    @pl.loop(0, rows)
    def _(i):
        for copy in own_pages(i):
            copy.start()

    @pl.loop(n_q + 2, n_col)
    def _(g):
        col_start(g)

    @pl.loop(0, n_row)
    def _(g):
        row_start(g)

    y_ref[...] = x_ref[...]

    col_pos = lax.broadcasted_iota(jnp.int32, (2 * heads, 2 * page * kv_heads), 1)
    row_pos = lax.broadcasted_iota(jnp.int32, (2 * heads, 2 * page * kv_heads), 0)
    same_head = (col_pos % kv_heads) == (row_pos % heads) // group_heads
    limit = jnp.where(same_head, col_pos // kv_heads - row_pos // heads, 4 * page)
    page_iota = lax.broadcasted_iota(jnp.int32, (page * kv_heads, head_dim), 0)
    page_pos = page_iota // kv_heads
    tile_head = lax.broadcasted_iota(jnp.int32, (8, head_dim), 0) % kv_heads

    @pl.loop(0, layers)
    def _(layer):
        col0 = layer * col_layer

        def project(ref):
            return jnp.dot(y_ref[...], ref[...], preferred_element_type=f32).astype(bf16).astype(f32)

        def put(dst, first, out):
            for h in range(CHUNK // head_dim):
                at = pl.multiple_of((first + h) * stride, 8)
                dst[pl.ds(at, tokens), :] = out[:, h * head_dim:(h + 1) * head_dim]

        @pl.loop(0, n_q // 2)
        def _(j):
            def body(refs):
                outs = [project(ref) for ref in refs]
                for u in range(2):
                    put(q_s, (2 * j + u) * (CHUNK // head_dim), outs[u])

            with_cols(col0 + 2 * j, 2, body)

        def body(refs):
            outs = [project(ref) for ref in refs]
            put(kn_s, 0, outs[0])
            put(vn_s, 0, outs[1])

        with_cols(col0 + n_q, 2, body)

        @pl.when(layer == 0)
        def _():
            for p, (src, dst) in enumerate(page_copies):
                pltpu.make_async_copy(src, dst, page_sem.at[p]).wait()

            @pl.loop(0, rows)
            def _(i):
                for copy in own_pages(i):
                    copy.wait()

        def attend(first):
            ids = [first + u for u in range(unroll)]
            scores, vals = [], []
            for i in ids:
                n = sc_ref[1, i]
                hits = [page_pos == n - page + t for t in range(2)]

                def updated(page_ref, new_ref):
                    val = page_ref[i, layer].astype(f32)
                    for t in range(2):
                        parts = [new_ref[pl.ds(g * stride + t * rows + i, 1), :] for g in range(kv_heads)]
                        new = jnp.broadcast_to(parts[0], (8, head_dim))
                        for g in range(1, kv_heads):
                            new = jnp.where(tile_head == g, parts[g], new)
                        val = jnp.where(hits[t], jnp.concatenate([new] * (page * kv_heads // 8), axis=0), val)
                    val = val.astype(bf16)
                    page_ref[i, layer] = val
                    return val

                keys = jnp.concatenate([p0k[i, layer], updated(p1k, kn_s)], axis=0)
                vals.append(updated(p1v, vn_s))
                qs = jnp.concatenate([q_s[pl.ds(t * rows + i, heads, stride=stride), :] for t in range(2)], axis=0)
                score = lax.dot_general(qs.astype(bf16), keys, (((1,), (1,)), ((), ())), preferred_element_type=f32) * head_dim ** -0.5
                scores.append(jnp.where(limit <= n, score, -jnp.inf))
            tops = [jnp.max(score, axis=1, keepdims=True) for score in scores]
            probs = [jnp.exp(score - top) for score, top in zip(scores, tops)]
            totals = [jnp.sum(prob, axis=1, keepdims=True) for prob in probs]
            for u, i in enumerate(ids):
                both = jnp.concatenate([p0v[i, layer], vals[u]], axis=0)
                out = jnp.dot(probs[u].astype(bf16), both, preferred_element_type=f32) / totals[u]
                for t in range(2):
                    o_s[pl.ds(t * rows + i, heads, stride=stride), :] = out[t * heads:(t + 1) * heads]

        unroll = min(UNROLL, rows)

        @pl.loop(0, rows // unroll)
        def _(block):
            attend(block * unroll)

        for h in range(heads):
            att[:, h * head_dim:(h + 1) * head_dim] = o_s[h * stride:h * stride + tokens, :].astype(bf16)

        @pl.loop(0, rows)
        def _(i):
            @pl.when(sc_ref[2, i] > 0)
            def _():
                slot = sc_ref[0, i]
                pltpu.make_async_copy(p1k.at[i, layer], k_out.at[slot, layer], out_sem).start()
                pltpu.make_async_copy(p1v.at[i, layer], v_out.at[slot, layer], out_sem).start()

        def span(j, count=1):
            return pl.ds(pl.multiple_of(j * CHUNK, CHUNK), count * CHUNK)

        @pl.loop(0, n_o // 2)
        def _(j):
            def body(refs):
                outs = [jnp.dot(att[...], ref[...], preferred_element_type=f32) for ref in refs]
                for u in range(2):
                    at = span(2 * j + u)
                    y_ref[:, at] = (y_ref[:, at].astype(f32) + outs[u]).astype(bf16)

            with_cols(col0 + n_q + 2 + 2 * j, 2, body)

        def up(first, count):
            def body(refs):
                ups = [jnp.dot(y_ref[...], ref[...], preferred_element_type=f32) for ref in refs]
                for u in range(count):
                    act[:, span(first + u)] = jax.nn.gelu(ups[u].astype(bf16).astype(f32), approximate=True).astype(bf16)

            with_cols(col0 + n_q + 2 + n_o + first, count, body)

        @pl.loop(0, n_u // 2)
        def _(j):
            up(2 * j, 2)

        if n_u % 2:
            up(n_u - 1, 1)

        acc[...] = y_ref[...].astype(f32)

        def down(first, count):
            def body(refs):
                out = acc[...]
                for u in range(count):
                    out += jnp.dot(act[:, span(first + u)], refs[u][...], preferred_element_type=f32)
                acc[...] = out

            with_rows(layer * n_u + first, count, body)

        @pl.loop(0, n_u // 2)
        def _(j):
            down(2 * j, 2)

        if n_u % 2:
            down(n_u - 1, 1)

        y_ref[...] = acc[...].astype(bf16)

    @pl.loop(0, rows)
    def _(i):
        @pl.when(sc_ref[2, i] > 0)
        def _():
            slot = sc_ref[0, i]
            pltpu.make_async_copy(p1k.at[i], k_out.at[slot], out_sem).wait()
            pltpu.make_async_copy(p1v.at[i], v_out.at[slot], out_sem).wait()


def decode(scalars, x, p0k, p0v, weights, k_pool, v_pool, page):
    w_query, w_key, w_value, w_out, w_up, w_down = weights
    layers, width, q_width = w_query.shape
    ff = w_up.shape[2]
    rows = x.shape[0] // 2
    page_rows, head_dim = k_pool.shape[2:]
    kv_heads = w_key.shape[2] // head_dim
    heads = q_width // head_dim
    tokens = 2 * rows
    stride = tokens + 8
    dims = (rows, layers, heads, kv_heads, head_dim, page, width, ff, stride)
    f32, bf16 = jnp.float32, jnp.bfloat16
    n_col = n_row = 16
    pool_shape = jax.ShapeDtypeStruct(k_pool.shape, k_pool.dtype)
    page_buf = pltpu.VMEM((rows, layers, page_rows, head_dim), bf16)
    weight_bytes = 2 * sum(w.size for w in weights)
    return pl.pallas_call(
        functools.partial(decode_kernel, dims),
        out_shape=[jax.ShapeDtypeStruct(x.shape, x.dtype), pool_shape, pool_shape],
        in_specs=[SMEM, VMEM] + [ANY] * 10,
        out_specs=[VMEM, ANY, ANY],
        input_output_aliases={10: 1, 11: 2},
        scratch_shapes=[
            pltpu.VMEM((n_col, width, CHUNK), bf16),
            pltpu.VMEM((n_row, CHUNK, width), bf16),
            page_buf, page_buf, page_buf, page_buf,
            pltpu.VMEM((heads * stride, head_dim), f32),
            pltpu.VMEM((kv_heads * stride, head_dim), f32),
            pltpu.VMEM((kv_heads * stride, head_dim), f32),
            pltpu.VMEM((heads * stride, head_dim), f32),
            pltpu.VMEM((tokens, q_width), bf16),
            pltpu.VMEM((tokens, ff), bf16),
            pltpu.VMEM((tokens, width), f32),
            pltpu.SemaphoreType.DMA((n_col,)),
            pltpu.SemaphoreType.DMA((n_row,)),
            pltpu.SemaphoreType.DMA((4,)),
            pltpu.SemaphoreType.DMA,
        ],
        compiler_params=pltpu.CompilerParams(vmem_limit_bytes=62 << 20),
        cost_estimate=pl.CostEstimate(flops=weight_bytes * tokens, bytes_accessed=weight_bytes, transcendentals=0),
        name="decode",
    )(scalars, x, p0k, p0v, *weights, k_pool, v_pool)


def rotate(arrays, shift, group_size):
    def branch(r):
        perm = [(i, (i + r) % group_size) for i in range(group_size)]
        return lambda args: tuple(lax.ppermute(a, 'kv', perm) for a in args) if r else args
    return lax.switch(shift, [branch(r) for r in range(group_size)], tuple(arrays))


def solution(mesh):
    group_size = mesh.shape['kv']
    side = math.isqrt(group_size // 2)
    pool_spec = P(('rep', 'kv'))
    tok_spec = P(None, ('rep', 'kv'), None)

    def device_fn(embeds, w_query, w_key, w_value, w_out, w_up, w_down, k_pool5, v_pool5, new_table, seq_lens, mig_src, mig_dst):
        me = lax.axis_index('kv')
        slots, layers, page, kv_heads, head_dim = k_pool5.shape
        rows, width = embeds.shape[1:]
        weights = (w_query, w_key, w_value, w_out, w_up, w_down)
        k_pool = k_pool5.reshape(slots, layers, page * kv_heads, head_dim)
        v_pool = v_pool5.reshape(slots, layers, page * kv_heads, head_dim)

        def local(ids):
            loc = ids - me * slots
            return jnp.where((loc >= 0) & (loc < slots), loc, -1)

        first_new, last_new = new_table[:, 0], new_table[:, 1]
        moved = first_new[None, :] == mig_dst[:, None]
        first_old = jnp.where(jnp.any(moved, axis=0), jnp.sum(jnp.where(moved, mig_src[:, None], 0), axis=0), first_new)
        home = jnp.arange(first_new.shape[0], dtype=jnp.int32) // rows
        worker = last_new // slots
        shift_of = (worker - home + group_size) % group_size
        first_dev = first_old // slots
        first_shift = (worker - first_dev + group_size) % group_size
        shift_ids = jnp.arange(group_size, dtype=jnp.int32)
        wanted = jnp.any(shift_of[None, :] == shift_ids[:, None], axis=1)

        mig = share(gather_migrated(local(mig_src), k_pool, v_pool), side)

        def take(vec, dev):
            return lax.dynamic_slice(vec, (dev * rows,), (rows,))

        def first_pages(shift, shift2, got_k, got_v):
            dest = (me + shift2) % group_size
            src_home = (dest - shift + group_size) % group_size
            slot = jnp.clip(take(first_old, src_home) - me * slots, 0, slots - 1)
            pk, pv = gather_pages(slot, k_pool, v_pool)
            pk, pv = rotate((pk, pv), shift2, group_size)
            if got_k is None:
                return pk, pv
            mine = (take(first_shift, (me - shift + group_size) % group_size) == shift2)[:, None, None, None]
            return jnp.where(mine, pk, got_k), jnp.where(mine, pv, got_v)

        def one_round(shift, y, k_new, v_new):
            src_home = (me - shift + group_size) % group_size
            in_round = shift_of == shift
            wanted2 = jnp.any(in_round[None, :] & (first_shift[None, :] == shift_ids[:, None]), axis=1)
            (x,) = rotate((embeds.reshape(2 * rows, width),), shift, group_size)
            first2 = jnp.argmax(wanted2).astype(jnp.int32)
            pk, pv = first_pages(shift, first2, None, None)

            def more(state):
                left, pk, pv = state
                shift2 = jnp.argmax(left).astype(jnp.int32)
                pk, pv = first_pages(shift, shift2, pk, pv)
                return left & (shift_ids != shift2), pk, pv

            _, pk, pv = lax.while_loop(lambda state: jnp.any(state[0]), more, (wanted2 & (shift_ids != first2), pk, pv))
            valid = take(shift_of, src_home) == shift
            slot = jnp.clip(take(last_new, src_home) - me * slots, 0, slots - 1)
            scalars = jnp.stack([slot, take(seq_lens, src_home), valid.astype(jnp.int32)])
            out, k_new, v_new = decode(scalars, x, pk, pv, weights, k_new, v_new, page)
            (back,) = rotate((out,), (group_size - shift) % group_size, group_size)
            mine = (take(shift_of, me) == shift)[None, :, None]
            return jnp.where(mine, back.reshape(2, rows, width), y), k_new, v_new

        k_new, v_new = migrate(local(mig_dst), local(mig_src), k_pool, v_pool, mig)

        def next_round(state):
            left, y, k_new, v_new = state
            shift = jnp.argmax(left).astype(jnp.int32)
            y, k_new, v_new = one_round(shift, y, k_new, v_new)
            return left & (shift_ids != shift), y, k_new, v_new

        _, y, k_new, v_new = lax.while_loop(lambda state: jnp.any(state[0]), next_round, (wanted, jnp.zeros_like(embeds), k_new, v_new))
        return y, k_new.reshape(k_pool5.shape), v_new.reshape(v_pool5.shape)

    return jax.shard_map(device_fn, mesh=mesh, in_specs=(tok_spec, P(), P(), P(), P(), P(), P(), pool_spec, pool_spec, P('rep', None), P('rep'), P('rep'), P('rep')), out_specs=(tok_spec, pool_spec, pool_spec), check_vma=False)
```

```python
import functools
import math

import jax
import jax.numpy as jnp
from jax import lax
from jax.experimental import pallas as pl
from jax.experimental.pallas import tpu as pltpu
from jax.sharding import PartitionSpec as P

ANY = pl.BlockSpec(memory_space=pl.ANY)
SMEM = pl.BlockSpec(memory_space=pltpu.SMEM)
VMEM = pl.BlockSpec(memory_space=pltpu.VMEM)
DMA = pltpu.SemaphoreType.DMA
CHUNK = 256
UNROLL = 8
LIMIT = 63 << 20
F32, BF16 = jnp.float32, jnp.bfloat16


def aligned(x, multiple):
    return x if isinstance(x, int) else pl.multiple_of(x, multiple)


class Dims:
    def __init__(self, rows, weights, k_pool, page):
        w_query, w_key, _, _, w_up, _ = weights
        self.layers, self.width, self.q_width = w_query.shape
        self.ff = w_up.shape[2]
        self.slots, _, self.page_rows, self.head_dim = k_pool.shape
        self.kv_heads = w_key.shape[2] // self.head_dim
        self.heads = self.q_width // self.head_dim
        self.page, self.rows = page, rows
        self.tokens = 2 * rows
        self.stride = self.tokens + 8
        self.n_q, self.n_o, self.n_u = self.q_width // CHUNK, self.width // CHUNK, self.ff // CHUNK
        self.col_layer = self.n_q + 2 + self.n_o + self.n_u

    def compute_scratch(self, n_col, n_row):
        return [
            pltpu.VMEM((n_col, self.width, CHUNK), BF16),
            pltpu.VMEM((n_row, CHUNK, self.width), BF16),
            pltpu.VMEM((self.heads * self.stride, self.head_dim), F32),
            pltpu.VMEM((self.kv_heads * self.stride, self.head_dim), F32),
            pltpu.VMEM((self.kv_heads * self.stride, self.head_dim), F32),
            pltpu.VMEM((self.heads * self.stride, self.head_dim), F32),
            pltpu.VMEM((self.tokens, self.q_width), BF16),
            pltpu.VMEM((self.tokens, self.ff), BF16),
            pltpu.VMEM((self.tokens, self.width), F32),
            DMA((n_col,)),
            DMA((n_row,)),
        ]

    def cost(self, layers):
        size = layers * self.width * (2 * self.q_width + 2 * self.kv_heads * self.head_dim + 2 * self.ff)
        return pl.CostEstimate(flops=2 * size * self.tokens, bytes_accessed=2 * size, transcendentals=0)


class Decoder:
    def __init__(self, dims, first, layers, weights, y_ref, scratch):
        self.d, self.first, self.layers, self.weights, self.y_ref = dims, first, layers, weights, y_ref
        (self.col_buf, self.row_buf, self.q_s, self.kn_s, self.vn_s, self.o_s, self.att, self.act, self.acc, self.col_sem, self.row_sem) = scratch
        self.n_col, self.n_row = self.col_buf.shape[0], self.row_buf.shape[0]
        self.zero = lax.axis_index('kv') * 0
        d = dims
        cols = 2 * d.page * d.kv_heads
        col_pos = lax.broadcasted_iota(jnp.int32, (2 * d.heads, cols), 1)
        row_pos = lax.broadcasted_iota(jnp.int32, (2 * d.heads, cols), 0)
        same_head = (col_pos % d.kv_heads) == (row_pos % d.heads) // (d.heads // d.kv_heads)
        self.limit = jnp.where(same_head, col_pos // d.kv_heads - row_pos // d.heads, 4 * d.page)
        self.page_pos = lax.broadcasted_iota(jnp.int32, (d.page_rows, d.head_dim), 0) // d.kv_heads
        self.tile_head = lax.broadcasted_iota(jnp.int32, (8, d.head_dim), 0) % d.kv_heads

    def layer_of(self, g, per_layer):
        return sum((g >= per_layer * l).astype(jnp.int32) for l in range(1, self.layers))

    def col_start(self, g):
        d = self.d
        wq, wk, wv, wo, wu, _ = self.weights

        @pl.when(g < self.layers * d.col_layer)
        def _():
            layer = self.layer_of(g, d.col_layer)
            pos = g - layer * d.col_layer
            slot = g % self.n_col

            def go(src, c):
                start = aligned(c * CHUNK, CHUNK)
                pltpu.make_async_copy(src.at[self.first + layer].at[:, pl.ds(start, CHUNK)], self.col_buf.at[slot], self.col_sem.at[slot]).start()

            @pl.when(pos < d.n_q)
            def _():
                go(wq, pos)

            @pl.when(pos == d.n_q)
            def _():
                go(wk, 0)

            @pl.when(pos == d.n_q + 1)
            def _():
                go(wv, 0)

            @pl.when((pos >= d.n_q + 2) & (pos < d.n_q + 2 + d.n_o))
            def _():
                go(wo, pos - (d.n_q + 2))

            @pl.when(pos >= d.n_q + 2 + d.n_o)
            def _():
                go(wu, pos - (d.n_q + 2 + d.n_o))

    def row_start(self, g):
        d = self.d
        wd = self.weights[5]

        @pl.when(g < self.layers * d.n_u)
        def _():
            layer = self.layer_of(g, d.n_u)
            slot = g % self.n_row
            start = aligned((g - layer * d.n_u) * CHUNK, CHUNK)
            pltpu.make_async_copy(wd.at[self.first + layer].at[pl.ds(start, CHUNK)], self.row_buf.at[slot], self.row_sem.at[slot]).start()

    def start_stream(self):
        @pl.loop(0, self.n_col)
        def _(g):
            self.col_start(g)

        @pl.loop(0, self.n_row)
        def _(g):
            self.row_start(g)

    def with_cols(self, g, count, body):
        slots = [(g + u) % self.n_col for u in range(count)]
        for slot in slots:
            pltpu.make_async_copy(self.weights[1].at[0], self.col_buf.at[slot], self.col_sem.at[slot]).wait()
        body([self.col_buf.at[slot] for slot in slots])
        for u in range(count):
            self.col_start(g + u + self.n_col)

    def with_rows(self, g, count, body):
        slots = [(g + u) % self.n_row for u in range(count)]
        for slot in slots:
            pltpu.make_async_copy(self.weights[5].at[0, pl.ds(0, CHUNK), :], self.row_buf.at[slot], self.row_sem.at[slot]).wait()
        body([self.row_buf.at[slot] for slot in slots])
        for u in range(count):
            self.row_start(g + u + self.n_row)

    def project(self, layer):
        d = self.d
        col0 = (self.zero + layer) * d.col_layer

        def product(ref):
            return jnp.dot(self.y_ref[...], ref[...], preferred_element_type=F32).astype(BF16).astype(F32)

        def put(dst, first, out):
            for h in range(CHUNK // d.head_dim):
                at = aligned((first + h) * d.stride, 8)
                dst[pl.ds(at, d.tokens), :] = out[:, h * d.head_dim:(h + 1) * d.head_dim]

        @pl.loop(0, d.n_q // 2)
        def _(j):
            def body(refs):
                outs = [product(ref) for ref in refs]
                for u in range(2):
                    put(self.q_s, (2 * j + u) * (CHUNK // d.head_dim), outs[u])

            self.with_cols(col0 + 2 * j, 2, body)

        def body(refs):
            outs = [product(ref) for ref in refs]
            put(self.kn_s, 0, outs[0])
            put(self.vn_s, 0, outs[1])

        self.with_cols(col0 + d.n_q, 2, body)

    def attend(self, lens, first_page, last_page, put_page):
        d = self.d
        unroll = min(UNROLL, d.rows)

        def some(first):
            ids = [first + u for u in range(unroll)]
            scores, vals = [], []
            for i in ids:
                n = lens(i)
                hits = [self.page_pos == n - d.page + t for t in range(2)]

                def updated(p, new_ref):
                    val = last_page(p, i).astype(F32)
                    for t in range(2):
                        parts = [new_ref[pl.ds(g * d.stride + t * d.rows + i, 1), :] for g in range(d.kv_heads)]
                        new = jnp.broadcast_to(parts[0], (8, d.head_dim))
                        for g in range(1, d.kv_heads):
                            new = jnp.where(self.tile_head == g, parts[g], new)
                        val = jnp.where(hits[t], jnp.concatenate([new] * (d.page_rows // 8), axis=0), val)
                    val = val.astype(BF16)
                    put_page(p, i, val)
                    return val

                keys = jnp.concatenate([first_page(0, i), updated(0, self.kn_s)], axis=0)
                vals.append(updated(1, self.vn_s))
                qs = jnp.concatenate([self.q_s[pl.ds(t * d.rows + i, d.heads, stride=d.stride), :] for t in range(2)], axis=0)
                score = lax.dot_general(qs.astype(BF16), keys, (((1,), (1,)), ((), ())), preferred_element_type=F32) * d.head_dim ** -0.5
                scores.append(jnp.where(self.limit <= n, score, -jnp.inf))
            tops = [jnp.max(score, axis=1, keepdims=True) for score in scores]
            probs = [jnp.exp(score - top) for score, top in zip(scores, tops)]
            totals = [jnp.sum(prob, axis=1, keepdims=True) for prob in probs]
            for u, i in enumerate(ids):
                both = jnp.concatenate([first_page(1, i), vals[u]], axis=0)
                out = jnp.dot(probs[u].astype(BF16), both, preferred_element_type=F32) / totals[u]
                for t in range(2):
                    self.o_s[pl.ds(t * d.rows + i, d.heads, stride=d.stride), :] = out[t * d.heads:(t + 1) * d.heads]

        @pl.loop(0, d.rows // unroll)
        def _(block):
            some(block * unroll)

        for h in range(d.heads):
            self.att[:, h * d.head_dim:(h + 1) * d.head_dim] = self.o_s[h * d.stride:h * d.stride + d.tokens, :].astype(BF16)

    def mix(self, layer, events=()):
        d = self.d
        layer = self.zero + layer
        col0 = layer * d.col_layer + d.n_q + 2
        pairs = d.n_u // 2

        def between(j, first):
            for k, run in events:
                if first <= k < first + pairs:
                    pl.when(j == k - first)(run)

        def span(j):
            return pl.ds(aligned(j * CHUNK, CHUNK), CHUNK)

        @pl.loop(0, d.n_o // 2)
        def _(j):
            def body(refs):
                outs = [jnp.dot(self.att[...], ref[...], preferred_element_type=F32) for ref in refs]
                for u in range(2):
                    at = span(2 * j + u)
                    self.y_ref[:, at] = (self.y_ref[:, at].astype(F32) + outs[u]).astype(BF16)

            self.with_cols(col0 + 2 * j, 2, body)

        def up(first, count):
            def body(refs):
                ups = [jnp.dot(self.y_ref[...], ref[...], preferred_element_type=F32) for ref in refs]
                for u in range(count):
                    self.act[:, span(first + u)] = jax.nn.gelu(ups[u].astype(BF16).astype(F32), approximate=True).astype(BF16)

            self.with_cols(col0 + d.n_o + first, count, body)

        def down(first, count):
            def body(refs):
                out = self.acc[...]
                for u in range(count):
                    out += jnp.dot(self.act[:, span(first + u)], refs[u][...], preferred_element_type=F32)
                self.acc[...] = out

            self.with_rows(layer * d.n_u + first, count, body)

        @pl.loop(0, d.n_u // 2)
        def _(j):
            between(j, 0)
            up(2 * j, 2)

        if d.n_u % 2:
            up(d.n_u - 1, 1)

        self.acc[...] = self.y_ref[...].astype(F32)

        @pl.loop(0, d.n_u // 2)
        def _(j):
            between(j, pairs)
            down(2 * j, 2)

        if d.n_u % 2:
            down(d.n_u - 1, 1)

        self.y_ref[...] = self.acc[...].astype(BF16)


class Exchange:
    STEPS = 11

    def __init__(self, side, layer, work, core_buf, ring_buf, out, send_sem, recv_sem):
        self.layer = layer
        self.work, self.core_buf, self.ring_buf, self.out, self.send_sem, self.recv_sem = work, core_buf, ring_buf, out, send_sem, recv_sem
        me = lax.axis_index('kv')
        core, x, y = me % 2, me // 2 % side, me // (2 * side)

        def pairings(pos, stride):
            return (((pos + 1) // 2 % 2, me + (1 - 2 * (pos % 2)) * stride), (pos // 2, me + (side - 1 - 2 * pos) * stride))

        xs, ys = pairings(x, 2), pairings(y, 2 * side)
        self.orders = [xs + ys, xs[::-1] + ys[::-1], ys + xs, ys[::-1] + xs[::-1]]
        self.partner = me + 1 - 2 * core
        self.peers = [self.partner] + [dev for _, dev in xs + ys]
        self.half = work.shape[1] // 2
        self.stream = self.half // 4
        self.base, self.other = core * self.half, (1 - core) * self.half
        self.held = [self.base + k * self.stream for k in range(4)]
        self.size = self.stream
        self.path, self.copies = [], []

    def send(self, src, dst, step, lane, dev):
        def copy():
            return pltpu.make_async_remote_copy(src(), dst(), self.send_sem.at[self.layer, step, lane], self.recv_sem.at[self.layer, step, lane], device_id={'kv': dev})

        copy().start()
        self.copies.append(copy)

    def units(self, ref, at, count):
        return lambda: ref.at[self.layer].at[pl.ds(at, count)]

    def results(self, at, count):
        return lambda: self.out.at[pl.ds(at, count)]

    def add(self, dst_at, buf, src_at, count):
        @pl.loop(0, count)
        def _(u):
            self.work[self.layer, dst_at + u] = self.work[self.layer, dst_at + u] + buf[self.layer, src_at + u]

    def halve(self, ring):
        self.size //= 2
        for k in range(4):
            bit, dev = self.orders[k][ring]
            src = self.units(self.work, self.held[k] + (1 - bit) * self.size, self.size)
            self.send(src, self.units(self.ring_buf, (k + 1) * self.stream - 2 * self.size, self.size), 1 + ring, k, dev)

    def halved(self, ring):
        for k in range(4):
            bit, _ = self.orders[k][ring]
            self.held[k] = self.held[k] + bit * self.size
            self.add(self.held[k], self.ring_buf, (k + 1) * self.stream - 2 * self.size, self.size)
        self.path.append(list(self.held))

    def double(self, ring):
        for k in range(4):
            at = self.results(self.path[ring][k], self.size)
            self.send(at, at, 8 - ring, k, self.orders[k][ring][1])
        self.size *= 2

    def step(self, k):
        for copy in self.copies:
            copy().wait()
        self.copies = []
        if k == 0:
            self.send(self.units(self.work, self.other, self.half), self.units(self.core_buf, 0, self.half), 0, 0, self.partner)
        elif k == 1:
            self.add(self.base, self.core_buf, 0, self.half)
            self.halve(0)
        elif k <= 4:
            self.halved(k - 2)
            self.halve(k - 1)
        elif k == 5:
            self.halved(3)
            for lane in range(4):
                for u in range(self.size):
                    self.out[self.held[lane] + u] = self.work[self.layer, self.held[lane] + u]
            self.double(3)
        elif k <= 8:
            self.double(8 - k)
        elif k == 9:
            at = self.results(self.base, self.half)
            self.send(at, at, 9, 0, self.partner)


def barrier_with(peers):
    barrier = pltpu.get_barrier_semaphore()
    for dev in peers:
        pl.semaphore_signal(barrier, inc=1, device_id={'kv': dev})
    pl.semaphore_wait(barrier, len(peers))


def first_layer_kernel(dims, side, group_size, entries, sc_ref, src_ref, x_ref, wq, wk, wv, wo, wu, wd, k_hbm, v_hbm,
                       y_ref, last_out, first_out, mig_out,
                       pool_k, pool_v, send_buf, first_buf, last_buf, work, core_buf, ring_buf, *rest):
    d = dims
    migs, rest = rest[:d.layers], rest[d.layers:]
    compute, (pool_sem, page_send, page_recv, mig_send, mig_recv, out_sem) = rest[:-6], rest[-6:]
    me = lax.axis_index('kv')
    ahead, behind = lax.rem(me + 1, group_size), lax.rem(me + group_size - 1, group_size)
    dec = Decoder(d, 0, 1, (wq, wk, wv, wo, wu, wd), y_ref, compute)
    pools = (pool_k, pool_v)
    exchanges = [Exchange(side, l, work, core_buf, ring_buf, migs[l], mig_send, mig_recv) for l in range(d.layers)]

    loads = [pltpu.make_async_copy(src, dst, pool_sem.at[p]) for p, (src, dst) in enumerate(((k_hbm, pool_k), (v_hbm, pool_v)))]
    for load in loads:
        load.start()
    dec.start_stream()
    barrier_with(exchanges[0].peers + [ahead, behind])
    y_ref[...] = x_ref[...]
    for load in loads:
        load.wait()

    def own(l):
        @pl.loop(0, entries)
        def _(e):
            slot = src_ref[e] - me * d.slots
            mine = (slot >= 0) & (slot < d.slots)
            slot = jnp.clip(slot, 0, d.slots - 1)
            for p in range(2):
                page = pools[p][slot, l]
                work[l, p * entries + e] = jnp.where(mine, page, jnp.zeros_like(page))

    def pack(l):
        @pl.loop(0, d.rows)
        def _(i):
            slot = sc_ref[0, i]
            for p in range(2):
                send_buf[l, p, i] = pools[p][slot, l]

    parts = 4
    size = d.rows // parts

    def first_copy(l, p, rows):
        dst = first_buf.at[p, rows] if l == 0 else first_out.at[l - 1, p, rows]
        return pltpu.make_async_remote_copy(send_buf.at[l, p, rows], dst, page_send.at[l, p], page_recv.at[l, p], device_id={'kv': ahead})

    def first_start(l, k):
        p, part = k % 2, k // 2
        first_copy(l, p, pl.ds(part * size, size)).start()

    def first_wait(l):
        for p in range(2):
            first_copy(l, p, pl.ds(0, d.rows)).wait()

    own(0)
    exchanges[0].step(0)
    pack(0)
    first_start(0, 0)
    first_start(0, 1)
    exchanges[0].step(1)
    first_start(0, 2)
    own(1)
    exchanges[0].step(2)
    first_start(0, 3)
    dec.project(0)
    exchanges[0].step(3)
    first_start(0, 4)
    pack(1)
    for k in range(4, 6):
        exchanges[0].step(k)
        first_start(0, k + 1)
    exchanges[1].step(0)
    exchanges[0].step(6)
    first_start(0, 7)
    exchanges[1].step(1)
    for k in range(7, 11):
        exchanges[0].step(k)
        exchanges[1].step(k - 5)
    first_wait(0)

    def last_page(p, i):
        entry = sc_ref[3, i]
        page = pools[p][sc_ref[1, i], 0]
        return jnp.where(entry >= 0, migs[0][p * entries + jnp.maximum(entry, 0)], page)

    def put_page(p, i, val):
        last_buf[p, i] = val

    dec.attend(lambda i: sc_ref[2, i], lambda p, i: first_buf[p, i], last_page, put_page)
    last_store = pltpu.make_async_copy(last_buf, last_out, out_sem.at[0])
    last_store.start()

    pairs = 2 * (d.n_u // 2)
    events = [(k * pairs // (2 * parts), functools.partial(first_start, 1, k)) for k in range(2 * parts)]
    events += [((k - 6) * pairs // 6, functools.partial(exchanges[1].step, k)) for k in range(6, 11)]
    dec.mix(0, sorted(events, key=lambda event: event[0]))
    mig_stores = [pltpu.make_async_copy(migs[l], mig_out.at[l], out_sem.at[1 + l]) for l in range(d.layers)]
    for store in mig_stores:
        store.start()
    first_wait(1)
    for store in [last_store] + mig_stores:
        store.wait()


def first_layer(side, group_size, d, scalars, mig_src, x, weights, k_pool, v_pool):
    entries = mig_src.shape[0]
    page = (d.page_rows, d.head_dim)
    struct = lambda *shape: jax.ShapeDtypeStruct(shape, BF16)
    return pl.pallas_call(
        functools.partial(first_layer_kernel, d, side, group_size, entries),
        out_shape=[
            struct(*x.shape), struct(2, d.rows, *page), struct(d.layers - 1, 2, d.rows, *page),
            struct(d.layers, 2 * entries, *page),
        ],
        in_specs=[SMEM, SMEM, VMEM] + [ANY] * 8,
        out_specs=[VMEM] + [ANY] * 3,
        scratch_shapes=[
            pltpu.VMEM(k_pool.shape, BF16),
            pltpu.VMEM(k_pool.shape, BF16),
            pltpu.VMEM((d.layers, 2, d.rows) + page, BF16),
            pltpu.VMEM((2, d.rows) + page, BF16),
            pltpu.VMEM((2, d.rows) + page, BF16),
            pltpu.VMEM((d.layers, 2 * entries) + page, BF16),
            pltpu.VMEM((d.layers, entries) + page, BF16),
            pltpu.VMEM((d.layers, entries) + page, BF16),
        ] + [pltpu.VMEM((2 * entries,) + page, BF16)] * d.layers + d.compute_scratch(12, 8) + [
            DMA((2,)),
            DMA((d.layers, 2)),
            DMA((d.layers, 2)),
            DMA((d.layers, 10, 4)),
            DMA((d.layers, 10, 4)),
            DMA((1 + d.layers,)),
        ],
        compiler_params=pltpu.CompilerParams(collective_id=1, has_side_effects=True, vmem_limit_bytes=LIMIT),
        cost_estimate=d.cost(1),
        name="first_layer",
    )(scalars, mig_src, x, *weights, k_pool, v_pool)


def last_layers_kernel(dims, entries, sc_ref, dst_ref, src_ref, h_ref, first_hbm, last0_hbm, mig_hbm, wq, wk, wv, wo, wu, wd, k_in, v_in,
                       y_ref, k_out, v_out, first_buf, last_buf, last0, mig, zero, *rest):
    compute, (first_sem, last_sem, stage_sem, fix_sem, put_sem) = rest[:-5], rest[-5:]
    d = dims
    later = d.layers - 1
    dec = Decoder(d, 1, later, (wq, wk, wv, wo, wu, wd), y_ref, compute)
    ins, outs = (k_in, v_in), (k_out, v_out)

    dec.start_stream()
    y_ref[...] = h_ref[...]
    first_load = pltpu.make_async_copy(first_hbm, first_buf, first_sem)
    first_load.start()

    @pl.loop(0, d.rows)
    def _(i):
        entry, slot = sc_ref[3, i], sc_ref[1, i]
        for l in range(later):
            for p in range(2):
                @pl.when(entry >= 0)
                def _():
                    pltpu.make_async_copy(mig_hbm.at[1 + l, p * entries + jnp.maximum(entry, 0)], last_buf.at[l, p, i], last_sem).start()

                @pl.when(entry < 0)
                def _():
                    pltpu.make_async_copy(ins[p].at[slot, 1 + l], last_buf.at[l, p, i], last_sem).start()

    stages = [pltpu.make_async_copy(mig_hbm, mig, stage_sem.at[0]), pltpu.make_async_copy(last0_hbm, last0, stage_sem.at[1])]
    for stage in stages:
        stage.start()
    zero[...] = jnp.zeros_like(zero)

    def fixes(run):
        @pl.loop(0, entries)
        def _(e):
            for p in range(2):
                @pl.when(dst_ref[e] >= 0)
                def _():
                    for l in range(d.layers):
                        run(pltpu.make_async_copy(mig.at[l, p * entries + e], outs[p].at[jnp.maximum(dst_ref[e], 0), l], fix_sem))

                @pl.when(src_ref[e] >= 0)
                def _():
                    run(pltpu.make_async_copy(zero, outs[p].at[jnp.maximum(src_ref[e], 0)], fix_sem))

    def puts(run, l):
        @pl.loop(0, d.rows)
        def _(i):
            for p in range(2):
                src = last0.at[p, i] if l == 0 else last_buf.at[l - 1, p, i]
                run(pltpu.make_async_copy(src, outs[p].at[sc_ref[1, i], l], put_sem))

    start, wait = lambda copy: copy.start(), lambda copy: copy.wait()
    for l in range(later):
        dec.project(l)
        if l == 0:
            first_load.wait()
            pltpu.make_async_copy(first_hbm, last_buf, last_sem).wait()
            for stage in stages:
                stage.wait()
            fixes(start)

        def put_page(p, i, val):
            last_buf[l, p, i] = val

        dec.attend(lambda i: sc_ref[2, i], lambda p, i: first_buf[l, p, i], lambda p, i: last_buf[l, p, i], put_page)
        if l == 0:
            fixes(wait)
            puts(start, 0)
        puts(start, 1 + l)
        dec.mix(l)
    for l in range(d.layers):
        puts(wait, l)


def last_layers(d, scalars, dst_local, src_local, h, first, last0, mig, weights, k_pool, v_pool):
    entries = dst_local.shape[0]
    page = (d.page_rows, d.head_dim)
    pool = jax.ShapeDtypeStruct(k_pool.shape, BF16)
    return pl.pallas_call(
        functools.partial(last_layers_kernel, d, entries),
        out_shape=[jax.ShapeDtypeStruct(h.shape, BF16), pool, pool],
        in_specs=[SMEM, SMEM, SMEM, VMEM] + [ANY] * 11,
        out_specs=[VMEM, ANY, ANY],
        input_output_aliases={13: 1, 14: 2},
        scratch_shapes=[
            pltpu.VMEM((d.layers - 1, 2, d.rows) + page, BF16),
            pltpu.VMEM((d.layers - 1, 2, d.rows) + page, BF16),
            pltpu.VMEM((2, d.rows) + page, BF16),
            pltpu.VMEM((d.layers, 2 * entries) + page, BF16),
            pltpu.VMEM((d.layers,) + page, BF16),
        ] + d.compute_scratch(16, 16) + [DMA, DMA, DMA((2,)), DMA, DMA],
        compiler_params=pltpu.CompilerParams(vmem_limit_bytes=LIMIT),
        cost_estimate=d.cost(d.layers - 1),
        name="last_layers",
    )(scalars, dst_local, src_local, h, first, last0, mig, *weights, k_pool, v_pool)


def gather_pages_kernel(idx_ref, k_hbm, v_hbm, k_out, v_out, sem):
    rows = k_out.shape[0]

    def copies(i):
        slot = jnp.maximum(idx_ref[i], 0)
        return (pltpu.make_async_copy(k_hbm.at[slot], k_out.at[i], sem), pltpu.make_async_copy(v_hbm.at[slot], v_out.at[i], sem))

    @pl.loop(0, rows)
    def _(i):
        @pl.when(idx_ref[i] >= 0)
        def _():
            for copy in copies(i):
                copy.start()

        @pl.when(idx_ref[i] < 0)
        def _():
            k_out[i] = jnp.zeros(k_out.shape[1:], k_out.dtype)
            v_out[i] = jnp.zeros(v_out.shape[1:], v_out.dtype)

    @pl.loop(0, rows)
    def _(i):
        @pl.when(idx_ref[i] >= 0)
        def _():
            for copy in copies(i):
                copy.wait()


def gather_pages(idx, k_pool, v_pool):
    shape = jax.ShapeDtypeStruct((idx.shape[0],) + k_pool.shape[1:], k_pool.dtype)
    return pl.pallas_call(
        gather_pages_kernel,
        out_shape=[shape, shape],
        in_specs=[SMEM, ANY, ANY],
        out_specs=[VMEM, VMEM],
        scratch_shapes=[DMA],
        compiler_params=pltpu.CompilerParams(vmem_limit_bytes=LIMIT),
        name="gather_pages",
    )(idx, k_pool, v_pool)


def share_kernel(side, k_hbm, v_hbm, k_out, v_out, work, core_buf, ring_buf, load_sem, send_sem, recv_sem, *migs):
    entries, layers = k_hbm.shape[:2]
    me_exchange = [Exchange(side, l, work, core_buf, ring_buf, migs[l], send_sem, recv_sem) for l in range(layers)]
    loads = [pltpu.make_async_copy(src.at[:, l], work.at[l, pl.ds(p * entries, entries)], load_sem.at[l, p]) for l in range(layers) for p, src in enumerate((k_hbm, v_hbm))]
    for load in loads:
        load.start()
    barrier_with(me_exchange[0].peers)
    for load in loads:
        load.wait()
    for k in range(Exchange.STEPS):
        for exchange in me_exchange:
            exchange.step(k)
    stores = [pltpu.make_async_copy(migs[l].at[pl.ds(p * entries, entries)], dst.at[:, l], load_sem.at[l, p]) for l in range(layers) for p, dst in enumerate((k_out, v_out))]
    for store in stores:
        store.start()
    for store in stores:
        store.wait()


def share(mig_k, mig_v, side):
    entries, layers = mig_k.shape[:2]
    page = mig_k.shape[2:]
    return pl.pallas_call(
        functools.partial(share_kernel, side),
        out_shape=[jax.ShapeDtypeStruct(mig_k.shape, BF16)] * 2,
        in_specs=[ANY, ANY],
        out_specs=[ANY, ANY],
        scratch_shapes=[
            pltpu.VMEM((layers, 2 * entries) + page, BF16),
            pltpu.VMEM((layers, entries) + page, BF16),
            pltpu.VMEM((layers, entries) + page, BF16),
            DMA((layers, 2)),
            DMA((layers, 10, 4)),
            DMA((layers, 10, 4)),
        ] + [pltpu.VMEM((2 * entries,) + page, BF16)] * layers,
        compiler_params=pltpu.CompilerParams(collective_id=0, has_side_effects=True, vmem_limit_bytes=LIMIT),
        name="share",
    )(mig_k, mig_v)


def migrate_kernel(dst_ref, src_ref, k_hbm, v_hbm, mk_hbm, mv_hbm, k_out, v_out, k_buf, v_buf, sem, fix_sem):
    entries = dst_ref.shape[0]
    pairs = ((k_hbm, mk_hbm, k_buf, k_out), (v_hbm, mv_hbm, v_buf, v_out))
    for p, (src, _, buf, _) in enumerate(pairs):
        pltpu.make_async_copy(src, buf, sem.at[p]).start()
    for p, (src, _, buf, _) in enumerate(pairs):
        pltpu.make_async_copy(src, buf, sem.at[p]).wait()

    @pl.loop(0, entries)
    def _(e):
        @pl.when(dst_ref[e] >= 0)
        def _():
            for _, mig, buf, _ in pairs:
                copy = pltpu.make_async_copy(mig.at[e], buf.at[jnp.maximum(dst_ref[e], 0)], fix_sem)
                copy.start()
                copy.wait()

        @pl.when(src_ref[e] >= 0)
        def _():
            for _, _, buf, _ in pairs:
                buf[jnp.maximum(src_ref[e], 0)] = jnp.zeros(buf.shape[1:], buf.dtype)

    for p, (_, _, buf, dst) in enumerate(pairs):
        pltpu.make_async_copy(buf, dst, sem.at[p]).start()
    for p, (_, _, buf, dst) in enumerate(pairs):
        pltpu.make_async_copy(buf, dst, sem.at[p]).wait()


def migrate(dst_local, src_local, k_pool, v_pool, mig_k, mig_v):
    shape = jax.ShapeDtypeStruct(k_pool.shape, k_pool.dtype)
    return pl.pallas_call(
        migrate_kernel,
        out_shape=[shape, shape],
        in_specs=[SMEM, SMEM, ANY, ANY, ANY, ANY],
        out_specs=[ANY, ANY],
        scratch_shapes=[pltpu.VMEM(k_pool.shape, k_pool.dtype), pltpu.VMEM(k_pool.shape, k_pool.dtype), DMA((2,)), DMA],
        compiler_params=pltpu.CompilerParams(vmem_limit_bytes=LIMIT),
        name="migrate",
    )(dst_local, src_local, k_pool, v_pool, mig_k, mig_v)


def decode_kernel(dims, sc_ref, x_ref, p0k_hbm, p0v_hbm, wq, wk, wv, wo, wu, wd, k_in, v_in, y_ref, k_out, v_out,
                  first_buf, last_buf, *rest):
    compute, (page_sem, put_sem) = rest[:-2], rest[-2:]
    d = dims
    dec = Decoder(d, 0, d.layers, (wq, wk, wv, wo, wu, wd), y_ref, compute)
    dec.start_stream()
    y_ref[...] = x_ref[...]
    loads = [pltpu.make_async_copy(src, first_buf.at[p], page_sem.at[p]) for p, src in enumerate((p0k_hbm, p0v_hbm))]
    for load in loads:
        load.start()

    def last_loads(run):
        @pl.loop(0, d.rows)
        def _(i):
            for p, src in enumerate((k_in, v_in)):
                run(pltpu.make_async_copy(src.at[sc_ref[0, i]], last_buf.at[p, i], page_sem.at[2]))

    def puts(run):
        @pl.loop(0, d.rows)
        def _(i):
            @pl.when(sc_ref[2, i] > 0)
            def _():
                for p, dst in enumerate((k_out, v_out)):
                    run(pltpu.make_async_copy(last_buf.at[p, i], dst.at[sc_ref[0, i]], put_sem))

    last_loads(lambda copy: copy.start())
    for load in loads:
        load.wait()
    last_loads(lambda copy: copy.wait())

    @pl.loop(0, d.layers)
    def _(layer):
        def put_page(p, i, val):
            last_buf[p, i, layer] = val

        dec.project(layer)
        dec.attend(lambda i: sc_ref[1, i], lambda p, i: first_buf[p, i, layer], lambda p, i: last_buf[p, i, layer], put_page)
        dec.mix(layer)

    puts(lambda copy: copy.start())
    puts(lambda copy: copy.wait())


def decode(d, scalars, x, p0k, p0v, weights, k_pool, v_pool):
    pool = jax.ShapeDtypeStruct(k_pool.shape, k_pool.dtype)
    pages = pltpu.VMEM((2, d.rows, d.layers, d.page_rows, d.head_dim), BF16)
    return pl.pallas_call(
        functools.partial(decode_kernel, d),
        out_shape=[jax.ShapeDtypeStruct(x.shape, x.dtype), pool, pool],
        in_specs=[SMEM, VMEM] + [ANY] * 10,
        out_specs=[VMEM, ANY, ANY],
        input_output_aliases={10: 1, 11: 2},
        scratch_shapes=[pages, pages] + d.compute_scratch(16, 16) + [DMA((3,)), DMA],
        compiler_params=pltpu.CompilerParams(vmem_limit_bytes=LIMIT),
        cost_estimate=d.cost(d.layers),
        name="decode",
    )(scalars, x, p0k, p0v, *weights, k_pool, v_pool)


def permute(arrays, shift, group_size):
    perm = [(i, (i + shift) % group_size) for i in range(group_size)]
    return tuple(lax.ppermute(a, 'kv', perm) for a in arrays)


def rotate(arrays, shift, group_size, beside=lambda: ()):
    def branch(r):
        return lambda args: (permute(args, r, group_size) if r else args, beside())

    return lax.switch(shift, [branch(r) for r in range(group_size)], tuple(arrays))


def rotate_bits(arrays, shift, group_size):
    arrays = tuple(arrays)
    bit = 1
    while bit < group_size:
        move = functools.partial(permute, shift=bit, group_size=group_size)
        arrays = lax.cond(shift // bit % 2 == 1, move, lambda args: args, arrays)
        bit *= 2
    return arrays


def copy_pools_kernel(k_hbm, v_hbm, k_out, v_out, k_buf, v_buf, sem):
    parts = 4
    size = k_buf.shape[0] // parts
    steps = [(src, buf, dst, sem.at[p, part], pl.ds(part * size, size)) for part in range(parts) for p, (src, buf, dst) in enumerate(((k_hbm, k_buf, k_out), (v_hbm, v_buf, v_out)))]
    for src, buf, _, s, rows in steps:
        pltpu.make_async_copy(src.at[rows], buf.at[rows], s).start()
    for src, buf, dst, s, rows in steps:
        pltpu.make_async_copy(src.at[rows], buf.at[rows], s).wait()
        pltpu.make_async_copy(buf.at[rows], dst.at[rows], s).start()
    for _, buf, dst, s, rows in steps:
        pltpu.make_async_copy(buf.at[rows], dst.at[rows], s).wait()


def copy_pools(k_pool, v_pool):
    size = 4 * k_pool.size
    return pl.pallas_call(
        copy_pools_kernel,
        out_shape=[jax.ShapeDtypeStruct(k_pool.shape, k_pool.dtype)] * 2,
        in_specs=[ANY, ANY],
        out_specs=[ANY, ANY],
        scratch_shapes=[pltpu.VMEM(k_pool.shape, k_pool.dtype), pltpu.VMEM(k_pool.shape, k_pool.dtype), DMA((2, 4))],
        compiler_params=pltpu.CompilerParams(vmem_limit_bytes=LIMIT),
        cost_estimate=pl.CostEstimate(flops=40 * size, bytes_accessed=2 * size, transcendentals=0),
        name="copy_pools",
    )(k_pool, v_pool)


def solution(mesh):
    group_size = mesh.shape['kv']
    side = math.isqrt(group_size // 2)
    pool_spec = P(('rep', 'kv'))
    tok_spec = P(None, ('rep', 'kv'), None)

    def device_fn(embeds, w_query, w_key, w_value, w_out, w_up, w_down, k_pool5, v_pool5, new_table, seq_lens, mig_src, mig_dst):
        me = lax.axis_index('kv')
        slots, layers, page, kv_heads, head_dim = k_pool5.shape
        rows, width = embeds.shape[1:]
        weights = (w_query, w_key, w_value, w_out, w_up, w_down)
        k_pool = k_pool5.reshape(slots, layers, page * kv_heads, head_dim)
        v_pool = v_pool5.reshape(slots, layers, page * kv_heads, head_dim)
        d = Dims(rows, weights, k_pool, page)
        ints = jnp.int32

        def local(ids):
            loc = ids - me * slots
            return jnp.where((loc >= 0) & (loc < slots), loc, -1)

        def take(vec, dev):
            return lax.dynamic_slice(vec, (dev * rows,), (rows,))

        def inside(ids):
            return jnp.clip(ids - me * slots, 0, slots - 1)

        first_new, last_new = new_table[:, 0], new_table[:, 1]
        moved = first_new[None, :] == mig_dst[:, None]
        first_old = jnp.where(jnp.any(moved, axis=0), jnp.sum(jnp.where(moved, mig_src[:, None], 0), axis=0), first_new)
        home = jnp.arange(first_new.shape[0], dtype=ints) // rows
        worker = last_new // slots
        shift_of = (worker - home + group_size) % group_size
        first_shift = (worker - first_old // slots + group_size) % group_size
        one_shift = shift_of[0]
        adjacent = jnp.all((shift_of == one_shift) & (first_shift == 1))

        def adjacent_path():
            src_home = (me - one_shift + group_size) % group_size
            next_home = (src_home + 1) % group_size
            last = take(last_new, src_home)
            hit = last[None, :] == mig_dst[:, None]
            entry = jnp.sum(jnp.where(hit, jnp.arange(1, mig_dst.shape[0] + 1, dtype=ints)[:, None], 0), axis=0) - 1
            scalars = jnp.stack([inside(take(first_old, next_home)), inside(last), take(seq_lens, src_home), entry])
            (x,), (k_new, v_new) = rotate((embeds.reshape(2 * rows, width),), one_shift, group_size, lambda: copy_pools(k_pool, v_pool))
            h, last0, first, mig = first_layer(side, group_size, d, scalars, mig_src, x, weights, k_pool, v_pool)
            y, k_new, v_new = last_layers(d, scalars, local(mig_dst), local(mig_src), h, first, last0, mig, weights, k_new, v_new)
            (y,), _ = rotate((y,), (group_size - one_shift) % group_size, group_size)
            return y.reshape(embeds.shape), k_new, v_new

        def general_path():
            shift_ids = jnp.arange(group_size, dtype=ints)
            wanted = jnp.any(shift_of[None, :] == shift_ids[:, None], axis=1)
            mig_k, mig_v = gather_pages(local(mig_src), k_pool, v_pool)
            mig_k, mig_v = share(mig_k, mig_v, side)
            k_new, v_new = migrate(local(mig_dst), local(mig_src), k_pool, v_pool, mig_k, mig_v)

            def one_round(shift, y, k_new, v_new):
                src_home = (me - shift + group_size) % group_size
                (x,) = rotate_bits((embeds.reshape(2 * rows, width),), shift, group_size)
                in_round = shift_of == shift
                wanted2 = jnp.any(in_round[None, :] & (first_shift[None, :] == shift_ids[:, None]), axis=1)

                def more(state):
                    left, pk, pv = state
                    shift2 = jnp.argmax(left).astype(ints)
                    dest_home = (me + shift2 - shift + group_size) % group_size
                    got = gather_pages(inside(take(first_old, dest_home)), k_pool, v_pool)
                    got_k, got_v = rotate_bits(got, shift2, group_size)
                    mine = (take(first_shift, src_home) == shift2)[:, None, None, None]
                    return left & (shift_ids != shift2), jnp.where(mine, got_k, pk), jnp.where(mine, got_v, pv)

                zeros = jnp.zeros((rows,) + k_pool.shape[1:], k_pool.dtype)
                _, pk, pv = lax.while_loop(lambda state: jnp.any(state[0]), more, (wanted2, zeros, zeros))
                valid = take(shift_of, src_home) == shift
                scalars = jnp.stack([inside(take(last_new, src_home)), take(seq_lens, src_home), valid.astype(ints)])
                out, k_new, v_new = decode(d, scalars, x, pk, pv, weights, k_new, v_new)
                (back,) = rotate_bits((out,), (group_size - shift) % group_size, group_size)
                mine = (take(shift_of, me) == shift)[None, :, None]
                return jnp.where(mine, back.reshape(embeds.shape), y), k_new, v_new

            def next_round(state):
                left, y, k_new, v_new = state
                shift = jnp.argmax(left).astype(ints)
                y, k_new, v_new = one_round(shift, y, k_new, v_new)
                return left & (shift_ids != shift), y, k_new, v_new

            _, y, k_new, v_new = lax.while_loop(lambda state: jnp.any(state[0]), next_round, (wanted, jnp.zeros_like(embeds), k_new, v_new))
            return y, k_new, v_new

        y, k_new, v_new = lax.cond(adjacent, adjacent_path, general_path)
        return y, k_new.reshape(k_pool5.shape), v_new.reshape(v_pool5.shape)

    return jax.shard_map(device_fn, mesh=mesh, in_specs=(tok_spec, P(), P(), P(), P(), P(), P(), pool_spec, pool_spec, P('rep', None), P('rep'), P('rep'), P('rep')), out_specs=(tok_spec, pool_spec, pool_spec), check_vma=False)
```

```python
import functools
import math

import jax
import jax.numpy as jnp
from jax import lax
from jax.experimental import pallas as pl
from jax.experimental.pallas import tpu as pltpu
from jax.sharding import PartitionSpec as P

ANY = pl.BlockSpec(memory_space=pl.ANY)
SMEM = pl.BlockSpec(memory_space=pltpu.SMEM)
VMEM = pl.BlockSpec(memory_space=pltpu.VMEM)
DMA = pltpu.SemaphoreType.DMA
CHUNK = 256
UNROLL = 8
LIMIT = 63 << 20
F32, BF16 = jnp.float32, jnp.bfloat16


def aligned(x, multiple):
    return x if isinstance(x, int) else pl.multiple_of(x, multiple)


class Dims:
    def __init__(self, rows, weights, k_pool, page):
        w_query, w_key, _, _, w_up, _ = weights
        self.layers, self.width, self.q_width = w_query.shape
        self.ff = w_up.shape[2]
        self.slots, _, self.page_rows, self.head_dim = k_pool.shape
        self.kv_heads = w_key.shape[2] // self.head_dim
        self.heads = self.q_width // self.head_dim
        self.page, self.rows = page, rows
        self.tokens = 2 * rows
        self.stride = self.tokens + 8
        self.n_q, self.n_o, self.n_u = self.q_width // CHUNK, self.width // CHUNK, self.ff // CHUNK
        self.col_layer = self.n_q + 2 + self.n_o + self.n_u

    def compute_scratch(self, n_col, n_row):
        return [
            pltpu.VMEM((n_col, self.width, CHUNK), BF16),
            pltpu.VMEM((n_row, CHUNK, self.width), BF16),
            pltpu.VMEM((self.heads * self.stride, self.head_dim), F32),
            pltpu.VMEM((self.kv_heads * self.stride, self.head_dim), F32),
            pltpu.VMEM((self.kv_heads * self.stride, self.head_dim), F32),
            pltpu.VMEM((self.heads * self.stride, self.head_dim), F32),
            pltpu.VMEM((self.tokens, self.q_width), BF16),
            pltpu.VMEM((self.tokens, self.ff), BF16),
            pltpu.VMEM((self.tokens, self.width), F32),
            DMA((n_col,)),
            DMA((n_row,)),
        ]

    def cost(self, layers):
        size = layers * self.width * (2 * self.q_width + 2 * self.kv_heads * self.head_dim + 2 * self.ff)
        return pl.CostEstimate(flops=2 * size * self.tokens, bytes_accessed=2 * size, transcendentals=0)


class Decoder:
    def __init__(self, dims, first, layers, weights, y_ref, scratch):
        self.d, self.first, self.layers, self.weights, self.y_ref = dims, first, layers, weights, y_ref
        (self.col_buf, self.row_buf, self.q_s, self.kn_s, self.vn_s, self.o_s, self.att, self.act, self.acc, self.col_sem, self.row_sem) = scratch
        self.n_col, self.n_row = self.col_buf.shape[0], self.row_buf.shape[0]
        self.zero = lax.axis_index('kv') * 0
        d = dims
        cols = 2 * d.page * d.kv_heads
        col_pos = lax.broadcasted_iota(jnp.int32, (2 * d.heads, cols), 1)
        row_pos = lax.broadcasted_iota(jnp.int32, (2 * d.heads, cols), 0)
        same_head = (col_pos % d.kv_heads) == (row_pos % d.heads) // (d.heads // d.kv_heads)
        self.limit = jnp.where(same_head, col_pos // d.kv_heads - row_pos // d.heads, 4 * d.page)
        self.page_pos = lax.broadcasted_iota(jnp.int32, (d.page_rows, d.head_dim), 0) // d.kv_heads
        self.tile_head = lax.broadcasted_iota(jnp.int32, (8, d.head_dim), 0) % d.kv_heads

    def layer_of(self, g, per_layer):
        return sum((g >= per_layer * l).astype(jnp.int32) for l in range(1, self.layers))

    def col_start(self, g):
        d = self.d
        wq, wk, wv, wo, wu, _ = self.weights

        @pl.when(g < self.layers * d.col_layer)
        def _():
            layer = self.layer_of(g, d.col_layer)
            pos = g - layer * d.col_layer
            slot = g % self.n_col

            def go(src, c):
                start = aligned(c * CHUNK, CHUNK)
                pltpu.make_async_copy(src.at[self.first + layer].at[:, pl.ds(start, CHUNK)], self.col_buf.at[slot], self.col_sem.at[slot]).start()

            @pl.when(pos < d.n_q)
            def _():
                go(wq, pos)

            @pl.when(pos == d.n_q)
            def _():
                go(wk, 0)

            @pl.when(pos == d.n_q + 1)
            def _():
                go(wv, 0)

            @pl.when((pos >= d.n_q + 2) & (pos < d.n_q + 2 + d.n_o))
            def _():
                go(wo, pos - (d.n_q + 2))

            @pl.when(pos >= d.n_q + 2 + d.n_o)
            def _():
                go(wu, pos - (d.n_q + 2 + d.n_o))

    def row_start(self, g):
        d = self.d
        wd = self.weights[5]

        @pl.when(g < self.layers * d.n_u)
        def _():
            layer = self.layer_of(g, d.n_u)
            slot = g % self.n_row
            start = aligned((g - layer * d.n_u) * CHUNK, CHUNK)
            pltpu.make_async_copy(wd.at[self.first + layer].at[pl.ds(start, CHUNK)], self.row_buf.at[slot], self.row_sem.at[slot]).start()

    def start_stream(self):
        @pl.loop(0, self.n_col)
        def _(g):
            self.col_start(g)

        @pl.loop(0, self.n_row)
        def _(g):
            self.row_start(g)

    def with_cols(self, g, count, body):
        slots = [(g + u) % self.n_col for u in range(count)]
        for slot in slots:
            pltpu.make_async_copy(self.weights[1].at[0], self.col_buf.at[slot], self.col_sem.at[slot]).wait()
        body([self.col_buf.at[slot] for slot in slots])
        for u in range(count):
            self.col_start(g + u + self.n_col)

    def with_rows(self, g, count, body):
        slots = [(g + u) % self.n_row for u in range(count)]
        for slot in slots:
            pltpu.make_async_copy(self.weights[5].at[0, pl.ds(0, CHUNK), :], self.row_buf.at[slot], self.row_sem.at[slot]).wait()
        body([self.row_buf.at[slot] for slot in slots])
        for u in range(count):
            self.row_start(g + u + self.n_row)

    def project(self, layer):
        d = self.d
        col0 = (self.zero + layer) * d.col_layer

        def product(ref):
            return jnp.dot(self.y_ref[...], ref[...], preferred_element_type=F32).astype(BF16).astype(F32)

        def put(dst, first, out):
            for h in range(CHUNK // d.head_dim):
                at = aligned((first + h) * d.stride, 8)
                dst[pl.ds(at, d.tokens), :] = out[:, h * d.head_dim:(h + 1) * d.head_dim]

        @pl.loop(0, d.n_q // 2)
        def _(j):
            def body(refs):
                outs = [product(ref) for ref in refs]
                for u in range(2):
                    put(self.q_s, (2 * j + u) * (CHUNK // d.head_dim), outs[u])

            self.with_cols(col0 + 2 * j, 2, body)

        def body(refs):
            outs = [product(ref) for ref in refs]
            put(self.kn_s, 0, outs[0])
            put(self.vn_s, 0, outs[1])

        self.with_cols(col0 + d.n_q, 2, body)

    def attend(self, lens, first_page, last_page, put_page, events=()):
        d = self.d
        unroll = min(UNROLL, d.rows)

        def some(first):
            ids = [first + u for u in range(unroll)]
            scores, vals = [], []
            for i in ids:
                n = lens(i)
                hits = [self.page_pos == n - d.page + t for t in range(2)]

                def updated(p, new_ref):
                    val = last_page(p, i).astype(F32)
                    for t in range(2):
                        parts = [new_ref[pl.ds(g * d.stride + t * d.rows + i, 1), :] for g in range(d.kv_heads)]
                        new = jnp.broadcast_to(parts[0], (8, d.head_dim))
                        for g in range(1, d.kv_heads):
                            new = jnp.where(self.tile_head == g, parts[g], new)
                        val = jnp.where(hits[t], jnp.concatenate([new] * (d.page_rows // 8), axis=0), val)
                    val = val.astype(BF16)
                    put_page(p, i, val)
                    return val

                keys = jnp.concatenate([first_page(0, i), updated(0, self.kn_s)], axis=0)
                vals.append(updated(1, self.vn_s))
                qs = jnp.concatenate([self.q_s[pl.ds(t * d.rows + i, d.heads, stride=d.stride), :] for t in range(2)], axis=0)
                score = lax.dot_general(qs.astype(BF16), keys, (((1,), (1,)), ((), ())), preferred_element_type=F32) * d.head_dim ** -0.5
                scores.append(jnp.where(self.limit <= n, score, -jnp.inf))
            tops = [jnp.max(score, axis=1, keepdims=True) for score in scores]
            probs = [jnp.exp(score - top) for score, top in zip(scores, tops)]
            totals = [jnp.sum(prob, axis=1, keepdims=True) for prob in probs]
            for u, i in enumerate(ids):
                both = jnp.concatenate([first_page(1, i), vals[u]], axis=0)
                out = jnp.dot(probs[u].astype(BF16), both, preferred_element_type=F32) / totals[u]
                for t in range(2):
                    self.o_s[pl.ds(t * d.rows + i, d.heads, stride=d.stride), :] = out[t * d.heads:(t + 1) * d.heads]

        @pl.loop(0, d.rows // unroll)
        def _(block):
            for k, run in events:
                pl.when(block == k)(run)
            some(block * unroll)

        for h in range(d.heads):
            self.att[:, h * d.head_dim:(h + 1) * d.head_dim] = self.o_s[h * d.stride:h * d.stride + d.tokens, :].astype(BF16)

    def mix(self, layer, events=()):
        d = self.d
        layer = self.zero + layer
        col0 = layer * d.col_layer + d.n_q + 2
        pairs = d.n_u // 2

        def between(j, first):
            for k, run in events:
                if first <= k < first + pairs:
                    pl.when(j == k - first)(run)

        def span(j):
            return pl.ds(aligned(j * CHUNK, CHUNK), CHUNK)

        @pl.loop(0, d.n_o // 2)
        def _(j):
            def body(refs):
                outs = [jnp.dot(self.att[...], ref[...], preferred_element_type=F32) for ref in refs]
                for u in range(2):
                    at = span(2 * j + u)
                    self.y_ref[:, at] = (self.y_ref[:, at].astype(F32) + outs[u]).astype(BF16)

            self.with_cols(col0 + 2 * j, 2, body)

        def up(first, count):
            def body(refs):
                ups = [jnp.dot(self.y_ref[...], ref[...], preferred_element_type=F32) for ref in refs]
                for u in range(count):
                    self.act[:, span(first + u)] = jax.nn.gelu(ups[u].astype(BF16).astype(F32), approximate=True).astype(BF16)

            self.with_cols(col0 + d.n_o + first, count, body)

        def down(first, count):
            def body(refs):
                out = self.acc[...]
                for u in range(count):
                    out += jnp.dot(self.act[:, span(first + u)], refs[u][...], preferred_element_type=F32)
                self.acc[...] = out

            self.with_rows(layer * d.n_u + first, count, body)

        @pl.loop(0, d.n_u // 2)
        def _(j):
            between(j, 0)
            up(2 * j, 2)

        if d.n_u % 2:
            up(d.n_u - 1, 1)

        self.acc[...] = self.y_ref[...].astype(F32)

        @pl.loop(0, d.n_u // 2)
        def _(j):
            between(j, pairs)
            down(2 * j, 2)

        if d.n_u % 2:
            down(d.n_u - 1, 1)

        self.y_ref[...] = self.acc[...].astype(BF16)


class Exchange:
    STEPS = 11

    def __init__(self, side, layer, work, core_buf, ring_buf, out, send_sem, recv_sem):
        self.layer = layer
        self.work, self.core_buf, self.ring_buf, self.out, self.send_sem, self.recv_sem = work, core_buf, ring_buf, out, send_sem, recv_sem
        me = lax.axis_index('kv')
        core, x, y = me % 2, me // 2 % side, me // (2 * side)

        def pairings(pos, stride):
            return (((pos + 1) // 2 % 2, me + (1 - 2 * (pos % 2)) * stride), (pos // 2, me + (side - 1 - 2 * pos) * stride))

        xs, ys = pairings(x, 2), pairings(y, 2 * side)
        self.orders = [xs + ys, xs[::-1] + ys[::-1], ys + xs, ys[::-1] + xs[::-1]]
        self.partner = me + 1 - 2 * core
        self.peers = [self.partner] + [dev for _, dev in xs + ys]
        self.half = work.shape[1] // 2
        self.stream = self.half // 4
        self.base, self.other = core * self.half, (1 - core) * self.half
        self.copies = []
        self.path = [[self.base + k * self.stream for k in range(4)]]
        for ring in range(4):
            self.path.append([self.path[-1][k] + self.orders[k][ring][0] * (self.stream >> (ring + 1)) for k in range(4)])

    def send(self, src, dst, step, lane, dev):
        def copy():
            return pltpu.make_async_remote_copy(src(), dst(), self.send_sem.at[self.layer, step, lane], self.recv_sem.at[self.layer, step, lane], device_id={'kv': dev})

        copy().start()
        self.copies.append(copy)

    def units(self, ref, at, count):
        return lambda: ref.at[self.layer].at[pl.ds(at, count)]

    def results(self, at, count):
        return lambda: self.out.at[pl.ds(at, count)]

    def add(self, dst_at, buf, src_at, count):
        @pl.loop(0, count)
        def _(u):
            self.work[self.layer, dst_at + u] = self.work[self.layer, dst_at + u] + buf[self.layer, src_at + u]

    def halve(self, ring):
        size = self.stream >> (ring + 1)
        for k in range(4):
            bit, dev = self.orders[k][ring]
            src = self.units(self.work, self.path[ring][k] + (1 - bit) * size, size)
            self.send(src, self.units(self.ring_buf, (k + 1) * self.stream - 2 * size, size), 1 + ring, k, dev)

    def halved(self, ring):
        size = self.stream >> (ring + 1)
        for k in range(4):
            self.add(self.path[ring + 1][k], self.ring_buf, (k + 1) * self.stream - 2 * size, size)

    def double(self, ring):
        for k in range(4):
            at = self.results(self.path[ring + 1][k], self.stream >> (ring + 1))
            self.send(at, at, 8 - ring, k, self.orders[k][ring][1])

    def step(self, k):
        for copy in self.copies:
            copy().wait()
        self.copies = []
        if k == 0:
            self.send(self.units(self.work, self.other, self.half), self.units(self.core_buf, 0, self.half), 0, 0, self.partner)
        elif k == 1:
            self.add(self.base, self.core_buf, 0, self.half)
            self.halve(0)
        elif k <= 4:
            self.halved(k - 2)
            self.halve(k - 1)
        elif k == 5:
            self.halved(3)
            for at in self.path[4]:
                for u in range(self.stream >> 4):
                    self.out[at + u] = self.work[self.layer, at + u]
            self.double(3)
        elif k <= 8:
            self.double(8 - k)
        elif k == 9:
            at = self.results(self.base, self.half)
            self.send(at, at, 9, 0, self.partner)


def barrier_with(peers):
    barrier = pltpu.get_barrier_semaphore()
    for dev in peers:
        pl.semaphore_signal(barrier, inc=1, device_id={'kv': dev})
    pl.semaphore_wait(barrier, len(peers))


def adjacent_kernel(dims, side, group_size, entries, table_s, lens_s, src_s, dst_s, table_v, embeds_v, wq, wk, wv, wo, wu, wd, k_hbm, v_hbm,
                    y_ref, info_s, last_out, mig_out,
                    send_buf, first_buf, last_buf, work, core_buf, ring_buf, mid_in, mid_out, x_in, plan_v, plan_s, *rest):
    d = dims
    migs, rest = rest[:d.layers], rest[d.layers:]
    pools, rest = [rest[2 * l:2 * l + 2] for l in range(d.layers)], rest[2 * d.layers:]
    compute, (pool_sem, plan_sem, x_send, x_recv, page_send, page_recv, mig_send, mig_recv, out_sem) = rest[:-9], rest[-9:]
    me = lax.axis_index('kv')
    ahead = lax.rem(me + 1, group_size)
    dec = Decoder(d, 0, d.layers, (wq, wk, wv, wo, wu, wd), y_ref, compute)
    exchanges = [Exchange(side, l, work, core_buf, ring_buf, migs[l], mig_send, mig_recv) for l in range(d.layers)]

    loads = [[pltpu.make_async_copy(src.at[:, l], pools[l][p], pool_sem.at[l, p]) for p, src in enumerate((k_hbm, v_hbm))] for l in range(d.layers)]
    for load in loads[0]:
        load.start()
    barrier = pltpu.get_barrier_semaphore()

    @pl.loop(1, group_size)
    def _(r):
        pl.semaphore_signal(barrier, inc=1, device_id={'kv': lax.rem(me + r, group_size)})

    shift = lax.rem(table_s[1, 0] // d.slots + group_size, group_size)
    src_home = lax.rem(me - shift + group_size, group_size)
    next_home = lax.rem(src_home + 1, group_size)
    pl.semaphore_wait(barrier, group_size - 1)

    groups = d.tokens // 8
    splits = group_size // groups
    cols = d.width // splits

    def piece(ref, m):
        return ref.at[m // splits, :, pl.ds(aligned(m % splits * cols, cols), cols)]

    def all_pieces(phase):
        some = mid_in.at[pl.ds(0, group_size - 1)]
        pltpu.make_async_remote_copy(some, some, x_send.at[phase], x_recv.at[phase], device_id={'kv': me}).wait()

    @pl.loop(1, group_size)
    def _(r):
        m = lax.rem(me + r, group_size)
        pltpu.make_async_remote_copy(piece(embeds_v, m), mid_in.at[me], x_send.at[0], x_recv.at[0], device_id={'kv': m}).start()

    mid_in[me] = piece(embeds_v, me)[...]

    def pass_on():
        all_pieces(0)

        @pl.loop(0, group_size)
        def _(m):
            mid_out[m] = mid_in[lax.rem(m - shift + group_size, group_size)]

        @pl.loop(1, group_size)
        def _(r):
            m = lax.rem(me + r, group_size)
            pltpu.make_async_remote_copy(mid_out.at[m], piece(x_in, me), x_send.at[1], x_recv.at[1], device_id={'kv': m}).start()

        piece(x_in, me)[...] = mid_out[me]

    def take_embeddings():
        all_pieces(1)
        y_ref[...] = x_in[...].reshape(d.tokens, d.width)

    last_ids = table_v[1:2, :]
    plan_v[...] = lax.fori_loop(0, entries, lambda e, acc: jnp.where(last_ids == dst_s[e], e, acc), jnp.full_like(last_ids, -1))
    plan_copy = pltpu.make_async_copy(plan_v, plan_s, plan_sem)

    def own(l):
        @pl.loop(0, entries)
        def _(e):
            slot = src_s[e] - me * d.slots
            mine = (slot >= 0) & (slot < d.slots)
            slot = jnp.clip(slot, 0, d.slots - 1)
            for p in range(2):
                page = pools[l][p][slot]
                work[l, p * entries + e] = jnp.where(mine, page, jnp.zeros_like(page))

    def pack(l):
        @pl.loop(0, d.rows)
        def _(i):
            slot = jnp.clip(table_s[0, next_home * d.rows + i] - me * d.slots, 0, d.slots - 1)
            for p in range(2):
                send_buf[l, p, i] = pools[l][p][slot]

    parts = 8
    size = d.rows // parts

    def first_copy(l, p, rows):
        return pltpu.make_async_remote_copy(send_buf.at[l, p, rows], first_buf.at[l, p, rows], page_send.at[l, p], page_recv.at[l, p], device_id={'kv': ahead})

    def first_start(l, *ks):
        for k in ks:
            first_copy(l, k % 2, pl.ds(k // 2 * size, size)).start()

    def first_wait(l):
        for p in range(2):
            first_copy(l, p, pl.ds(0, d.rows)).wait()

    def check():
        seq = lax.broadcasted_iota(jnp.int32, (1, table_v.shape[1]), 1)
        worker = lax.rem(seq // d.rows + shift, group_size)
        before = lax.rem(worker + group_size - 1, group_size)
        first, last = table_v[0:1, :], table_v[1:2, :]
        bad = (last < worker * d.slots) | (last >= worker * d.slots + d.slots) | (first < before * d.slots) | (first >= before * d.slots + d.slots)
        bad = lax.fori_loop(0, entries, lambda e, acc: acc | (first == dst_s[e]).astype(jnp.int32), bad.astype(jnp.int32))
        info_s[0] = shift
        info_s[1] = 1 - jnp.max(bad)

    first_step, second_step = exchanges[0].step, exchanges[1].step
    for load in loads[0]:
        load.wait()
    own(0)
    first_step(0)
    for l in range(1, d.layers):
        for load in loads[l]:
            load.start()
    dec.start_stream()
    plan_copy.start()
    pack(0)
    first_start(0, 0, 1)
    first_step(1)
    first_start(0, 2, 3)
    pass_on()
    first_step(2)
    first_start(0, 4, 5)
    for l in range(1, d.layers):
        for load in loads[l]:
            load.wait()
    own(1)
    first_step(3)
    first_start(0, 6, 7)
    pack(1)
    first_step(4)
    first_start(0, 8, 9)
    take_embeddings()
    first_step(5)
    first_start(0, 10)
    second_step(0)
    check()
    first_step(6)
    first_start(0, 11)
    second_step(1)
    dec.project(0)
    first_step(7)
    first_start(0, 12)
    second_step(2)
    plan_copy.wait()
    first_step(8)
    first_start(0, 13)
    second_step(3)
    first_step(9)
    first_start(0, 14, 15)
    second_step(4)
    first_step(10)
    first_wait(0)

    def attend(l, events):
        def last_page(p, i):
            entry = plan_s[0, src_home * d.rows + i]
            slot = jnp.clip(table_s[1, src_home * d.rows + i] - me * d.slots, 0, d.slots - 1)
            return jnp.where(entry >= 0, migs[l][p * entries + jnp.maximum(entry, 0)], pools[l][p][slot])

        def put_page(p, i, val):
            last_buf[p, i] = val

        dec.attend(lambda i: lens_s[src_home * d.rows + i], lambda p, i: first_buf[l, p, i], last_page, put_page, events)
        store = pltpu.make_async_copy(last_buf, last_out.at[l], out_sem.at[0])
        store.start()
        return store

    blocks = d.rows // min(UNROLL, d.rows)
    pairs = 2 * (d.n_u // 2)
    events = [(k * pairs // (2 * parts), functools.partial(first_start, 1, k)) for k in range(2 * parts)]
    events += [((k - 7) * pairs // 6, functools.partial(second_step, k)) for k in range(7, 11)]
    last_store = attend(0, [(0, functools.partial(second_step, 5)), (blocks * 3 // 4, functools.partial(second_step, 6))])
    dec.mix(0, sorted(events, key=lambda event: event[0]))
    for l in range(1, d.layers):
        dec.project(l)
        first_wait(l)
        last_store.wait()
        last_store = attend(l, [])
        if l == 1:
            mig_stores = [pltpu.make_async_copy(migs[k], mig_out.at[k], out_sem.at[1 + k]) for k in range(d.layers)]
            for store in mig_stores:
                store.start()
        dec.mix(l)
    for store in [last_store] + mig_stores:
        store.wait()


def decode_adjacent(side, group_size, d, table, seq_lens, mig_src, mig_dst, embeds, weights, k_pool, v_pool):
    entries = mig_src.shape[0]
    page = (d.page_rows, d.head_dim)
    struct = lambda *shape: jax.ShapeDtypeStruct(shape, BF16)
    groups = d.tokens // 8
    mid = pltpu.VMEM((group_size, 8, d.width * groups // group_size), BF16)
    return pl.pallas_call(
        functools.partial(adjacent_kernel, d, side, group_size, entries),
        out_shape=[struct(d.tokens, d.width), jax.ShapeDtypeStruct((2,), jnp.int32), struct(d.layers, 2, d.rows, *page), struct(d.layers, 2 * entries, *page)],
        in_specs=[SMEM] * 4 + [VMEM] * 2 + [ANY] * 8,
        out_specs=[VMEM, SMEM, ANY, ANY],
        scratch_shapes=[
            pltpu.VMEM((d.layers, 2, d.rows) + page, BF16),
            pltpu.VMEM((d.layers, 2, d.rows) + page, BF16),
            pltpu.VMEM((2, d.rows) + page, BF16),
            pltpu.VMEM((d.layers, 2 * entries) + page, BF16),
            pltpu.VMEM((d.layers, entries) + page, BF16),
            pltpu.VMEM((d.layers, entries) + page, BF16),
            mid,
            mid,
            pltpu.VMEM((groups, 8, d.width), BF16),
            pltpu.VMEM((1, table.shape[1]), jnp.int32),
            pltpu.SMEM((1, table.shape[1]), jnp.int32),
        ] + [pltpu.VMEM((2 * entries,) + page, BF16)] * d.layers + [pltpu.VMEM((d.slots,) + page, BF16)] * (2 * d.layers) + d.compute_scratch(10, 8) + [
            DMA((d.layers, 2)),
            DMA,
            DMA((2,)),
            DMA((2,)),
            DMA((d.layers, 2)),
            DMA((d.layers, 2)),
            DMA((d.layers, 10, 4)),
            DMA((d.layers, 10, 4)),
            DMA((1 + d.layers,)),
        ],
        compiler_params=pltpu.CompilerParams(collective_id=1, has_side_effects=True, vmem_limit_bytes=LIMIT),
        cost_estimate=d.cost(d.layers),
        name="decode_adjacent",
    )(table, seq_lens, mig_src, mig_dst, table, embeds.reshape(groups, 8, d.width), *weights, k_pool, v_pool)


def fill_pools_kernel(dims, group_size, entries, info_s, table_s, src_s, dst_s, k_hbm, v_hbm, last_hbm, mig_hbm, k_out, v_out, k_buf, v_buf, sem, fix_sem):
    d = dims
    me = lax.axis_index('kv')
    src_home = lax.rem(me - info_s[0] + group_size, group_size)
    pools = ((k_hbm, k_buf, k_out), (v_hbm, v_buf, v_out))
    parts = 4
    size = d.slots // parts

    def moves(out):
        return [pltpu.make_async_copy(*((buf.at[at], dst.at[at]) if out else (src.at[at], buf.at[at])), sem.at[p, part])
                for part in range(parts) for at in [pl.ds(part * size, size)] for p, (src, buf, dst) in enumerate(pools)]

    def local(slot):
        slot = slot - me * d.slots
        return (slot >= 0) & (slot < d.slots), jnp.clip(slot, 0, d.slots - 1)

    def migrated(run):
        @pl.loop(0, entries)
        def _(e):
            mine, slot = local(dst_s[e])

            @pl.when(mine)
            def _():
                for p, (_, buf, _) in enumerate(pools):
                    for l in range(d.layers):
                        run(pltpu.make_async_copy(mig_hbm.at[l, p * entries + e], buf.at[slot, l], fix_sem))

    def updated(run):
        @pl.loop(0, d.rows)
        def _(i):
            _, slot = local(table_s[1, src_home * d.rows + i])
            for p, (_, buf, _) in enumerate(pools):
                for l in range(d.layers):
                    run(pltpu.make_async_copy(last_hbm.at[l, p, i], buf.at[slot, l], fix_sem))

    start, wait = lambda copy: copy.start(), lambda copy: copy.wait()
    for copy in moves(False):
        copy.start()
    for copy in moves(False):
        copy.wait()
    migrated(start)
    migrated(wait)
    updated(start)

    @pl.loop(0, entries)
    def _(e):
        mine, slot = local(src_s[e])

        @pl.when(mine)
        def _():
            for _, buf, _ in pools:
                buf[slot] = jnp.zeros(buf.shape[1:], buf.dtype)

    updated(wait)
    for copy in moves(True):
        copy.start()
    for copy in moves(True):
        copy.wait()


def fill_pools(group_size, d, info, table, mig_src, mig_dst, k_pool, v_pool, last, mig):
    entries = mig_src.shape[0]
    size = 4 * k_pool.size
    return pl.pallas_call(
        functools.partial(fill_pools_kernel, d, group_size, entries),
        out_shape=[jax.ShapeDtypeStruct(k_pool.shape, k_pool.dtype)] * 2,
        in_specs=[SMEM] * 4 + [ANY] * 4,
        out_specs=[ANY, ANY],
        scratch_shapes=[pltpu.VMEM(k_pool.shape, k_pool.dtype), pltpu.VMEM(k_pool.shape, k_pool.dtype), DMA((2, 4)), DMA],
        compiler_params=pltpu.CompilerParams(vmem_limit_bytes=LIMIT),
        cost_estimate=pl.CostEstimate(flops=40 * size, bytes_accessed=2 * size, transcendentals=0),
        name="fill_pools",
    )(info, table, mig_src, mig_dst, k_pool, v_pool, last, mig)


def gather_pages_kernel(idx_ref, k_hbm, v_hbm, k_out, v_out, sem):
    rows = k_out.shape[0]

    def copies(i):
        slot = jnp.maximum(idx_ref[i], 0)
        return (pltpu.make_async_copy(k_hbm.at[slot], k_out.at[i], sem), pltpu.make_async_copy(v_hbm.at[slot], v_out.at[i], sem))

    @pl.loop(0, rows)
    def _(i):
        @pl.when(idx_ref[i] >= 0)
        def _():
            for copy in copies(i):
                copy.start()

        @pl.when(idx_ref[i] < 0)
        def _():
            k_out[i] = jnp.zeros(k_out.shape[1:], k_out.dtype)
            v_out[i] = jnp.zeros(v_out.shape[1:], v_out.dtype)

    @pl.loop(0, rows)
    def _(i):
        @pl.when(idx_ref[i] >= 0)
        def _():
            for copy in copies(i):
                copy.wait()


def gather_pages(idx, k_pool, v_pool):
    shape = jax.ShapeDtypeStruct((idx.shape[0],) + k_pool.shape[1:], k_pool.dtype)
    return pl.pallas_call(
        gather_pages_kernel,
        out_shape=[shape, shape],
        in_specs=[SMEM, ANY, ANY],
        out_specs=[VMEM, VMEM],
        scratch_shapes=[DMA],
        compiler_params=pltpu.CompilerParams(vmem_limit_bytes=LIMIT),
        name="gather_pages",
    )(idx, k_pool, v_pool)


def share_kernel(side, k_hbm, v_hbm, k_out, v_out, work, core_buf, ring_buf, load_sem, send_sem, recv_sem, *migs):
    entries, layers = k_hbm.shape[:2]
    me_exchange = [Exchange(side, l, work, core_buf, ring_buf, migs[l], send_sem, recv_sem) for l in range(layers)]
    loads = [pltpu.make_async_copy(src.at[:, l], work.at[l, pl.ds(p * entries, entries)], load_sem.at[l, p]) for l in range(layers) for p, src in enumerate((k_hbm, v_hbm))]
    for load in loads:
        load.start()
    barrier_with(me_exchange[0].peers)
    for load in loads:
        load.wait()
    for k in range(Exchange.STEPS):
        for exchange in me_exchange:
            exchange.step(k)
    stores = [pltpu.make_async_copy(migs[l].at[pl.ds(p * entries, entries)], dst.at[:, l], load_sem.at[l, p]) for l in range(layers) for p, dst in enumerate((k_out, v_out))]
    for store in stores:
        store.start()
    for store in stores:
        store.wait()


def share(mig_k, mig_v, side):
    entries, layers = mig_k.shape[:2]
    page = mig_k.shape[2:]
    return pl.pallas_call(
        functools.partial(share_kernel, side),
        out_shape=[jax.ShapeDtypeStruct(mig_k.shape, BF16)] * 2,
        in_specs=[ANY, ANY],
        out_specs=[ANY, ANY],
        scratch_shapes=[
            pltpu.VMEM((layers, 2 * entries) + page, BF16),
            pltpu.VMEM((layers, entries) + page, BF16),
            pltpu.VMEM((layers, entries) + page, BF16),
            DMA((layers, 2)),
            DMA((layers, 10, 4)),
            DMA((layers, 10, 4)),
        ] + [pltpu.VMEM((2 * entries,) + page, BF16)] * layers,
        compiler_params=pltpu.CompilerParams(collective_id=0, has_side_effects=True, vmem_limit_bytes=LIMIT),
        name="share",
    )(mig_k, mig_v)


def migrate_kernel(dst_ref, src_ref, k_hbm, v_hbm, mk_hbm, mv_hbm, k_out, v_out, k_buf, v_buf, sem, fix_sem):
    entries = dst_ref.shape[0]
    pairs = ((k_hbm, mk_hbm, k_buf, k_out), (v_hbm, mv_hbm, v_buf, v_out))
    for p, (src, _, buf, _) in enumerate(pairs):
        pltpu.make_async_copy(src, buf, sem.at[p]).start()
    for p, (src, _, buf, _) in enumerate(pairs):
        pltpu.make_async_copy(src, buf, sem.at[p]).wait()

    @pl.loop(0, entries)
    def _(e):
        @pl.when(dst_ref[e] >= 0)
        def _():
            for _, mig, buf, _ in pairs:
                copy = pltpu.make_async_copy(mig.at[e], buf.at[jnp.maximum(dst_ref[e], 0)], fix_sem)
                copy.start()
                copy.wait()

        @pl.when(src_ref[e] >= 0)
        def _():
            for _, _, buf, _ in pairs:
                buf[jnp.maximum(src_ref[e], 0)] = jnp.zeros(buf.shape[1:], buf.dtype)

    for p, (_, _, buf, dst) in enumerate(pairs):
        pltpu.make_async_copy(buf, dst, sem.at[p]).start()
    for p, (_, _, buf, dst) in enumerate(pairs):
        pltpu.make_async_copy(buf, dst, sem.at[p]).wait()


def migrate(dst_local, src_local, k_pool, v_pool, mig_k, mig_v):
    shape = jax.ShapeDtypeStruct(k_pool.shape, k_pool.dtype)
    return pl.pallas_call(
        migrate_kernel,
        out_shape=[shape, shape],
        in_specs=[SMEM, SMEM, ANY, ANY, ANY, ANY],
        out_specs=[ANY, ANY],
        scratch_shapes=[pltpu.VMEM(k_pool.shape, k_pool.dtype), pltpu.VMEM(k_pool.shape, k_pool.dtype), DMA((2,)), DMA],
        compiler_params=pltpu.CompilerParams(vmem_limit_bytes=LIMIT),
        name="migrate",
    )(dst_local, src_local, k_pool, v_pool, mig_k, mig_v)


def decode_kernel(dims, sc_ref, x_ref, p0k_hbm, p0v_hbm, wq, wk, wv, wo, wu, wd, k_in, v_in, y_ref, k_out, v_out,
                  first_buf, last_buf, *rest):
    compute, (page_sem, put_sem) = rest[:-2], rest[-2:]
    d = dims
    dec = Decoder(d, 0, d.layers, (wq, wk, wv, wo, wu, wd), y_ref, compute)
    dec.start_stream()
    y_ref[...] = x_ref[...]
    loads = [pltpu.make_async_copy(src, first_buf.at[p], page_sem.at[p]) for p, src in enumerate((p0k_hbm, p0v_hbm))]
    for load in loads:
        load.start()

    def last_loads(run):
        @pl.loop(0, d.rows)
        def _(i):
            for p, src in enumerate((k_in, v_in)):
                run(pltpu.make_async_copy(src.at[sc_ref[0, i]], last_buf.at[p, i], page_sem.at[2]))

    def puts(run):
        @pl.loop(0, d.rows)
        def _(i):
            @pl.when(sc_ref[2, i] > 0)
            def _():
                for p, dst in enumerate((k_out, v_out)):
                    run(pltpu.make_async_copy(last_buf.at[p, i], dst.at[sc_ref[0, i]], put_sem))

    last_loads(lambda copy: copy.start())
    for load in loads:
        load.wait()
    last_loads(lambda copy: copy.wait())

    @pl.loop(0, d.layers)
    def _(layer):
        def put_page(p, i, val):
            last_buf[p, i, layer] = val

        dec.project(layer)
        dec.attend(lambda i: sc_ref[1, i], lambda p, i: first_buf[p, i, layer], lambda p, i: last_buf[p, i, layer], put_page)
        dec.mix(layer)

    puts(lambda copy: copy.start())
    puts(lambda copy: copy.wait())


def decode(d, scalars, x, p0k, p0v, weights, k_pool, v_pool):
    pool = jax.ShapeDtypeStruct(k_pool.shape, k_pool.dtype)
    pages = pltpu.VMEM((2, d.rows, d.layers, d.page_rows, d.head_dim), BF16)
    return pl.pallas_call(
        functools.partial(decode_kernel, d),
        out_shape=[jax.ShapeDtypeStruct(x.shape, x.dtype), pool, pool],
        in_specs=[SMEM, VMEM] + [ANY] * 10,
        out_specs=[VMEM, ANY, ANY],
        input_output_aliases={10: 1, 11: 2},
        scratch_shapes=[pages, pages] + d.compute_scratch(16, 16) + [DMA((3,)), DMA],
        compiler_params=pltpu.CompilerParams(vmem_limit_bytes=LIMIT),
        cost_estimate=d.cost(d.layers),
        name="decode",
    )(scalars, x, p0k, p0v, *weights, k_pool, v_pool)


def permute(arrays, shift, group_size):
    perm = [(i, (i + shift) % group_size) for i in range(group_size)]
    return tuple(lax.ppermute(a, 'kv', perm) for a in arrays)


def rotate(arrays, shift, group_size, beside=lambda: ()):
    def branch(r):
        return lambda args: (permute(args, r, group_size) if r else args, beside())

    return lax.switch(shift, [branch(r) for r in range(group_size)], tuple(arrays))


def rotate_bits(arrays, shift, group_size):
    arrays = tuple(arrays)
    bit = 1
    while bit < group_size:
        move = functools.partial(permute, shift=bit, group_size=group_size)
        arrays = lax.cond(shift // bit % 2 == 1, move, lambda args: args, arrays)
        bit *= 2
    return arrays


def solution(mesh):
    group_size = mesh.shape['kv']
    side = math.isqrt(group_size // 2)
    pool_spec = P(('rep', 'kv'))
    tok_spec = P(None, ('rep', 'kv'), None)

    def device_fn(embeds, w_query, w_key, w_value, w_out, w_up, w_down, k_pool5, v_pool5, new_table, seq_lens, mig_src, mig_dst):
        me = lax.axis_index('kv')
        slots, layers, page, kv_heads, head_dim = k_pool5.shape
        rows, width = embeds.shape[1:]
        weights = (w_query, w_key, w_value, w_out, w_up, w_down)
        k_pool = k_pool5.reshape(slots, layers, page * kv_heads, head_dim)
        v_pool = v_pool5.reshape(slots, layers, page * kv_heads, head_dim)
        d = Dims(rows, weights, k_pool, page)
        ints = jnp.int32

        def local(ids):
            loc = ids - me * slots
            return jnp.where((loc >= 0) & (loc < slots), loc, -1)

        def take(vec, dev):
            return lax.dynamic_slice(vec, (dev * rows,), (rows,))

        def inside(ids):
            return jnp.clip(ids - me * slots, 0, slots - 1)

        def general_path():
            first_new, last_new = new_table[:, 0], new_table[:, 1]
            moved = first_new[None, :] == mig_dst[:, None]
            first_old = jnp.where(jnp.any(moved, axis=0), jnp.sum(jnp.where(moved, mig_src[:, None], 0), axis=0), first_new)
            home = jnp.arange(first_new.shape[0], dtype=ints) // rows
            worker = last_new // slots
            shift_of = (worker - home + group_size) % group_size
            first_shift = (worker - first_old // slots + group_size) % group_size
            shift_ids = jnp.arange(group_size, dtype=ints)
            wanted = jnp.any(shift_of[None, :] == shift_ids[:, None], axis=1)
            mig_k, mig_v = gather_pages(local(mig_src), k_pool, v_pool)
            mig_k, mig_v = share(mig_k, mig_v, side)
            k_new, v_new = migrate(local(mig_dst), local(mig_src), k_pool, v_pool, mig_k, mig_v)

            def one_round(shift, y, k_new, v_new):
                src_home = (me - shift + group_size) % group_size
                (x,) = rotate_bits((embeds.reshape(2 * rows, width),), shift, group_size)
                in_round = shift_of == shift
                wanted2 = jnp.any(in_round[None, :] & (first_shift[None, :] == shift_ids[:, None]), axis=1)

                def more(state):
                    left, pk, pv = state
                    shift2 = jnp.argmax(left).astype(ints)
                    dest_home = (me + shift2 - shift + group_size) % group_size
                    got = gather_pages(inside(take(first_old, dest_home)), k_pool, v_pool)
                    got_k, got_v = rotate_bits(got, shift2, group_size)
                    mine = (take(first_shift, src_home) == shift2)[:, None, None, None]
                    return left & (shift_ids != shift2), jnp.where(mine, got_k, pk), jnp.where(mine, got_v, pv)

                zeros = jnp.zeros((rows,) + k_pool.shape[1:], k_pool.dtype)
                _, pk, pv = lax.while_loop(lambda state: jnp.any(state[0]), more, (wanted2, zeros, zeros))
                valid = take(shift_of, src_home) == shift
                scalars = jnp.stack([inside(take(last_new, src_home)), take(seq_lens, src_home), valid.astype(ints)])
                out, k_new, v_new = decode(d, scalars, x, pk, pv, weights, k_new, v_new)
                (back,) = rotate_bits((out,), (group_size - shift) % group_size, group_size)
                mine = (take(shift_of, me) == shift)[None, :, None]
                return jnp.where(mine, back.reshape(embeds.shape), y), k_new, v_new

            def next_round(state):
                left, y, k_new, v_new = state
                shift = jnp.argmax(left).astype(ints)
                y, k_new, v_new = one_round(shift, y, k_new, v_new)
                return left & (shift_ids != shift), y, k_new, v_new

            _, y, k_new, v_new = lax.while_loop(lambda state: jnp.any(state[0]), next_round, (wanted, jnp.zeros_like(embeds), k_new, v_new))
            return y, k_new, v_new

        table = new_table.T
        y, info, last, mig = decode_adjacent(side, group_size, d, table, seq_lens, mig_src, mig_dst, embeds, weights, k_pool, v_pool)
        (y,), (k_new, v_new) = rotate((y,), (group_size - info[0]) % group_size, group_size, lambda: fill_pools(group_size, d, info, table, mig_src, mig_dst, k_pool, v_pool, last, mig))
        _, y, k_new, v_new = lax.while_loop(lambda state: state[0] == 0, lambda state: (jnp.ones_like(state[0]),) + general_path(), (info[1], y.reshape(embeds.shape), k_new, v_new))
        return y, k_new.reshape(k_pool5.shape), v_new.reshape(v_pool5.shape)

    return jax.shard_map(device_fn, mesh=mesh, in_specs=(tok_spec, P(), P(), P(), P(), P(), P(), pool_spec, pool_spec, P('rep', None), P('rep'), P('rep'), P('rep')), out_specs=(tok_spec, pool_spec, pool_spec), check_vma=False)
```

```python
import functools
import math

import jax
import jax.numpy as jnp
from jax import lax
from jax.experimental import pallas as pl
from jax.experimental.pallas import tpu as pltpu
from jax.sharding import PartitionSpec as P

ANY = pl.BlockSpec(memory_space=pl.ANY)
SMEM = pl.BlockSpec(memory_space=pltpu.SMEM)
VMEM = pl.BlockSpec(memory_space=pltpu.VMEM)
DMA = pltpu.SemaphoreType.DMA
CHUNK = 256
UNROLL = 8
LIMIT = 63 << 20
F32, BF16 = jnp.float32, jnp.bfloat16


def aligned(x, multiple):
    return x if isinstance(x, int) else pl.multiple_of(x, multiple)


class Dims:
    def __init__(self, rows, weights, k_pool, page):
        w_query, w_key, _, _, w_up, _ = weights
        self.layers, self.width, self.q_width = w_query.shape
        self.ff = w_up.shape[2]
        self.slots, _, self.page_rows, self.head_dim = k_pool.shape
        self.kv_heads = w_key.shape[2] // self.head_dim
        self.heads = self.q_width // self.head_dim
        self.page, self.rows = page, rows
        self.tokens = 2 * rows
        self.stride = self.tokens + 8
        self.n_q, self.n_o, self.n_u = self.q_width // CHUNK, self.width // CHUNK, self.ff // CHUNK
        self.col_layer = self.n_q + 2 + self.n_o + self.n_u

    def compute_scratch(self, n_col, n_row):
        return [
            pltpu.VMEM((n_col, self.width, CHUNK), BF16),
            pltpu.VMEM((n_row, CHUNK, self.width), BF16),
            pltpu.VMEM((self.heads * self.stride, self.head_dim), F32),
            pltpu.VMEM((self.kv_heads * self.stride, self.head_dim), F32),
            pltpu.VMEM((self.kv_heads * self.stride, self.head_dim), F32),
            pltpu.VMEM((self.heads * self.stride, self.head_dim), F32),
            pltpu.VMEM((self.tokens, self.q_width), BF16),
            pltpu.VMEM((self.tokens, self.ff), BF16),
            pltpu.VMEM((self.tokens, self.width), F32),
            DMA((n_col,)),
            DMA((n_row,)),
        ]

    def cost(self, layers):
        size = layers * self.width * (2 * self.q_width + 2 * self.kv_heads * self.head_dim + 2 * self.ff)
        return pl.CostEstimate(flops=2 * size * self.tokens, bytes_accessed=2 * size, transcendentals=0)


class Decoder:
    def __init__(self, dims, first, layers, weights, y_ref, scratch):
        self.d, self.first, self.layers, self.weights, self.y_ref = dims, first, layers, weights, y_ref
        (self.col_buf, self.row_buf, self.q_s, self.kn_s, self.vn_s, self.o_s, self.att, self.act, self.acc, self.col_sem, self.row_sem) = scratch
        self.n_col, self.n_row = self.col_buf.shape[0], self.row_buf.shape[0]
        self.zero = lax.axis_index('kv') * 0
        d = dims
        cols = 2 * d.page * d.kv_heads
        col_pos = lax.broadcasted_iota(jnp.int32, (2 * d.heads, cols), 1)
        row_pos = lax.broadcasted_iota(jnp.int32, (2 * d.heads, cols), 0)
        same_head = (col_pos % d.kv_heads) == (row_pos % d.heads) // (d.heads // d.kv_heads)
        self.limit = jnp.where(same_head, col_pos // d.kv_heads - row_pos // d.heads, 4 * d.page)
        self.page_pos = lax.broadcasted_iota(jnp.int32, (d.page_rows, d.head_dim), 0) // d.kv_heads
        self.tile_head = lax.broadcasted_iota(jnp.int32, (8, d.head_dim), 0) % d.kv_heads

    def layer_of(self, g, per_layer):
        return sum((g >= per_layer * l).astype(jnp.int32) for l in range(1, self.layers))

    def col_start(self, g):
        d = self.d
        wq, wk, wv, wo, wu, _ = self.weights

        @pl.when(g < self.layers * d.col_layer)
        def _():
            layer = self.layer_of(g, d.col_layer)
            pos = g - layer * d.col_layer
            slot = g % self.n_col

            def go(src, c):
                start = aligned(c * CHUNK, CHUNK)
                pltpu.make_async_copy(src.at[self.first + layer].at[:, pl.ds(start, CHUNK)], self.col_buf.at[slot], self.col_sem.at[slot]).start()

            @pl.when(pos < d.n_q)
            def _():
                go(wq, pos)

            @pl.when(pos == d.n_q)
            def _():
                go(wk, 0)

            @pl.when(pos == d.n_q + 1)
            def _():
                go(wv, 0)

            @pl.when((pos >= d.n_q + 2) & (pos < d.n_q + 2 + d.n_o))
            def _():
                go(wo, pos - (d.n_q + 2))

            @pl.when(pos >= d.n_q + 2 + d.n_o)
            def _():
                go(wu, pos - (d.n_q + 2 + d.n_o))

    def row_start(self, g):
        d = self.d
        wd = self.weights[5]

        @pl.when(g < self.layers * d.n_u)
        def _():
            layer = self.layer_of(g, d.n_u)
            slot = g % self.n_row
            start = aligned((g - layer * d.n_u) * CHUNK, CHUNK)
            pltpu.make_async_copy(wd.at[self.first + layer].at[pl.ds(start, CHUNK)], self.row_buf.at[slot], self.row_sem.at[slot]).start()

    def start_stream(self):
        @pl.loop(0, self.n_col)
        def _(g):
            self.col_start(g)

        @pl.loop(0, self.n_row)
        def _(g):
            self.row_start(g)

    def with_cols(self, g, count, body):
        slots = [(g + u) % self.n_col for u in range(count)]
        for slot in slots:
            pltpu.make_async_copy(self.weights[1].at[0], self.col_buf.at[slot], self.col_sem.at[slot]).wait()
        body([self.col_buf.at[slot] for slot in slots])
        for u in range(count):
            self.col_start(g + u + self.n_col)

    def with_rows(self, g, count, body):
        slots = [(g + u) % self.n_row for u in range(count)]
        for slot in slots:
            pltpu.make_async_copy(self.weights[5].at[0, pl.ds(0, CHUNK), :], self.row_buf.at[slot], self.row_sem.at[slot]).wait()
        body([self.row_buf.at[slot] for slot in slots])
        for u in range(count):
            self.row_start(g + u + self.n_row)

    def project(self, layer):
        d = self.d
        col0 = (self.zero + layer) * d.col_layer

        def product(ref):
            return jnp.dot(self.y_ref[...], ref[...], preferred_element_type=F32).astype(BF16).astype(F32)

        def put(dst, first, out):
            for h in range(CHUNK // d.head_dim):
                at = aligned((first + h) * d.stride, 8)
                dst[pl.ds(at, d.tokens), :] = out[:, h * d.head_dim:(h + 1) * d.head_dim]

        @pl.loop(0, d.n_q // 2)
        def _(j):
            def body(refs):
                outs = [product(ref) for ref in refs]
                for u in range(2):
                    put(self.q_s, (2 * j + u) * (CHUNK // d.head_dim), outs[u])

            self.with_cols(col0 + 2 * j, 2, body)

        def body(refs):
            outs = [product(ref) for ref in refs]
            put(self.kn_s, 0, outs[0])
            put(self.vn_s, 0, outs[1])

        self.with_cols(col0 + d.n_q, 2, body)

    def insert(self, page, n, row):
        d = self.d
        val = page.astype(F32)
        for t in range(2):
            new = jnp.broadcast_to(row(t, 0), (8, d.head_dim))
            for g in range(1, d.kv_heads):
                new = jnp.where(self.tile_head == g, row(t, g), new)
            val = jnp.where(self.page_pos == n - d.page + t, jnp.concatenate([new] * (d.page_rows // 8), axis=0), val)
        return val.astype(BF16)

    def attend(self, lens, first_page, last_page, put_page, events=(), begin=0, count=None):
        d = self.d
        count = count or d.rows
        unroll = min(UNROLL, count)

        def some(first):
            ids = [first + u for u in range(unroll)]
            scores, vals = [], []
            for i in ids:
                n = lens(i)

                def updated(p, new_ref):
                    val = self.insert(last_page(p, i), n, lambda t, g: new_ref[pl.ds(g * d.stride + t * d.rows + i, 1), :])
                    put_page(p, i, val)
                    return val

                keys = jnp.concatenate([first_page(0, i), updated(0, self.kn_s)], axis=0)
                vals.append(updated(1, self.vn_s))
                qs = jnp.concatenate([self.q_s[pl.ds(t * d.rows + i, d.heads, stride=d.stride), :] for t in range(2)], axis=0)
                score = lax.dot_general(qs.astype(BF16), keys, (((1,), (1,)), ((), ())), preferred_element_type=F32) * d.head_dim ** -0.5
                scores.append(jnp.where(self.limit <= n, score, -jnp.inf))
            tops = [jnp.max(score, axis=1, keepdims=True) for score in scores]
            probs = [jnp.exp(score - top) for score, top in zip(scores, tops)]
            totals = [jnp.sum(prob, axis=1, keepdims=True) for prob in probs]
            for u, i in enumerate(ids):
                both = jnp.concatenate([first_page(1, i), vals[u]], axis=0)
                out = jnp.dot(probs[u].astype(BF16), both, preferred_element_type=F32) / totals[u]
                for t in range(2):
                    self.o_s[pl.ds(t * d.rows + i, d.heads, stride=d.stride), :] = out[t * d.heads:(t + 1) * d.heads]

        @pl.loop(0, count // unroll)
        def _(block):
            for k, run in events:
                pl.when(block == k)(run)
            some(begin + block * unroll)

    def gather_heads(self):
        d = self.d
        for h in range(d.heads):
            self.att[:, h * d.head_dim:(h + 1) * d.head_dim] = self.o_s[h * d.stride:h * d.stride + d.tokens, :].astype(BF16)

    def mix(self, layer, events=()):
        d = self.d
        layer = self.zero + layer
        col0 = layer * d.col_layer + d.n_q + 2
        pairs = d.n_u // 2

        def between(j, first):
            for k, run in events:
                if first <= k < first + pairs:
                    pl.when(j == k - first)(run)

        def span(j):
            return pl.ds(aligned(j * CHUNK, CHUNK), CHUNK)

        @pl.loop(0, d.n_o // 2)
        def _(j):
            def body(refs):
                outs = [jnp.dot(self.att[...], ref[...], preferred_element_type=F32) for ref in refs]
                for u in range(2):
                    at = span(2 * j + u)
                    self.y_ref[:, at] = (self.y_ref[:, at].astype(F32) + outs[u]).astype(BF16)

            self.with_cols(col0 + 2 * j, 2, body)

        def up(first, count):
            def body(refs):
                ups = [jnp.dot(self.y_ref[...], ref[...], preferred_element_type=F32) for ref in refs]
                for u in range(count):
                    self.act[:, span(first + u)] = jax.nn.gelu(ups[u].astype(BF16).astype(F32), approximate=True).astype(BF16)

            self.with_cols(col0 + d.n_o + first, count, body)

        def down(first, count):
            def body(refs):
                out = self.acc[...]
                for u in range(count):
                    out += jnp.dot(self.act[:, span(first + u)], refs[u][...], preferred_element_type=F32)
                self.acc[...] = out

            self.with_rows(layer * d.n_u + first, count, body)

        @pl.loop(0, d.n_u // 2)
        def _(j):
            between(j, 0)
            up(2 * j, 2)

        if d.n_u % 2:
            up(d.n_u - 1, 1)

        self.acc[...] = self.y_ref[...].astype(F32)

        @pl.loop(0, d.n_u // 2)
        def _(j):
            between(j, pairs)
            down(2 * j, 2)

        if d.n_u % 2:
            down(d.n_u - 1, 1)

        self.y_ref[...] = self.acc[...].astype(BF16)


class Exchange:
    STEPS = 11

    def __init__(self, side, layer, work, core_buf, ring_buf, out, send_sem, recv_sem):
        self.layer = layer
        self.work, self.core_buf, self.ring_buf, self.out, self.send_sem, self.recv_sem = work, core_buf, ring_buf, out, send_sem, recv_sem
        me = lax.axis_index('kv')
        core, x, y = me % 2, me // 2 % side, me // (2 * side)

        def pairings(pos, stride):
            return (((pos + 1) // 2 % 2, me + (1 - 2 * (pos % 2)) * stride), (pos // 2, me + (side - 1 - 2 * pos) * stride))

        xs, ys = pairings(x, 2), pairings(y, 2 * side)
        self.orders = [xs + ys, xs[::-1] + ys[::-1], ys + xs, ys[::-1] + xs[::-1]]
        self.partner = me + 1 - 2 * core
        self.peers = [self.partner] + [dev for _, dev in xs + ys]
        self.half = work.shape[1] // 2
        self.stream = self.half // 4
        self.base, self.other = core * self.half, (1 - core) * self.half
        self.copies, self.done = [], 0
        self.path = [[self.base + k * self.stream for k in range(4)]]
        self.away = []
        for ring in range(4):
            size = self.stream >> (ring + 1)
            self.away.append([self.path[-1][k] + (1 - self.orders[k][ring][0]) * size for k in range(4)])
            self.path.append([self.path[-1][k] + self.orders[k][ring][0] * size for k in range(4)])

    def send(self, src, dst, step, lane, dev):
        def copy():
            return pltpu.make_async_remote_copy(src(), dst(), self.send_sem.at[self.layer, step, lane], self.recv_sem.at[self.layer, step, lane], device_id={'kv': dev})

        copy().start()
        self.copies.append(copy)

    def units(self, ref, at, count):
        return lambda: ref.at[self.layer].at[pl.ds(at, count)]

    def results(self, at, count):
        return lambda: self.out.at[pl.ds(at, count)]

    def add(self, dst_at, buf, src_at, count):
        @pl.loop(0, count)
        def _(u):
            self.work[self.layer, dst_at + u] = self.work[self.layer, dst_at + u] + buf[self.layer, src_at + u]

    def halve(self, ring, k):
        size = self.stream >> (ring + 1)
        src = self.units(self.work, self.away[ring][k], size)
        self.send(src, self.units(self.ring_buf, (k + 1) * self.stream - 2 * size, size), 1 + ring, k, self.orders[k][ring][1])

    def halved(self, ring, k):
        size = self.stream >> (ring + 1)
        self.add(self.path[ring + 1][k], self.ring_buf, (k + 1) * self.stream - 2 * size, size)

    def double(self, ring, k):
        at = self.results(self.path[ring + 1][k], self.stream >> (ring + 1))
        self.send(at, at, 8 - ring, k, self.orders[k][ring][1])

    def step(self):
        step, self.done = self.done, self.done + 1
        started, self.copies = self.copies, []
        if step in (1, 9, 10):
            for copy in started:
                copy().wait()
        if step == 0:
            self.send(self.units(self.work, self.other, self.half), self.units(self.core_buf, 0, self.half), 0, 0, self.partner)
        elif step == 1:
            self.add(self.base, self.core_buf, 0, self.half)
            for k in range(4):
                self.halve(0, k)
        elif step < 9:
            for k in range(4):
                started[k]().wait()
                if step < 6:
                    self.halved(step - 2, k)
                if step < 5:
                    self.halve(step - 1, k)
                    continue
                if step == 5:
                    for u in range(self.stream >> 4):
                        self.out[self.path[4][k] + u] = self.work[self.layer, self.path[4][k] + u]
                self.double(8 - step, k)
        elif step == 9:
            at = self.results(self.base, self.half)
            self.send(at, at, 9, 0, self.partner)


def adjacent_kernel(dims, side, group_size, entries, src_s, dst_s, table_hbm, lens_hbm, embeds_hbm, wq, wk, wv, wo, wu, wd, k_hbm, v_hbm,
                    ya_ref, yb_ref, info_s, last_out, mig_out,
                    table_s, lens_s, table_v, embeds_v, y_ref, send_buf, got_buf, last_buf, new_buf, work, core_buf, ring_buf, mid_in, mid_out, x_in, plan_v, plan_s, *rest):
    d = dims
    migs, rest = rest[:d.layers], rest[d.layers:]
    pools, rest = [rest[2 * l:2 * l + 2] for l in range(d.layers)], rest[2 * d.layers:]
    compute, (load_sem, pool_sem, plan_sem, x_send, x_recv, page_send, page_recv, new_send, new_recv, mig_send, mig_recv, out_sem) = rest[:-12], rest[-12:]
    half = d.rows // 2
    me = lax.axis_index('kv')
    ahead, behind = lax.rem(me + 1, group_size), lax.rem(me + group_size - 1, group_size)
    dec = Decoder(d, 0, d.layers, (wq, wk, wv, wo, wu, wd), y_ref, compute)
    exchanges = [Exchange(side, l, work, core_buf, ring_buf, migs[l], mig_send, mig_recv) for l in range(d.layers)]

    def scope(name, run, *args):
        with jax.named_scope(name):
            return run(*args)

    pool_loads = [[pltpu.make_async_copy(src.at[:, l], pools[l][p], pool_sem.at[l, p]) for p, src in enumerate((k_hbm, v_hbm))] for l in range(d.layers)]
    embeds_load, table_load, lens_load, table_load_v = [
        pltpu.make_async_copy(src, dst, load_sem.at[i]) for i, (src, dst) in enumerate(((embeds_hbm, embeds_v), (table_hbm, table_s), (lens_hbm, lens_s), (table_hbm, table_v)))]
    for load in [embeds_load] + pool_loads[0] + [table_load, table_load_v, lens_load]:
        load.start()
    barrier = pltpu.get_barrier_semaphore()

    @pl.loop(1, group_size)
    def _(r):
        pl.semaphore_signal(barrier, inc=1, device_id={'kv': lax.rem(me + r, group_size)})

    scope("barrier", lambda: pl.semaphore_wait(barrier, group_size - 1))

    groups = d.tokens // 8
    splits = group_size // groups
    cols = d.width // splits

    def piece(ref, m):
        return ref.at[m // splits, :, pl.ds(aligned(m % splits * cols, cols), cols)]

    def all_pieces(phase):
        some = mid_in.at[pl.ds(0, group_size - 1)]
        pltpu.make_async_remote_copy(some, some, x_send.at[phase], x_recv.at[phase], device_id={'kv': me}).wait()

    def send_embeddings():
        embeds_load.wait()

        @pl.loop(1, group_size)
        def _(r):
            m = lax.rem(me + r, group_size)
            pltpu.make_async_remote_copy(piece(embeds_v, m), mid_in.at[me], x_send.at[0], x_recv.at[0], device_id={'kv': m}).start()

        mid_in[me] = piece(embeds_v, me)[...]

    def load_tables():
        for load in (table_load, lens_load, table_load_v):
            load.wait()
        return lax.rem(table_s[1, 0] // d.slots + group_size, group_size)

    scope("pool_wait_0", lambda: [load.wait() for load in pool_loads[0]])

    def own(l):
        @pl.loop(0, entries)
        def _(e):
            slot = src_s[e] - me * d.slots
            mine = (slot >= 0) & (slot < d.slots)
            slot = jnp.clip(slot, 0, d.slots - 1)
            for p in range(2):
                page = pools[l][p][slot]
                work[l, p * entries + e] = jnp.where(mine, page, jnp.zeros_like(page))

    def step(l):
        scope(f"exchange_{l}_{exchanges[l].done}", exchanges[l].step)

    step_0, step_1 = functools.partial(step, 0), functools.partial(step, 1)

    scope("own_0", own, 0)
    step_0()
    for l in range(1, d.layers):
        for load in pool_loads[l]:
            load.start()
    scope("start_stream", dec.start_stream)
    shift = scope("load_tables", load_tables)
    home_a = lax.rem(me - shift + group_size, group_size)
    home_b = lax.rem(home_a + 1, group_size)

    def clipped(slot):
        return jnp.clip(slot - me * d.slots, 0, d.slots - 1)

    def first_here(l, p, i):
        return pools[l][p][clipped(table_s[0, home_b * d.rows + i])]

    def last_here(l, p, i):
        return pools[l][p][clipped(table_s[1, home_a * d.rows + i])]

    def migrated(l, p, home, i, page):
        entry = plan_s[0, home * d.rows + i]
        return jnp.where(entry >= 0, migs[l][p * entries + jnp.maximum(entry, 0)], page)

    def pack(l):
        @pl.loop(0, half)
        def _(i):
            for p in range(2):
                send_buf[l, 0, p, i] = first_here(l, p, i)
                send_buf[l, 1, p, i] = last_here(l, p, half + i)

    parts = 4
    size = half // parts

    def page_copy(l, way, p, rows):
        return pltpu.make_async_remote_copy(
            send_buf.at[l, way, p, rows], got_buf.at[l, way, p, rows], page_send.at[l, way, p], page_recv.at[l, way, p], device_id={'kv': (ahead, behind)[way]})

    pieces = [iter([(p, part) for part in range(parts) for p in range(2)]) for _ in range(d.layers)]

    def pages_start(l):
        p, part = next(pieces[l])
        for way in range(2):
            page_copy(l, way, p, pl.ds(part * size, size)).start()

    pages_0, pages_1 = functools.partial(pages_start, 0), functools.partial(pages_start, 1)

    def pages_wait(l):
        for way in range(2):
            for p in range(2):
                page_copy(l, way, p, pl.ds(0, half)).wait()

    def pass_on():
        all_pieces(0)
        later = me // splits * 8 % d.rows // half

        @pl.loop(0, group_size)
        def _(m):
            mid_out[m] = mid_in[lax.rem(m - shift + later + group_size, group_size)]

        @pl.loop(1, group_size)
        def _(r):
            m = lax.rem(me + r, group_size)
            pltpu.make_async_remote_copy(mid_out.at[m], piece(x_in, me), x_send.at[1], x_recv.at[1], device_id={'kv': m}).start()

        piece(x_in, me)[...] = mid_out[me]

    def take_embeddings():
        all_pieces(1)
        y_ref[...] = x_in[...].reshape(d.tokens, d.width)

    plan_copy = pltpu.make_async_copy(plan_v, plan_s, plan_sem)

    def plan():
        seq = lax.broadcasted_iota(jnp.int32, (1, table_v.shape[1]), 1)
        worker = lax.rem(seq // d.rows + shift, group_size)
        before = lax.rem(worker + group_size - 1, group_size)
        first, last = table_v[0:1, :], table_v[1:2, :]
        bad = (last < worker * d.slots) | (last >= worker * d.slots + d.slots) | (first < before * d.slots) | (first >= before * d.slots + d.slots)

        def entry(e, state):
            plan, bad = state
            return jnp.where(last == dst_s[e], e, plan), bad | (first == dst_s[e]).astype(jnp.int32)

        plan, bad = lax.fori_loop(0, entries, entry, (jnp.full_like(last, -1), bad.astype(jnp.int32)))
        plan_v[...] = plan
        plan_copy.start()
        info_s[0] = shift
        info_s[1] = 1 - jnp.max(bad)

    def new_copies(l):
        return [pltpu.make_async_remote_copy(
            ref.at[pl.ds(g * d.stride + t * d.rows + half, half)], new_buf.at[l, p, g, t], new_send.at[l, p, g, t], new_recv.at[l, p, g, t], device_id={'kv': ahead})
            for p, ref in enumerate((dec.kn_s, dec.vn_s)) for g in range(d.kv_heads) for t in range(2)]

    def project(l):
        dec.project(l)
        for copy in new_copies(l):
            copy.start()

    scope("pack_0", pack, 0)
    step_0()
    scope("send_embeddings", send_embeddings)
    pages_0()
    scope("plan", plan)
    step_0()
    pages_0()
    step_0()
    pages_0()
    scope("pass_on", pass_on)
    step_0()
    pages_0()
    for l in range(1, d.layers):
        for load in pool_loads[l]:
            load.wait()
    step_0()
    pages_0()
    scope("own_1", own, 1)
    step_0()
    pages_0()
    scope("pack_1", pack, 1)
    step_0()
    pages_0()
    scope("take_embeddings", take_embeddings)
    step_0()
    pages_0()
    scope("project_0", project, 0)
    step_0()
    plan_copy.wait()
    step_0()
    scope("pages_wait_0", pages_wait, 0)

    def attend(l, events_a, events_b):
        def put_page(p, i, val):
            last_buf[p, i] = val

        dec.attend(lambda i: lens_s[home_a * d.rows + i], lambda p, i: got_buf[l, 0, p, i],
                   lambda p, i: migrated(l, p, home_a, i, last_here(l, p, i)), put_page, events_a, 0, half)
        dec.attend(lambda i: lens_s[home_b * d.rows + i], lambda p, i: first_here(l, p, i),
                   lambda p, i: migrated(l, p, home_b, i, got_buf[l, 1, p, i - half]), lambda p, i, val: None, events_b, half, half)
        dec.gather_heads()

    def finish_pages(l):
        for copy in new_copies(l):
            copy.wait()

        @pl.loop(0, half)
        def _(i):
            row = half + i
            for p in range(2):
                page = migrated(l, p, home_a, row, last_here(l, p, row))
                last_buf[p, row] = dec.insert(page, lens_s[home_a * d.rows + row], lambda t, g: new_buf[l, p, g, t, pl.ds(i, 1), :])

        pltpu.make_async_copy(last_buf, last_out.at[l], out_sem.at[0]).start()

    def last_wait(l):
        pltpu.make_async_copy(last_buf, last_out.at[l], out_sem.at[0]).wait()

    def event(run):
        return lambda: run()

    blocks = half // min(UNROLL, half)
    pairs = 2 * (d.n_u // 2)
    with jax.named_scope("attend_0"):
        attend(0, [(0, event(step_1))], [(0, event(step_1))])
    events = [((2 * k + 1) * pairs // (4 * parts), event(pages_1)) for k in range(2 * parts)]
    events += [(k * (pairs - 1) // 8, event(step_1)) for k in range(Exchange.STEPS - 2)]
    events += [(pairs - 1, functools.partial(scope, "finish_0", finish_pages, 0))]
    with jax.named_scope("mix_0"):
        dec.mix(0, sorted(events, key=lambda event: event[0]))
    for l in range(1, d.layers):
        scope(f"project_{l}", project, l)
        scope(f"pages_wait_{l}", pages_wait, l)
        last_wait(l - 1)
        with jax.named_scope(f"attend_{l}"):
            attend(l, [], [])
        if l == 1:
            mig_stores = [pltpu.make_async_copy(migs[k], mig_out.at[k], out_sem.at[1 + k]) for k in range(d.layers)]
            for store in mig_stores:
                store.start()
        with jax.named_scope(f"mix_{l}"):
            dec.mix(l, [(pairs // 2, functools.partial(finish_pages, l))])
    for t in range(2):
        ya_ref[t] = y_ref[pl.ds(t * d.rows, half), :]
        yb_ref[t] = y_ref[pl.ds(t * d.rows + half, half), :]
    last_wait(d.layers - 1)
    for store in mig_stores:
        store.wait()


def decode_adjacent(side, group_size, d, table, seq_lens, mig_src, mig_dst, embeds, weights, k_pool, v_pool):
    entries = mig_src.shape[0]
    half = d.rows // 2
    page = (d.page_rows, d.head_dim)
    struct = lambda *shape: jax.ShapeDtypeStruct(shape, BF16)
    groups = d.tokens // 8
    mid = pltpu.VMEM((group_size, 8, d.width * groups // group_size), BF16)
    return pl.pallas_call(
        functools.partial(adjacent_kernel, d, side, group_size, entries),
        out_shape=[struct(2, half, d.width), struct(2, half, d.width), jax.ShapeDtypeStruct((2,), jnp.int32), struct(d.layers, 2, d.rows, *page), struct(d.layers, 2 * entries, *page)],
        in_specs=[SMEM] * 2 + [ANY] * 11,
        out_specs=[VMEM, VMEM, SMEM, ANY, ANY],
        scratch_shapes=[
            pltpu.SMEM(table.shape, jnp.int32),
            pltpu.SMEM(seq_lens.shape, jnp.int32),
            pltpu.VMEM(table.shape, jnp.int32),
            pltpu.VMEM((groups, 8, d.width), BF16),
            pltpu.VMEM((d.tokens, d.width), BF16),
            pltpu.VMEM((d.layers, 2, 2, half) + page, BF16),
            pltpu.VMEM((d.layers, 2, 2, half) + page, BF16),
            pltpu.VMEM((2, d.rows) + page, BF16),
            pltpu.VMEM((d.layers, 2, d.kv_heads, 2, half, d.head_dim), F32),
            pltpu.VMEM((d.layers, 2 * entries) + page, BF16),
            pltpu.VMEM((d.layers, entries) + page, BF16),
            pltpu.VMEM((d.layers, entries) + page, BF16),
            mid,
            mid,
            pltpu.VMEM((groups, 8, d.width), BF16),
            pltpu.VMEM((1, table.shape[1]), jnp.int32),
            pltpu.SMEM((1, table.shape[1]), jnp.int32),
        ] + [pltpu.VMEM((2 * entries,) + page, BF16)] * d.layers + [pltpu.VMEM((d.slots,) + page, BF16)] * (2 * d.layers) + d.compute_scratch(10, 8) + [
            DMA((4,)),
            DMA((d.layers, 2)),
            DMA,
            DMA((2,)),
            DMA((2,)),
            DMA((d.layers, 2, 2)),
            DMA((d.layers, 2, 2)),
            DMA((d.layers, 2, d.kv_heads, 2)),
            DMA((d.layers, 2, d.kv_heads, 2)),
            DMA((d.layers, 10, 4)),
            DMA((d.layers, 10, 4)),
            DMA((1 + d.layers,)),
        ],
        compiler_params=pltpu.CompilerParams(collective_id=1, has_side_effects=True, skip_device_barrier=True, vmem_limit_bytes=LIMIT),
        cost_estimate=d.cost(d.layers),
        name="decode_adjacent",
    )(mig_src, mig_dst, table, seq_lens, embeds.reshape(groups, 8, d.width), *weights, k_pool, v_pool)


def fill_pools_kernel(dims, group_size, entries, info_s, table_s, src_s, dst_s, k_hbm, v_hbm, last_hbm, mig_hbm, k_out, v_out, k_buf, v_buf, sem, fix_sem):
    d = dims
    me = lax.axis_index('kv')
    src_home = lax.rem(me - info_s[0] + group_size, group_size)
    pools = ((k_hbm, k_buf, k_out), (v_hbm, v_buf, v_out))
    parts = 4
    size = d.slots // parts

    def moves(out):
        return [pltpu.make_async_copy(*((buf.at[at], dst.at[at]) if out else (src.at[at], buf.at[at])), sem.at[p, part])
                for part in range(parts) for at in [pl.ds(part * size, size)] for p, (src, buf, dst) in enumerate(pools)]

    def local(slot):
        slot = slot - me * d.slots
        return (slot >= 0) & (slot < d.slots), jnp.clip(slot, 0, d.slots - 1)

    def migrated(run):
        @pl.loop(0, entries)
        def _(e):
            mine, slot = local(dst_s[e])

            @pl.when(mine)
            def _():
                for p, (_, buf, _) in enumerate(pools):
                    for l in range(d.layers):
                        run(pltpu.make_async_copy(mig_hbm.at[l, p * entries + e], buf.at[slot, l], fix_sem))

    def updated(run):
        @pl.loop(0, d.rows)
        def _(i):
            _, slot = local(table_s[1, src_home * d.rows + i])
            for p, (_, buf, _) in enumerate(pools):
                for l in range(d.layers):
                    run(pltpu.make_async_copy(last_hbm.at[l, p, i], buf.at[slot, l], fix_sem))

    start, wait = lambda copy: copy.start(), lambda copy: copy.wait()
    for copy in moves(False):
        copy.start()
    for copy in moves(False):
        copy.wait()
    migrated(start)
    migrated(wait)
    updated(start)

    @pl.loop(0, entries)
    def _(e):
        mine, slot = local(src_s[e])

        @pl.when(mine)
        def _():
            for _, buf, _ in pools:
                buf[slot] = jnp.zeros(buf.shape[1:], buf.dtype)

    updated(wait)
    for copy in moves(True):
        copy.start()
    for copy in moves(True):
        copy.wait()


def fill_pools(group_size, d, info, table, mig_src, mig_dst, k_pool, v_pool, last, mig):
    entries = mig_src.shape[0]
    size = 4 * k_pool.size
    return pl.pallas_call(
        functools.partial(fill_pools_kernel, d, group_size, entries),
        out_shape=[jax.ShapeDtypeStruct(k_pool.shape, k_pool.dtype)] * 2,
        in_specs=[SMEM] * 4 + [ANY] * 4,
        out_specs=[ANY, ANY],
        scratch_shapes=[pltpu.VMEM(k_pool.shape, k_pool.dtype), pltpu.VMEM(k_pool.shape, k_pool.dtype), DMA((2, 4)), DMA],
        compiler_params=pltpu.CompilerParams(vmem_limit_bytes=LIMIT),
        cost_estimate=pl.CostEstimate(flops=40 * size, bytes_accessed=2 * size, transcendentals=0),
        name="fill_pools",
    )(info, table, mig_src, mig_dst, k_pool, v_pool, last, mig)


def gather_pages_kernel(idx_ref, k_hbm, v_hbm, k_out, v_out, sem):
    rows = k_out.shape[0]

    def copies(i):
        slot = jnp.maximum(idx_ref[i], 0)
        return (pltpu.make_async_copy(k_hbm.at[slot], k_out.at[i], sem), pltpu.make_async_copy(v_hbm.at[slot], v_out.at[i], sem))

    @pl.loop(0, rows)
    def _(i):
        @pl.when(idx_ref[i] >= 0)
        def _():
            for copy in copies(i):
                copy.start()

        @pl.when(idx_ref[i] < 0)
        def _():
            k_out[i] = jnp.zeros(k_out.shape[1:], k_out.dtype)
            v_out[i] = jnp.zeros(v_out.shape[1:], v_out.dtype)

    @pl.loop(0, rows)
    def _(i):
        @pl.when(idx_ref[i] >= 0)
        def _():
            for copy in copies(i):
                copy.wait()


def gather_pages(idx, k_pool, v_pool):
    shape = jax.ShapeDtypeStruct((idx.shape[0],) + k_pool.shape[1:], k_pool.dtype)
    return pl.pallas_call(
        gather_pages_kernel,
        out_shape=[shape, shape],
        in_specs=[SMEM, ANY, ANY],
        out_specs=[VMEM, VMEM],
        scratch_shapes=[DMA],
        compiler_params=pltpu.CompilerParams(vmem_limit_bytes=LIMIT),
        name="gather_pages",
    )(idx, k_pool, v_pool)


def share_kernel(side, k_hbm, v_hbm, k_out, v_out, work, core_buf, ring_buf, load_sem, send_sem, recv_sem, result):
    entries = k_hbm.shape[0]
    exchange = Exchange(side, 0, work, core_buf, ring_buf, result, send_sem, recv_sem)
    units = [pl.ds(p * entries, entries) for p in range(2)]
    for p, src in enumerate((k_hbm, v_hbm)):
        pltpu.make_async_copy(src, work.at[0].at[units[p]], load_sem.at[p]).start()
    for p, src in enumerate((k_hbm, v_hbm)):
        pltpu.make_async_copy(src, work.at[0].at[units[p]], load_sem.at[p]).wait()
    for _ in range(Exchange.STEPS):
        exchange.step()
    for p, dst in enumerate((k_out, v_out)):
        pltpu.make_async_copy(result.at[units[p]], dst, load_sem.at[p]).start()
    for p, dst in enumerate((k_out, v_out)):
        pltpu.make_async_copy(result.at[units[p]], dst, load_sem.at[p]).wait()


def share(side, mig_k, mig_v):
    entries = mig_k.shape[0]
    page = mig_k.shape[1:]
    return pl.pallas_call(
        functools.partial(share_kernel, side),
        out_shape=[jax.ShapeDtypeStruct(mig_k.shape, BF16)] * 2,
        in_specs=[ANY, ANY],
        out_specs=[ANY, ANY],
        scratch_shapes=[pltpu.VMEM((1, n * entries) + page, BF16) for n in (2, 1, 1)] + [DMA((2,)), DMA((1, 10, 4)), DMA((1, 10, 4)), pltpu.VMEM((2 * entries,) + page, BF16)],
        compiler_params=pltpu.CompilerParams(has_side_effects=True, vmem_limit_bytes=LIMIT),
        name="share",
    )(mig_k, mig_v)


def migrate_kernel(dst_ref, src_ref, k_hbm, v_hbm, mk_hbm, mv_hbm, k_out, v_out, k_buf, v_buf, sem, fix_sem):
    entries = dst_ref.shape[0]
    pairs = ((k_hbm, mk_hbm, k_buf, k_out), (v_hbm, mv_hbm, v_buf, v_out))
    for p, (src, _, buf, _) in enumerate(pairs):
        pltpu.make_async_copy(src, buf, sem.at[p]).start()
    for p, (src, _, buf, _) in enumerate(pairs):
        pltpu.make_async_copy(src, buf, sem.at[p]).wait()

    @pl.loop(0, entries)
    def _(e):
        @pl.when(dst_ref[e] >= 0)
        def _():
            for _, mig, buf, _ in pairs:
                copy = pltpu.make_async_copy(mig.at[e], buf.at[jnp.maximum(dst_ref[e], 0)], fix_sem)
                copy.start()
                copy.wait()

        @pl.when(src_ref[e] >= 0)
        def _():
            for _, _, buf, _ in pairs:
                buf[jnp.maximum(src_ref[e], 0)] = jnp.zeros(buf.shape[1:], buf.dtype)

    for p, (_, _, buf, dst) in enumerate(pairs):
        pltpu.make_async_copy(buf, dst, sem.at[p]).start()
    for p, (_, _, buf, dst) in enumerate(pairs):
        pltpu.make_async_copy(buf, dst, sem.at[p]).wait()


def migrate(dst_local, src_local, k_pool, v_pool, mig_k, mig_v):
    shape = jax.ShapeDtypeStruct(k_pool.shape, k_pool.dtype)
    return pl.pallas_call(
        migrate_kernel,
        out_shape=[shape, shape],
        in_specs=[SMEM, SMEM, ANY, ANY, ANY, ANY],
        out_specs=[ANY, ANY],
        scratch_shapes=[pltpu.VMEM(k_pool.shape, k_pool.dtype), pltpu.VMEM(k_pool.shape, k_pool.dtype), DMA((2,)), DMA],
        compiler_params=pltpu.CompilerParams(vmem_limit_bytes=LIMIT),
        name="migrate",
    )(dst_local, src_local, k_pool, v_pool, mig_k, mig_v)


def decode_kernel(dims, sc_ref, x_ref, p0k_hbm, p0v_hbm, wq, wk, wv, wo, wu, wd, k_in, v_in, y_ref, k_out, v_out,
                  first_buf, last_buf, *rest):
    compute, (page_sem, put_sem) = rest[:-2], rest[-2:]
    d = dims
    dec = Decoder(d, 0, d.layers, (wq, wk, wv, wo, wu, wd), y_ref, compute)
    dec.start_stream()
    y_ref[...] = x_ref[...]
    loads = [pltpu.make_async_copy(src, first_buf.at[p], page_sem.at[p]) for p, src in enumerate((p0k_hbm, p0v_hbm))]
    for load in loads:
        load.start()

    def last_loads(run):
        @pl.loop(0, d.rows)
        def _(i):
            for p, src in enumerate((k_in, v_in)):
                run(pltpu.make_async_copy(src.at[sc_ref[0, i]], last_buf.at[p, i], page_sem.at[2]))

    def puts(run):
        @pl.loop(0, d.rows)
        def _(i):
            @pl.when(sc_ref[2, i] > 0)
            def _():
                for p, dst in enumerate((k_out, v_out)):
                    run(pltpu.make_async_copy(last_buf.at[p, i], dst.at[sc_ref[0, i]], put_sem))

    last_loads(lambda copy: copy.start())
    for load in loads:
        load.wait()
    last_loads(lambda copy: copy.wait())

    @pl.loop(0, d.layers)
    def _(layer):
        def put_page(p, i, val):
            last_buf[p, i, layer] = val

        dec.project(layer)
        dec.attend(lambda i: sc_ref[1, i], lambda p, i: first_buf[p, i, layer], lambda p, i: last_buf[p, i, layer], put_page)
        dec.gather_heads()
        dec.mix(layer)

    puts(lambda copy: copy.start())
    puts(lambda copy: copy.wait())


def decode(d, scalars, x, p0k, p0v, weights, k_pool, v_pool):
    pool = jax.ShapeDtypeStruct(k_pool.shape, k_pool.dtype)
    pages = pltpu.VMEM((2, d.rows, d.layers, d.page_rows, d.head_dim), BF16)
    return pl.pallas_call(
        functools.partial(decode_kernel, d),
        out_shape=[jax.ShapeDtypeStruct(x.shape, x.dtype), pool, pool],
        in_specs=[SMEM, VMEM] + [ANY] * 10,
        out_specs=[VMEM, ANY, ANY],
        input_output_aliases={10: 1, 11: 2},
        scratch_shapes=[pages, pages] + d.compute_scratch(16, 16) + [DMA((3,)), DMA],
        compiler_params=pltpu.CompilerParams(vmem_limit_bytes=LIMIT),
        cost_estimate=d.cost(d.layers),
        name="decode",
    )(scalars, x, p0k, p0v, *weights, k_pool, v_pool)


def permute(arrays, shift, group_size):
    if shift == group_size // 2:
        return permute(permute(arrays, shift // 2, group_size), shift // 2, group_size)
    perm = [(i, (i + shift) % group_size) for i in range(group_size)]
    return jax.tree.map(lambda a: lax.ppermute(a, 'kv', perm), arrays) if shift else arrays


def rotate_back(first, second, shift, group_size, beside):
    def branch(r):
        def run(args):
            parts = permute(args[0], -r % group_size, group_size), permute(args[1], (1 - r) % group_size, group_size)
            return jnp.concatenate(parts, axis=1), beside()

        return run

    return lax.switch(shift, [branch(r) for r in range(group_size)], (first, second))


def rotate_bits(arrays, shift, group_size):
    arrays = tuple(arrays)
    bit = 1
    while bit < group_size:
        move = functools.partial(permute, shift=bit, group_size=group_size)
        arrays = lax.cond(shift // bit % 2 == 1, move, lambda args: args, arrays)
        bit *= 2
    return arrays


def solution(mesh):
    group_size = mesh.shape['kv']
    side = math.isqrt(group_size // 2)
    pool_spec = P(('rep', 'kv'))
    tok_spec = P(None, ('rep', 'kv'), None)

    def device_fn(embeds, w_query, w_key, w_value, w_out, w_up, w_down, k_pool5, v_pool5, new_table, seq_lens, mig_src, mig_dst):
        me = lax.axis_index('kv')
        slots, layers, page, kv_heads, head_dim = k_pool5.shape
        rows, width = embeds.shape[1:]
        weights = (w_query, w_key, w_value, w_out, w_up, w_down)
        k_pool = k_pool5.reshape(slots, layers, page * kv_heads, head_dim)
        v_pool = v_pool5.reshape(slots, layers, page * kv_heads, head_dim)
        d = Dims(rows, weights, k_pool, page)
        ints = jnp.int32

        def local(ids):
            loc = ids - me * slots
            return jnp.where((loc >= 0) & (loc < slots), loc, -1)

        def take(vec, dev):
            return lax.dynamic_slice(vec, (dev * rows,), (rows,))

        def inside(ids):
            return jnp.clip(ids - me * slots, 0, slots - 1)

        def general_path():
            first_new, last_new = new_table[:, 0], new_table[:, 1]
            moved = first_new[None, :] == mig_dst[:, None]
            first_old = jnp.where(jnp.any(moved, axis=0), jnp.sum(jnp.where(moved, mig_src[:, None], 0), axis=0), first_new)
            home = jnp.arange(first_new.shape[0], dtype=ints) // rows
            worker = last_new // slots
            shift_of = (worker - home + group_size) % group_size
            first_shift = (worker - first_old // slots + group_size) % group_size
            shift_ids = jnp.arange(group_size, dtype=ints)
            wanted = jnp.any(shift_of[None, :] == shift_ids[:, None], axis=1)
            mig_k, mig_v = gather_pages(local(mig_src), k_pool, v_pool)
            by_layer = tuple(m.swapaxes(0, 1) for m in (mig_k, mig_v))
            mig_k, mig_v = (m.swapaxes(0, 1) for m in lax.map(lambda pages: tuple(share(side, *pages)), by_layer))
            k_new, v_new = migrate(local(mig_dst), local(mig_src), k_pool, v_pool, mig_k, mig_v)

            def one_round(shift, y, k_new, v_new):
                src_home = (me - shift + group_size) % group_size
                (x,) = rotate_bits((embeds.reshape(2 * rows, width),), shift, group_size)
                in_round = shift_of == shift
                wanted2 = jnp.any(in_round[None, :] & (first_shift[None, :] == shift_ids[:, None]), axis=1)

                def more(state):
                    left, pk, pv = state
                    shift2 = jnp.argmax(left).astype(ints)
                    dest_home = (me + shift2 - shift + group_size) % group_size
                    got = gather_pages(inside(take(first_old, dest_home)), k_pool, v_pool)
                    got_k, got_v = rotate_bits(got, shift2, group_size)
                    mine = (take(first_shift, src_home) == shift2)[:, None, None, None]
                    return left & (shift_ids != shift2), jnp.where(mine, got_k, pk), jnp.where(mine, got_v, pv)

                zeros = jnp.zeros((rows,) + k_pool.shape[1:], k_pool.dtype)
                _, pk, pv = lax.while_loop(lambda state: jnp.any(state[0]), more, (wanted2, zeros, zeros))
                valid = take(shift_of, src_home) == shift
                scalars = jnp.stack([inside(take(last_new, src_home)), take(seq_lens, src_home), valid.astype(ints)])
                out, k_new, v_new = decode(d, scalars, x, pk, pv, weights, k_new, v_new)
                (back,) = rotate_bits((out,), (group_size - shift) % group_size, group_size)
                mine = (take(shift_of, me) == shift)[None, :, None]
                return jnp.where(mine, back.reshape(embeds.shape), y), k_new, v_new

            def next_round(state):
                left, y, k_new, v_new = state
                shift = jnp.argmax(left).astype(ints)
                y, k_new, v_new = one_round(shift, y, k_new, v_new)
                return left & (shift_ids != shift), y, k_new, v_new

            _, y, k_new, v_new = lax.while_loop(lambda state: jnp.any(state[0]), next_round, (wanted, jnp.zeros_like(embeds), k_new, v_new))
            return y, k_new, v_new

        table = new_table.T
        ya, yb, info, last, mig = decode_adjacent(side, group_size, d, table, seq_lens, mig_src, mig_dst, embeds, weights, k_pool, v_pool)
        y, (k_new, v_new) = rotate_back(ya, yb, info[0], group_size, lambda: fill_pools(group_size, d, info, table, mig_src, mig_dst, k_pool, v_pool, last, mig))
        _, y, k_new, v_new = lax.while_loop(lambda state: state[0] == 0, lambda state: (jnp.ones_like(state[0]),) + general_path(), (info[1], y, k_new, v_new))
        return y, k_new.reshape(k_pool5.shape), v_new.reshape(v_pool5.shape)

    return jax.shard_map(device_fn, mesh=mesh, in_specs=(tok_spec, P(), P(), P(), P(), P(), P(), pool_spec, pool_spec, P('rep', None), P('rep'), P('rep'), P('rep')), out_specs=(tok_spec, pool_spec, pool_spec), check_vma=False)
```

```python
import functools
import math

import jax
import jax.numpy as jnp
from jax import lax
from jax.experimental import pallas as pl
from jax.experimental.pallas import tpu as pltpu
from jax.sharding import PartitionSpec as P

ANY = pl.BlockSpec(memory_space=pl.ANY)
SMEM = pl.BlockSpec(memory_space=pltpu.SMEM)
VMEM = pl.BlockSpec(memory_space=pltpu.VMEM)
DMA = pltpu.SemaphoreType.DMA
CHUNK = 256
UNROLL = 8
LIMIT = 63 << 20
F32, BF16 = jnp.float32, jnp.bfloat16


def aligned(x, multiple):
    return x if isinstance(x, int) else pl.multiple_of(x, multiple)


class Dims:
    def __init__(self, rows, weights, k_pool, page):
        w_query, w_key, _, _, w_up, _ = weights
        self.layers, self.width, self.q_width = w_query.shape
        self.ff = w_up.shape[2]
        self.slots, _, self.page_rows, self.head_dim = k_pool.shape
        self.kv_heads = w_key.shape[2] // self.head_dim
        self.heads = self.q_width // self.head_dim
        self.page, self.rows = page, rows
        self.tokens = 2 * rows
        self.stride = self.tokens + 8
        self.n_q, self.n_o, self.n_u = self.q_width // CHUNK, self.width // CHUNK, self.ff // CHUNK
        self.col_layer = self.n_q + 2 + self.n_o + self.n_u

    def compute_scratch(self, n_col, n_row):
        return [
            pltpu.VMEM((n_col, self.width, CHUNK), BF16),
            pltpu.VMEM((n_row, CHUNK, self.width), BF16),
            pltpu.VMEM((self.heads * self.stride, self.head_dim), F32),
            pltpu.VMEM((self.kv_heads * self.stride, self.head_dim), F32),
            pltpu.VMEM((self.kv_heads * self.stride, self.head_dim), F32),
            pltpu.VMEM((self.heads * self.stride, self.head_dim), F32),
            pltpu.VMEM((self.tokens, self.q_width), BF16),
            pltpu.VMEM((self.tokens, self.ff), BF16),
            pltpu.VMEM((self.tokens, self.width), F32),
            DMA((n_col,)),
            DMA((n_row,)),
        ]

    def cost(self, layers):
        size = layers * self.width * (2 * self.q_width + 2 * self.kv_heads * self.head_dim + 2 * self.ff)
        return pl.CostEstimate(flops=2 * size * self.tokens, bytes_accessed=2 * size, transcendentals=0)


class Decoder:
    def __init__(self, dims, first, layers, weights, y_ref, scratch, group=2, unroll=UNROLL):
        self.group, self.unroll = group, unroll
        self.d, self.first, self.layers, self.weights, self.y_ref = dims, first, layers, weights, y_ref
        (self.col_buf, self.row_buf, self.q_s, self.kn_s, self.vn_s, self.o_s, self.att, self.act, self.acc, self.col_sem, self.row_sem) = scratch
        self.n_col, self.n_row = self.col_buf.shape[0], self.row_buf.shape[0]
        self.zero = lax.axis_index('kv') * 0
        d = dims
        cols = 2 * d.page * d.kv_heads
        col_pos = lax.broadcasted_iota(jnp.int32, (2 * d.heads, cols), 1)
        row_pos = lax.broadcasted_iota(jnp.int32, (2 * d.heads, cols), 0)
        same_head = (col_pos % d.kv_heads) == (row_pos % d.heads) // (d.heads // d.kv_heads)
        self.limit = jnp.where(same_head, col_pos // d.kv_heads - row_pos // d.heads, 4 * d.page)
        self.page_pos = lax.broadcasted_iota(jnp.int32, (d.page_rows, d.head_dim), 0) // d.kv_heads
        self.tile_head = lax.broadcasted_iota(jnp.int32, (8, d.head_dim), 0) % d.kv_heads

    def layer_of(self, g, per_layer):
        return sum((g >= per_layer * l).astype(jnp.int32) for l in range(1, self.layers))

    def col_start(self, g):
        d = self.d
        wq, wk, wv, wo, wu, _ = self.weights

        @pl.when(g < self.layers * d.col_layer)
        def _():
            layer = self.layer_of(g, d.col_layer)
            pos = g - layer * d.col_layer
            slot = g % self.n_col

            def go(src, c):
                start = aligned(c * CHUNK, CHUNK)
                pltpu.make_async_copy(src.at[self.first + layer].at[:, pl.ds(start, CHUNK)], self.col_buf.at[slot], self.col_sem.at[slot]).start()

            @pl.when(pos < d.n_q)
            def _():
                go(wq, pos)

            @pl.when(pos == d.n_q)
            def _():
                go(wk, 0)

            @pl.when(pos == d.n_q + 1)
            def _():
                go(wv, 0)

            @pl.when((pos >= d.n_q + 2) & (pos < d.n_q + 2 + d.n_o))
            def _():
                go(wo, pos - (d.n_q + 2))

            @pl.when(pos >= d.n_q + 2 + d.n_o)
            def _():
                go(wu, pos - (d.n_q + 2 + d.n_o))

    def row_start(self, g):
        d = self.d
        wd = self.weights[5]

        @pl.when(g < self.layers * d.n_u)
        def _():
            layer = self.layer_of(g, d.n_u)
            slot = g % self.n_row
            start = aligned((g - layer * d.n_u) * CHUNK, CHUNK)
            pltpu.make_async_copy(wd.at[self.first + layer].at[pl.ds(start, CHUNK)], self.row_buf.at[slot], self.row_sem.at[slot]).start()

    def start_stream(self):
        @pl.loop(0, self.n_col)
        def _(g):
            self.col_start(g)

        @pl.loop(0, self.n_row)
        def _(g):
            self.row_start(g)

    def with_cols(self, g, count, body):
        slots = [(g + u) % self.n_col for u in range(count)]
        for slot in slots:
            pltpu.make_async_copy(self.weights[1].at[0], self.col_buf.at[slot], self.col_sem.at[slot]).wait()
        body([self.col_buf.at[slot] for slot in slots])
        for u in range(count):
            self.col_start(g + u + self.n_col)

    def with_rows(self, g, count, body):
        slots = [(g + u) % self.n_row for u in range(count)]
        for slot in slots:
            pltpu.make_async_copy(self.weights[5].at[0, pl.ds(0, CHUNK), :], self.row_buf.at[slot], self.row_sem.at[slot]).wait()
        body([self.row_buf.at[slot] for slot in slots])
        for u in range(count):
            self.row_start(g + u + self.n_row)

    def project(self, layer):
        d = self.d
        col0 = (self.zero + layer) * d.col_layer

        def product(ref):
            return jnp.dot(self.y_ref[...], ref[...], preferred_element_type=F32).astype(BF16).astype(F32)

        def put(dst, first, out):
            for h in range(CHUNK // d.head_dim):
                at = aligned((first + h) * d.stride, 8)
                dst[pl.ds(at, d.tokens), :] = out[:, h * d.head_dim:(h + 1) * d.head_dim]

        many = self.group

        @pl.loop(0, d.n_q // many)
        def _(j):
            def body(refs):
                outs = [product(ref) for ref in refs]
                for u in range(many):
                    put(self.q_s, (many * j + u) * (CHUNK // d.head_dim), outs[u])

            self.with_cols(col0 + many * j, many, body)

        def body(refs):
            outs = [product(ref) for ref in refs]
            put(self.kn_s, 0, outs[0])
            put(self.vn_s, 0, outs[1])

        self.with_cols(col0 + d.n_q, 2, body)

    def insert(self, page, n, row):
        d = self.d
        val = page.astype(F32)
        for t in range(2):
            new = jnp.broadcast_to(row(t, 0), (8, d.head_dim))
            for g in range(1, d.kv_heads):
                new = jnp.where(self.tile_head == g, row(t, g), new)
            val = jnp.where(self.page_pos == n - d.page + t, jnp.concatenate([new] * (d.page_rows // 8), axis=0), val)
        return val.astype(BF16)

    def attend(self, lens, first_page, last_page, put_page, events=(), begin=0, count=None):
        d = self.d
        count = count or d.rows
        unroll = min(self.unroll, count)

        def some(first):
            ids = [first + u for u in range(unroll)]
            scores, vals = [], []
            for i in ids:
                n = lens(i)

                def updated(p, new_ref):
                    val = self.insert(last_page(p, i), n, lambda t, g: new_ref[pl.ds(g * d.stride + t * d.rows + i, 1), :])
                    put_page(p, i, val)
                    return val

                keys = jnp.concatenate([first_page(0, i), updated(0, self.kn_s)], axis=0)
                vals.append(updated(1, self.vn_s))
                qs = jnp.concatenate([self.q_s[pl.ds(t * d.rows + i, d.heads, stride=d.stride), :] for t in range(2)], axis=0)
                score = lax.dot_general(qs.astype(BF16), keys, (((1,), (1,)), ((), ())), preferred_element_type=F32) * d.head_dim ** -0.5
                scores.append(jnp.where(self.limit <= n, score, -jnp.inf))
            tops = [jnp.max(score, axis=1, keepdims=True) for score in scores]
            probs = [jnp.exp(score - top) for score, top in zip(scores, tops)]
            totals = [jnp.sum(prob, axis=1, keepdims=True) for prob in probs]
            for u, i in enumerate(ids):
                both = jnp.concatenate([first_page(1, i), vals[u]], axis=0)
                out = jnp.dot(probs[u].astype(BF16), both, preferred_element_type=F32) / totals[u]
                for t in range(2):
                    self.o_s[pl.ds(t * d.rows + i, d.heads, stride=d.stride), :] = out[t * d.heads:(t + 1) * d.heads]

        @pl.loop(0, count // unroll)
        def _(block):
            for k, run in events:
                pl.when(block == k)(run)
            some(begin + block * unroll)

    def gather_heads(self):
        d = self.d
        for h in range(d.heads):
            self.att[:, h * d.head_dim:(h + 1) * d.head_dim] = self.o_s[h * d.stride:h * d.stride + d.tokens, :].astype(BF16)

    def mix(self, layer, events=()):
        d = self.d
        layer = self.zero + layer
        col0 = layer * d.col_layer + d.n_q + 2
        many = self.group
        pairs = d.n_u // many

        def between(j, first):
            for k, run in events:
                if first <= k < first + pairs:
                    pl.when(j == k - first)(run)

        def span(j):
            return pl.ds(aligned(j * CHUNK, CHUNK), CHUNK)

        @pl.loop(0, d.n_o // many)
        def _(j):
            def body(refs):
                outs = [jnp.dot(self.att[...], ref[...], preferred_element_type=F32) for ref in refs]
                for u in range(many):
                    at = span(many * j + u)
                    self.y_ref[:, at] = (self.y_ref[:, at].astype(F32) + outs[u]).astype(BF16)

            self.with_cols(col0 + many * j, many, body)

        def up(first, count):
            def body(refs):
                ups = [jnp.dot(self.y_ref[...], ref[...], preferred_element_type=F32) for ref in refs]
                for u in range(count):
                    self.act[:, span(first + u)] = jax.nn.gelu(ups[u].astype(BF16).astype(F32), approximate=True).astype(BF16)

            self.with_cols(col0 + d.n_o + first, count, body)

        def down(first, count):
            def body(refs):
                out = self.acc[...]
                for u in range(count):
                    out += jnp.dot(self.act[:, span(first + u)], refs[u][...], preferred_element_type=F32)
                self.acc[...] = out

            self.with_rows(layer * d.n_u + first, count, body)

        @pl.loop(0, pairs)
        def _(j):
            between(j, 0)
            up(many * j, many)

        if d.n_u % many:
            up(d.n_u - 1, 1)

        self.acc[...] = self.y_ref[...].astype(F32)

        @pl.loop(0, pairs)
        def _(j):
            between(j, pairs)
            down(many * j, many)

        if d.n_u % many:
            down(d.n_u - 1, 1)

        self.y_ref[...] = self.acc[...].astype(BF16)


class Exchange:
    STEPS = 11

    def __init__(self, side, layer, work, core_buf, ring_buf, out, send_sem, recv_sem):
        self.layer = layer
        self.work, self.core_buf, self.ring_buf, self.out, self.send_sem, self.recv_sem = work, core_buf, ring_buf, out, send_sem, recv_sem
        me = lax.axis_index('kv')
        core, x, y = me % 2, me // 2 % side, me // (2 * side)

        def pairings(pos, stride):
            return (((pos + 1) // 2 % 2, me + (1 - 2 * (pos % 2)) * stride), (pos // 2, me + (side - 1 - 2 * pos) * stride))

        xs, ys = pairings(x, 2), pairings(y, 2 * side)
        self.orders = [xs + ys, xs[::-1] + ys[::-1], ys + xs, ys[::-1] + xs[::-1]]
        self.partner = me + 1 - 2 * core
        self.peers = [self.partner] + [dev for _, dev in xs + ys]
        self.half = work.shape[1] // 2
        self.stream = self.half // 4
        self.base, self.other = core * self.half, (1 - core) * self.half
        self.copies, self.done = [], 0
        self.path = [[self.base + k * self.stream for k in range(4)]]
        self.away = []
        for ring in range(4):
            size = self.stream >> (ring + 1)
            self.away.append([self.path[-1][k] + (1 - self.orders[k][ring][0]) * size for k in range(4)])
            self.path.append([self.path[-1][k] + self.orders[k][ring][0] * size for k in range(4)])

    def send(self, src, dst, step, lane, dev):
        def copy():
            return pltpu.make_async_remote_copy(src(), dst(), self.send_sem.at[self.layer, step, lane], self.recv_sem.at[self.layer, step, lane], device_id={'kv': dev})

        copy().start()
        self.copies.append(copy)

    def units(self, ref, at, count):
        return lambda: ref.at[self.layer].at[pl.ds(at, count)]

    def results(self, at, count):
        return lambda: self.out.at[pl.ds(at, count)]

    def add(self, dst_at, buf, src_at, count):
        @pl.loop(0, count)
        def _(u):
            self.work[self.layer, dst_at + u] = self.work[self.layer, dst_at + u] + buf[self.layer, src_at + u]

    def halve(self, ring, k):
        size = self.stream >> (ring + 1)
        src = self.units(self.work, self.away[ring][k], size)
        self.send(src, self.units(self.ring_buf, (k + 1) * self.stream - 2 * size, size), 1 + ring, k, self.orders[k][ring][1])

    def halved(self, ring, k):
        size = self.stream >> (ring + 1)
        self.add(self.path[ring + 1][k], self.ring_buf, (k + 1) * self.stream - 2 * size, size)

    def double(self, ring, k):
        at = self.results(self.path[ring + 1][k], self.stream >> (ring + 1))
        self.send(at, at, 8 - ring, k, self.orders[k][ring][1])

    def step(self):
        step, self.done = self.done, self.done + 1
        started, self.copies = self.copies, []
        if step in (1, 9, 10):
            for copy in started:
                copy().wait()
        if step == 0:
            self.send(self.units(self.work, self.other, self.half), self.units(self.core_buf, 0, self.half), 0, 0, self.partner)
        elif step == 1:
            self.add(self.base, self.core_buf, 0, self.half)
            for k in range(4):
                self.halve(0, k)
        elif step < 9:
            for k in range(4):
                started[k]().wait()
                if step < 6:
                    self.halved(step - 2, k)
                if step < 5:
                    self.halve(step - 1, k)
                    continue
                if step == 5:
                    for u in range(self.stream >> 4):
                        self.out[self.path[4][k] + u] = self.work[self.layer, self.path[4][k] + u]
                self.double(8 - step, k)
        elif step == 9:
            at = self.results(self.base, self.half)
            self.send(at, at, 9, 0, self.partner)


def adjacent_kernel(dims, side, group_size, entries, src_s, dst_s, table_hbm, lens_hbm, embeds_hbm, wq, wk, wv, wo, wu, wd, k_hbm, v_hbm,
                    ya_ref, yb_ref, info_s, last_out,
                    table_s, lens_s, table_v, embeds_v, y_ref, send_buf, got_buf, last_buf, new_buf, work, core_buf, ring_buf, mid_in, mid_out, x_in, plan_v, plan_s, *rest):
    d = dims
    migs, rest = rest[:d.layers], rest[d.layers:]
    pools, rest = [rest[2 * l:2 * l + 2] for l in range(d.layers)], rest[2 * d.layers:]
    compute, (load_sem, pool_sem, plan_sem, x_send, x_recv, page_send, page_recv, new_send, new_recv, mig_send, mig_recv, out_sem) = rest[:-12], rest[-12:]
    half = d.rows // 2
    me = lax.axis_index('kv')
    ahead, behind = lax.rem(me + 1, group_size), lax.rem(me + group_size - 1, group_size)
    dec = Decoder(d, 0, d.layers, (wq, wk, wv, wo, wu, wd), y_ref, compute)
    exchanges = [Exchange(side, l, work, core_buf, ring_buf, migs[l], mig_send, mig_recv) for l in range(d.layers)]

    def scope(name, run, *args):
        with jax.named_scope(name):
            return run(*args)

    pool_loads = [[pltpu.make_async_copy(src.at[:, l], pools[l][p], pool_sem.at[l, p]) for p, src in enumerate((k_hbm, v_hbm))] for l in range(d.layers)]
    embeds_load, table_load, lens_load, table_load_v = [
        pltpu.make_async_copy(src, dst, load_sem.at[i]) for i, (src, dst) in enumerate(((embeds_hbm, embeds_v), (table_hbm, table_s), (lens_hbm, lens_s), (table_hbm, table_v)))]
    for load in [embeds_load] + pool_loads[0] + [table_load, table_load_v, lens_load]:
        load.start()
    barrier = pltpu.get_barrier_semaphore()

    @pl.loop(1, group_size)
    def _(r):
        pl.semaphore_signal(barrier, inc=1, device_id={'kv': lax.rem(me + r, group_size)})

    scope("barrier", lambda: pl.semaphore_wait(barrier, group_size - 1))

    groups = d.tokens // 8
    splits = group_size // groups
    cols = d.width // splits

    def piece(ref, m):
        return ref.at[m // splits, :, pl.ds(aligned(m % splits * cols, cols), cols)]

    def all_pieces(phase):
        some = mid_in.at[pl.ds(0, group_size - 1)]
        pltpu.make_async_remote_copy(some, some, x_send.at[phase], x_recv.at[phase], device_id={'kv': me}).wait()

    def send_embeddings():
        embeds_load.wait()

        @pl.loop(1, group_size)
        def _(r):
            m = lax.rem(me + r, group_size)
            pltpu.make_async_remote_copy(piece(embeds_v, m), mid_in.at[me], x_send.at[0], x_recv.at[0], device_id={'kv': m}).start()

        mid_in[me] = piece(embeds_v, me)[...]

    def load_tables():
        for load in (table_load, lens_load, table_load_v):
            load.wait()
        return lax.rem(table_s[1, 0] // d.slots + group_size, group_size)

    scope("pool_wait_0", lambda: [load.wait() for load in pool_loads[0]])

    def own(l):
        @pl.loop(0, entries)
        def _(e):
            slot = src_s[e] - me * d.slots
            mine = (slot >= 0) & (slot < d.slots)
            slot = jnp.clip(slot, 0, d.slots - 1)
            for p in range(2):
                page = pools[l][p][slot]
                work[l, p * entries + e] = jnp.where(mine, page, jnp.zeros_like(page))

    def step(l):
        scope(f"exchange_{l}_{exchanges[l].done}", exchanges[l].step)

    step_0, step_1 = functools.partial(step, 0), functools.partial(step, 1)

    scope("own_0", own, 0)
    step_0()
    for l in range(1, d.layers):
        for load in pool_loads[l]:
            load.start()
    scope("start_stream", dec.start_stream)
    shift = scope("load_tables", load_tables)
    home_a = lax.rem(me - shift + group_size, group_size)
    home_b = lax.rem(home_a + 1, group_size)

    def clipped(slot):
        return jnp.clip(slot - me * d.slots, 0, d.slots - 1)

    def first_here(l, p, i):
        return pools[l][p][clipped(table_s[0, home_b * d.rows + i])]

    def last_here(l, p, i):
        return pools[l][p][clipped(table_s[1, home_a * d.rows + i])]

    def migrated(l, p, home, i, page):
        entry = plan_s[0, home * d.rows + i]
        return jnp.where(entry >= 0, migs[l][p * entries + jnp.maximum(entry, 0)], page)

    def pack(l):
        @pl.loop(0, half)
        def _(i):
            for p in range(2):
                send_buf[l, 0, p, i] = first_here(l, p, i)
                send_buf[l, 1, p, i] = last_here(l, p, half + i)

    parts = 4
    size = half // parts

    def page_copy(l, way, p, rows):
        return pltpu.make_async_remote_copy(
            send_buf.at[l, way, p, rows], got_buf.at[l, way, p, rows], page_send.at[l, way, p], page_recv.at[l, way, p], device_id={'kv': (ahead, behind)[way]})

    pieces = [iter([(p, part) for part in range(parts) for p in range(2)]) for _ in range(d.layers)]

    def pages_start(l):
        p, part = next(pieces[l])
        for way in range(2):
            page_copy(l, way, p, pl.ds(part * size, size)).start()

    pages_0, pages_1 = functools.partial(pages_start, 0), functools.partial(pages_start, 1)

    def pages_wait(l):
        for way in range(2):
            for p in range(2):
                page_copy(l, way, p, pl.ds(0, half)).wait()

    def pass_on():
        all_pieces(0)
        later = me // splits * 8 % d.rows // half

        @pl.loop(0, group_size)
        def _(m):
            mid_out[m] = mid_in[lax.rem(m - shift + later + group_size, group_size)]

        @pl.loop(1, group_size)
        def _(r):
            m = lax.rem(me + r, group_size)
            pltpu.make_async_remote_copy(mid_out.at[m], piece(x_in, me), x_send.at[1], x_recv.at[1], device_id={'kv': m}).start()

        piece(x_in, me)[...] = mid_out[me]

    def take_embeddings():
        all_pieces(1)
        y_ref[...] = x_in[...].reshape(d.tokens, d.width)

    plan_copy = pltpu.make_async_copy(plan_v, plan_s, plan_sem)

    def plan():
        seq = lax.broadcasted_iota(jnp.int32, (1, table_v.shape[1]), 1)
        worker = lax.rem(seq // d.rows + shift, group_size)
        before = lax.rem(worker + group_size - 1, group_size)
        first, last = table_v[0:1, :], table_v[1:2, :]
        bad = (last < worker * d.slots) | (last >= worker * d.slots + d.slots) | (first < before * d.slots) | (first >= before * d.slots + d.slots)

        def entry(e, state):
            plan, bad = state
            return jnp.where(last == dst_s[e], e, plan), bad | (first == dst_s[e]).astype(jnp.int32)

        plan, bad = lax.fori_loop(0, entries, entry, (jnp.full_like(last, -1), bad.astype(jnp.int32)))
        plan_v[...] = plan
        plan_copy.start()
        info_s[0] = shift
        info_s[1] = 1 - jnp.max(bad)

    def new_copies(l):
        return [pltpu.make_async_remote_copy(
            ref.at[pl.ds(g * d.stride + t * d.rows + half, half)], new_buf.at[l, p, g, t], new_send.at[l, p, g, t], new_recv.at[l, p, g, t], device_id={'kv': ahead})
            for p, ref in enumerate((dec.kn_s, dec.vn_s)) for g in range(d.kv_heads) for t in range(2)]

    def project(l):
        dec.project(l)
        for copy in new_copies(l):
            copy.start()

    scope("pack_0", pack, 0)
    step_0()
    scope("send_embeddings", send_embeddings)
    pages_0()
    scope("plan", plan)
    step_0()
    pages_0()
    step_0()
    pages_0()
    scope("pass_on", pass_on)
    step_0()
    pages_0()
    for l in range(1, d.layers):
        for load in pool_loads[l]:
            load.wait()
    step_0()
    pages_0()
    scope("own_1", own, 1)
    step_0()
    pages_0()
    scope("pack_1", pack, 1)
    step_0()
    pages_0()
    scope("take_embeddings", take_embeddings)
    step_1()
    step_0()
    pages_0()
    scope("project_0", project, 0)
    step_1()
    step_0()
    plan_copy.wait()
    step_0()
    scope("pages_wait_0", pages_wait, 0)

    def attend(l, events_a, events_b):
        def put_page(p, i, val):
            last_buf[p, i] = val

        dec.attend(lambda i: lens_s[home_a * d.rows + i], lambda p, i: got_buf[l, 0, p, i],
                   lambda p, i: migrated(l, p, home_a, i, last_here(l, p, i)), put_page, events_a, 0, half)
        dec.attend(lambda i: lens_s[home_b * d.rows + i], lambda p, i: first_here(l, p, i),
                   lambda p, i: migrated(l, p, home_b, i, got_buf[l, 1, p, i - half]), lambda p, i, val: None, events_b, half, half)
        dec.gather_heads()

    def finish_pages(l):
        for copy in new_copies(l):
            copy.wait()

        @pl.loop(0, half)
        def _(i):
            row = half + i
            for p in range(2):
                page = migrated(l, p, home_a, row, last_here(l, p, row))
                last_buf[p, row] = dec.insert(page, lens_s[home_a * d.rows + row], lambda t, g: new_buf[l, p, g, t, pl.ds(i, 1), :])

        pltpu.make_async_copy(last_buf, last_out.at[l], out_sem).start()

    def last_wait(l):
        pltpu.make_async_copy(last_buf, last_out.at[l], out_sem).wait()

    def event(run):
        return lambda: run()

    blocks = half // min(UNROLL, half)
    pairs = 2 * (d.n_u // 2)
    with jax.named_scope("attend_0"):
        attend(0, [(0, event(step_1))], [(0, event(step_1))])
    events = [((2 * k + 1) * pairs // (4 * parts), event(pages_1)) for k in range(2 * parts)]
    events += [(k * (pairs - 1) // 7, event(step_1)) for k in range(Exchange.STEPS - 4)]
    events += [(pairs - 1, functools.partial(scope, "finish_0", finish_pages, 0))]
    with jax.named_scope("mix_0"):
        dec.mix(0, sorted(events, key=lambda event: event[0]))
    for l in range(1, d.layers):
        scope(f"project_{l}", project, l)
        scope(f"pages_wait_{l}", pages_wait, l)
        last_wait(l - 1)
        with jax.named_scope(f"attend_{l}"):
            attend(l, [], [])
        with jax.named_scope(f"mix_{l}"):
            dec.mix(l, [(pairs // 2, functools.partial(finish_pages, l))])
    for t in range(2):
        ya_ref[t] = y_ref[pl.ds(t * d.rows, half), :]
        yb_ref[t] = y_ref[pl.ds(t * d.rows + half, half), :]
    last_wait(d.layers - 1)


def decode_adjacent(side, group_size, d, table, seq_lens, mig_src, mig_dst, embeds, weights, k_pool, v_pool):
    entries = mig_src.shape[0]
    half = d.rows // 2
    page = (d.page_rows, d.head_dim)
    struct = lambda *shape: jax.ShapeDtypeStruct(shape, BF16)
    groups = d.tokens // 8
    mid = pltpu.VMEM((group_size, 8, d.width * groups // group_size), BF16)
    return pl.pallas_call(
        functools.partial(adjacent_kernel, d, side, group_size, entries),
        out_shape=[struct(2, half, d.width), struct(2, half, d.width), jax.ShapeDtypeStruct((2,), jnp.int32), struct(d.layers, 2, d.rows, *page)],
        in_specs=[SMEM] * 2 + [ANY] * 11,
        out_specs=[VMEM, VMEM, SMEM, ANY],
        scratch_shapes=[
            pltpu.SMEM(table.shape, jnp.int32),
            pltpu.SMEM(seq_lens.shape, jnp.int32),
            pltpu.VMEM(table.shape, jnp.int32),
            pltpu.VMEM((groups, 8, d.width), BF16),
            pltpu.VMEM((d.tokens, d.width), BF16),
            pltpu.VMEM((d.layers, 2, 2, half) + page, BF16),
            pltpu.VMEM((d.layers, 2, 2, half) + page, BF16),
            pltpu.VMEM((2, d.rows) + page, BF16),
            pltpu.VMEM((d.layers, 2, d.kv_heads, 2, half, d.head_dim), F32),
            pltpu.VMEM((d.layers, 2 * entries) + page, BF16),
            pltpu.VMEM((d.layers, entries) + page, BF16),
            pltpu.VMEM((d.layers, entries) + page, BF16),
            mid,
            mid,
            pltpu.VMEM((groups, 8, d.width), BF16),
            pltpu.VMEM((1, table.shape[1]), jnp.int32),
            pltpu.SMEM((1, table.shape[1]), jnp.int32),
        ] + [pltpu.VMEM((2 * entries,) + page, BF16)] * d.layers + [pltpu.VMEM((d.slots,) + page, BF16)] * (2 * d.layers) + d.compute_scratch(10, 8) + [
            DMA((4,)),
            DMA((d.layers, 2)),
            DMA,
            DMA((2,)),
            DMA((2,)),
            DMA((d.layers, 2, 2)),
            DMA((d.layers, 2, 2)),
            DMA((d.layers, 2, d.kv_heads, 2)),
            DMA((d.layers, 2, d.kv_heads, 2)),
            DMA((d.layers, 10, 4)),
            DMA((d.layers, 10, 4)),
            DMA,
        ],
        compiler_params=pltpu.CompilerParams(collective_id=1, has_side_effects=True, skip_device_barrier=True, vmem_limit_bytes=LIMIT),
        cost_estimate=d.cost(d.layers),
        name="decode_adjacent",
    )(mig_src, mig_dst, table, seq_lens, embeds.reshape(groups, 8, d.width), *weights, k_pool, v_pool)


def fill_pools_kernel(dims, group_size, info_s, table_s, src_s, k_hbm, v_hbm, last_hbm, k_out, v_out, k_buf, v_buf, sem, put_sem):
    d = dims
    me = lax.axis_index('kv')
    home = lax.rem(me - info_s[0] + group_size, group_size)
    pools = ((k_hbm, k_buf, k_out), (v_hbm, v_buf, v_out))
    parts = sem.shape[1]
    size = d.slots // parts

    def moves(part, out):
        at = pl.ds(part * size, size)
        return [pltpu.make_async_copy(*((buf.at[at], dst.at[at]) if out else (src.at[at], buf.at[at])), sem.at[p, part]) for p, (src, buf, dst) in enumerate(pools)]

    def start(copies):
        for copy in copies:
            copy.start()

    def wait(copies):
        for copy in copies:
            copy.wait()

    def within(ids, count, part, run):
        @pl.loop(0, count)
        def _(i):
            slot = ids(i) - me * d.slots
            here = (slot >= part * size) & (slot < part * size + size)
            slot = jnp.clip(slot, 0, d.slots - 1)
            pl.when(here)(lambda: run(i, slot))

    def row_copies(i, slot):
        return [pltpu.make_async_copy(last_hbm.at[:, p, i], buf.at[slot], put_sem) for p, (_, buf, _) in enumerate(pools)]

    def clear(i, slot):
        for _, buf, _ in pools:
            buf[slot] = jnp.zeros(buf.shape[1:], buf.dtype)

    def last_id(i):
        return table_s[1, home * d.rows + i]

    @pl.loop(0, parts)
    def _(part):
        start(moves(part, False))

    @pl.loop(0, parts)
    def _(part):
        wait(moves(part, False))
        within(last_id, d.rows, part, lambda i, slot: start(row_copies(i, slot)))
        within(lambda e: src_s[e], src_s.shape[0], part, clear)
        within(last_id, d.rows, part, lambda i, slot: wait(row_copies(i, slot)))
        start(moves(part, True))

    @pl.loop(0, parts)
    def _(part):
        wait(moves(part, True))


def fill_pools(group_size, d, info, table, mig_src, k_pool, v_pool, last):
    size = 4 * k_pool.size
    return pl.pallas_call(
        functools.partial(fill_pools_kernel, d, group_size),
        out_shape=[jax.ShapeDtypeStruct(k_pool.shape, k_pool.dtype)] * 2,
        in_specs=[SMEM] * 3 + [ANY] * 3,
        out_specs=[ANY, ANY],
        scratch_shapes=[pltpu.VMEM(k_pool.shape, k_pool.dtype), pltpu.VMEM(k_pool.shape, k_pool.dtype), DMA((2, 4)), DMA],
        compiler_params=pltpu.CompilerParams(vmem_limit_bytes=LIMIT),
        cost_estimate=pl.CostEstimate(flops=40 * size, bytes_accessed=2 * size, transcendentals=0),
        name="fill_pools",
    )(info, table, mig_src, k_pool, v_pool, last)


def gather_pages_kernel(idx_ref, k_hbm, v_hbm, k_out, v_out, sem):
    rows = k_out.shape[0]

    def copies(i):
        slot = jnp.maximum(idx_ref[i], 0)
        return (pltpu.make_async_copy(k_hbm.at[slot], k_out.at[i], sem), pltpu.make_async_copy(v_hbm.at[slot], v_out.at[i], sem))

    @pl.loop(0, rows)
    def _(i):
        @pl.when(idx_ref[i] >= 0)
        def _():
            for copy in copies(i):
                copy.start()

        @pl.when(idx_ref[i] < 0)
        def _():
            k_out[i] = jnp.zeros(k_out.shape[1:], k_out.dtype)
            v_out[i] = jnp.zeros(v_out.shape[1:], v_out.dtype)

    @pl.loop(0, rows)
    def _(i):
        @pl.when(idx_ref[i] >= 0)
        def _():
            for copy in copies(i):
                copy.wait()


def gather_pages(idx, k_pool, v_pool):
    shape = jax.ShapeDtypeStruct((idx.shape[0],) + k_pool.shape[1:], k_pool.dtype)
    return pl.pallas_call(
        gather_pages_kernel,
        out_shape=[shape, shape],
        in_specs=[SMEM, ANY, ANY],
        out_specs=[VMEM, VMEM],
        scratch_shapes=[DMA],
        compiler_params=pltpu.CompilerParams(vmem_limit_bytes=LIMIT),
        name="gather_pages",
    )(idx, k_pool, v_pool)


def share_kernel(side, k_hbm, v_hbm, k_out, v_out, work, core_buf, ring_buf, load_sem, send_sem, recv_sem, result):
    entries = k_hbm.shape[0]
    exchange = Exchange(side, 0, work, core_buf, ring_buf, result, send_sem, recv_sem)
    units = [pl.ds(p * entries, entries) for p in range(2)]
    for p, src in enumerate((k_hbm, v_hbm)):
        pltpu.make_async_copy(src, work.at[0].at[units[p]], load_sem.at[p]).start()
    for p, src in enumerate((k_hbm, v_hbm)):
        pltpu.make_async_copy(src, work.at[0].at[units[p]], load_sem.at[p]).wait()
    for _ in range(Exchange.STEPS):
        exchange.step()
    for p, dst in enumerate((k_out, v_out)):
        pltpu.make_async_copy(result.at[units[p]], dst, load_sem.at[p]).start()
    for p, dst in enumerate((k_out, v_out)):
        pltpu.make_async_copy(result.at[units[p]], dst, load_sem.at[p]).wait()


def share(side, mig_k, mig_v):
    entries = mig_k.shape[0]
    page = mig_k.shape[1:]
    return pl.pallas_call(
        functools.partial(share_kernel, side),
        out_shape=[jax.ShapeDtypeStruct(mig_k.shape, BF16)] * 2,
        in_specs=[ANY, ANY],
        out_specs=[ANY, ANY],
        scratch_shapes=[pltpu.VMEM((1, n * entries) + page, BF16) for n in (2, 1, 1)] + [DMA((2,)), DMA((1, 10, 4)), DMA((1, 10, 4)), pltpu.VMEM((2 * entries,) + page, BF16)],
        compiler_params=pltpu.CompilerParams(has_side_effects=True, vmem_limit_bytes=LIMIT),
        name="share",
    )(mig_k, mig_v)


def migrate_kernel(dst_ref, src_ref, k_hbm, v_hbm, mk_hbm, mv_hbm, k_out, v_out, k_buf, v_buf, sem, fix_sem):
    entries = dst_ref.shape[0]
    pairs = ((k_hbm, mk_hbm, k_buf, k_out), (v_hbm, mv_hbm, v_buf, v_out))
    for p, (src, _, buf, _) in enumerate(pairs):
        pltpu.make_async_copy(src, buf, sem.at[p]).start()
    for p, (src, _, buf, _) in enumerate(pairs):
        pltpu.make_async_copy(src, buf, sem.at[p]).wait()

    @pl.loop(0, entries)
    def _(e):
        @pl.when(dst_ref[e] >= 0)
        def _():
            for _, mig, buf, _ in pairs:
                copy = pltpu.make_async_copy(mig.at[e], buf.at[jnp.maximum(dst_ref[e], 0)], fix_sem)
                copy.start()
                copy.wait()

        @pl.when(src_ref[e] >= 0)
        def _():
            for _, _, buf, _ in pairs:
                buf[jnp.maximum(src_ref[e], 0)] = jnp.zeros(buf.shape[1:], buf.dtype)

    for p, (_, _, buf, dst) in enumerate(pairs):
        pltpu.make_async_copy(buf, dst, sem.at[p]).start()
    for p, (_, _, buf, dst) in enumerate(pairs):
        pltpu.make_async_copy(buf, dst, sem.at[p]).wait()


def migrate(dst_local, src_local, k_pool, v_pool, mig_k, mig_v):
    shape = jax.ShapeDtypeStruct(k_pool.shape, k_pool.dtype)
    return pl.pallas_call(
        migrate_kernel,
        out_shape=[shape, shape],
        in_specs=[SMEM, SMEM, ANY, ANY, ANY, ANY],
        out_specs=[ANY, ANY],
        scratch_shapes=[pltpu.VMEM(k_pool.shape, k_pool.dtype), pltpu.VMEM(k_pool.shape, k_pool.dtype), DMA((2,)), DMA],
        compiler_params=pltpu.CompilerParams(vmem_limit_bytes=LIMIT),
        name="migrate",
    )(dst_local, src_local, k_pool, v_pool, mig_k, mig_v)


def decode_kernel(dims, sc_ref, x_ref, p0k_hbm, p0v_hbm, wq, wk, wv, wo, wu, wd, k_in, v_in, y_ref, k_out, v_out,
                  first_buf, last_buf, *rest):
    compute, (page_sem, put_sem) = rest[:-2], rest[-2:]
    d = dims
    dec = Decoder(d, 0, d.layers, (wq, wk, wv, wo, wu, wd), y_ref, compute, 1, 2)
    dec.start_stream()
    y_ref[...] = x_ref[...]
    loads = [pltpu.make_async_copy(src, first_buf.at[p], page_sem.at[p]) for p, src in enumerate((p0k_hbm, p0v_hbm))]
    for load in loads:
        load.start()

    def last_loads(run):
        @pl.loop(0, d.rows)
        def _(i):
            for p, src in enumerate((k_in, v_in)):
                run(pltpu.make_async_copy(src.at[sc_ref[0, i]], last_buf.at[p, i], page_sem.at[2]))

    def puts(run):
        @pl.loop(0, d.rows)
        def _(i):
            @pl.when(sc_ref[2, i] > 0)
            def _():
                for p, dst in enumerate((k_out, v_out)):
                    run(pltpu.make_async_copy(last_buf.at[p, i], dst.at[sc_ref[0, i]], put_sem))

    last_loads(lambda copy: copy.start())
    for load in loads:
        load.wait()
    last_loads(lambda copy: copy.wait())

    @pl.loop(0, d.layers)
    def _(layer):
        def put_page(p, i, val):
            last_buf[p, i, layer] = val

        dec.project(layer)
        dec.attend(lambda i: sc_ref[1, i], lambda p, i: first_buf[p, i, layer], lambda p, i: last_buf[p, i, layer], put_page)
        dec.gather_heads()
        dec.mix(layer)

    puts(lambda copy: copy.start())
    puts(lambda copy: copy.wait())


def decode(d, scalars, x, p0k, p0v, weights, k_pool, v_pool):
    pool = jax.ShapeDtypeStruct(k_pool.shape, k_pool.dtype)
    pages = pltpu.VMEM((2, d.rows, d.layers, d.page_rows, d.head_dim), BF16)
    return pl.pallas_call(
        functools.partial(decode_kernel, d),
        out_shape=[jax.ShapeDtypeStruct(x.shape, x.dtype), pool, pool],
        in_specs=[SMEM, VMEM] + [ANY] * 10,
        out_specs=[VMEM, ANY, ANY],
        input_output_aliases={10: 1, 11: 2},
        scratch_shapes=[pages, pages] + d.compute_scratch(16, 16) + [DMA((3,)), DMA],
        compiler_params=pltpu.CompilerParams(vmem_limit_bytes=LIMIT),
        cost_estimate=d.cost(d.layers),
        name="decode",
    )(scalars, x, p0k, p0v, *weights, k_pool, v_pool)


def permute(arrays, shift, group_size):
    if shift == group_size // 2:
        return permute(permute(arrays, shift // 2, group_size), shift // 2, group_size)
    perm = [(i, (i + shift) % group_size) for i in range(group_size)]
    return jax.tree.map(lambda a: lax.ppermute(a, 'kv', perm), arrays) if shift else arrays


def rotate_back(first, second, shift, group_size, beside):
    def branch(r):
        def run(args):
            parts = permute(args[0], -r % group_size, group_size), permute(args[1], (1 - r) % group_size, group_size)
            return jnp.concatenate(parts, axis=1), beside()

        return run

    return lax.switch(shift, [branch(r) for r in range(group_size)], (first, second))


def rotate(arrays, shift, group_size):
    stride = math.isqrt(2 * group_size)
    for count, move in ((shift // stride, stride), (shift % stride, 1)):
        arrays = lax.fori_loop(0, count, lambda _, a: permute(a, move, group_size), arrays)
    return arrays


def solution(mesh):
    group_size = mesh.shape['kv']
    side = math.isqrt(group_size // 2)
    pool_spec = P(('rep', 'kv'))
    tok_spec = P(None, ('rep', 'kv'), None)

    def device_fn(embeds, w_query, w_key, w_value, w_out, w_up, w_down, k_pool5, v_pool5, new_table, seq_lens, mig_src, mig_dst):
        me = lax.axis_index('kv')
        slots, layers, page, kv_heads, head_dim = k_pool5.shape
        rows, width = embeds.shape[1:]
        weights = (w_query, w_key, w_value, w_out, w_up, w_down)
        k_pool = k_pool5.reshape(slots, layers, page * kv_heads, head_dim)
        v_pool = v_pool5.reshape(slots, layers, page * kv_heads, head_dim)
        d = Dims(rows, weights, k_pool, page)
        ints = jnp.int32

        def local(ids):
            loc = ids - me * slots
            return jnp.where((loc >= 0) & (loc < slots), loc, -1)

        def take(vec, dev):
            return lax.dynamic_slice(vec, (dev * rows,), (rows,))

        def inside(ids):
            return jnp.clip(ids - me * slots, 0, slots - 1)

        def general_path():
            first_new, last_new = new_table[:, 0], new_table[:, 1]
            moved = first_new[None, :] == mig_dst[:, None]
            first_old = jnp.where(jnp.any(moved, axis=0), jnp.sum(jnp.where(moved, mig_src[:, None], 0), axis=0), first_new)
            home = jnp.arange(first_new.shape[0], dtype=ints) // rows
            worker = last_new // slots
            shift_of = (worker - home + group_size) % group_size
            first_shift = (worker - first_old // slots + group_size) % group_size
            shift_ids = jnp.arange(group_size, dtype=ints)
            wanted = jnp.any(shift_of[None, :] == shift_ids[:, None], axis=1)
            mig_k, mig_v = gather_pages(local(mig_src), k_pool, v_pool)
            by_layer = tuple(m.swapaxes(0, 1) for m in (mig_k, mig_v))
            mig_k, mig_v = (m.swapaxes(0, 1) for m in lax.map(lambda pages: tuple(share(side, *pages)), by_layer))
            k_new, v_new = migrate(local(mig_dst), local(mig_src), k_pool, v_pool, mig_k, mig_v)

            def one_round(shift, y, k_new, v_new):
                src_home = (me - shift + group_size) % group_size
                x = rotate(embeds.reshape(2 * rows, width), shift, group_size)
                in_round = shift_of == shift
                wanted2 = jnp.any(in_round[None, :] & (first_shift[None, :] == shift_ids[:, None]), axis=1)

                def more(state):
                    left, pk, pv = state
                    shift2 = jnp.argmax(left).astype(ints)
                    dest_home = (me + shift2 - shift + group_size) % group_size
                    got = gather_pages(inside(take(first_old, dest_home)), k_pool, v_pool)
                    got_k, got_v = rotate(tuple(got), shift2, group_size)
                    mine = (take(first_shift, src_home) == shift2)[:, None, None, None]
                    return left & (shift_ids != shift2), jnp.where(mine, got_k, pk), jnp.where(mine, got_v, pv)

                zeros = jnp.zeros((rows,) + k_pool.shape[1:], k_pool.dtype)
                _, pk, pv = lax.while_loop(lambda state: jnp.any(state[0]), more, (wanted2, zeros, zeros))
                valid = take(shift_of, src_home) == shift
                scalars = jnp.stack([inside(take(last_new, src_home)), take(seq_lens, src_home), valid.astype(ints)])
                out, k_new, v_new = decode(d, scalars, x, pk, pv, weights, k_new, v_new)
                back = rotate(out, (group_size - shift) % group_size, group_size)
                mine = (take(shift_of, me) == shift)[None, :, None]
                return jnp.where(mine, back.reshape(embeds.shape), y), k_new, v_new

            def next_round(state):
                left, y, k_new, v_new = state
                shift = jnp.argmax(left).astype(ints)
                y, k_new, v_new = one_round(shift, y, k_new, v_new)
                return left & (shift_ids != shift), y, k_new, v_new

            _, y, k_new, v_new = lax.while_loop(lambda state: jnp.any(state[0]), next_round, (wanted, jnp.zeros_like(embeds), k_new, v_new))
            return y, k_new, v_new

        table = new_table.T
        ya, yb, info, last = decode_adjacent(side, group_size, d, table, seq_lens, mig_src, mig_dst, embeds, weights, k_pool, v_pool)
        y, (k_new, v_new) = rotate_back(ya, yb, info[0], group_size, lambda: fill_pools(group_size, d, info, table, mig_src, k_pool, v_pool, last))
        _, y, k_new, v_new = lax.while_loop(lambda state: state[0] == 0, lambda state: (jnp.ones_like(state[0]),) + general_path(), (info[1], y, k_new, v_new))
        return y, k_new.reshape(k_pool5.shape), v_new.reshape(v_pool5.shape)

    return jax.shard_map(device_fn, mesh=mesh, in_specs=(tok_spec, P(), P(), P(), P(), P(), P(), pool_spec, pool_spec, P('rep', None), P('rep'), P('rep'), P('rep')), out_specs=(tok_spec, pool_spec, pool_spec), check_vma=False)
```

```python
import functools
import math

import jax
import jax.numpy as jnp
from jax import lax
from jax.experimental import pallas as pl
from jax.experimental.pallas import tpu as pltpu
from jax.sharding import PartitionSpec as P

ANY = pl.BlockSpec(memory_space=pl.ANY)
SMEM = pl.BlockSpec(memory_space=pltpu.SMEM)
VMEM = pl.BlockSpec(memory_space=pltpu.VMEM)
DMA = pltpu.SemaphoreType.DMA
CHUNK = 256
UNROLL = 8
LANES = 128
HALF = CHUNK // 2
PAIR = (0, 1)
LIMIT = 63 << 20
F32, BF16 = jnp.float32, jnp.bfloat16


def iota(shape, axis):
    return lax.broadcasted_iota(jnp.int32, shape, axis)


def dot(a, b):
    return jnp.dot(a, b, preferred_element_type=F32)


def local_slot(ids, me, slots):
    return jnp.clip(ids - me * slots, 0, slots - 1)


def aligned(x, multiple):
    return x if isinstance(x, int) else pl.multiple_of(x, multiple)


class Dims:
    def __init__(self, rows, weights, k_pool, page):
        w_query, w_key, _, _, w_up, _ = weights
        self.layers, self.width, self.q_width = w_query.shape
        self.ff = w_up.shape[2]
        self.slots, _, self.page_rows, self.head_dim = k_pool.shape
        self.kv_heads = w_key.shape[2] // self.head_dim
        self.heads = self.q_width // self.head_dim
        self.page, self.rows = page, rows
        self.tokens = 2 * rows
        self.stride = self.tokens + 8
        self.n_q, self.n_o, self.n_u = self.q_width // CHUNK, self.width // CHUNK, self.ff // CHUNK
        self.col_layer = self.n_q + 2 + self.n_o + self.n_u

    def compute_scratch(self, n_col, n_row):
        return [
            pltpu.VMEM((n_col, self.width, CHUNK), BF16),
            pltpu.VMEM((n_row, CHUNK, self.width), BF16),
            pltpu.VMEM((self.heads * self.stride, self.head_dim), F32),
            pltpu.VMEM((self.kv_heads * self.stride, self.head_dim), F32),
            pltpu.VMEM((self.kv_heads * self.stride, self.head_dim), F32),
            pltpu.VMEM((self.heads * self.stride, self.head_dim), F32),
            pltpu.VMEM((self.tokens, self.q_width), BF16),
            pltpu.VMEM((self.tokens, self.ff), BF16),
            pltpu.VMEM((self.tokens, self.width), F32),
            DMA((n_col,)),
            DMA((n_row,)),
        ]

    def cost(self, layers):
        size = layers * self.width * (2 * self.q_width + 2 * self.kv_heads * self.head_dim + 2 * self.ff)
        return pl.CostEstimate(flops=2 * size * self.tokens, bytes_accessed=2 * size, transcendentals=0)


class Decoder:
    def __init__(self, dims, first, layers, weights, y_ref, scratch, group=2, unroll=UNROLL, shared=False):
        self.group, self.unroll, self.shared = group, unroll, shared
        self.d, self.first, self.layers, self.weights, self.y_ref = dims, first, layers, weights, y_ref
        (self.col_buf, self.row_buf, self.q_s, self.kn_s, self.vn_s, self.o_s, self.att, self.act, self.acc, self.col_sem, self.row_sem) = scratch
        self.n_col, self.n_row = self.col_buf.shape[0], self.row_buf.shape[0]
        self.zero = lax.axis_index('kv') * 0
        d = dims
        self.whole, self.begin = d.ff // 2 // CHUNK, lax.axis_index('kv') % 2 * (d.ff // 2)
        self.cols = layers * d.col_layer - shared * (d.n_u - self.whole)
        self.downs = layers * d.n_u - shared * (d.n_u - self.whole)
        cols = 2 * d.page * d.kv_heads
        col_pos = iota((2 * d.heads, cols), 1)
        row_pos = iota((2 * d.heads, cols), 0)
        same_head = (col_pos % d.kv_heads) == (row_pos % d.heads) // (d.heads // d.kv_heads)
        self.limit = jnp.where(same_head, col_pos // d.kv_heads - row_pos // d.heads, 4 * d.page)
        self.page_pos = iota((d.page_rows, d.head_dim), 0) // d.kv_heads
        self.tile_head = iota((8, d.head_dim), 0) % d.kv_heads

    def layer_of(self, g, per_layer):
        return sum((g >= per_layer * l).astype(jnp.int32) for l in range(1, self.layers))

    def col_start(self, g):
        d = self.d
        wq, wk, wv, wo, wu, _ = self.weights

        @pl.when(g < self.cols)
        def _():
            layer = self.layer_of(g, d.col_layer)
            pos = g - layer * d.col_layer
            slot = g % self.n_col

            def go(src, c, begin=0):
                start = aligned(c * CHUNK + begin, LANES)
                pltpu.make_async_copy(src.at[self.first + layer].at[:, pl.ds(start, CHUNK)], self.col_buf.at[slot], self.col_sem.at[slot]).start()

            @pl.when(pos < d.n_q)
            def _():
                go(wq, pos)

            @pl.when(pos == d.n_q)
            def _():
                go(wk, 0)

            @pl.when(pos == d.n_q + 1)
            def _():
                go(wv, 0)

            @pl.when((pos >= d.n_q + 2) & (pos < d.n_q + 2 + d.n_o))
            def _():
                go(wo, pos - (d.n_q + 2))

            @pl.when(pos >= d.n_q + 2 + d.n_o)
            def _():
                go(wu, pos - (d.n_q + 2 + d.n_o), self.begin * (layer == self.layers - 1) if self.shared else 0)

    def row_start(self, g):
        d = self.d
        wd = self.weights[5]

        @pl.when(g < self.downs)
        def _():
            layer = self.layer_of(g, d.n_u)
            slot = g % self.n_row
            start = aligned((g - layer * d.n_u) * CHUNK + (self.begin * (layer == self.layers - 1) if self.shared else 0), LANES)
            pltpu.make_async_copy(wd.at[self.first + layer].at[pl.ds(start, CHUNK)], self.row_buf.at[slot], self.row_sem.at[slot]).start()

    def start_stream(self):
        @pl.loop(0, self.n_col)
        def _(g):
            self.col_start(g)

        @pl.loop(0, self.n_row)
        def _(g):
            self.row_start(g)

    def with_cols(self, g, count, body):
        slots = [(g + u) % self.n_col for u in range(count)]
        for slot in slots:
            pltpu.make_async_copy(self.weights[1].at[0], self.col_buf.at[slot], self.col_sem.at[slot]).wait()
        body([self.col_buf.at[slot] for slot in slots])
        for u in range(count):
            self.col_start(g + u + self.n_col)

    def with_rows(self, g, count, body):
        slots = [(g + u) % self.n_row for u in range(count)]
        for slot in slots:
            pltpu.make_async_copy(self.weights[5].at[0, pl.ds(0, CHUNK), :], self.row_buf.at[slot], self.row_sem.at[slot]).wait()
        body([self.row_buf.at[slot] for slot in slots])
        for u in range(count):
            self.row_start(g + u + self.n_row)

    def project(self, layer):
        d = self.d
        col0 = (self.zero + layer) * d.col_layer

        def product(ref):
            return dot(self.y_ref[...], ref[...]).astype(BF16).astype(F32)

        def put(dst, first, out):
            for h in range(CHUNK // d.head_dim):
                at = aligned((first + h) * d.stride, 8)
                dst[pl.ds(at, d.tokens), :] = out[:, h * d.head_dim:(h + 1) * d.head_dim]

        many = self.group

        @pl.loop(0, d.n_q // many)
        def _(j):
            def body(refs):
                outs = [product(ref) for ref in refs]
                for u in range(many):
                    put(self.q_s, (many * j + u) * (CHUNK // d.head_dim), outs[u])

            self.with_cols(col0 + many * j, many, body)

        def body(refs):
            outs = [product(ref) for ref in refs]
            put(self.kn_s, 0, outs[0])
            put(self.vn_s, 0, outs[1])

        self.with_cols(col0 + d.n_q, 2, body)

    def insert(self, page, n, row):
        d = self.d
        val = page.astype(F32)
        for t in PAIR:
            new = jnp.broadcast_to(row(t, 0), (8, d.head_dim))
            for g in range(1, d.kv_heads):
                new = jnp.where(self.tile_head == g, row(t, g), new)
            val = jnp.where(self.page_pos == n - d.page + t, jnp.concatenate([new] * (d.page_rows // 8), axis=0), val)
        return val.astype(BF16)

    def attend(self, lens, first_page, last_page, put_page, events=(), begin=0, count=None):
        d = self.d
        count = count or d.rows
        unroll = min(self.unroll, count)

        def some(first):
            ids = [first + u for u in range(unroll)]
            scores, vals = [], []
            for i in ids:
                n = lens(i)

                def updated(p, new_ref):
                    val = self.insert(last_page(p, i), n, lambda t, g: new_ref[pl.ds(g * d.stride + t * d.rows + i, 1), :])
                    put_page(p, i, val)
                    return val

                keys = jnp.concatenate([first_page(0, i), updated(0, self.kn_s)], axis=0)
                vals.append(updated(1, self.vn_s))
                qs = jnp.concatenate([self.q_s[pl.ds(t * d.rows + i, d.heads, stride=d.stride), :] for t in PAIR], axis=0)
                score = lax.dot_general(qs.astype(BF16), keys, (((1,), (1,)), ((), ())), preferred_element_type=F32) * d.head_dim ** -0.5
                scores.append(jnp.where(self.limit <= n, score, -jnp.inf))
            tops = [jnp.max(score, axis=1, keepdims=True) for score in scores]
            probs = [jnp.exp(score - top) for score, top in zip(scores, tops)]
            totals = [jnp.sum(prob, axis=1, keepdims=True) for prob in probs]
            for u, i in enumerate(ids):
                both = jnp.concatenate([first_page(1, i), vals[u]], axis=0)
                out = dot(probs[u].astype(BF16), both) / totals[u]
                for t in PAIR:
                    self.o_s[pl.ds(t * d.rows + i, d.heads, stride=d.stride), :] = out[t * d.heads:(t + 1) * d.heads]

        @pl.loop(0, count // unroll)
        def _(block):
            for k, run in events:
                pl.when(block == k)(run)
            some(begin + block * unroll)

    def gather_heads(self):
        d = self.d
        for h in range(d.heads):
            self.att[:, h * d.head_dim:(h + 1) * d.head_dim] = self.o_s[h * d.stride:h * d.stride + d.tokens, :].astype(BF16)

    def span(self, j):
        return pl.ds(aligned(j * CHUNK, CHUNK), CHUNK)

    def out_project(self, layer, after=None):
        d, many = self.d, self.group

        @pl.loop(0, d.n_o // many)
        def _(j):
            def body(refs):
                outs = [dot(self.att[...], ref[...]) for ref in refs]
                for u in range(many):
                    at = self.span(many * j + u)
                    self.y_ref[:, at] = (self.y_ref[:, at].astype(F32) + outs[u]).astype(BF16)

            self.with_cols(layer * d.col_layer + d.n_q + len(PAIR) + many * j, many, body)
            if after:
                after(j)

    def mix(self, layer, events=()):
        d = self.d
        layer = self.zero + layer
        col0 = layer * d.col_layer + d.n_q + 2
        many = self.group
        pairs = d.n_u // many

        def between(j, first):
            for k, run in events:
                if first <= k < first + pairs:
                    pl.when(j == k - first)(run)

        self.out_project(layer)

        def up(first, count):
            def body(refs):
                ups = [dot(self.y_ref[...], ref[...]) for ref in refs]
                for u in range(count):
                    self.act[:, self.span(first + u)] = jax.nn.gelu(ups[u].astype(BF16).astype(F32), approximate=True).astype(BF16)

            self.with_cols(col0 + d.n_o + first, count, body)

        def down(first, count):
            def body(refs):
                out = self.acc[...]
                for u in range(count):
                    out += dot(self.act[:, self.span(first + u)], refs[u][...])
                self.acc[...] = out

            self.with_rows(layer * d.n_u + first, count, body)

        @pl.loop(0, pairs)
        def _(j):
            between(j, 0)
            up(many * j, many)

        if d.n_u % many:
            up(d.n_u - 1, 1)

        self.acc[...] = self.y_ref[...].astype(F32)

        @pl.loop(0, pairs)
        def _(j):
            between(j, pairs)
            down(many * j, many)

        if d.n_u % many:
            down(d.n_u - 1, 1)

        self.y_ref[...] = self.acc[...].astype(BF16)


    def half_start(self):
        layer, at = self.first + self.layers - 1, pl.ds(aligned(self.begin + self.whole * CHUNK, LANES), HALF)
        return (pltpu.make_async_copy(self.weights[4].at[layer].at[:, at], self.half_col, self.half_sem.at[0]),
                pltpu.make_async_copy(self.weights[5].at[layer].at[at], self.half_row, self.half_sem.at[1]))

    def mix_shared(self, layer, send_hidden, wait_hidden, swap_sums, events=()):
        d = self.d
        layer = self.zero + layer
        col0 = layer * d.col_layer + d.n_q + 2
        many = self.group
        rows = d.tokens
        offset = d.ff // 2

        self.out_project(layer, send_hidden)

        self.acc[...] = self.y_ref[...].astype(F32)
        self.acc_other[...] = jnp.zeros_like(self.acc_other)
        wait_hidden()

        def hidden():
            return jnp.concatenate([self.y_ref[...], self.y_other[...]], axis=0)

        def activate(up, at, size):
            val = jax.nn.gelu(up.astype(BF16).astype(F32), approximate=True).astype(BF16)
            self.act[:, pl.ds(aligned(at, LANES), size)] = val[:rows]
            self.act[:, pl.ds(aligned(at + offset, LANES), size)] = val[rows:]

        @pl.loop(0, self.whole // many)
        def _(j):
            for k, run in events:
                pl.when(j == k)(run)

            def body(refs):
                ups = [dot(hidden(), ref[...]) for ref in refs]
                for u in range(many):
                    activate(ups[u], (many * j + u) * CHUNK, CHUNK)

            self.with_cols(col0 + d.n_o + many * j, many, body)

        tail = self.whole % many
        for u in range(tail):
            def body(refs, at=(self.whole - tail + u) * CHUNK):
                activate(dot(hidden(), refs[0][...]), at, CHUNK)

            self.with_cols(col0 + d.n_o + self.whole - tail + u, 1, body)
        for copy in self.half_start():
            copy.wait()
        activate(dot(hidden(), self.half_col[...]), self.whole * CHUNK, HALF)

        def acts(at, size):
            return jnp.concatenate([self.act[:, pl.ds(aligned(at, LANES), size)], self.act[:, pl.ds(aligned(at + offset, LANES), size)]], axis=0)

        def add(out):
            self.acc[...] += out[:rows]
            self.acc_other[...] += out[rows:]

        @pl.loop(0, self.whole // many)
        def _(j):
            def body(refs):
                add(sum(dot(acts((many * j + u) * CHUNK, CHUNK), refs[u][...]) for u in range(many)))

            self.with_rows(layer * d.n_u + many * j, many, body)

        for u in range(tail):
            def body(refs, at=(self.whole - tail + u) * CHUNK):
                add(dot(acts(at, CHUNK), refs[0][...]))

            self.with_rows(layer * d.n_u + self.whole - tail + u, 1, body)
        add(dot(acts(self.whole * CHUNK, HALF), self.half_row[...]))
        self.y_ref[...] = (self.acc[...] + swap_sums()).astype(BF16)


class Exchange:
    STEPS = 11

    def __init__(self, side, layer, work, core_buf, ring_buf, out, send_sem, recv_sem):
        self.layer = layer
        self.work, self.core_buf, self.ring_buf, self.out, self.send_sem, self.recv_sem = work, core_buf, ring_buf, out, send_sem, recv_sem
        me = lax.axis_index('kv')
        core, x, y = me % 2, me // 2 % side, me // (2 * side)

        def pairings(pos, stride):
            return (((pos + 1) // 2 % 2, me + (1 - 2 * (pos % 2)) * stride), (pos // 2, me + (side - 1 - 2 * pos) * stride))

        xs, ys = pairings(x, 2), pairings(y, 2 * side)
        self.orders = [xs + ys, xs[::-1] + ys[::-1], ys + xs, ys[::-1] + xs[::-1]]
        self.partner = me + 1 - 2 * core
        self.peers = [self.partner] + [dev for _, dev in xs + ys]
        self.half = work.shape[1] // 2
        self.stream = self.half // 4
        self.base, self.other = core * self.half, (1 - core) * self.half
        self.copies, self.done = [], 0
        self.path = [[self.base + k * self.stream for k in range(4)]]
        self.away = []
        for ring in range(4):
            size = self.stream >> (ring + 1)
            self.away.append([self.path[-1][k] + (1 - self.orders[k][ring][0]) * size for k in range(4)])
            self.path.append([self.path[-1][k] + self.orders[k][ring][0] * size for k in range(4)])

    def send(self, src, dst, step, lane, dev):
        def copy():
            return pltpu.make_async_remote_copy(src(), dst(), self.send_sem.at[self.layer, step, lane], self.recv_sem.at[self.layer, step, lane], device_id={'kv': dev})

        copy().start()
        self.copies.append(copy)

    def units(self, ref, at, count):
        return lambda: ref.at[self.layer].at[pl.ds(at, count)]

    def results(self, at, count):
        return lambda: self.out.at[pl.ds(at, count)]

    def add(self, dst_at, buf, src_at, count):
        @pl.loop(0, count)
        def _(u):
            self.work[self.layer, dst_at + u] = self.work[self.layer, dst_at + u] + buf[self.layer, src_at + u]

    def halve(self, ring, k):
        size = self.stream >> (ring + 1)
        src = self.units(self.work, self.away[ring][k], size)
        self.send(src, self.units(self.ring_buf, (k + 1) * self.stream - 2 * size, size), 1 + ring, k, self.orders[k][ring][1])

    def halved(self, ring, k):
        size = self.stream >> (ring + 1)
        self.add(self.path[ring + 1][k], self.ring_buf, (k + 1) * self.stream - 2 * size, size)

    def double(self, ring, k):
        at = self.results(self.path[ring + 1][k], self.stream >> (ring + 1))
        self.send(at, at, 8 - ring, k, self.orders[k][ring][1])

    def step(self):
        step, self.done = self.done, self.done + 1
        started, self.copies = self.copies, []
        if step in (1, 9, 10):
            for copy in started:
                copy().wait()
        if step == 0:
            self.send(self.units(self.work, self.other, self.half), self.units(self.core_buf, 0, self.half), 0, 0, self.partner)
        elif step == 1:
            self.add(self.base, self.core_buf, 0, self.half)
            for k in range(4):
                self.halve(0, k)
        elif step < 9:
            for k in range(4):
                started[k]().wait()
                if step < 6:
                    self.halved(step - 2, k)
                if step < 5:
                    self.halve(step - 1, k)
                    continue
                if step == 5:
                    for u in range(self.stream >> 4):
                        self.out[self.path[4][k] + u] = self.work[self.layer, self.path[4][k] + u]
                self.double(8 - step, k)
        elif step == 9:
            at = self.results(self.base, self.half)
            self.send(at, at, 9, 0, self.partner)


def adjacent_kernel(dims, side, group_size, entries, src_s, dst_s, table_hbm, lens_hbm, embeds_hbm, wq, wk, wv, wo, wu, wd, k_hbm, v_hbm,
                    ya_ref, yb_ref, info_s, last_out,
                    table_s, lens_s, table_v, embeds_v, y_ref, send_buf, got_buf, last_buf, new_buf, work, core_buf, ring_buf, mid_in, mid_out, x_in, plan_v, plan_s, y_other, acc_other, sums_in, half_col, half_row, *rest):
    d = dims
    migs, rest = rest[:d.layers], rest[d.layers:]
    pools, rest = [rest[2 * l:2 * l + 2] for l in range(d.layers)], rest[2 * d.layers:]
    compute, (load_sem, pool_sem, plan_sem, x_send, x_recv, page_send, page_recv, new_send, new_recv, mig_send, mig_recv, out_sem, half_sem, pair_send, pair_recv) = rest[:-15], rest[-15:]
    half = d.rows // 2
    me = lax.axis_index('kv')
    ahead, behind = lax.rem(me + 1, group_size), lax.rem(me + group_size - 1, group_size)
    dec = Decoder(d, 0, d.layers, (wq, wk, wv, wo, wu, wd), y_ref, compute, shared=True)
    dec.y_other, dec.acc_other, dec.half_col, dec.half_row, dec.half_sem = y_other, acc_other, half_col, half_row, half_sem
    exchanges = [Exchange(side, l, work, core_buf, ring_buf, migs[l], mig_send, mig_recv) for l in range(d.layers)]

    def scope(name, run, *args):
        with jax.named_scope(name):
            return run(*args)

    pool_loads = [[pltpu.make_async_copy(src.at[:, l], pools[l][p], pool_sem.at[l, p]) for p, src in enumerate((k_hbm, v_hbm))] for l in range(d.layers)]
    embeds_load, table_load, lens_load, table_load_v = [
        pltpu.make_async_copy(src, dst, load_sem.at[i]) for i, (src, dst) in enumerate(((embeds_hbm, embeds_v), (table_hbm, table_s), (lens_hbm, lens_s), (table_hbm, table_v)))]
    for load in [embeds_load] + pool_loads[0] + [table_load, table_load_v, lens_load]:
        load.start()
    barrier = pltpu.get_barrier_semaphore()

    @pl.loop(1, group_size)
    def _(r):
        pl.semaphore_signal(barrier, inc=1, device_id={'kv': lax.rem(me + r, group_size)})

    scope("barrier", lambda: pl.semaphore_wait(barrier, group_size - 1))

    groups = d.tokens // 8
    splits = group_size // groups
    cols = d.width // splits

    def piece(ref, m):
        return ref.at[m // splits, :, pl.ds(aligned(m % splits * cols, cols), cols)]

    def all_pieces(phase):
        some = mid_in.at[pl.ds(0, group_size - 1)]
        pltpu.make_async_remote_copy(some, some, x_send.at[phase], x_recv.at[phase], device_id={'kv': me}).wait()

    def send_embeddings():
        embeds_load.wait()

        @pl.loop(1, group_size)
        def _(r):
            m = lax.rem(me + r, group_size)
            pltpu.make_async_remote_copy(piece(embeds_v, m), mid_in.at[me], x_send.at[0], x_recv.at[0], device_id={'kv': m}).start()

        mid_in[me] = piece(embeds_v, me)[...]

    def load_tables():
        for load in (table_load, lens_load, table_load_v):
            load.wait()
        return lax.rem(table_s[1, 0] // d.slots + group_size, group_size)

    scope("pool_wait_0", lambda: [load.wait() for load in pool_loads[0]])

    def own(l):
        @pl.loop(0, entries)
        def _(e):
            slot = src_s[e] - me * d.slots
            mine = (slot >= 0) & (slot < d.slots)
            slot = local_slot(src_s[e], me, d.slots)
            for p in PAIR:
                page = pools[l][p][slot]
                work[l, p * entries + e] = jnp.where(mine, page, jnp.zeros_like(page))

    def step(l):
        scope(f"exchange_{l}_{exchanges[l].done}", exchanges[l].step)

    step_0, step_1 = functools.partial(step, 0), functools.partial(step, 1)

    scope("own_0", own, 0)
    step_0()
    for l in range(1, d.layers):
        for load in pool_loads[l]:
            load.start()
    scope("start_stream", dec.start_stream)
    for copy in dec.half_start():
        copy.start()
    shift = scope("load_tables", load_tables)
    home_a = lax.rem(me - shift + group_size, group_size)
    home_b = lax.rem(home_a + 1, group_size)

    def clipped(slot):
        return local_slot(slot, me, d.slots)

    def first_here(l, p, i):
        return pools[l][p][clipped(table_s[0, home_b * d.rows + i])]

    def last_here(l, p, i):
        return pools[l][p][clipped(table_s[1, home_a * d.rows + i])]

    def migrated(l, p, home, i, page):
        entry = plan_s[0, home * d.rows + i]
        return jnp.where(entry >= 0, migs[l][p * entries + jnp.maximum(entry, 0)], page)

    def pack(l):
        @pl.loop(0, half)
        def _(i):
            for p in PAIR:
                send_buf[l, 0, p, i] = first_here(l, p, i)
                send_buf[l, 1, p, i] = last_here(l, p, half + i)

    parts = 4
    size = half // parts

    def page_copy(l, way, p, rows):
        return pltpu.make_async_remote_copy(
            send_buf.at[l, way, p, rows], got_buf.at[l, way, p, rows], page_send.at[l, way, p], page_recv.at[l, way, p], device_id={'kv': (ahead, behind)[way]})

    pieces = [iter([(p, part) for part in range(parts) for p in PAIR]) for _ in range(d.layers)]

    def pages_start(l):
        p, part = next(pieces[l])
        for way in PAIR:
            page_copy(l, way, p, pl.ds(part * size, size)).start()

    pages_0, pages_1 = functools.partial(pages_start, 0), functools.partial(pages_start, 1)

    def pages_wait(l):
        for way in PAIR:
            for p in PAIR:
                page_copy(l, way, p, pl.ds(0, half)).wait()

    def pass_on():
        all_pieces(0)
        later = me // splits * 8 % d.rows // half

        @pl.loop(0, group_size)
        def _(m):
            mid_out[m] = mid_in[lax.rem(m - shift + later + group_size, group_size)]

        @pl.loop(1, group_size)
        def _(r):
            m = lax.rem(me + r, group_size)
            pltpu.make_async_remote_copy(mid_out.at[m], piece(x_in, me), x_send.at[1], x_recv.at[1], device_id={'kv': m}).start()

        piece(x_in, me)[...] = mid_out[me]

    def take_embeddings():
        all_pieces(1)
        y_ref[...] = x_in[...].reshape(d.tokens, d.width)

    plan_copy = pltpu.make_async_copy(plan_v, plan_s, plan_sem)

    def plan():
        seq = iota((1, table_v.shape[1]), 1)
        worker = lax.rem(seq // d.rows + shift, group_size)
        before = lax.rem(worker + group_size - 1, group_size)
        first, last = table_v[0:1, :], table_v[1:2, :]
        bad = (last < worker * d.slots) | (last >= worker * d.slots + d.slots) | (first < before * d.slots) | (first >= before * d.slots + d.slots)

        def entry(e, state):
            plan, bad = state
            return jnp.where(last == dst_s[e], e, plan), bad | (first == dst_s[e]).astype(jnp.int32)

        plan, bad = lax.fori_loop(0, entries, entry, (jnp.full_like(last, -1), bad.astype(jnp.int32)))
        plan_v[...] = plan
        plan_copy.start()
        info_s[0] = shift
        info_s[1] = 1 - jnp.max(bad)

    def new_copies(l):
        return [pltpu.make_async_remote_copy(
            ref.at[pl.ds(g * d.stride + t * d.rows + half, half)], new_buf.at[l, p, g, t], new_send.at[l, p, g, t], new_recv.at[l, p, g, t], device_id={'kv': ahead})
            for p, ref in enumerate((dec.kn_s, dec.vn_s)) for g in range(d.kv_heads) for t in PAIR]

    def project(l):
        dec.project(l)
        for copy in new_copies(l):
            copy.start()

    scope("pack_0", pack, 0)
    step_0()
    scope("send_embeddings", send_embeddings)
    pages_0()
    scope("plan", plan)
    step_0()
    pages_0()
    step_0()
    pages_0()
    scope("pass_on", pass_on)
    step_0()
    pages_0()
    for l in range(1, d.layers):
        for load in pool_loads[l]:
            load.wait()
    step_0()
    pages_0()
    scope("own_1", own, 1)
    step_0()
    pages_0()
    scope("pack_1", pack, 1)
    step_0()
    pages_0()
    scope("take_embeddings", take_embeddings)
    step_1()
    step_0()
    pages_0()
    scope("project_0", project, 0)
    step_1()
    step_0()
    plan_copy.wait()
    step_0()
    scope("pages_wait_0", pages_wait, 0)

    def attend(l, events_a, events_b):
        def put_page(p, i, val):
            last_buf[p, i] = val

        dec.attend(lambda i: lens_s[home_a * d.rows + i], lambda p, i: got_buf[l, 0, p, i],
                   lambda p, i: migrated(l, p, home_a, i, last_here(l, p, i)), put_page, events_a, 0, half)
        dec.attend(lambda i: lens_s[home_b * d.rows + i], lambda p, i: first_here(l, p, i),
                   lambda p, i: migrated(l, p, home_b, i, got_buf[l, 1, p, i - half]), lambda p, i, val: None, events_b, half, half)
        dec.gather_heads()

    def finish_pages(l):
        for copy in new_copies(l):
            copy.wait()

        @pl.loop(0, half)
        def _(i):
            row = half + i
            for p in PAIR:
                page = migrated(l, p, home_a, row, last_here(l, p, row))
                last_buf[p, row] = dec.insert(page, lens_s[home_a * d.rows + row], lambda t, g: new_buf[l, p, g, t, pl.ds(i, 1), :])

        pltpu.make_async_copy(last_buf, last_out.at[l], out_sem).start()

    def last_wait(l):
        pltpu.make_async_copy(last_buf, last_out.at[l], out_sem).wait()

    def event(run):
        return lambda: run()

    blocks = half // min(UNROLL, half)
    pairs = 2 * (d.n_u // 2)
    with jax.named_scope("attend_0"):
        attend(0, [(0, event(step_1))], [(0, event(step_1))])
    events = [((2 * k + 1) * pairs // (4 * parts), event(pages_1)) for k in range(2 * parts)]
    events += [(k * (pairs - 1) // 7, event(step_1)) for k in range(Exchange.STEPS - 4)]
    events += [(pairs - 1, functools.partial(scope, "finish_0", finish_pages, 0))]
    with jax.named_scope("mix_0"):
        dec.mix(0, sorted(events, key=lambda event: event[0]))
    def hidden_copy(at):
        return pltpu.make_async_remote_copy(y_ref.at[:, at], y_other.at[:, at], pair_send.at[0], pair_recv.at[0], device_id={'kv': exchanges[0].partner})

    def send_hidden(j):
        hidden_copy(pl.ds(aligned(j * dec.group * CHUNK, CHUNK), dec.group * CHUNK)).start()

    def wait_hidden():
        hidden_copy(pl.ds(0, d.width)).wait()

    def swap_sums():
        copy = pltpu.make_async_remote_copy(acc_other, sums_in, pair_send.at[1], pair_recv.at[1], device_id={'kv': exchanges[0].partner})
        copy.start()
        copy.wait()
        return sums_in[...]

    for l in range(1, d.layers):
        scope(f"project_{l}", project, l)
        scope(f"pages_wait_{l}", pages_wait, l)
        last_wait(l - 1)
        with jax.named_scope(f"attend_{l}"):
            attend(l, [], [])
        finish = [(1, functools.partial(finish_pages, l))]
        with jax.named_scope(f"mix_{l}"):
            if l == d.layers - 1:
                dec.mix_shared(l, send_hidden, wait_hidden, swap_sums, finish)
            else:
                dec.mix(l, finish)
    for t in PAIR:
        ya_ref[t] = y_ref[pl.ds(t * d.rows, half), :]
        yb_ref[t] = y_ref[pl.ds(t * d.rows + half, half), :]
    last_wait(d.layers - 1)


def decode_adjacent(side, group_size, d, table, seq_lens, mig_src, mig_dst, embeds, weights, k_pool, v_pool):
    entries = mig_src.shape[0]
    half = d.rows // 2
    page = (d.page_rows, d.head_dim)
    struct = lambda *shape: jax.ShapeDtypeStruct(shape, BF16)
    groups = d.tokens // 8
    mid = pltpu.VMEM((group_size, 8, d.width * groups // group_size), BF16)
    return pl.pallas_call(
        functools.partial(adjacent_kernel, d, side, group_size, entries),
        out_shape=[struct(2, half, d.width), struct(2, half, d.width), jax.ShapeDtypeStruct((2,), jnp.int32), struct(d.layers, 2, d.rows, *page)],
        in_specs=[SMEM] * 2 + [ANY] * 11,
        out_specs=[VMEM, VMEM, SMEM, ANY],
        scratch_shapes=[
            pltpu.SMEM(table.shape, jnp.int32),
            pltpu.SMEM(seq_lens.shape, jnp.int32),
            pltpu.VMEM(table.shape, jnp.int32),
            pltpu.VMEM((groups, 8, d.width), BF16),
            pltpu.VMEM((d.tokens, d.width), BF16),
        ] + [pltpu.VMEM((d.layers, 2, 2, half) + page, BF16)] * len(PAIR) + [
            pltpu.VMEM((2, d.rows) + page, BF16),
            pltpu.VMEM((d.layers, 2, d.kv_heads, 2, half, d.head_dim), F32),
            pltpu.VMEM((d.layers, 2 * entries) + page, BF16),
        ] + [pltpu.VMEM((d.layers, entries) + page, BF16)] * len(PAIR) + [
            mid,
            mid,
            pltpu.VMEM((groups, 8, d.width), BF16),
            pltpu.VMEM((1, table.shape[1]), jnp.int32),
            pltpu.SMEM((1, table.shape[1]), jnp.int32),
            pltpu.VMEM((d.tokens, d.width), BF16),
            pltpu.VMEM((d.tokens, d.width), F32),
            pltpu.VMEM((d.tokens, d.width), F32),
            pltpu.VMEM((d.width, HALF), BF16),
            pltpu.VMEM((HALF, d.width), BF16),
        ] + [pltpu.VMEM((2 * entries,) + page, BF16)] * d.layers + [pltpu.VMEM((d.slots,) + page, BF16)] * (2 * d.layers) + d.compute_scratch(8, 6) + [
            DMA((4,)),
            DMA((d.layers, 2)),
            DMA,
        ] + [DMA(shape) for shape in ((2,), (d.layers, 2, 2), (d.layers, 2, d.kv_heads, 2), (d.layers, 10, 4)) for _ in PAIR] + [DMA] + [DMA((2,))] * 3,
        compiler_params=pltpu.CompilerParams(collective_id=1, has_side_effects=True, skip_device_barrier=True, vmem_limit_bytes=LIMIT),
        cost_estimate=d.cost(d.layers),
        name="decode_adjacent",
    )(mig_src, mig_dst, table, seq_lens, embeds.reshape(groups, 8, d.width), *weights, k_pool, v_pool)


def fill_pools_kernel(dims, group_size, info_s, table_s, src_s, k_hbm, v_hbm, last_hbm, k_out, v_out, k_buf, v_buf, sem, put_sem):
    d = dims
    me = lax.axis_index('kv')
    home = lax.rem(me - info_s[0] + group_size, group_size)
    pools = ((k_hbm, k_buf, k_out), (v_hbm, v_buf, v_out))
    parts = sem.shape[1]
    size = d.slots // parts

    def moves(part, out):
        at = pl.ds(part * size, size)
        return [pltpu.make_async_copy(*((buf.at[at], dst.at[at]) if out else (src.at[at], buf.at[at])), sem.at[p, part]) for p, (src, buf, dst) in enumerate(pools)]

    def all_parts(out, run):
        @pl.loop(0, parts)
        def _(part):
            for copy in moves(part, out):
                run(copy)

    start, wait = lambda copy: copy.start(), lambda copy: copy.wait()
    all_parts(False, start)
    all_parts(False, wait)

    @pl.loop(0, d.rows)
    def _(i):
        slot = local_slot(table_s[1, home * d.rows + i], me, d.slots)
        for p, (_, buf, _) in enumerate(pools):
            pltpu.make_async_copy(last_hbm.at[:, p, i], buf.at[slot], put_sem).start()

    @pl.loop(0, src_s.shape[0])
    def _(e):
        slot = src_s[e] - me * d.slots

        @pl.when((slot >= 0) & (slot < d.slots))
        def _():
            for _, buf, _ in pools:
                buf[local_slot(src_s[e], me, d.slots)] = jnp.zeros(buf.shape[1:], buf.dtype)

    for src, buf, _ in pools:
        pltpu.make_async_copy(src.at[pl.ds(0, d.rows)], buf.at[pl.ds(0, d.rows)], put_sem).wait()
    all_parts(True, start)
    all_parts(True, wait)


def fill_pools(group_size, d, info, table, mig_src, k_pool, v_pool, last):
    return pl.pallas_call(
        functools.partial(fill_pools_kernel, d, group_size),
        out_shape=[jax.ShapeDtypeStruct(k_pool.shape, k_pool.dtype)] * 2,
        in_specs=[SMEM] * 3 + [ANY] * 3,
        out_specs=[ANY, ANY],
        scratch_shapes=[pltpu.VMEM(k_pool.shape, k_pool.dtype), pltpu.VMEM(k_pool.shape, k_pool.dtype), DMA((2, 4)), DMA],
        compiler_params=pltpu.CompilerParams(vmem_limit_bytes=LIMIT),
        cost_estimate=d.cost(1),
        name="fill_pools",
    )(info, table, mig_src, k_pool, v_pool, last)


def gather_pages_kernel(idx_ref, k_hbm, v_hbm, k_out, v_out, sem):
    rows = k_out.shape[0]

    def copies(i):
        slot = jnp.maximum(idx_ref[i], 0)
        return (pltpu.make_async_copy(k_hbm.at[slot], k_out.at[i], sem), pltpu.make_async_copy(v_hbm.at[slot], v_out.at[i], sem))

    @pl.loop(0, rows)
    def _(i):
        @pl.when(idx_ref[i] >= 0)
        def _():
            for copy in copies(i):
                copy.start()

        @pl.when(idx_ref[i] < 0)
        def _():
            k_out[i] = jnp.zeros(k_out.shape[1:], k_out.dtype)
            v_out[i] = jnp.zeros(v_out.shape[1:], v_out.dtype)

    @pl.loop(0, rows)
    def _(i):
        @pl.when(idx_ref[i] >= 0)
        def _():
            for copy in copies(i):
                copy.wait()


def gather_pages(idx, k_pool, v_pool):
    shape = jax.ShapeDtypeStruct((idx.shape[0],) + k_pool.shape[1:], k_pool.dtype)
    return pl.pallas_call(
        gather_pages_kernel,
        out_shape=[shape, shape],
        in_specs=[SMEM, ANY, ANY],
        out_specs=[VMEM, VMEM],
        scratch_shapes=[DMA],
        compiler_params=pltpu.CompilerParams(vmem_limit_bytes=LIMIT),
        name="gather_pages",
    )(idx, k_pool, v_pool)


def share_kernel(side, k_hbm, v_hbm, k_out, v_out, work, core_buf, ring_buf, load_sem, send_sem, recv_sem, result):
    entries = k_hbm.shape[0]
    exchange = Exchange(side, 0, work, core_buf, ring_buf, result, send_sem, recv_sem)
    units = [pl.ds(p * entries, entries) for p in PAIR]
    for p, src in enumerate((k_hbm, v_hbm)):
        pltpu.make_async_copy(src, work.at[0].at[units[p]], load_sem.at[p]).start()
    for p, src in enumerate((k_hbm, v_hbm)):
        pltpu.make_async_copy(src, work.at[0].at[units[p]], load_sem.at[p]).wait()
    for _ in range(Exchange.STEPS):
        exchange.step()
    for p, dst in enumerate((k_out, v_out)):
        pltpu.make_async_copy(result.at[units[p]], dst, load_sem.at[p]).start()
    for p, dst in enumerate((k_out, v_out)):
        pltpu.make_async_copy(result.at[units[p]], dst, load_sem.at[p]).wait()


def share(side, mig_k, mig_v):
    entries = mig_k.shape[0]
    page = mig_k.shape[1:]
    return pl.pallas_call(
        functools.partial(share_kernel, side),
        out_shape=[jax.ShapeDtypeStruct(mig_k.shape, BF16)] * 2,
        in_specs=[ANY, ANY],
        out_specs=[ANY, ANY],
        scratch_shapes=[pltpu.VMEM((1, n * entries) + page, BF16) for n in (2, 1, 1)] + [DMA((2,)), DMA((1, 10, 4)), DMA((1, 10, 4)), pltpu.VMEM((2 * entries,) + page, BF16)],
        compiler_params=pltpu.CompilerParams(has_side_effects=True, vmem_limit_bytes=LIMIT),
        name="share",
    )(mig_k, mig_v)


def migrate_kernel(dst_ref, src_ref, k_hbm, v_hbm, mk_hbm, mv_hbm, k_out, v_out, k_buf, v_buf, sem, fix_sem):
    entries = dst_ref.shape[0]
    pairs = ((k_hbm, mk_hbm, k_buf, k_out), (v_hbm, mv_hbm, v_buf, v_out))
    for p, (src, _, buf, _) in enumerate(pairs):
        pltpu.make_async_copy(src, buf, sem.at[p]).start()
    for p, (src, _, buf, _) in enumerate(pairs):
        pltpu.make_async_copy(src, buf, sem.at[p]).wait()

    @pl.loop(0, entries)
    def _(e):
        @pl.when(dst_ref[e] >= 0)
        def _():
            for _, mig, buf, _ in pairs:
                copy = pltpu.make_async_copy(mig.at[e], buf.at[jnp.maximum(dst_ref[e], 0)], fix_sem)
                copy.start()
                copy.wait()

        @pl.when(src_ref[e] >= 0)
        def _():
            for _, _, buf, _ in pairs:
                buf[jnp.maximum(src_ref[e], 0)] = jnp.zeros(buf.shape[1:], buf.dtype)

    for p, (_, _, buf, dst) in enumerate(pairs):
        pltpu.make_async_copy(buf, dst, sem.at[p]).start()
    for p, (_, _, buf, dst) in enumerate(pairs):
        pltpu.make_async_copy(buf, dst, sem.at[p]).wait()


def migrate(dst_local, src_local, k_pool, v_pool, mig_k, mig_v):
    shape = jax.ShapeDtypeStruct(k_pool.shape, k_pool.dtype)
    return pl.pallas_call(
        migrate_kernel,
        out_shape=[shape, shape],
        in_specs=[SMEM, SMEM, ANY, ANY, ANY, ANY],
        out_specs=[ANY, ANY],
        scratch_shapes=[pltpu.VMEM(k_pool.shape, k_pool.dtype), pltpu.VMEM(k_pool.shape, k_pool.dtype), DMA((2,)), DMA],
        compiler_params=pltpu.CompilerParams(vmem_limit_bytes=LIMIT),
        name="migrate",
    )(dst_local, src_local, k_pool, v_pool, mig_k, mig_v)


def decode_kernel(dims, sc_ref, x_ref, p0k_hbm, p0v_hbm, wq, wk, wv, wo, wu, wd, k_in, v_in, y_ref, k_out, v_out,
                  first_buf, last_buf, *rest):
    compute, (page_sem, put_sem) = rest[:-2], rest[-2:]
    d = dims
    dec = Decoder(d, 0, d.layers, (wq, wk, wv, wo, wu, wd), y_ref, compute, 1, 2)
    dec.start_stream()
    y_ref[...] = x_ref[...]
    loads = [pltpu.make_async_copy(src, first_buf.at[p], page_sem.at[p]) for p, src in enumerate((p0k_hbm, p0v_hbm))]
    for load in loads:
        load.start()

    def last_loads(run):
        @pl.loop(0, d.rows)
        def _(i):
            for p, src in enumerate((k_in, v_in)):
                run(pltpu.make_async_copy(src.at[sc_ref[0, i]], last_buf.at[p, i], page_sem.at[2]))

    def puts(run):
        @pl.loop(0, d.rows)
        def _(i):
            @pl.when(sc_ref[2, i] > 0)
            def _():
                for p, dst in enumerate((k_out, v_out)):
                    run(pltpu.make_async_copy(last_buf.at[p, i], dst.at[sc_ref[0, i]], put_sem))

    last_loads(lambda copy: copy.start())
    for load in loads:
        load.wait()
    last_loads(lambda copy: copy.wait())

    @pl.loop(0, d.layers)
    def _(layer):
        def put_page(p, i, val):
            last_buf[p, i, layer] = val

        dec.project(layer)
        dec.attend(lambda i: sc_ref[1, i], lambda p, i: first_buf[p, i, layer], lambda p, i: last_buf[p, i, layer], put_page)
        dec.gather_heads()
        dec.mix(layer)

    puts(lambda copy: copy.start())
    puts(lambda copy: copy.wait())


def decode(d, scalars, x, p0k, p0v, weights, k_pool, v_pool):
    pool = jax.ShapeDtypeStruct(k_pool.shape, k_pool.dtype)
    pages = pltpu.VMEM((2, d.rows, d.layers, d.page_rows, d.head_dim), BF16)
    return pl.pallas_call(
        functools.partial(decode_kernel, d),
        out_shape=[jax.ShapeDtypeStruct(x.shape, x.dtype), pool, pool],
        in_specs=[SMEM, VMEM] + [ANY] * 10,
        out_specs=[VMEM, ANY, ANY],
        input_output_aliases={10: 1, 11: 2},
        scratch_shapes=[pages, pages] + d.compute_scratch(16, 16) + [DMA((3,)), DMA],
        compiler_params=pltpu.CompilerParams(vmem_limit_bytes=LIMIT),
        cost_estimate=d.cost(d.layers),
        name="decode",
    )(scalars, x, p0k, p0v, *weights, k_pool, v_pool)


def permute(arrays, shift, group_size):
    if shift == group_size // 2:
        return permute(permute(arrays, shift // 2, group_size), shift // 2, group_size)
    perm = [(i, (i + shift) % group_size) for i in range(group_size)]
    return jax.tree.map(lambda a: lax.ppermute(a, 'kv', perm), arrays) if shift else arrays


def rotate_back(first, second, shift, group_size, beside):
    def branch(r):
        def run(args):
            parts = permute(args[0], -r % group_size, group_size), permute(args[1], (1 - r) % group_size, group_size)
            return jnp.concatenate(parts, axis=1), beside()

        return run

    return lax.switch(shift, [branch(r) for r in range(group_size)], (first, second))


def rotate(arrays, shift, group_size):
    stride = math.isqrt(2 * group_size)
    for count, move in ((shift // stride, stride), (shift % stride, 1)):
        arrays = lax.fori_loop(0, count, lambda _, a: permute(a, move, group_size), arrays)
    return arrays


def solution(mesh):
    group_size = mesh.shape['kv']
    side = math.isqrt(group_size // 2)
    pool_spec = P(('rep', 'kv'))
    tok_spec = P(None, ('rep', 'kv'), None)

    def device_fn(embeds, w_query, w_key, w_value, w_out, w_up, w_down, k_pool5, v_pool5, new_table, seq_lens, mig_src, mig_dst):
        me = lax.axis_index('kv')
        slots, layers, page, kv_heads, head_dim = k_pool5.shape
        rows, width = embeds.shape[1:]
        weights = (w_query, w_key, w_value, w_out, w_up, w_down)
        k_pool = k_pool5.reshape(slots, layers, page * kv_heads, head_dim)
        v_pool = v_pool5.reshape(slots, layers, page * kv_heads, head_dim)
        d = Dims(rows, weights, k_pool, page)
        ints = jnp.int32

        def local(ids):
            loc = ids - me * slots
            return jnp.where((loc >= 0) & (loc < slots), loc, -1)

        def take(vec, dev):
            return lax.dynamic_slice(vec, (dev * rows,), (rows,))

        def inside(ids):
            return local_slot(ids, me, slots)

        def general_path():
            first_new, last_new = new_table[:, 0], new_table[:, 1]
            moved = first_new[None, :] == mig_dst[:, None]
            first_old = jnp.where(jnp.any(moved, axis=0), jnp.sum(jnp.where(moved, mig_src[:, None], 0), axis=0), first_new)
            home = jnp.arange(first_new.shape[0], dtype=ints) // rows
            worker = last_new // slots
            shift_of = (worker - home + group_size) % group_size
            first_shift = (worker - first_old // slots + group_size) % group_size
            shift_ids = jnp.arange(group_size, dtype=ints)
            wanted = jnp.any(shift_of[None, :] == shift_ids[:, None], axis=1)
            mig_k, mig_v = gather_pages(local(mig_src), k_pool, v_pool)
            by_layer = tuple(m.swapaxes(0, 1) for m in (mig_k, mig_v))
            mig_k, mig_v = (m.swapaxes(0, 1) for m in lax.map(lambda pages: tuple(share(side, *pages)), by_layer))
            k_new, v_new = migrate(local(mig_dst), local(mig_src), k_pool, v_pool, mig_k, mig_v)

            def one_round(shift, y, k_new, v_new):
                src_home = (me - shift + group_size) % group_size
                x = rotate(embeds.reshape(2 * rows, width), shift, group_size)
                in_round = shift_of == shift
                wanted2 = jnp.any(in_round[None, :] & (first_shift[None, :] == shift_ids[:, None]), axis=1)

                def more(state):
                    left, pk, pv = state
                    shift2 = jnp.argmax(left).astype(ints)
                    dest_home = (me + shift2 - shift + group_size) % group_size
                    got = gather_pages(inside(take(first_old, dest_home)), k_pool, v_pool)
                    got_k, got_v = rotate(tuple(got), shift2, group_size)
                    mine = (take(first_shift, src_home) == shift2)[:, None, None, None]
                    return left & (shift_ids != shift2), jnp.where(mine, got_k, pk), jnp.where(mine, got_v, pv)

                zeros = jnp.zeros((rows,) + k_pool.shape[1:], k_pool.dtype)
                _, pk, pv = lax.while_loop(lambda state: jnp.any(state[0]), more, (wanted2, zeros, zeros))
                valid = take(shift_of, src_home) == shift
                scalars = jnp.stack([inside(take(last_new, src_home)), take(seq_lens, src_home), valid.astype(ints)])
                out, k_new, v_new = decode(d, scalars, x, pk, pv, weights, k_new, v_new)
                back = rotate(out, (group_size - shift) % group_size, group_size)
                mine = (take(shift_of, me) == shift)[None, :, None]
                return jnp.where(mine, back.reshape(embeds.shape), y), k_new, v_new

            def next_round(state):
                left, y, k_new, v_new = state
                shift = jnp.argmax(left).astype(ints)
                y, k_new, v_new = one_round(shift, y, k_new, v_new)
                return left & (shift_ids != shift), y, k_new, v_new

            _, y, k_new, v_new = lax.while_loop(lambda state: jnp.any(state[0]), next_round, (wanted, jnp.zeros_like(embeds), k_new, v_new))
            return y, k_new, v_new

        table = new_table.T
        ya, yb, info, last = decode_adjacent(side, group_size, d, table, seq_lens, mig_src, mig_dst, embeds, weights, k_pool, v_pool)
        y, (k_new, v_new) = rotate_back(ya, yb, info[0], group_size, lambda: fill_pools(group_size, d, info, table, mig_src, k_pool, v_pool, last))
        _, y, k_new, v_new = lax.while_loop(lambda state: state[0] == 0, lambda state: (jnp.ones_like(state[0]),) + general_path(), (info[1], y, k_new, v_new))
        return y, k_new.reshape(k_pool5.shape), v_new.reshape(v_pool5.shape)

    return jax.shard_map(device_fn, mesh=mesh, in_specs=(tok_spec, P(), P(), P(), P(), P(), P(), pool_spec, pool_spec, P('rep', None), P('rep'), P('rep'), P('rep')), out_specs=(tok_spec, pool_spec, pool_spec), check_vma=False)
```

```python
import functools
import math

import jax
import jax.numpy as jnp
from jax import lax
from jax.experimental import pallas as pl
from jax.experimental.pallas import tpu as pltpu
from jax.sharding import PartitionSpec as P

ANY = pl.BlockSpec(memory_space=pl.ANY)
SMEM = pl.BlockSpec(memory_space=pltpu.SMEM)
VMEM = pl.BlockSpec(memory_space=pltpu.VMEM)
DMA = pltpu.SemaphoreType.DMA
CHUNK = 256
UNROLL = 8
LANES = 128
HALF = CHUNK // 2
PAIR = (0, 1)
LIMIT = 63 << 20
F32, BF16 = jnp.float32, jnp.bfloat16


def iota(shape, axis):
    return lax.broadcasted_iota(jnp.int32, shape, axis)


def dot(a, b):
    return jnp.dot(a, b, preferred_element_type=F32)


def local_slot(ids, me, slots):
    return jnp.clip(ids - me * slots, 0, slots - 1)


def aligned(x, multiple):
    return x if isinstance(x, int) else pl.multiple_of(x, multiple)


class Dims:
    def __init__(self, rows, weights, k_pool, page):
        w_query, w_key, _, _, w_up, _ = weights
        self.layers, self.width, self.q_width = w_query.shape
        self.ff = w_up.shape[2]
        self.slots, _, self.page_rows, self.head_dim = k_pool.shape
        self.kv_heads = w_key.shape[2] // self.head_dim
        self.heads = self.q_width // self.head_dim
        self.page, self.rows = page, rows
        self.tokens = 2 * rows
        self.stride = self.tokens + 8
        self.n_q, self.n_o, self.n_u = self.q_width // CHUNK, self.width // CHUNK, self.ff // CHUNK

    def compute_scratch(self, n_col, n_row):
        return [
            pltpu.VMEM((n_col, self.width, CHUNK), BF16),
            pltpu.VMEM((n_row, CHUNK, self.width), BF16),
            pltpu.VMEM((self.heads * self.stride, self.head_dim), F32),
            pltpu.VMEM((self.kv_heads * self.stride, self.head_dim), F32),
            pltpu.VMEM((self.kv_heads * self.stride, self.head_dim), F32),
            pltpu.VMEM((self.heads * self.stride, self.head_dim), F32),
            pltpu.VMEM((self.tokens, self.q_width), BF16),
            pltpu.VMEM((self.tokens, self.ff), BF16),
            pltpu.VMEM((self.tokens, self.width), F32),
            DMA((n_col,)),
            DMA((n_row,)),
        ]

    def cost(self, layers):
        size = layers * self.width * (2 * self.q_width + 2 * self.kv_heads * self.head_dim + 2 * self.ff)
        return pl.CostEstimate(flops=2 * size * self.tokens, bytes_accessed=2 * size, transcendentals=0)


class Decoder:
    def __init__(self, dims, first, layers, weights, y_ref, scratch, group=2, unroll=UNROLL, shared=False):
        self.group, self.unroll, self.shared = group, unroll, shared
        self.d, self.first, self.layers, self.weights, self.y_ref = dims, first, layers, weights, y_ref
        (self.col_buf, self.row_buf, self.q_s, self.kn_s, self.vn_s, self.o_s, self.att, self.act, self.acc, self.col_sem, self.row_sem) = scratch
        self.n_col, self.n_row = self.col_buf.shape[0], self.row_buf.shape[0]
        self.zero = lax.axis_index('kv') * 0
        d = dims
        self.whole = d.ff // 2 // CHUNK if shared else d.n_u
        self.begin = lax.axis_index('kv') % 2 * (d.ff // 2) if shared else 0
        self.col_layer = d.n_q + 2 + d.n_o + self.whole
        cols = 2 * d.page * d.kv_heads
        col_pos = iota((2 * d.heads, cols), 1)
        row_pos = iota((2 * d.heads, cols), 0)
        same_head = (col_pos % d.kv_heads) == (row_pos % d.heads) // (d.heads // d.kv_heads)
        self.limit = jnp.where(same_head, col_pos // d.kv_heads - row_pos // d.heads, 4 * d.page)
        self.page_pos = iota((d.page_rows, d.head_dim), 0) // d.kv_heads
        self.tile_head = iota((8, d.head_dim), 0) % d.kv_heads

    def layer_of(self, g, per_layer):
        return sum((g >= per_layer * l).astype(jnp.int32) for l in range(1, self.layers))

    def col_start(self, g):
        d = self.d
        wq, wk, wv, wo, wu, _ = self.weights

        @pl.when(g < self.layers * self.col_layer)
        def _():
            layer = self.layer_of(g, self.col_layer)
            pos = g - layer * self.col_layer
            slot = g % self.n_col

            def go(src, c, begin=0):
                start = aligned(c * CHUNK + begin, LANES)
                pltpu.make_async_copy(src.at[self.first + layer].at[:, pl.ds(start, CHUNK)], self.col_buf.at[slot], self.col_sem.at[slot]).start()

            @pl.when(pos < d.n_q)
            def _():
                go(wq, pos)

            @pl.when(pos == d.n_q)
            def _():
                go(wk, 0)

            @pl.when(pos == d.n_q + 1)
            def _():
                go(wv, 0)

            @pl.when((pos >= d.n_q + 2) & (pos < d.n_q + 2 + d.n_o))
            def _():
                go(wo, pos - (d.n_q + 2))

            @pl.when(pos >= d.n_q + 2 + d.n_o)
            def _():
                go(wu, pos - (d.n_q + 2 + d.n_o), self.begin)

    def row_start(self, g):
        d = self.d
        wd = self.weights[5]

        @pl.when(g < self.layers * self.whole)
        def _():
            layer = self.layer_of(g, self.whole)
            slot = g % self.n_row
            start = aligned((g - layer * self.whole) * CHUNK + self.begin, LANES)
            pltpu.make_async_copy(wd.at[self.first + layer].at[pl.ds(start, CHUNK)], self.row_buf.at[slot], self.row_sem.at[slot]).start()

    def start_stream(self):
        @pl.loop(0, self.n_col)
        def _(g):
            self.col_start(g)

        @pl.loop(0, self.n_row)
        def _(g):
            self.row_start(g)

    def with_cols(self, g, count, body):
        slots = [(g + u) % self.n_col for u in range(count)]
        for slot in slots:
            pltpu.make_async_copy(self.weights[1].at[0], self.col_buf.at[slot], self.col_sem.at[slot]).wait()
        body([self.col_buf.at[slot] for slot in slots])
        for u in range(count):
            self.col_start(g + u + self.n_col)

    def with_rows(self, g, count, body):
        slots = [(g + u) % self.n_row for u in range(count)]
        for slot in slots:
            pltpu.make_async_copy(self.weights[5].at[0, pl.ds(0, CHUNK), :], self.row_buf.at[slot], self.row_sem.at[slot]).wait()
        body([self.row_buf.at[slot] for slot in slots])
        for u in range(count):
            self.row_start(g + u + self.n_row)

    def project(self, layer):
        d = self.d
        col0 = (self.zero + layer) * self.col_layer

        def product(ref):
            return dot(self.y_ref[...], ref[...]).astype(BF16).astype(F32)

        def put(dst, first, out):
            for h in range(CHUNK // d.head_dim):
                at = aligned((first + h) * d.stride, 8)
                dst[pl.ds(at, d.tokens), :] = out[:, h * d.head_dim:(h + 1) * d.head_dim]

        many = self.group

        @pl.loop(0, d.n_q // many)
        def _(j):
            def body(refs):
                outs = [product(ref) for ref in refs]
                for u in range(many):
                    put(self.q_s, (many * j + u) * (CHUNK // d.head_dim), outs[u])

            self.with_cols(col0 + many * j, many, body)

        def body(refs):
            outs = [product(ref) for ref in refs]
            put(self.kn_s, 0, outs[0])
            put(self.vn_s, 0, outs[1])

        self.with_cols(col0 + d.n_q, 2, body)

    def insert(self, page, n, row):
        d = self.d
        val = page.astype(F32)
        for t in PAIR:
            new = jnp.broadcast_to(row(t, 0), (8, d.head_dim))
            for g in range(1, d.kv_heads):
                new = jnp.where(self.tile_head == g, row(t, g), new)
            val = jnp.where(self.page_pos == n - d.page + t, jnp.concatenate([new] * (d.page_rows // 8), axis=0), val)
        return val.astype(BF16)

    def attend(self, lens, first_page, last_page, put_page, events=(), begin=0, count=None):
        d = self.d
        count = count or d.rows
        unroll = min(self.unroll, count)

        def some(first):
            ids = [first + u for u in range(unroll)]
            scores, vals = [], []
            for i in ids:
                n = lens(i)

                def updated(p, new_ref):
                    val = self.insert(last_page(p, i), n, lambda t, g: new_ref[pl.ds(g * d.stride + t * d.rows + i, 1), :])
                    put_page(p, i, val)
                    return val

                keys = jnp.concatenate([first_page(0, i), updated(0, self.kn_s)], axis=0)
                vals.append(updated(1, self.vn_s))
                qs = jnp.concatenate([self.q_s[pl.ds(t * d.rows + i, d.heads, stride=d.stride), :] for t in PAIR], axis=0)
                score = lax.dot_general(qs.astype(BF16), keys, (((1,), (1,)), ((), ())), preferred_element_type=F32) * d.head_dim ** -0.5
                scores.append(jnp.where(self.limit <= n, score, -jnp.inf))
            tops = [jnp.max(score, axis=1, keepdims=True) for score in scores]
            probs = [jnp.exp(score - top) for score, top in zip(scores, tops)]
            totals = [jnp.sum(prob, axis=1, keepdims=True) for prob in probs]
            for u, i in enumerate(ids):
                both = jnp.concatenate([first_page(1, i), vals[u]], axis=0)
                out = dot(probs[u].astype(BF16), both) / totals[u]
                for t in PAIR:
                    self.o_s[pl.ds(t * d.rows + i, d.heads, stride=d.stride), :] = out[t * d.heads:(t + 1) * d.heads]

        @pl.loop(0, count // unroll)
        def _(block):
            for k, run in events:
                pl.when(block == k)(run)
            some(begin + block * unroll)

    def gather_heads(self):
        d = self.d
        for h in range(d.heads):
            self.att[:, h * d.head_dim:(h + 1) * d.head_dim] = self.o_s[h * d.stride:h * d.stride + d.tokens, :].astype(BF16)

    def span(self, j):
        return pl.ds(aligned(j * CHUNK, CHUNK), CHUNK)

    def out_project(self, layer, after=None):
        d, many = self.d, self.group

        @pl.loop(0, d.n_o // many)
        def _(j):
            def body(refs):
                outs = [dot(self.att[...], ref[...]) for ref in refs]
                for u in range(many):
                    at = self.span(many * j + u)
                    self.y_ref[:, at] = (self.y_ref[:, at].astype(F32) + outs[u]).astype(BF16)

            self.with_cols(layer * self.col_layer + d.n_q + len(PAIR) + many * j, many, body)
            if after:
                after(j)

    def mix(self, layer, events=()):
        d = self.d
        layer = self.zero + layer
        col0 = layer * self.col_layer + d.n_q + 2
        many = self.group
        pairs = d.n_u // many

        def between(j, first):
            for k, run in events:
                if first <= k < first + pairs:
                    pl.when(j == k - first)(run)

        self.out_project(layer)

        def up(first, count):
            def body(refs):
                ups = [dot(self.y_ref[...], ref[...]) for ref in refs]
                for u in range(count):
                    self.act[:, self.span(first + u)] = jax.nn.gelu(ups[u].astype(BF16).astype(F32), approximate=True).astype(BF16)

            self.with_cols(col0 + d.n_o + first, count, body)

        def down(first, count):
            def body(refs):
                out = self.acc[...]
                for u in range(count):
                    out += dot(self.act[:, self.span(first + u)], refs[u][...])
                self.acc[...] = out

            self.with_rows(layer * self.whole + first, count, body)

        @pl.loop(0, pairs)
        def _(j):
            between(j, 0)
            up(many * j, many)

        if d.n_u % many:
            up(d.n_u - 1, 1)

        self.acc[...] = self.y_ref[...].astype(F32)

        @pl.loop(0, pairs)
        def _(j):
            between(j, pairs)
            down(many * j, many)

        if d.n_u % many:
            down(d.n_u - 1, 1)

        self.y_ref[...] = self.acc[...].astype(BF16)


    def half_loads(self, layer):
        at = pl.ds(aligned(self.begin + self.whole * CHUNK, LANES), HALF)
        return (pltpu.make_async_copy(self.weights[4].at[layer].at[:, at], self.half_col, self.half_sem.at[0]),
                pltpu.make_async_copy(self.weights[5].at[layer].at[at], self.half_row, self.half_sem.at[1]))

    def mix_shared(self, layer, send_hidden, wait_hidden, swap_sums, events=()):
        d = self.d
        half_loads, next_loads = self.half_loads(layer), self.half_loads(layer + 1) if layer + 1 < d.layers else ()
        layer = self.zero + layer
        col0 = layer * self.col_layer + d.n_q + 2
        many = self.group
        rows = d.tokens
        offset = d.ff // 2
        pairs = self.whole // many

        def between(j, first):
            for k, run in events:
                if first <= k < first + pairs:
                    pl.when(j == k - first)(run)

        self.out_project(layer, send_hidden)

        self.acc[...] = self.y_ref[...].astype(F32)
        self.acc_other[...] = jnp.zeros_like(self.acc_other)
        wait_hidden()

        def hidden():
            return jnp.concatenate([self.y_ref[...], self.y_other[...]], axis=0)

        def activate(up, at, size):
            val = jax.nn.gelu(up.astype(BF16).astype(F32), approximate=True).astype(BF16)
            self.act[:, pl.ds(aligned(at, LANES), size)] = val[:rows]
            self.act[:, pl.ds(aligned(at + offset, LANES), size)] = val[rows:]

        @pl.loop(0, pairs)
        def _(j):
            between(j, 0)

            def body(refs):
                ups = [dot(hidden(), ref[...]) for ref in refs]
                for u in range(many):
                    activate(ups[u], (many * j + u) * CHUNK, CHUNK)

            self.with_cols(col0 + d.n_o + many * j, many, body)

        tail = self.whole % many
        for u in range(tail):
            def body(refs, at=(self.whole - tail + u) * CHUNK):
                activate(dot(hidden(), refs[0][...]), at, CHUNK)

            self.with_cols(col0 + d.n_o + self.whole - tail + u, 1, body)
        for copy in half_loads:
            copy.wait()
        activate(dot(hidden(), self.half_col[...]), self.whole * CHUNK, HALF)

        def acts(at, size):
            return jnp.concatenate([self.act[:, pl.ds(aligned(at, LANES), size)], self.act[:, pl.ds(aligned(at + offset, LANES), size)]], axis=0)

        def add(out):
            self.acc[...] += out[:rows]
            self.acc_other[...] += out[rows:]

        @pl.loop(0, pairs)
        def _(j):
            between(j, pairs)

            def body(refs):
                add(sum(dot(acts((many * j + u) * CHUNK, CHUNK), refs[u][...]) for u in range(many)))

            self.with_rows(layer * self.whole + many * j, many, body)

        for u in range(tail):
            def body(refs, at=(self.whole - tail + u) * CHUNK):
                add(dot(acts(at, CHUNK), refs[0][...]))

            self.with_rows(layer * self.whole + self.whole - tail + u, 1, body)
        add(dot(acts(self.whole * CHUNK, HALF), self.half_row[...]))
        for copy in next_loads:
            copy.start()
        self.y_ref[...] = (self.acc[...] + swap_sums()).astype(BF16)


class Exchange:
    STEPS = 11

    def __init__(self, side, layer, work, core_buf, ring_buf, out, send_sem, recv_sem):
        self.layer = layer
        self.work, self.core_buf, self.ring_buf, self.out, self.send_sem, self.recv_sem = work, core_buf, ring_buf, out, send_sem, recv_sem
        me = lax.axis_index('kv')
        core, x, y = me % 2, me // 2 % side, me // (2 * side)

        def pairings(pos, stride):
            return (((pos + 1) // 2 % 2, me + (1 - 2 * (pos % 2)) * stride), (pos // 2, me + (side - 1 - 2 * pos) * stride))

        xs, ys = pairings(x, 2), pairings(y, 2 * side)
        self.orders = [xs + ys, xs[::-1] + ys[::-1], ys + xs, ys[::-1] + xs[::-1]]
        self.partner = me + 1 - 2 * core
        self.peers = [self.partner] + [dev for _, dev in xs + ys]
        self.half = work.shape[1] // 2
        self.stream = self.half // 4
        self.base, self.other = core * self.half, (1 - core) * self.half
        self.copies, self.done = [], 0
        self.path = [[self.base + k * self.stream for k in range(4)]]
        self.away = []
        for ring in range(4):
            size = self.stream >> (ring + 1)
            self.away.append([self.path[-1][k] + (1 - self.orders[k][ring][0]) * size for k in range(4)])
            self.path.append([self.path[-1][k] + self.orders[k][ring][0] * size for k in range(4)])

    def send(self, src, dst, step, lane, dev):
        def copy():
            return pltpu.make_async_remote_copy(src(), dst(), self.send_sem.at[self.layer, step, lane], self.recv_sem.at[self.layer, step, lane], device_id={'kv': dev})

        copy().start()
        self.copies.append(copy)

    def units(self, ref, at, count):
        return lambda: ref.at[self.layer].at[pl.ds(at, count)]

    def results(self, at, count):
        return lambda: self.out.at[pl.ds(at, count)]

    def add(self, dst_at, buf, src_at, count):
        @pl.loop(0, count)
        def _(u):
            self.work[self.layer, dst_at + u] = self.work[self.layer, dst_at + u] + buf[self.layer, src_at + u]

    def halve(self, ring, k):
        size = self.stream >> (ring + 1)
        src = self.units(self.work, self.away[ring][k], size)
        self.send(src, self.units(self.ring_buf, (k + 1) * self.stream - 2 * size, size), 1 + ring, k, self.orders[k][ring][1])

    def halved(self, ring, k):
        size = self.stream >> (ring + 1)
        self.add(self.path[ring + 1][k], self.ring_buf, (k + 1) * self.stream - 2 * size, size)

    def double(self, ring, k):
        at = self.results(self.path[ring + 1][k], self.stream >> (ring + 1))
        self.send(at, at, 8 - ring, k, self.orders[k][ring][1])

    def step(self):
        step, self.done = self.done, self.done + 1
        started, self.copies = self.copies, []
        if step in (1, 9, 10):
            for copy in started:
                copy().wait()
        if step == 0:
            self.send(self.units(self.work, self.other, self.half), self.units(self.core_buf, 0, self.half), 0, 0, self.partner)
        elif step == 1:
            self.add(self.base, self.core_buf, 0, self.half)
            for k in range(4):
                self.halve(0, k)
        elif step < 9:
            for k in range(4):
                started[k]().wait()
                if step < 6:
                    self.halved(step - 2, k)
                if step < 5:
                    self.halve(step - 1, k)
                    continue
                if step == 5:
                    for u in range(self.stream >> 4):
                        self.out[self.path[4][k] + u] = self.work[self.layer, self.path[4][k] + u]
                self.double(8 - step, k)
        elif step == 9:
            at = self.results(self.base, self.half)
            self.send(at, at, 9, 0, self.partner)


def adjacent_kernel(dims, side, group_size, entries, src_s, dst_s, table_hbm, lens_hbm, embeds_hbm, wq, wk, wv, wo, wu, wd, k_hbm, v_hbm,
                    ya_ref, yb_ref, info_s, last_out,
                    table_s, lens_s, table_v, embeds_v, y_ref, send_buf, got_buf, last_buf, new_buf, work, core_buf, ring_buf, mid_in, mid_out, x_in, plan_v, plan_s, y_other, acc_other, sums_in, half_col, half_row, *rest):
    d = dims
    migs, rest = rest[:d.layers], rest[d.layers:]
    pools, rest = [rest[2 * l:2 * l + 2] for l in range(d.layers)], rest[2 * d.layers:]
    compute, (load_sem, pool_sem, plan_sem, x_send, x_recv, page_send, page_recv, new_send, new_recv, mig_send, mig_recv, out_sem, half_sem, pair_send, pair_recv) = rest[:-15], rest[-15:]
    half = d.rows // 2
    me = lax.axis_index('kv')
    ahead, behind = lax.rem(me + 1, group_size), lax.rem(me + group_size - 1, group_size)
    dec = Decoder(d, 0, d.layers, (wq, wk, wv, wo, wu, wd), y_ref, compute, shared=True)
    dec.y_other, dec.acc_other, dec.half_col, dec.half_row, dec.half_sem = y_other, acc_other, half_col, half_row, half_sem
    exchanges = [Exchange(side, l, work, core_buf, ring_buf, migs[l], mig_send, mig_recv) for l in range(d.layers)]

    def scope(name, run, *args):
        with jax.named_scope(name):
            return run(*args)

    pool_loads = [[pltpu.make_async_copy(src.at[:, l], pools[l][p], pool_sem.at[l, p]) for p, src in enumerate((k_hbm, v_hbm))] for l in range(d.layers)]
    embeds_load, table_load, lens_load, table_load_v = [
        pltpu.make_async_copy(src, dst, load_sem.at[i]) for i, (src, dst) in enumerate(((embeds_hbm, embeds_v), (table_hbm, table_s), (lens_hbm, lens_s), (table_hbm, table_v)))]
    for load in [embeds_load] + pool_loads[0] + [table_load, table_load_v, lens_load]:
        load.start()
    barrier = pltpu.get_barrier_semaphore()

    @pl.loop(1, group_size)
    def _(r):
        pl.semaphore_signal(barrier, inc=1, device_id={'kv': lax.rem(me + r, group_size)})

    scope("barrier", lambda: pl.semaphore_wait(barrier, group_size - 1))

    groups = d.tokens // 8
    splits = group_size // groups
    cols = d.width // splits

    def piece(ref, m):
        return ref.at[m // splits, :, pl.ds(aligned(m % splits * cols, cols), cols)]

    def all_pieces(phase):
        some = mid_in.at[pl.ds(0, group_size - 1)]
        pltpu.make_async_remote_copy(some, some, x_send.at[phase], x_recv.at[phase], device_id={'kv': me}).wait()

    def send_embeddings():
        embeds_load.wait()

        @pl.loop(1, group_size)
        def _(r):
            m = lax.rem(me + r, group_size)
            pltpu.make_async_remote_copy(piece(embeds_v, m), mid_in.at[me], x_send.at[0], x_recv.at[0], device_id={'kv': m}).start()

        mid_in[me] = piece(embeds_v, me)[...]

    def load_tables():
        for load in (table_load, lens_load, table_load_v):
            load.wait()
        return lax.rem(table_s[1, 0] // d.slots + group_size, group_size)

    scope("pool_wait_0", lambda: [load.wait() for load in pool_loads[0]])

    def own(l):
        @pl.loop(0, entries)
        def _(e):
            slot = src_s[e] - me * d.slots
            mine = (slot >= 0) & (slot < d.slots)
            slot = local_slot(src_s[e], me, d.slots)
            for p in PAIR:
                page = pools[l][p][slot]
                work[l, p * entries + e] = jnp.where(mine, page, jnp.zeros_like(page))

    def step(l):
        scope(f"exchange_{l}_{exchanges[l].done}", exchanges[l].step)

    step_0, step_1 = functools.partial(step, 0), functools.partial(step, 1)

    scope("own_0", own, 0)
    step_0()
    for l in range(1, d.layers):
        for load in pool_loads[l]:
            load.start()
    scope("start_stream", dec.start_stream)
    for copy in dec.half_loads(0):
        copy.start()
    shift = scope("load_tables", load_tables)
    home_a = lax.rem(me - shift + group_size, group_size)
    home_b = lax.rem(home_a + 1, group_size)

    def clipped(slot):
        return local_slot(slot, me, d.slots)

    def first_here(l, p, i):
        return pools[l][p][clipped(table_s[0, home_b * d.rows + i])]

    def last_here(l, p, i):
        return pools[l][p][clipped(table_s[1, home_a * d.rows + i])]

    def migrated(l, p, home, i, page):
        entry = plan_s[0, home * d.rows + i]
        return jnp.where(entry >= 0, migs[l][p * entries + jnp.maximum(entry, 0)], page)

    def pack(l):
        @pl.loop(0, half)
        def _(i):
            for p in PAIR:
                send_buf[l, 0, p, i] = first_here(l, p, i)
                send_buf[l, 1, p, i] = last_here(l, p, half + i)

    parts = 4
    size = half // parts

    def page_copy(l, way, p, rows):
        return pltpu.make_async_remote_copy(
            send_buf.at[l, way, p, rows], got_buf.at[l, way, p, rows], page_send.at[l, way, p], page_recv.at[l, way, p], device_id={'kv': (ahead, behind)[way]})

    pieces = [iter([(p, part) for part in range(parts) for p in PAIR]) for _ in range(d.layers)]

    def pages_start(l):
        p, part = next(pieces[l])
        for way in PAIR:
            page_copy(l, way, p, pl.ds(part * size, size)).start()

    pages_0, pages_1 = functools.partial(pages_start, 0), functools.partial(pages_start, 1)

    def pages_wait(l):
        for way in PAIR:
            for p in PAIR:
                page_copy(l, way, p, pl.ds(0, half)).wait()

    def pass_on():
        all_pieces(0)
        later = me // splits * 8 % d.rows // half

        @pl.loop(0, group_size)
        def _(m):
            mid_out[m] = mid_in[lax.rem(m - shift + later + group_size, group_size)]

        @pl.loop(1, group_size)
        def _(r):
            m = lax.rem(me + r, group_size)
            pltpu.make_async_remote_copy(mid_out.at[m], piece(x_in, me), x_send.at[1], x_recv.at[1], device_id={'kv': m}).start()

        piece(x_in, me)[...] = mid_out[me]

    def take_embeddings():
        all_pieces(1)
        y_ref[...] = x_in[...].reshape(d.tokens, d.width)

    plan_copy = pltpu.make_async_copy(plan_v, plan_s, plan_sem)

    def plan():
        seq = iota((1, table_v.shape[1]), 1)
        worker = lax.rem(seq // d.rows + shift, group_size)
        before = lax.rem(worker + group_size - 1, group_size)
        first, last = table_v[0:1, :], table_v[1:2, :]
        bad = (last < worker * d.slots) | (last >= worker * d.slots + d.slots) | (first < before * d.slots) | (first >= before * d.slots + d.slots)

        def entry(e, state):
            plan, bad = state
            return jnp.where(last == dst_s[e], e, plan), bad | (first == dst_s[e]).astype(jnp.int32)

        plan, bad = lax.fori_loop(0, entries, entry, (jnp.full_like(last, -1), bad.astype(jnp.int32)))
        plan_v[...] = plan
        plan_copy.start()
        info_s[0] = shift
        info_s[1] = 1 - jnp.max(bad)

    def new_copies(l):
        return [pltpu.make_async_remote_copy(
            ref.at[pl.ds(g * d.stride + t * d.rows + half, half)], new_buf.at[l, p, g, t], new_send.at[l, p, g, t], new_recv.at[l, p, g, t], device_id={'kv': ahead})
            for p, ref in enumerate((dec.kn_s, dec.vn_s)) for g in range(d.kv_heads) for t in PAIR]

    def project(l):
        dec.project(l)
        for copy in new_copies(l):
            copy.start()

    scope("pack_0", pack, 0)
    step_0()
    scope("send_embeddings", send_embeddings)
    pages_0()
    scope("plan", plan)
    step_0()
    pages_0()
    step_0()
    pages_0()
    scope("pass_on", pass_on)
    step_0()
    pages_0()
    for l in range(1, d.layers):
        for load in pool_loads[l]:
            load.wait()
    step_0()
    pages_0()
    scope("own_1", own, 1)
    step_0()
    pages_0()
    scope("pack_1", pack, 1)
    step_0()
    pages_0()
    scope("take_embeddings", take_embeddings)
    step_1()
    step_0()
    pages_0()
    scope("project_0", project, 0)
    step_1()
    step_0()
    plan_copy.wait()
    step_1()
    step_0()
    scope("pages_wait_0", pages_wait, 0)

    def attend(l, events_a, events_b):
        def put_page(p, i, val):
            last_buf[p, i] = val

        dec.attend(lambda i: lens_s[home_a * d.rows + i], lambda p, i: got_buf[l, 0, p, i],
                   lambda p, i: migrated(l, p, home_a, i, last_here(l, p, i)), put_page, events_a, 0, half)
        dec.attend(lambda i: lens_s[home_b * d.rows + i], lambda p, i: first_here(l, p, i),
                   lambda p, i: migrated(l, p, home_b, i, got_buf[l, 1, p, i - half]), lambda p, i, val: None, events_b, half, half)
        dec.gather_heads()

    def finish_pages(l):
        for copy in new_copies(l):
            copy.wait()

        @pl.loop(0, half)
        def _(i):
            row = half + i
            for p in PAIR:
                page = migrated(l, p, home_a, row, last_here(l, p, row))
                last_buf[p, row] = dec.insert(page, lens_s[home_a * d.rows + row], lambda t, g: new_buf[l, p, g, t, pl.ds(i, 1), :])

        pltpu.make_async_copy(last_buf, last_out.at[l], out_sem).start()

    def last_wait(l):
        pltpu.make_async_copy(last_buf, last_out.at[l], out_sem).wait()

    def event(run):
        return lambda: run()

    def hidden_copy(at):
        return pltpu.make_async_remote_copy(y_ref.at[:, at], y_other.at[:, at], pair_send.at[0], pair_recv.at[0], device_id={'kv': exchanges[0].partner})

    def send_hidden(j):
        hidden_copy(pl.ds(aligned(j * dec.group * CHUNK, CHUNK), dec.group * CHUNK)).start()

    def wait_hidden():
        hidden_copy(pl.ds(0, d.width)).wait()

    def swap_sums():
        copy = pltpu.make_async_remote_copy(acc_other, sums_in, pair_send.at[1], pair_recv.at[1], device_id={'kv': exchanges[0].partner})
        copy.start()
        copy.wait()
        return sums_in[...]

    blocks = half // min(UNROLL, half)
    last_pair = 2 * (dec.whole // dec.group) - 1
    for l in range(d.layers):
        between_a, between_b, events = (), (), []
        if l:
            scope(f"project_{l}", project, l)
            scope(f"pages_wait_{l}", pages_wait, l)
            last_wait(l - 1)
        else:
            between_a, between_b = [(0, event(step_1)), (blocks // 2, event(pages_1))], [(blocks // 2, event(pages_1))]
            events = [(k * last_pair // 7, event(pages_1)) for k in range(2 * parts - 2)]
            events += [(k * last_pair // 6, event(step_1)) for k in range(Exchange.STEPS - 4)]
        with jax.named_scope(f"attend_{l}"):
            attend(l, between_a, between_b)
        events += [(last_pair, functools.partial(scope, f"finish_{l}", finish_pages, l))]
        with jax.named_scope(f"mix_{l}"):
            dec.mix_shared(l, send_hidden, wait_hidden, swap_sums, sorted(events, key=lambda event: event[0]))
    for t in PAIR:
        ya_ref[t] = y_ref[pl.ds(t * d.rows, half), :]
        yb_ref[t] = y_ref[pl.ds(t * d.rows + half, half), :]
    last_wait(d.layers - 1)


def decode_adjacent(side, group_size, d, table, seq_lens, mig_src, mig_dst, embeds, weights, k_pool, v_pool):
    entries = mig_src.shape[0]
    half = d.rows // 2
    page = (d.page_rows, d.head_dim)
    struct = lambda *shape: jax.ShapeDtypeStruct(shape, BF16)
    groups = d.tokens // 8
    mid = pltpu.VMEM((group_size, 8, d.width * groups // group_size), BF16)
    return pl.pallas_call(
        functools.partial(adjacent_kernel, d, side, group_size, entries),
        out_shape=[struct(2, half, d.width), struct(2, half, d.width), jax.ShapeDtypeStruct((2,), jnp.int32), struct(d.layers, 2, d.rows, *page)],
        in_specs=[SMEM] * 2 + [ANY] * 11,
        out_specs=[VMEM, VMEM, SMEM, ANY],
        scratch_shapes=[
            pltpu.SMEM(table.shape, jnp.int32),
            pltpu.SMEM(seq_lens.shape, jnp.int32),
            pltpu.VMEM(table.shape, jnp.int32),
            pltpu.VMEM((groups, 8, d.width), BF16),
            pltpu.VMEM((d.tokens, d.width), BF16),
        ] + [pltpu.VMEM((d.layers, 2, 2, half) + page, BF16)] * len(PAIR) + [
            pltpu.VMEM((2, d.rows) + page, BF16),
            pltpu.VMEM((d.layers, 2, d.kv_heads, 2, half, d.head_dim), F32),
            pltpu.VMEM((d.layers, 2 * entries) + page, BF16),
        ] + [pltpu.VMEM((d.layers, entries) + page, BF16)] * len(PAIR) + [
            mid,
            mid,
            pltpu.VMEM((groups, 8, d.width), BF16),
            pltpu.VMEM((1, table.shape[1]), jnp.int32),
            pltpu.SMEM((1, table.shape[1]), jnp.int32),
            pltpu.VMEM((d.tokens, d.width), BF16),
            pltpu.VMEM((d.tokens, d.width), F32),
            pltpu.VMEM((d.tokens, d.width), F32),
            pltpu.VMEM((d.width, HALF), BF16),
            pltpu.VMEM((HALF, d.width), BF16),
        ] + [pltpu.VMEM((2 * entries,) + page, BF16)] * d.layers + [pltpu.VMEM((d.slots,) + page, BF16)] * (2 * d.layers) + d.compute_scratch(8, 6) + [
            DMA((4,)),
            DMA((d.layers, 2)),
            DMA,
        ] + [DMA(shape) for shape in ((2,), (d.layers, 2, 2), (d.layers, 2, d.kv_heads, 2), (d.layers, 10, 4)) for _ in PAIR] + [DMA] + [DMA((2,))] * 3,
        compiler_params=pltpu.CompilerParams(collective_id=1, has_side_effects=True, skip_device_barrier=True, vmem_limit_bytes=LIMIT),
        cost_estimate=d.cost(d.layers),
        name="decode_adjacent",
    )(mig_src, mig_dst, table, seq_lens, embeds.reshape(groups, 8, d.width), *weights, k_pool, v_pool)


def fill_pools_kernel(dims, group_size, info_s, table_s, src_s, k_hbm, v_hbm, last_hbm, k_out, v_out, k_buf, v_buf, last, zero, sem, last_sem, put_sem):
    d = dims
    me = lax.axis_index('kv')
    home = lax.rem(me - info_s[0] + group_size, group_size)
    pools = ((k_hbm, k_buf, k_out), (v_hbm, v_buf, v_out))
    parts = sem.shape[1]
    size = d.slots // parts
    last_load = pltpu.make_async_copy(last_hbm, last, last_sem)

    def moves(part, out):
        at = pl.ds(part * size, size)
        return [pltpu.make_async_copy(*((buf.at[at], dst.at[at]) if out else (src.at[at], buf.at[at])), sem.at[p, part]) for p, (src, buf, dst) in enumerate(pools)]

    def all_parts(run):
        pl.loop(0, parts)(run)

    def start(copies):
        for copy in copies:
            copy.start()

    def wait(copies):
        for copy in copies:
            copy.wait()

    def puts(run):
        @pl.loop(0, d.rows)
        def _(i):
            slot = local_slot(table_s[1, home * d.rows + i], me, d.slots)
            run([pltpu.make_async_copy(last.at[:, p, i], dst.at[slot], put_sem) for p, (_, _, dst) in enumerate(pools)])

        @pl.loop(0, src_s.shape[0])
        def _(e):
            slot = src_s[e] - me * d.slots

            @pl.when((slot >= 0) & (slot < d.slots))
            def _():
                run([pltpu.make_async_copy(zero, dst.at[local_slot(src_s[e], me, d.slots)], put_sem) for _, _, dst in pools])

    all_parts(lambda part: start(moves(part, False)))
    last_load.start()
    zero[...] = jnp.zeros_like(zero)

    @all_parts
    def _(part):
        wait(moves(part, False))
        start(moves(part, True))

    last_load.wait()
    all_parts(lambda part: wait(moves(part, True)))
    puts(start)
    puts(wait)


def fill_pools(group_size, d, info, table, mig_src, k_pool, v_pool, last):
    return pl.pallas_call(
        functools.partial(fill_pools_kernel, d, group_size),
        out_shape=[jax.ShapeDtypeStruct(k_pool.shape, k_pool.dtype)] * 2,
        in_specs=[SMEM] * 3 + [ANY] * 3,
        out_specs=[ANY, ANY],
        scratch_shapes=[pltpu.VMEM(shape, BF16) for shape in (k_pool.shape, k_pool.shape, last.shape, k_pool.shape[1:])] + [DMA((2, 4)), DMA, DMA],
        compiler_params=pltpu.CompilerParams(vmem_limit_bytes=LIMIT),
        cost_estimate=d.cost(1),
        name="fill_pools",
    )(info, table, mig_src, k_pool, v_pool, last)


def gather_pages_kernel(idx_ref, k_hbm, v_hbm, k_out, v_out, sem):
    rows = k_out.shape[0]

    def copies(i):
        slot = jnp.maximum(idx_ref[i], 0)
        return (pltpu.make_async_copy(k_hbm.at[slot], k_out.at[i], sem), pltpu.make_async_copy(v_hbm.at[slot], v_out.at[i], sem))

    @pl.loop(0, rows)
    def _(i):
        @pl.when(idx_ref[i] >= 0)
        def _():
            for copy in copies(i):
                copy.start()

        @pl.when(idx_ref[i] < 0)
        def _():
            k_out[i] = jnp.zeros(k_out.shape[1:], k_out.dtype)
            v_out[i] = jnp.zeros(v_out.shape[1:], v_out.dtype)

    @pl.loop(0, rows)
    def _(i):
        @pl.when(idx_ref[i] >= 0)
        def _():
            for copy in copies(i):
                copy.wait()


def gather_pages(idx, k_pool, v_pool):
    shape = jax.ShapeDtypeStruct((idx.shape[0],) + k_pool.shape[1:], k_pool.dtype)
    return pl.pallas_call(
        gather_pages_kernel,
        out_shape=[shape, shape],
        in_specs=[SMEM, ANY, ANY],
        out_specs=[VMEM, VMEM],
        scratch_shapes=[DMA],
        compiler_params=pltpu.CompilerParams(vmem_limit_bytes=LIMIT),
        name="gather_pages",
    )(idx, k_pool, v_pool)


def share_kernel(side, k_hbm, v_hbm, k_out, v_out, work, core_buf, ring_buf, load_sem, send_sem, recv_sem, result):
    entries = k_hbm.shape[0]
    exchange = Exchange(side, 0, work, core_buf, ring_buf, result, send_sem, recv_sem)
    units = [pl.ds(p * entries, entries) for p in PAIR]
    for p, src in enumerate((k_hbm, v_hbm)):
        pltpu.make_async_copy(src, work.at[0].at[units[p]], load_sem.at[p]).start()
    for p, src in enumerate((k_hbm, v_hbm)):
        pltpu.make_async_copy(src, work.at[0].at[units[p]], load_sem.at[p]).wait()
    for _ in range(Exchange.STEPS):
        exchange.step()
    for p, dst in enumerate((k_out, v_out)):
        pltpu.make_async_copy(result.at[units[p]], dst, load_sem.at[p]).start()
    for p, dst in enumerate((k_out, v_out)):
        pltpu.make_async_copy(result.at[units[p]], dst, load_sem.at[p]).wait()


def share(side, mig_k, mig_v):
    entries = mig_k.shape[0]
    page = mig_k.shape[1:]
    return pl.pallas_call(
        functools.partial(share_kernel, side),
        out_shape=[jax.ShapeDtypeStruct(mig_k.shape, BF16)] * 2,
        in_specs=[ANY, ANY],
        out_specs=[ANY, ANY],
        scratch_shapes=[pltpu.VMEM((1, n * entries) + page, BF16) for n in (2, 1, 1)] + [DMA((2,)), DMA((1, 10, 4)), DMA((1, 10, 4)), pltpu.VMEM((2 * entries,) + page, BF16)],
        compiler_params=pltpu.CompilerParams(has_side_effects=True, vmem_limit_bytes=LIMIT),
        name="share",
    )(mig_k, mig_v)


def migrate_kernel(dst_ref, src_ref, k_hbm, v_hbm, mk_hbm, mv_hbm, k_out, v_out, k_buf, v_buf, sem, fix_sem):
    entries = dst_ref.shape[0]
    pairs = ((k_hbm, mk_hbm, k_buf, k_out), (v_hbm, mv_hbm, v_buf, v_out))
    for p, (src, _, buf, _) in enumerate(pairs):
        pltpu.make_async_copy(src, buf, sem.at[p]).start()
    for p, (src, _, buf, _) in enumerate(pairs):
        pltpu.make_async_copy(src, buf, sem.at[p]).wait()

    @pl.loop(0, entries)
    def _(e):
        @pl.when(dst_ref[e] >= 0)
        def _():
            for _, mig, buf, _ in pairs:
                copy = pltpu.make_async_copy(mig.at[e], buf.at[jnp.maximum(dst_ref[e], 0)], fix_sem)
                copy.start()
                copy.wait()

        @pl.when(src_ref[e] >= 0)
        def _():
            for _, _, buf, _ in pairs:
                buf[jnp.maximum(src_ref[e], 0)] = jnp.zeros(buf.shape[1:], buf.dtype)

    for p, (_, _, buf, dst) in enumerate(pairs):
        pltpu.make_async_copy(buf, dst, sem.at[p]).start()
    for p, (_, _, buf, dst) in enumerate(pairs):
        pltpu.make_async_copy(buf, dst, sem.at[p]).wait()


def migrate(dst_local, src_local, k_pool, v_pool, mig_k, mig_v):
    shape = jax.ShapeDtypeStruct(k_pool.shape, k_pool.dtype)
    return pl.pallas_call(
        migrate_kernel,
        out_shape=[shape, shape],
        in_specs=[SMEM, SMEM, ANY, ANY, ANY, ANY],
        out_specs=[ANY, ANY],
        scratch_shapes=[pltpu.VMEM(k_pool.shape, k_pool.dtype), pltpu.VMEM(k_pool.shape, k_pool.dtype), DMA((2,)), DMA],
        compiler_params=pltpu.CompilerParams(vmem_limit_bytes=LIMIT),
        name="migrate",
    )(dst_local, src_local, k_pool, v_pool, mig_k, mig_v)


def decode_kernel(dims, sc_ref, x_ref, p0k_hbm, p0v_hbm, wq, wk, wv, wo, wu, wd, k_in, v_in, y_ref, k_out, v_out,
                  first_buf, last_buf, *rest):
    compute, (page_sem, put_sem) = rest[:-2], rest[-2:]
    d = dims
    dec = Decoder(d, 0, d.layers, (wq, wk, wv, wo, wu, wd), y_ref, compute, 1, 2)
    dec.start_stream()
    y_ref[...] = x_ref[...]
    loads = [pltpu.make_async_copy(src, first_buf.at[p], page_sem.at[p]) for p, src in enumerate((p0k_hbm, p0v_hbm))]
    for load in loads:
        load.start()

    def last_loads(run):
        @pl.loop(0, d.rows)
        def _(i):
            for p, src in enumerate((k_in, v_in)):
                run(pltpu.make_async_copy(src.at[sc_ref[0, i]], last_buf.at[p, i], page_sem.at[2]))

    def puts(run):
        @pl.loop(0, d.rows)
        def _(i):
            @pl.when(sc_ref[2, i] > 0)
            def _():
                for p, dst in enumerate((k_out, v_out)):
                    run(pltpu.make_async_copy(last_buf.at[p, i], dst.at[sc_ref[0, i]], put_sem))

    last_loads(lambda copy: copy.start())
    for load in loads:
        load.wait()
    last_loads(lambda copy: copy.wait())

    @pl.loop(0, d.layers)
    def _(layer):
        def put_page(p, i, val):
            last_buf[p, i, layer] = val

        dec.project(layer)
        dec.attend(lambda i: sc_ref[1, i], lambda p, i: first_buf[p, i, layer], lambda p, i: last_buf[p, i, layer], put_page)
        dec.gather_heads()
        dec.mix(layer)

    puts(lambda copy: copy.start())
    puts(lambda copy: copy.wait())


def decode(d, scalars, x, p0k, p0v, weights, k_pool, v_pool):
    pool = jax.ShapeDtypeStruct(k_pool.shape, k_pool.dtype)
    pages = pltpu.VMEM((2, d.rows, d.layers, d.page_rows, d.head_dim), BF16)
    return pl.pallas_call(
        functools.partial(decode_kernel, d),
        out_shape=[jax.ShapeDtypeStruct(x.shape, x.dtype), pool, pool],
        in_specs=[SMEM, VMEM] + [ANY] * 10,
        out_specs=[VMEM, ANY, ANY],
        input_output_aliases={10: 1, 11: 2},
        scratch_shapes=[pages, pages] + d.compute_scratch(16, 16) + [DMA((3,)), DMA],
        compiler_params=pltpu.CompilerParams(vmem_limit_bytes=LIMIT),
        cost_estimate=d.cost(d.layers),
        name="decode",
    )(scalars, x, p0k, p0v, *weights, k_pool, v_pool)


def permute(arrays, shift, group_size):
    if shift == group_size // 2:
        return permute(permute(arrays, shift // 2, group_size), shift // 2, group_size)
    perm = [(i, (i + shift) % group_size) for i in range(group_size)]
    return jax.tree.map(lambda a: lax.ppermute(a, 'kv', perm), arrays) if shift else arrays


def rotate_back(first, second, shift, group_size, beside):
    def branch(r):
        def run(args):
            parts = permute(args[0], -r % group_size, group_size), permute(args[1], (1 - r) % group_size, group_size)
            return jnp.concatenate(parts, axis=1), beside()

        return run

    return lax.switch(shift, [branch(r) for r in range(group_size)], (first, second))


def rotate(arrays, shift, group_size):
    stride = math.isqrt(2 * group_size)
    for count, move in ((shift // stride, stride), (shift % stride, 1)):
        arrays = lax.fori_loop(0, count, lambda _, a: permute(a, move, group_size), arrays)
    return arrays


def solution(mesh):
    group_size = mesh.shape['kv']
    side = math.isqrt(group_size // 2)
    pool_spec = P(('rep', 'kv'))
    tok_spec = P(None, ('rep', 'kv'), None)

    def device_fn(embeds, w_query, w_key, w_value, w_out, w_up, w_down, k_pool5, v_pool5, new_table, seq_lens, mig_src, mig_dst):
        me = lax.axis_index('kv')
        slots, layers, page, kv_heads, head_dim = k_pool5.shape
        rows, width = embeds.shape[1:]
        weights = (w_query, w_key, w_value, w_out, w_up, w_down)
        k_pool = k_pool5.reshape(slots, layers, page * kv_heads, head_dim)
        v_pool = v_pool5.reshape(slots, layers, page * kv_heads, head_dim)
        d = Dims(rows, weights, k_pool, page)
        ints = jnp.int32

        def local(ids):
            loc = ids - me * slots
            return jnp.where((loc >= 0) & (loc < slots), loc, -1)

        def take(vec, dev):
            return lax.dynamic_slice(vec, (dev * rows,), (rows,))

        def inside(ids):
            return local_slot(ids, me, slots)

        def general_path():
            first_new, last_new = new_table[:, 0], new_table[:, 1]
            moved = first_new[None, :] == mig_dst[:, None]
            first_old = jnp.where(jnp.any(moved, axis=0), jnp.sum(jnp.where(moved, mig_src[:, None], 0), axis=0), first_new)
            home = jnp.arange(first_new.shape[0], dtype=ints) // rows
            worker = last_new // slots
            shift_of = (worker - home + group_size) % group_size
            first_shift = (worker - first_old // slots + group_size) % group_size
            shift_ids = jnp.arange(group_size, dtype=ints)
            wanted = jnp.any(shift_of[None, :] == shift_ids[:, None], axis=1)
            mig_k, mig_v = gather_pages(local(mig_src), k_pool, v_pool)
            by_layer = tuple(m.swapaxes(0, 1) for m in (mig_k, mig_v))
            mig_k, mig_v = (m.swapaxes(0, 1) for m in lax.map(lambda pages: tuple(share(side, *pages)), by_layer))
            k_new, v_new = migrate(local(mig_dst), local(mig_src), k_pool, v_pool, mig_k, mig_v)

            def one_round(shift, y, k_new, v_new):
                src_home = (me - shift + group_size) % group_size
                x = rotate(embeds.reshape(2 * rows, width), shift, group_size)
                in_round = shift_of == shift
                wanted2 = jnp.any(in_round[None, :] & (first_shift[None, :] == shift_ids[:, None]), axis=1)

                def more(state):
                    left, pk, pv = state
                    shift2 = jnp.argmax(left).astype(ints)
                    dest_home = (me + shift2 - shift + group_size) % group_size
                    got = gather_pages(inside(take(first_old, dest_home)), k_pool, v_pool)
                    got_k, got_v = rotate(tuple(got), shift2, group_size)
                    mine = (take(first_shift, src_home) == shift2)[:, None, None, None]
                    return left & (shift_ids != shift2), jnp.where(mine, got_k, pk), jnp.where(mine, got_v, pv)

                zeros = jnp.zeros((rows,) + k_pool.shape[1:], k_pool.dtype)
                _, pk, pv = lax.while_loop(lambda state: jnp.any(state[0]), more, (wanted2, zeros, zeros))
                valid = take(shift_of, src_home) == shift
                scalars = jnp.stack([inside(take(last_new, src_home)), take(seq_lens, src_home), valid.astype(ints)])
                out, k_new, v_new = decode(d, scalars, x, pk, pv, weights, k_new, v_new)
                back = rotate(out, (group_size - shift) % group_size, group_size)
                mine = (take(shift_of, me) == shift)[None, :, None]
                return jnp.where(mine, back.reshape(embeds.shape), y), k_new, v_new

            def next_round(state):
                left, y, k_new, v_new = state
                shift = jnp.argmax(left).astype(ints)
                y, k_new, v_new = one_round(shift, y, k_new, v_new)
                return left & (shift_ids != shift), y, k_new, v_new

            _, y, k_new, v_new = lax.while_loop(lambda state: jnp.any(state[0]), next_round, (wanted, jnp.zeros_like(embeds), k_new, v_new))
            return y, k_new, v_new

        table = new_table.T
        ya, yb, info, last = decode_adjacent(side, group_size, d, table, seq_lens, mig_src, mig_dst, embeds, weights, k_pool, v_pool)
        y, (k_new, v_new) = rotate_back(ya, yb, info[0], group_size, lambda: fill_pools(group_size, d, info, table, mig_src, k_pool, v_pool, last))
        _, y, k_new, v_new = lax.while_loop(lambda state: state[0] == 0, lambda state: (jnp.ones_like(state[0]),) + general_path(), (info[1], y, k_new, v_new))
        return y, k_new.reshape(k_pool5.shape), v_new.reshape(v_pool5.shape)

    return jax.shard_map(device_fn, mesh=mesh, in_specs=(tok_spec, P(), P(), P(), P(), P(), P(), pool_spec, pool_spec, P('rep', None), P('rep'), P('rep'), P('rep')), out_specs=(tok_spec, pool_spec, pool_spec), check_vma=False)
```

```python
import functools
import math

import jax
import jax.numpy as jnp
from jax import lax
from jax.experimental import pallas as pl
from jax.experimental.pallas import tpu as pltpu
from jax.sharding import PartitionSpec as P

ANY = pl.BlockSpec(memory_space=pl.ANY)
SMEM = pl.BlockSpec(memory_space=pltpu.SMEM)
VMEM = pl.BlockSpec(memory_space=pltpu.VMEM)
DMA = pltpu.SemaphoreType.DMA
CHUNK = 256
UNROLL = 8
LANES = 128
HALF = CHUNK // 2
PAIR = (0, 1)
LIMIT = 63 << 20
F32, BF16 = jnp.float32, jnp.bfloat16


def iota(shape, axis):
    return lax.broadcasted_iota(jnp.int32, shape, axis)


def dot(a, b):
    return jnp.dot(a, b, preferred_element_type=F32)


def local_slot(ids, me, slots):
    return jnp.clip(ids - me * slots, 0, slots - 1)


def aligned(x, multiple):
    return x if isinstance(x, int) else pl.multiple_of(x, multiple)


class Dims:
    def __init__(self, rows, weights, k_pool, page):
        w_query, w_key, _, _, w_up, _ = weights
        self.layers, self.width, self.q_width = w_query.shape
        self.ff = w_up.shape[2]
        self.slots, _, self.page_rows, self.head_dim = k_pool.shape
        self.kv_heads = w_key.shape[2] // self.head_dim
        self.heads = self.q_width // self.head_dim
        self.page, self.rows = page, rows
        self.tokens = 2 * rows
        self.stride = self.tokens + 8
        self.n_q, self.n_o, self.n_u = self.q_width // CHUNK, self.width // CHUNK, self.ff // CHUNK

    def compute_scratch(self, n_col, n_row):
        return [
            pltpu.VMEM((n_col, self.width, CHUNK), BF16),
            pltpu.VMEM((n_row, CHUNK, self.width), BF16),
            pltpu.VMEM((self.heads * self.stride, self.head_dim), F32),
            pltpu.VMEM((self.kv_heads * self.stride, self.head_dim), F32),
            pltpu.VMEM((self.kv_heads * self.stride, self.head_dim), F32),
            pltpu.VMEM((self.heads * self.stride, self.head_dim), F32),
            pltpu.VMEM((self.tokens, self.q_width), BF16),
            pltpu.VMEM((self.tokens, self.ff), BF16),
            pltpu.VMEM((self.tokens, self.width), F32),
            DMA((n_col,)),
            DMA((n_row,)),
        ]

    def cost(self, layers):
        size = layers * self.width * (2 * self.q_width + 2 * self.kv_heads * self.head_dim + 2 * self.ff)
        return pl.CostEstimate(flops=2 * size * self.tokens, bytes_accessed=2 * size, transcendentals=0)


class Decoder:
    def __init__(self, dims, first, layers, weights, y_ref, scratch, group=2, unroll=UNROLL, shared=False):
        self.group, self.unroll, self.shared = group, unroll, shared
        self.d, self.first, self.layers, self.weights, self.y_ref = dims, first, layers, weights, y_ref
        (self.col_buf, self.row_buf, self.q_s, self.kn_s, self.vn_s, self.o_s, self.att, self.act, self.acc, self.col_sem, self.row_sem) = scratch
        self.n_col, self.n_row = self.col_buf.shape[0], self.row_buf.shape[0]
        self.zero = lax.axis_index('kv') * 0
        d = dims
        self.whole = d.ff // 2 // CHUNK if shared else d.n_u
        self.begin = lax.axis_index('kv') % 2 * (d.ff // 2) if shared else 0
        self.col_layer = d.n_q + 2 + d.n_o + self.whole
        cols = 2 * d.page * d.kv_heads
        col_pos = iota((2 * d.heads, cols), 1)
        row_pos = iota((2 * d.heads, cols), 0)
        same_head = (col_pos % d.kv_heads) == (row_pos % d.heads) // (d.heads // d.kv_heads)
        self.limit = jnp.where(same_head, col_pos // d.kv_heads - row_pos // d.heads, 4 * d.page)
        self.page_pos = iota((d.page_rows, d.head_dim), 0) // d.kv_heads
        self.tile_head = iota((8, d.head_dim), 0) % d.kv_heads

    def layer_of(self, g, per_layer):
        return sum((g >= per_layer * l).astype(jnp.int32) for l in range(1, self.layers))

    def col_start(self, g):
        d = self.d
        wq, wk, wv, wo, wu, _ = self.weights

        @pl.when(g < self.layers * self.col_layer)
        def _():
            layer = self.layer_of(g, self.col_layer)
            pos = g - layer * self.col_layer
            slot = g % self.n_col

            def go(src, c, begin=0):
                start = aligned(c * CHUNK + begin, LANES)
                pltpu.make_async_copy(src.at[self.first + layer].at[:, pl.ds(start, CHUNK)], self.col_buf.at[slot], self.col_sem.at[slot]).start()

            @pl.when(pos < d.n_q)
            def _():
                go(wq, pos)

            @pl.when(pos == d.n_q)
            def _():
                go(wk, 0)

            @pl.when(pos == d.n_q + 1)
            def _():
                go(wv, 0)

            @pl.when((pos >= d.n_q + 2) & (pos < d.n_q + 2 + d.n_o))
            def _():
                go(wo, pos - (d.n_q + 2))

            @pl.when(pos >= d.n_q + 2 + d.n_o)
            def _():
                go(wu, pos - (d.n_q + 2 + d.n_o), self.begin)

    def row_start(self, g):
        d = self.d
        wd = self.weights[5]

        @pl.when(g < self.layers * self.whole)
        def _():
            layer = self.layer_of(g, self.whole)
            slot = g % self.n_row
            start = aligned((g - layer * self.whole) * CHUNK + self.begin, LANES)
            pltpu.make_async_copy(wd.at[self.first + layer].at[pl.ds(start, CHUNK)], self.row_buf.at[slot], self.row_sem.at[slot]).start()

    def start_stream(self):
        @pl.loop(0, self.n_col)
        def _(g):
            self.col_start(g)

        @pl.loop(0, self.n_row)
        def _(g):
            self.row_start(g)

    def with_cols(self, g, count, body):
        slots = [(g + u) % self.n_col for u in range(count)]
        for slot in slots:
            pltpu.make_async_copy(self.weights[1].at[0], self.col_buf.at[slot], self.col_sem.at[slot]).wait()
        body([self.col_buf.at[slot] for slot in slots])
        for u in range(count):
            self.col_start(g + u + self.n_col)

    def with_rows(self, g, count, body):
        slots = [(g + u) % self.n_row for u in range(count)]
        for slot in slots:
            pltpu.make_async_copy(self.weights[5].at[0, pl.ds(0, CHUNK), :], self.row_buf.at[slot], self.row_sem.at[slot]).wait()
        body([self.row_buf.at[slot] for slot in slots])
        for u in range(count):
            self.row_start(g + u + self.n_row)

    def project(self, layer):
        d = self.d
        col0 = (self.zero + layer) * self.col_layer

        def product(ref):
            return dot(self.y_ref[...], ref[...]).astype(BF16).astype(F32)

        def put(dst, first, out):
            for h in range(CHUNK // d.head_dim):
                at = aligned((first + h) * d.stride, 8)
                dst[pl.ds(at, d.tokens), :] = out[:, h * d.head_dim:(h + 1) * d.head_dim]

        many = self.group

        @pl.loop(0, d.n_q // many)
        def _(j):
            def body(refs):
                outs = [product(ref) for ref in refs]
                for u in range(many):
                    put(self.q_s, (many * j + u) * (CHUNK // d.head_dim), outs[u])

            self.with_cols(col0 + many * j, many, body)

        def body(refs):
            outs = [product(ref) for ref in refs]
            put(self.kn_s, 0, outs[0])
            put(self.vn_s, 0, outs[1])

        self.with_cols(col0 + d.n_q, 2, body)

    def insert(self, page, n, row):
        d = self.d
        val = page.astype(F32)
        for t in PAIR:
            new = jnp.broadcast_to(row(t, 0), (8, d.head_dim))
            for g in range(1, d.kv_heads):
                new = jnp.where(self.tile_head == g, row(t, g), new)
            val = jnp.where(self.page_pos == n - d.page + t, jnp.concatenate([new] * (d.page_rows // 8), axis=0), val)
        return val.astype(BF16)

    def attend(self, lens, first_page, last_page, put_page, events=(), begin=0, count=None):
        d = self.d
        count = count or d.rows
        unroll = min(self.unroll, count)

        def some(first):
            ids = [first + u for u in range(unroll)]
            scores, vals = [], []
            for i in ids:
                n = lens(i)

                def updated(p, new_ref):
                    val = self.insert(last_page(p, i), n, lambda t, g: new_ref[pl.ds(g * d.stride + t * d.rows + i, 1), :])
                    put_page(p, i, val)
                    return val

                keys = jnp.concatenate([first_page(0, i), updated(0, self.kn_s)], axis=0)
                vals.append(updated(1, self.vn_s))
                qs = jnp.concatenate([self.q_s[pl.ds(t * d.rows + i, d.heads, stride=d.stride), :] for t in PAIR], axis=0)
                score = lax.dot_general(qs.astype(BF16), keys, (((1,), (1,)), ((), ())), preferred_element_type=F32) * d.head_dim ** -0.5
                scores.append(jnp.where(self.limit <= n, score, -jnp.inf))
            tops = [jnp.max(score, axis=1, keepdims=True) for score in scores]
            probs = [jnp.exp(score - top) for score, top in zip(scores, tops)]
            totals = [jnp.sum(prob, axis=1, keepdims=True) for prob in probs]
            for u, i in enumerate(ids):
                both = jnp.concatenate([first_page(1, i), vals[u]], axis=0)
                out = dot(probs[u].astype(BF16), both) / totals[u]
                for t in PAIR:
                    self.o_s[pl.ds(t * d.rows + i, d.heads, stride=d.stride), :] = out[t * d.heads:(t + 1) * d.heads]

        @pl.loop(0, count // unroll)
        def _(block):
            for k, run in events:
                pl.when(block == k)(run)
            some(begin + block * unroll)

    def gather_heads(self):
        d = self.d
        for h in range(d.heads):
            self.att[:, h * d.head_dim:(h + 1) * d.head_dim] = self.o_s[h * d.stride:h * d.stride + d.tokens, :].astype(BF16)

    def span(self, j):
        return pl.ds(aligned(j * CHUNK, CHUNK), CHUNK)

    def out_project(self, layer, after=None):
        d, many = self.d, self.group

        @pl.loop(0, d.n_o // many)
        def _(j):
            def body(refs):
                outs = [dot(self.att[...], ref[...]) for ref in refs]
                for u in range(many):
                    at = self.span(many * j + u)
                    self.y_ref[:, at] = (self.y_ref[:, at].astype(F32) + outs[u]).astype(BF16)

            self.with_cols(layer * self.col_layer + d.n_q + len(PAIR) + many * j, many, body)
            if after:
                after(j)

    def mix(self, layer, events=()):
        d = self.d
        layer = self.zero + layer
        col0 = layer * self.col_layer + d.n_q + 2
        many = self.group
        pairs = d.n_u // many

        def between(j, first):
            for k, run in events:
                if first <= k < first + pairs:
                    pl.when(j == k - first)(run)

        self.out_project(layer)

        def up(first, count):
            def body(refs):
                ups = [dot(self.y_ref[...], ref[...]) for ref in refs]
                for u in range(count):
                    self.act[:, self.span(first + u)] = jax.nn.gelu(ups[u].astype(BF16).astype(F32), approximate=True).astype(BF16)

            self.with_cols(col0 + d.n_o + first, count, body)

        def down(first, count):
            def body(refs):
                out = self.acc[...]
                for u in range(count):
                    out += dot(self.act[:, self.span(first + u)], refs[u][...])
                self.acc[...] = out

            self.with_rows(layer * self.whole + first, count, body)

        @pl.loop(0, pairs)
        def _(j):
            between(j, 0)
            up(many * j, many)

        if d.n_u % many:
            up(d.n_u - 1, 1)

        self.acc[...] = self.y_ref[...].astype(F32)

        @pl.loop(0, pairs)
        def _(j):
            between(j, pairs)
            down(many * j, many)

        if d.n_u % many:
            down(d.n_u - 1, 1)

        self.y_ref[...] = self.acc[...].astype(BF16)


    def half_loads(self, layer):
        at = pl.ds(aligned(self.begin + self.whole * CHUNK, LANES), HALF)
        return (pltpu.make_async_copy(self.weights[4].at[layer].at[:, at], self.half_col, self.half_sem.at[0]),
                pltpu.make_async_copy(self.weights[5].at[layer].at[at], self.half_row, self.half_sem.at[1]))

    def mix_shared(self, layer, send_hidden, wait_hidden, swap_sums, events=()):
        d = self.d
        half_loads, next_loads = self.half_loads(layer), self.half_loads(layer + 1) if layer + 1 < d.layers else ()
        layer = self.zero + layer
        col0 = layer * self.col_layer + d.n_q + 2
        many = self.group
        rows = d.tokens
        offset = d.ff // 2
        pairs = self.whole // many

        def between(j, first):
            for k, run in events:
                if first <= k < first + pairs:
                    pl.when(j == k - first)(run)

        self.out_project(layer, send_hidden)

        self.acc[...] = self.y_ref[...].astype(F32)
        self.acc_other[...] = jnp.zeros_like(self.acc_other)
        wait_hidden()

        def hidden():
            return jnp.concatenate([self.y_ref[...], self.y_other[...]], axis=0)

        def activate(up, at, size):
            val = jax.nn.gelu(up.astype(BF16).astype(F32), approximate=True).astype(BF16)
            self.act[:, pl.ds(aligned(at, LANES), size)] = val[:rows]
            self.act[:, pl.ds(aligned(at + offset, LANES), size)] = val[rows:]

        @pl.loop(0, pairs)
        def _(j):
            between(j, 0)

            def body(refs):
                ups = [dot(hidden(), ref[...]) for ref in refs]
                for u in range(many):
                    activate(ups[u], (many * j + u) * CHUNK, CHUNK)

            self.with_cols(col0 + d.n_o + many * j, many, body)

        tail = self.whole % many
        for u in range(tail):
            def body(refs, at=(self.whole - tail + u) * CHUNK):
                activate(dot(hidden(), refs[0][...]), at, CHUNK)

            self.with_cols(col0 + d.n_o + self.whole - tail + u, 1, body)
        for copy in half_loads:
            copy.wait()
        activate(dot(hidden(), self.half_col[...]), self.whole * CHUNK, HALF)

        def acts(at, size):
            return jnp.concatenate([self.act[:, pl.ds(aligned(at, LANES), size)], self.act[:, pl.ds(aligned(at + offset, LANES), size)]], axis=0)

        def add(out):
            self.acc[...] += out[:rows]
            self.acc_other[...] += out[rows:]

        @pl.loop(0, pairs)
        def _(j):
            between(j, pairs)

            def body(refs):
                add(sum(dot(acts((many * j + u) * CHUNK, CHUNK), refs[u][...]) for u in range(many)))

            self.with_rows(layer * self.whole + many * j, many, body)

        for u in range(tail):
            def body(refs, at=(self.whole - tail + u) * CHUNK):
                add(dot(acts(at, CHUNK), refs[0][...]))

            self.with_rows(layer * self.whole + self.whole - tail + u, 1, body)
        add(dot(acts(self.whole * CHUNK, HALF), self.half_row[...]))
        for copy in next_loads:
            copy.start()
        self.y_ref[...] = (self.acc[...] + swap_sums()).astype(BF16)


class Exchange:
    STEPS = 11

    def __init__(self, side, layer, work, core_buf, ring_buf, out, send_sem, recv_sem):
        self.layer = layer
        self.work, self.core_buf, self.ring_buf, self.out, self.send_sem, self.recv_sem = work, core_buf, ring_buf, out, send_sem, recv_sem
        me = lax.axis_index('kv')
        core, x, y = me % 2, me // 2 % side, me // (2 * side)

        def pairings(pos, stride):
            return (((pos + 1) // 2 % 2, me + (1 - 2 * (pos % 2)) * stride), (pos // 2, me + (side - 1 - 2 * pos) * stride))

        xs, ys = pairings(x, 2), pairings(y, 2 * side)
        self.orders = [xs + ys, xs[::-1] + ys[::-1], ys + xs, ys[::-1] + xs[::-1]]
        self.partner = me + 1 - 2 * core
        self.peers = [self.partner] + [dev for _, dev in xs + ys]
        self.half = work.shape[1] // 2
        self.stream = self.half // 4
        self.base, self.other = core * self.half, (1 - core) * self.half
        self.copies, self.done = [], 0
        self.path = [[self.base + k * self.stream for k in range(4)]]
        self.away = []
        for ring in range(4):
            size = self.stream >> (ring + 1)
            self.away.append([self.path[-1][k] + (1 - self.orders[k][ring][0]) * size for k in range(4)])
            self.path.append([self.path[-1][k] + self.orders[k][ring][0] * size for k in range(4)])

    def send(self, src, dst, step, lane, dev):
        def copy():
            return pltpu.make_async_remote_copy(src(), dst(), self.send_sem.at[self.layer, step, lane], self.recv_sem.at[self.layer, step, lane], device_id={'kv': dev})

        copy().start()
        self.copies.append(copy)

    def units(self, ref, at, count):
        return lambda: ref.at[self.layer].at[pl.ds(at, count)]

    def results(self, at, count):
        return lambda: self.out.at[pl.ds(at, count)]

    def add(self, dst_at, buf, src_at, count):
        @pl.loop(0, count)
        def _(u):
            self.work[self.layer, dst_at + u] = self.work[self.layer, dst_at + u] + buf[self.layer, src_at + u]

    def halve(self, ring, k):
        size = self.stream >> (ring + 1)
        src = self.units(self.work, self.away[ring][k], size)
        self.send(src, self.units(self.ring_buf, (k + 1) * self.stream - 2 * size, size), 1 + ring, k, self.orders[k][ring][1])

    def halved(self, ring, k):
        size = self.stream >> (ring + 1)
        self.add(self.path[ring + 1][k], self.ring_buf, (k + 1) * self.stream - 2 * size, size)

    def double(self, ring, k):
        at = self.results(self.path[ring + 1][k], self.stream >> (ring + 1))
        self.send(at, at, 8 - ring, k, self.orders[k][ring][1])

    def step(self):
        step, self.done = self.done, self.done + 1
        started, self.copies = self.copies, []
        if step in (1, 9, 10):
            for copy in started:
                copy().wait()
        if step == 0:
            self.send(self.units(self.work, self.other, self.half), self.units(self.core_buf, 0, self.half), 0, 0, self.partner)
        elif step == 1:
            self.add(self.base, self.core_buf, 0, self.half)
            for k in range(4):
                self.halve(0, k)
        elif step < 9:
            for k in range(4):
                started[k]().wait()
                if step < 6:
                    self.halved(step - 2, k)
                if step < 5:
                    self.halve(step - 1, k)
                    continue
                if step == 5:
                    for u in range(self.stream >> 4):
                        self.out[self.path[4][k] + u] = self.work[self.layer, self.path[4][k] + u]
                self.double(8 - step, k)
        elif step == 9:
            at = self.results(self.base, self.half)
            self.send(at, at, 9, 0, self.partner)


def adjacent_kernel(dims, side, group_size, entries, src_s, dst_s, table_hbm, lens_hbm, embeds_hbm, wq, wk, wv, wo, wu, wd, k_hbm, v_hbm,
                    ya_ref, yb_ref, info_s, last_out,
                    table_s, lens_s, table_v, embeds_v, y_ref, send_buf, got_buf, last_buf, new_buf, work, core_buf, ring_buf, mid_in, mid_out, x_in, plan_v, plan_s, y_other, acc_other, sums_in, half_col, half_row, *rest):
    d = dims
    migs, rest = rest[:d.layers], rest[d.layers:]
    pools, rest = [rest[2 * l:2 * l + 2] for l in range(d.layers)], rest[2 * d.layers:]
    compute, (load_sem, pool_sem, plan_sem, x_send, x_recv, page_send, page_recv, new_send, new_recv, mig_send, mig_recv, out_sem, half_sem, pair_send, pair_recv) = rest[:-15], rest[-15:]
    half = d.rows // 2
    me = lax.axis_index('kv')
    ahead, behind = lax.rem(me + 1, group_size), lax.rem(me + group_size - 1, group_size)
    dec = Decoder(d, 0, d.layers, (wq, wk, wv, wo, wu, wd), y_ref, compute, shared=True)
    dec.y_other, dec.acc_other, dec.half_col, dec.half_row, dec.half_sem = y_other, acc_other, half_col, half_row, half_sem
    exchanges = [Exchange(side, l, work, core_buf, ring_buf, migs[l], mig_send, mig_recv) for l in range(d.layers)]

    def scope(name, run, *args):
        with jax.named_scope(name):
            return run(*args)

    pool_loads = [[pltpu.make_async_copy(src.at[:, l], pools[l][p], pool_sem.at[l, p]) for p, src in enumerate((k_hbm, v_hbm))] for l in range(d.layers)]
    embeds_load, table_load, lens_load, table_load_v = [
        pltpu.make_async_copy(src, dst, load_sem.at[i]) for i, (src, dst) in enumerate(((embeds_hbm, embeds_v), (table_hbm, table_s), (lens_hbm, lens_s), (table_hbm, table_v)))]
    for load in [embeds_load] + pool_loads[0] + [table_load, table_load_v, lens_load]:
        load.start()
    barrier = pltpu.get_barrier_semaphore()

    @pl.loop(1, group_size)
    def _(r):
        pl.semaphore_signal(barrier, inc=1, device_id={'kv': lax.rem(me + r, group_size)})

    scope("barrier", lambda: pl.semaphore_wait(barrier, group_size - 1))

    groups = d.tokens // 8
    splits = group_size // groups
    cols = d.width // splits

    def piece(ref, m):
        return ref.at[m // splits, :, pl.ds(aligned(m % splits * cols, cols), cols)]

    def all_pieces(phase):
        some = mid_in.at[pl.ds(0, group_size - 1)]
        pltpu.make_async_remote_copy(some, some, x_send.at[phase], x_recv.at[phase], device_id={'kv': me}).wait()

    def send_embeddings():
        embeds_load.wait()

        @pl.loop(1, group_size)
        def _(r):
            m = lax.rem(me + r, group_size)
            pltpu.make_async_remote_copy(piece(embeds_v, m), mid_in.at[me], x_send.at[0], x_recv.at[0], device_id={'kv': m}).start()

        mid_in[me] = piece(embeds_v, me)[...]

    def load_tables():
        for load in (table_load, lens_load, table_load_v):
            load.wait()
        return lax.rem(table_s[1, 0] // d.slots + group_size, group_size)

    scope("pool_wait_0", lambda: [load.wait() for load in pool_loads[0]])

    def own(l):
        @pl.loop(0, entries)
        def _(e):
            slot = src_s[e] - me * d.slots
            mine = (slot >= 0) & (slot < d.slots)
            slot = local_slot(src_s[e], me, d.slots)
            for p in PAIR:
                page = pools[l][p][slot]
                work[l, p * entries + e] = jnp.where(mine, page, jnp.zeros_like(page))

    def step(l):
        scope(f"exchange_{l}_{exchanges[l].done}", exchanges[l].step)

    step_0, step_1 = functools.partial(step, 0), functools.partial(step, 1)

    scope("own_0", own, 0)
    step_0()
    for l in range(1, d.layers):
        for load in pool_loads[l]:
            load.start()
    scope("start_stream", dec.start_stream)
    for copy in dec.half_loads(0):
        copy.start()
    shift = scope("load_tables", load_tables)
    home_a = lax.rem(me - shift + group_size, group_size)
    home_b = lax.rem(home_a + 1, group_size)

    def clipped(slot):
        return local_slot(slot, me, d.slots)

    def first_here(l, p, i):
        return pools[l][p][clipped(table_s[0, home_b * d.rows + i])]

    def last_here(l, p, i):
        return pools[l][p][clipped(table_s[1, home_a * d.rows + i])]

    def migrated(l, p, home, i, page):
        entry = plan_s[0, home * d.rows + i]
        return jnp.where(entry >= 0, migs[l][p * entries + jnp.maximum(entry, 0)], page)

    def pack(l):
        @pl.loop(0, half)
        def _(i):
            for p in PAIR:
                send_buf[l, 0, p, i] = first_here(l, p, i)
                send_buf[l, 1, p, i] = last_here(l, p, half + i)

    parts = 4
    size = half // parts

    def page_copy(l, way, p, rows):
        return pltpu.make_async_remote_copy(
            send_buf.at[l, way, p, rows], got_buf.at[l, way, p, rows], page_send.at[l, way, p], page_recv.at[l, way, p], device_id={'kv': (ahead, behind)[way]})

    pieces = [iter([(p, part) for part in range(parts) for p in PAIR]) for _ in range(d.layers)]

    def pages_start(l):
        p, part = next(pieces[l])
        for way in PAIR:
            page_copy(l, way, p, pl.ds(part * size, size)).start()

    pages_0, pages_1 = functools.partial(pages_start, 0), functools.partial(pages_start, 1)

    def pages_wait(l):
        for way in PAIR:
            for p in PAIR:
                page_copy(l, way, p, pl.ds(0, half)).wait()

    def pass_on():
        all_pieces(0)
        later = me // splits * 8 % d.rows // half

        @pl.loop(0, group_size)
        def _(m):
            mid_out[m] = mid_in[lax.rem(m - shift + later + group_size, group_size)]

        @pl.loop(1, group_size)
        def _(r):
            m = lax.rem(me + r, group_size)
            pltpu.make_async_remote_copy(mid_out.at[m], piece(x_in, me), x_send.at[1], x_recv.at[1], device_id={'kv': m}).start()

        piece(x_in, me)[...] = mid_out[me]

    def take_embeddings():
        all_pieces(1)
        y_ref[...] = x_in[...].reshape(d.tokens, d.width)

    plan_copy = pltpu.make_async_copy(plan_v, plan_s, plan_sem)

    def plan():
        seq = iota((1, table_v.shape[1]), 1)
        worker = lax.rem(seq // d.rows + shift, group_size)
        before = lax.rem(worker + group_size - 1, group_size)
        first, last = table_v[0:1, :], table_v[1:2, :]
        bad = (last < worker * d.slots) | (last >= worker * d.slots + d.slots) | (first < before * d.slots) | (first >= before * d.slots + d.slots)

        def entry(e, state):
            plan, bad = state
            return jnp.where(last == dst_s[e], e, plan), bad | (first == dst_s[e]).astype(jnp.int32)

        plan, bad = lax.fori_loop(0, entries, entry, (jnp.full_like(last, -1), bad.astype(jnp.int32)))
        plan_v[...] = plan
        plan_copy.start()
        info_s[0] = shift
        info_s[1] = 1 - jnp.max(bad)

    def new_copies(l):
        return [pltpu.make_async_remote_copy(
            ref.at[pl.ds(g * d.stride + t * d.rows + half, half)], new_buf.at[l, p, g, t], new_send.at[l, p, g, t], new_recv.at[l, p, g, t], device_id={'kv': ahead})
            for p, ref in enumerate((dec.kn_s, dec.vn_s)) for g in range(d.kv_heads) for t in PAIR]

    def project(l):
        dec.project(l)
        for copy in new_copies(l):
            copy.start()

    scope("pack_0", pack, 0)
    step_0()
    scope("send_embeddings", send_embeddings)
    pages_0()
    scope("plan", plan)
    step_0()
    pages_0()
    for l in range(1, d.layers):
        for load in pool_loads[l]:
            load.wait()
    scope("own_1", own, 1)

    def both():
        step_0()
        pages_0()
        step_1()

    both()
    scope("pass_on", pass_on)
    both()
    both()
    scope("pack_1", pack, 1)
    both()
    scope("take_embeddings", take_embeddings)
    both()
    scope("project_0", project, 0)
    both()
    plan_copy.wait()
    step_0()
    step_1()
    step_0()
    step_1()
    scope("pages_wait_0", pages_wait, 0)

    def attend(l, events_a, events_b):
        def put_page(p, i, val):
            last_buf[p, i] = val

        dec.attend(lambda i: lens_s[home_a * d.rows + i], lambda p, i: got_buf[l, 0, p, i],
                   lambda p, i: migrated(l, p, home_a, i, last_here(l, p, i)), put_page, events_a, 0, half)
        dec.attend(lambda i: lens_s[home_b * d.rows + i], lambda p, i: first_here(l, p, i),
                   lambda p, i: migrated(l, p, home_b, i, got_buf[l, 1, p, i - half]), lambda p, i, val: None, events_b, half, half)
        dec.gather_heads()

    def finish_pages(l):
        for copy in new_copies(l):
            copy.wait()

        @pl.loop(0, half)
        def _(i):
            row = half + i
            for p in PAIR:
                page = migrated(l, p, home_a, row, last_here(l, p, row))
                last_buf[p, row] = dec.insert(page, lens_s[home_a * d.rows + row], lambda t, g: new_buf[l, p, g, t, pl.ds(i, 1), :])

        pltpu.make_async_copy(last_buf, last_out.at[l], out_sem).start()

    def last_wait(l):
        pltpu.make_async_copy(last_buf, last_out.at[l], out_sem).wait()

    def event(run):
        return lambda: run()

    def hidden_copy(at):
        return pltpu.make_async_remote_copy(y_ref.at[:, at], y_other.at[:, at], pair_send.at[0], pair_recv.at[0], device_id={'kv': exchanges[0].partner})

    def send_hidden(j):
        hidden_copy(pl.ds(aligned(j * dec.group * CHUNK, CHUNK), dec.group * CHUNK)).start()

    def wait_hidden():
        hidden_copy(pl.ds(0, d.width)).wait()

    def swap_sums():
        copy = pltpu.make_async_remote_copy(acc_other, sums_in, pair_send.at[1], pair_recv.at[1], device_id={'kv': exchanges[0].partner})
        copy.start()
        copy.wait()
        return sums_in[...]

    blocks = half // min(UNROLL, half)
    last_pair = 2 * (dec.whole // dec.group) - 1
    for l in range(d.layers):
        between_a, between_b, events = (), (), []
        if l:
            scope(f"project_{l}", project, l)
            scope(f"pages_wait_{l}", pages_wait, l)
            last_wait(l - 1)
        else:
            between_a, between_b = [(0, event(step_1)), (blocks // 2, event(pages_1))], [(0, event(step_1)), (blocks // 2, event(pages_1))]
            events = [(k * last_pair // 7, event(pages_1)) for k in range(2 * parts - 2)]
            events += [(1, event(step_1))]
        with jax.named_scope(f"attend_{l}"):
            attend(l, between_a, between_b)
        events += [(last_pair, functools.partial(scope, f"finish_{l}", finish_pages, l))]
        with jax.named_scope(f"mix_{l}"):
            dec.mix_shared(l, send_hidden, wait_hidden, swap_sums, sorted(events, key=lambda event: event[0]))
    for t in PAIR:
        ya_ref[t] = y_ref[pl.ds(t * d.rows, half), :]
        yb_ref[t] = y_ref[pl.ds(t * d.rows + half, half), :]
    last_wait(d.layers - 1)


def decode_adjacent(side, group_size, d, table, seq_lens, mig_src, mig_dst, embeds, weights, k_pool, v_pool):
    entries = mig_src.shape[0]
    half = d.rows // 2
    page = (d.page_rows, d.head_dim)
    struct = lambda *shape: jax.ShapeDtypeStruct(shape, BF16)
    groups = d.tokens // 8
    mid = pltpu.VMEM((group_size, 8, d.width * groups // group_size), BF16)
    return pl.pallas_call(
        functools.partial(adjacent_kernel, d, side, group_size, entries),
        out_shape=[struct(2, half, d.width), struct(2, half, d.width), jax.ShapeDtypeStruct((2,), jnp.int32), struct(d.layers, 2, d.rows, *page)],
        in_specs=[SMEM] * 2 + [ANY] * 11,
        out_specs=[VMEM, VMEM, SMEM, ANY],
        scratch_shapes=[
            pltpu.SMEM(table.shape, jnp.int32),
            pltpu.SMEM(seq_lens.shape, jnp.int32),
            pltpu.VMEM(table.shape, jnp.int32),
            pltpu.VMEM((groups, 8, d.width), BF16),
            pltpu.VMEM((d.tokens, d.width), BF16),
        ] + [pltpu.VMEM((d.layers, 2, 2, half) + page, BF16)] * len(PAIR) + [
            pltpu.VMEM((2, d.rows) + page, BF16),
            pltpu.VMEM((d.layers, 2, d.kv_heads, 2, half, d.head_dim), F32),
            pltpu.VMEM((d.layers, 2 * entries) + page, BF16),
        ] + [pltpu.VMEM((d.layers, entries) + page, BF16)] * len(PAIR) + [
            mid,
            mid,
            pltpu.VMEM((groups, 8, d.width), BF16),
            pltpu.VMEM((1, table.shape[1]), jnp.int32),
            pltpu.SMEM((1, table.shape[1]), jnp.int32),
            pltpu.VMEM((d.tokens, d.width), BF16),
            pltpu.VMEM((d.tokens, d.width), F32),
            pltpu.VMEM((d.tokens, d.width), F32),
            pltpu.VMEM((d.width, HALF), BF16),
            pltpu.VMEM((HALF, d.width), BF16),
        ] + [pltpu.VMEM((2 * entries,) + page, BF16)] * d.layers + [pltpu.VMEM((d.slots,) + page, BF16)] * (2 * d.layers) + d.compute_scratch(8, 6) + [
            DMA((4,)),
            DMA((d.layers, 2)),
            DMA,
        ] + [DMA(shape) for shape in ((2,), (d.layers, 2, 2), (d.layers, 2, d.kv_heads, 2), (d.layers, 10, 4)) for _ in PAIR] + [DMA] + [DMA((2,))] * 3,
        compiler_params=pltpu.CompilerParams(collective_id=1, has_side_effects=True, skip_device_barrier=True, vmem_limit_bytes=LIMIT),
        cost_estimate=d.cost(d.layers),
        name="decode_adjacent",
    )(mig_src, mig_dst, table, seq_lens, embeds.reshape(groups, 8, d.width), *weights, k_pool, v_pool)


def fill_pools_kernel(dims, group_size, info_s, table_s, src_s, k_hbm, v_hbm, last_hbm, k_out, v_out, k_buf, v_buf, sem, put_sem):
    d = dims
    me = lax.axis_index('kv')
    home = lax.rem(me - info_s[0] + group_size, group_size)
    pools = ((k_hbm, k_buf, k_out), (v_hbm, v_buf, v_out))
    parts = sem.shape[1]
    size = d.slots // parts

    def moves(part, out):
        at = pl.ds(part * size, size)
        return [pltpu.make_async_copy(*((buf.at[at], dst.at[at]) if out else (src.at[at], buf.at[at])), sem.at[p, part]) for p, (src, buf, dst) in enumerate(pools)]

    def all_parts(out, run):
        @pl.loop(0, parts)
        def _(part):
            for copy in moves(part, out):
                run(copy)

    start, wait = lambda copy: copy.start(), lambda copy: copy.wait()
    all_parts(False, start)
    all_parts(False, wait)

    @pl.loop(0, d.rows)
    def _(i):
        slot = local_slot(table_s[1, home * d.rows + i], me, d.slots)
        for p, (_, buf, _) in enumerate(pools):
            pltpu.make_async_copy(last_hbm.at[:, p, i], buf.at[slot], put_sem).start()

    @pl.loop(0, src_s.shape[0])
    def _(e):
        slot = src_s[e] - me * d.slots

        @pl.when((slot >= 0) & (slot < d.slots))
        def _():
            for _, buf, _ in pools:
                buf[local_slot(src_s[e], me, d.slots)] = jnp.zeros(buf.shape[1:], buf.dtype)

    for src, buf, _ in pools:
        pltpu.make_async_copy(src.at[pl.ds(0, d.rows)], buf.at[pl.ds(0, d.rows)], put_sem).wait()
    all_parts(True, start)
    all_parts(True, wait)


def fill_pools(group_size, d, info, table, mig_src, k_pool, v_pool, last):
    return pl.pallas_call(
        functools.partial(fill_pools_kernel, d, group_size),
        out_shape=[jax.ShapeDtypeStruct(k_pool.shape, k_pool.dtype)] * 2,
        in_specs=[SMEM] * 3 + [ANY] * 3,
        out_specs=[ANY, ANY],
        scratch_shapes=[pltpu.VMEM(k_pool.shape, k_pool.dtype), pltpu.VMEM(k_pool.shape, k_pool.dtype), DMA((2, 4)), DMA],
        compiler_params=pltpu.CompilerParams(vmem_limit_bytes=LIMIT),
        cost_estimate=d.cost(1),
        name="fill_pools",
    )(info, table, mig_src, k_pool, v_pool, last)


def gather_pages_kernel(idx_ref, k_hbm, v_hbm, k_out, v_out, sem):
    rows = k_out.shape[0]

    def copies(i):
        slot = jnp.maximum(idx_ref[i], 0)
        return (pltpu.make_async_copy(k_hbm.at[slot], k_out.at[i], sem), pltpu.make_async_copy(v_hbm.at[slot], v_out.at[i], sem))

    @pl.loop(0, rows)
    def _(i):
        @pl.when(idx_ref[i] >= 0)
        def _():
            for copy in copies(i):
                copy.start()

        @pl.when(idx_ref[i] < 0)
        def _():
            k_out[i] = jnp.zeros(k_out.shape[1:], k_out.dtype)
            v_out[i] = jnp.zeros(v_out.shape[1:], v_out.dtype)

    @pl.loop(0, rows)
    def _(i):
        @pl.when(idx_ref[i] >= 0)
        def _():
            for copy in copies(i):
                copy.wait()


def gather_pages(idx, k_pool, v_pool):
    shape = jax.ShapeDtypeStruct((idx.shape[0],) + k_pool.shape[1:], k_pool.dtype)
    return pl.pallas_call(
        gather_pages_kernel,
        out_shape=[shape, shape],
        in_specs=[SMEM, ANY, ANY],
        out_specs=[VMEM, VMEM],
        scratch_shapes=[DMA],
        compiler_params=pltpu.CompilerParams(vmem_limit_bytes=LIMIT),
        name="gather_pages",
    )(idx, k_pool, v_pool)


def share_kernel(side, k_hbm, v_hbm, k_out, v_out, work, core_buf, ring_buf, load_sem, send_sem, recv_sem, result):
    entries = k_hbm.shape[0]
    exchange = Exchange(side, 0, work, core_buf, ring_buf, result, send_sem, recv_sem)
    units = [pl.ds(p * entries, entries) for p in PAIR]
    for p, src in enumerate((k_hbm, v_hbm)):
        pltpu.make_async_copy(src, work.at[0].at[units[p]], load_sem.at[p]).start()
    for p, src in enumerate((k_hbm, v_hbm)):
        pltpu.make_async_copy(src, work.at[0].at[units[p]], load_sem.at[p]).wait()
    for _ in range(Exchange.STEPS):
        exchange.step()
    for p, dst in enumerate((k_out, v_out)):
        pltpu.make_async_copy(result.at[units[p]], dst, load_sem.at[p]).start()
    for p, dst in enumerate((k_out, v_out)):
        pltpu.make_async_copy(result.at[units[p]], dst, load_sem.at[p]).wait()


def share(side, mig_k, mig_v):
    entries = mig_k.shape[0]
    page = mig_k.shape[1:]
    return pl.pallas_call(
        functools.partial(share_kernel, side),
        out_shape=[jax.ShapeDtypeStruct(mig_k.shape, BF16)] * 2,
        in_specs=[ANY, ANY],
        out_specs=[ANY, ANY],
        scratch_shapes=[pltpu.VMEM((1, n * entries) + page, BF16) for n in (2, 1, 1)] + [DMA((2,)), DMA((1, 10, 4)), DMA((1, 10, 4)), pltpu.VMEM((2 * entries,) + page, BF16)],
        compiler_params=pltpu.CompilerParams(has_side_effects=True, vmem_limit_bytes=LIMIT),
        name="share",
    )(mig_k, mig_v)


def migrate_kernel(dst_ref, src_ref, k_hbm, v_hbm, mk_hbm, mv_hbm, k_out, v_out, k_buf, v_buf, sem, fix_sem):
    entries = dst_ref.shape[0]
    pairs = ((k_hbm, mk_hbm, k_buf, k_out), (v_hbm, mv_hbm, v_buf, v_out))
    for p, (src, _, buf, _) in enumerate(pairs):
        pltpu.make_async_copy(src, buf, sem.at[p]).start()
    for p, (src, _, buf, _) in enumerate(pairs):
        pltpu.make_async_copy(src, buf, sem.at[p]).wait()

    @pl.loop(0, entries)
    def _(e):
        @pl.when(dst_ref[e] >= 0)
        def _():
            for _, mig, buf, _ in pairs:
                copy = pltpu.make_async_copy(mig.at[e], buf.at[jnp.maximum(dst_ref[e], 0)], fix_sem)
                copy.start()
                copy.wait()

        @pl.when(src_ref[e] >= 0)
        def _():
            for _, _, buf, _ in pairs:
                buf[jnp.maximum(src_ref[e], 0)] = jnp.zeros(buf.shape[1:], buf.dtype)

    for p, (_, _, buf, dst) in enumerate(pairs):
        pltpu.make_async_copy(buf, dst, sem.at[p]).start()
    for p, (_, _, buf, dst) in enumerate(pairs):
        pltpu.make_async_copy(buf, dst, sem.at[p]).wait()


def migrate(dst_local, src_local, k_pool, v_pool, mig_k, mig_v):
    shape = jax.ShapeDtypeStruct(k_pool.shape, k_pool.dtype)
    return pl.pallas_call(
        migrate_kernel,
        out_shape=[shape, shape],
        in_specs=[SMEM, SMEM, ANY, ANY, ANY, ANY],
        out_specs=[ANY, ANY],
        scratch_shapes=[pltpu.VMEM(k_pool.shape, k_pool.dtype), pltpu.VMEM(k_pool.shape, k_pool.dtype), DMA((2,)), DMA],
        compiler_params=pltpu.CompilerParams(vmem_limit_bytes=LIMIT),
        name="migrate",
    )(dst_local, src_local, k_pool, v_pool, mig_k, mig_v)


def decode_kernel(dims, sc_ref, x_ref, p0k_hbm, p0v_hbm, wq, wk, wv, wo, wu, wd, k_in, v_in, y_ref, k_out, v_out,
                  first_buf, last_buf, *rest):
    compute, (page_sem, put_sem) = rest[:-2], rest[-2:]
    d = dims
    dec = Decoder(d, 0, d.layers, (wq, wk, wv, wo, wu, wd), y_ref, compute, 1, 2)
    dec.start_stream()
    y_ref[...] = x_ref[...]
    loads = [pltpu.make_async_copy(src, first_buf.at[p], page_sem.at[p]) for p, src in enumerate((p0k_hbm, p0v_hbm))]
    for load in loads:
        load.start()

    def last_loads(run):
        @pl.loop(0, d.rows)
        def _(i):
            for p, src in enumerate((k_in, v_in)):
                run(pltpu.make_async_copy(src.at[sc_ref[0, i]], last_buf.at[p, i], page_sem.at[2]))

    def puts(run):
        @pl.loop(0, d.rows)
        def _(i):
            @pl.when(sc_ref[2, i] > 0)
            def _():
                for p, dst in enumerate((k_out, v_out)):
                    run(pltpu.make_async_copy(last_buf.at[p, i], dst.at[sc_ref[0, i]], put_sem))

    last_loads(lambda copy: copy.start())
    for load in loads:
        load.wait()
    last_loads(lambda copy: copy.wait())

    @pl.loop(0, d.layers)
    def _(layer):
        def put_page(p, i, val):
            last_buf[p, i, layer] = val

        dec.project(layer)
        dec.attend(lambda i: sc_ref[1, i], lambda p, i: first_buf[p, i, layer], lambda p, i: last_buf[p, i, layer], put_page)
        dec.gather_heads()
        dec.mix(layer)

    puts(lambda copy: copy.start())
    puts(lambda copy: copy.wait())


def decode(d, scalars, x, p0k, p0v, weights, k_pool, v_pool):
    pool = jax.ShapeDtypeStruct(k_pool.shape, k_pool.dtype)
    pages = pltpu.VMEM((2, d.rows, d.layers, d.page_rows, d.head_dim), BF16)
    return pl.pallas_call(
        functools.partial(decode_kernel, d),
        out_shape=[jax.ShapeDtypeStruct(x.shape, x.dtype), pool, pool],
        in_specs=[SMEM, VMEM] + [ANY] * 10,
        out_specs=[VMEM, ANY, ANY],
        input_output_aliases={10: 1, 11: 2},
        scratch_shapes=[pages, pages] + d.compute_scratch(16, 16) + [DMA((3,)), DMA],
        compiler_params=pltpu.CompilerParams(vmem_limit_bytes=LIMIT),
        cost_estimate=d.cost(d.layers),
        name="decode",
    )(scalars, x, p0k, p0v, *weights, k_pool, v_pool)


def permute(arrays, shift, group_size):
    if shift == group_size // 2:
        return permute(permute(arrays, shift // 2, group_size), shift // 2, group_size)
    perm = [(i, (i + shift) % group_size) for i in range(group_size)]
    return jax.tree.map(lambda a: lax.ppermute(a, 'kv', perm), arrays) if shift else arrays


def rotate_back(first, second, shift, group_size, beside):
    def branch(r):
        def run(args):
            parts = permute(args[0], -r % group_size, group_size), permute(args[1], (1 - r) % group_size, group_size)
            return jnp.concatenate(parts, axis=1), beside()

        return run

    return lax.switch(shift, [branch(r) for r in range(group_size)], (first, second))


def rotate(arrays, shift, group_size):
    stride = math.isqrt(2 * group_size)
    for count, move in ((shift // stride, stride), (shift % stride, 1)):
        arrays = lax.fori_loop(0, count, lambda _, a: permute(a, move, group_size), arrays)
    return arrays


def solution(mesh):
    group_size = mesh.shape['kv']
    side = math.isqrt(group_size // 2)
    pool_spec = P(('rep', 'kv'))
    tok_spec = P(None, ('rep', 'kv'), None)

    def device_fn(embeds, w_query, w_key, w_value, w_out, w_up, w_down, k_pool5, v_pool5, new_table, seq_lens, mig_src, mig_dst):
        me = lax.axis_index('kv')
        slots, layers, page, kv_heads, head_dim = k_pool5.shape
        rows, width = embeds.shape[1:]
        weights = (w_query, w_key, w_value, w_out, w_up, w_down)
        k_pool = k_pool5.reshape(slots, layers, page * kv_heads, head_dim)
        v_pool = v_pool5.reshape(slots, layers, page * kv_heads, head_dim)
        d = Dims(rows, weights, k_pool, page)
        ints = jnp.int32

        def local(ids):
            loc = ids - me * slots
            return jnp.where((loc >= 0) & (loc < slots), loc, -1)

        def take(vec, dev):
            return lax.dynamic_slice(vec, (dev * rows,), (rows,))

        def inside(ids):
            return local_slot(ids, me, slots)

        def general_path():
            first_new, last_new = new_table[:, 0], new_table[:, 1]
            moved = first_new[None, :] == mig_dst[:, None]
            first_old = jnp.where(jnp.any(moved, axis=0), jnp.sum(jnp.where(moved, mig_src[:, None], 0), axis=0), first_new)
            home = jnp.arange(first_new.shape[0], dtype=ints) // rows
            worker = last_new // slots
            shift_of = (worker - home + group_size) % group_size
            first_shift = (worker - first_old // slots + group_size) % group_size
            shift_ids = jnp.arange(group_size, dtype=ints)
            wanted = jnp.any(shift_of[None, :] == shift_ids[:, None], axis=1)
            mig_k, mig_v = gather_pages(local(mig_src), k_pool, v_pool)
            by_layer = tuple(m.swapaxes(0, 1) for m in (mig_k, mig_v))
            mig_k, mig_v = (m.swapaxes(0, 1) for m in lax.map(lambda pages: tuple(share(side, *pages)), by_layer))
            k_new, v_new = migrate(local(mig_dst), local(mig_src), k_pool, v_pool, mig_k, mig_v)

            def one_round(shift, y, k_new, v_new):
                src_home = (me - shift + group_size) % group_size
                x = rotate(embeds.reshape(2 * rows, width), shift, group_size)
                in_round = shift_of == shift
                wanted2 = jnp.any(in_round[None, :] & (first_shift[None, :] == shift_ids[:, None]), axis=1)

                def more(state):
                    left, pk, pv = state
                    shift2 = jnp.argmax(left).astype(ints)
                    dest_home = (me + shift2 - shift + group_size) % group_size
                    got = gather_pages(inside(take(first_old, dest_home)), k_pool, v_pool)
                    got_k, got_v = rotate(tuple(got), shift2, group_size)
                    mine = (take(first_shift, src_home) == shift2)[:, None, None, None]
                    return left & (shift_ids != shift2), jnp.where(mine, got_k, pk), jnp.where(mine, got_v, pv)

                zeros = jnp.zeros((rows,) + k_pool.shape[1:], k_pool.dtype)
                _, pk, pv = lax.while_loop(lambda state: jnp.any(state[0]), more, (wanted2, zeros, zeros))
                valid = take(shift_of, src_home) == shift
                scalars = jnp.stack([inside(take(last_new, src_home)), take(seq_lens, src_home), valid.astype(ints)])
                out, k_new, v_new = decode(d, scalars, x, pk, pv, weights, k_new, v_new)
                back = rotate(out, (group_size - shift) % group_size, group_size)
                mine = (take(shift_of, me) == shift)[None, :, None]
                return jnp.where(mine, back.reshape(embeds.shape), y), k_new, v_new

            def next_round(state):
                left, y, k_new, v_new = state
                shift = jnp.argmax(left).astype(ints)
                y, k_new, v_new = one_round(shift, y, k_new, v_new)
                return left & (shift_ids != shift), y, k_new, v_new

            _, y, k_new, v_new = lax.while_loop(lambda state: jnp.any(state[0]), next_round, (wanted, jnp.zeros_like(embeds), k_new, v_new))
            return y, k_new, v_new

        table = new_table.T
        ya, yb, info, last = decode_adjacent(side, group_size, d, table, seq_lens, mig_src, mig_dst, embeds, weights, k_pool, v_pool)
        y, (k_new, v_new) = rotate_back(ya, yb, info[0], group_size, lambda: fill_pools(group_size, d, info, table, mig_src, k_pool, v_pool, last))
        _, y, k_new, v_new = lax.while_loop(lambda state: state[0] == 0, lambda state: (jnp.ones_like(state[0]),) + general_path(), (info[1], y, k_new, v_new))
        return y, k_new.reshape(k_pool5.shape), v_new.reshape(v_pool5.shape)

    return jax.shard_map(device_fn, mesh=mesh, in_specs=(tok_spec, P(), P(), P(), P(), P(), P(), pool_spec, pool_spec, P('rep', None), P('rep'), P('rep'), P('rep')), out_specs=(tok_spec, pool_spec, pool_spec), check_vma=False)
```

```python
import functools
import math

import jax
import jax.numpy as jnp
from jax import lax
from jax.experimental import pallas as pl
from jax.experimental.pallas import tpu as pltpu
from jax.sharding import PartitionSpec as P

ANY = pl.BlockSpec(memory_space=pl.ANY)
SMEM = pl.BlockSpec(memory_space=pltpu.SMEM)
VMEM = pl.BlockSpec(memory_space=pltpu.VMEM)
DMA = pltpu.SemaphoreType.DMA
CHUNK = 256
UNROLL = 8
MLP_GROUP = 3
LANES = 128
HALF = CHUNK // 2
PAIR = (0, 1)
LIMIT = 1023 << 16
F32, BF16 = jnp.float32, jnp.bfloat16


def iota(shape, axis):
    return lax.broadcasted_iota(jnp.int32, shape, axis)


def dot(a, b):
    return jnp.dot(a, b, preferred_element_type=F32)


def local_slot(ids, me, slots):
    return jnp.clip(ids - me * slots, 0, slots - 1)


def aligned(x, multiple):
    return x if isinstance(x, int) else pl.multiple_of(x, multiple)


class Dims:
    def __init__(self, rows, weights, k_pool, page):
        w_query, w_key, _, _, w_up, _ = weights
        self.layers, self.width, self.q_width = w_query.shape
        self.ff = w_up.shape[2]
        self.slots, _, self.page_rows, self.head_dim = k_pool.shape
        self.kv_heads = w_key.shape[2] // self.head_dim
        self.heads = self.q_width // self.head_dim
        self.page, self.rows = page, rows
        self.tokens = 2 * rows
        self.stride = self.tokens + 8
        self.n_q, self.n_o, self.n_u = self.q_width // CHUNK, self.width // CHUNK, self.ff // CHUNK

    def compute_scratch(self, n_col, n_row):
        return [
            pltpu.VMEM((n_col, self.width, CHUNK), BF16),
            pltpu.VMEM((n_row, CHUNK, self.width), BF16),
            pltpu.VMEM((self.heads * self.stride, self.head_dim), F32),
            pltpu.VMEM((self.kv_heads * self.stride, self.head_dim), F32),
            pltpu.VMEM((self.kv_heads * self.stride, self.head_dim), F32),
            pltpu.VMEM((self.heads * self.stride, self.head_dim), F32),
            pltpu.VMEM((self.tokens, self.q_width), BF16),
            pltpu.VMEM((self.tokens, self.ff), BF16),
            pltpu.VMEM((self.tokens, self.width), F32),
            DMA((n_col,)),
            DMA((n_row,)),
        ]

    def cost(self, layers):
        size = layers * self.width * (2 * self.q_width + 2 * self.kv_heads * self.head_dim + 2 * self.ff)
        return pl.CostEstimate(flops=2 * size * self.tokens, bytes_accessed=2 * size, transcendentals=0)


class Decoder:
    def __init__(self, dims, first, layers, weights, y_ref, scratch, group=2, unroll=UNROLL, shared=False):
        self.group, self.unroll, self.shared = group, unroll, shared
        self.d, self.first, self.layers, self.weights, self.y_ref = dims, first, layers, weights, y_ref
        (self.col_buf, self.row_buf, self.q_s, self.kn_s, self.vn_s, self.o_s, self.att, self.act, self.acc, self.col_sem, self.row_sem) = scratch
        self.n_col, self.n_row = self.col_buf.shape[0], self.row_buf.shape[0]
        self.zero = lax.axis_index('kv') * 0
        d = dims
        self.whole = d.ff // 2 // CHUNK if shared else d.n_u
        self.begin = lax.axis_index('kv') % 2 * (d.ff // 2) if shared else 0
        self.col_layer = d.n_q + 2 + d.n_o + self.whole
        cols = 2 * d.page * d.kv_heads
        col_pos = iota((2 * d.heads, cols), 1)
        row_pos = iota((2 * d.heads, cols), 0)
        same_head = (col_pos % d.kv_heads) == (row_pos % d.heads) // (d.heads // d.kv_heads)
        self.limit = jnp.where(same_head, col_pos // d.kv_heads - row_pos // d.heads, 4 * d.page)
        self.page_pos = iota((d.page_rows, d.head_dim), 0) // d.kv_heads
        self.tile_head = iota((8, d.head_dim), 0) % d.kv_heads

    def layer_of(self, g, per_layer):
        return sum((g >= per_layer * l).astype(jnp.int32) for l in range(1, self.layers))

    def col_start(self, g):
        d = self.d
        wq, wk, wv, wo, wu, _ = self.weights

        @pl.when(g < self.layers * self.col_layer)
        def _():
            layer = self.layer_of(g, self.col_layer)
            pos = g - layer * self.col_layer
            slot = g % self.n_col

            def go(src, c, begin=0):
                start = aligned(c * CHUNK + begin, LANES)
                pltpu.make_async_copy(src.at[self.first + layer].at[:, pl.ds(start, CHUNK)], self.col_buf.at[slot], self.col_sem.at[slot]).start()

            @pl.when(pos < d.n_q)
            def _():
                go(wq, pos)

            @pl.when(pos == d.n_q)
            def _():
                go(wk, 0)

            @pl.when(pos == d.n_q + 1)
            def _():
                go(wv, 0)

            @pl.when((pos >= d.n_q + 2) & (pos < d.n_q + 2 + d.n_o))
            def _():
                go(wo, pos - (d.n_q + 2))

            @pl.when(pos >= d.n_q + 2 + d.n_o)
            def _():
                go(wu, pos - (d.n_q + 2 + d.n_o), self.begin)

    def row_start(self, g):
        d = self.d
        wd = self.weights[5]

        @pl.when(g < self.layers * self.whole)
        def _():
            layer = self.layer_of(g, self.whole)
            slot = g % self.n_row
            start = aligned((g - layer * self.whole) * CHUNK + self.begin, LANES)
            pltpu.make_async_copy(wd.at[self.first + layer].at[pl.ds(start, CHUNK)], self.row_buf.at[slot], self.row_sem.at[slot]).start()

    def start_stream(self):
        @pl.loop(0, self.n_col)
        def _(g):
            self.col_start(g)

        @pl.loop(0, self.n_row)
        def _(g):
            self.row_start(g)

    def with_cols(self, g, count, body):
        slots = [(g + u) % self.n_col for u in range(count)]
        for slot in slots:
            pltpu.make_async_copy(self.weights[1].at[0], self.col_buf.at[slot], self.col_sem.at[slot]).wait()
        body([self.col_buf.at[slot] for slot in slots])
        for u in range(count):
            self.col_start(g + u + self.n_col)

    def with_rows(self, g, count, body):
        slots = [(g + u) % self.n_row for u in range(count)]
        for slot in slots:
            pltpu.make_async_copy(self.weights[5].at[0, pl.ds(0, CHUNK), :], self.row_buf.at[slot], self.row_sem.at[slot]).wait()
        body([self.row_buf.at[slot] for slot in slots])
        for u in range(count):
            self.row_start(g + u + self.n_row)

    def project(self, layer):
        d = self.d
        col0 = (self.zero + layer) * self.col_layer

        def product(ref):
            return dot(self.y_ref[...], ref[...]).astype(BF16).astype(F32)

        def put(dst, first, out):
            for h in range(CHUNK // d.head_dim):
                at = aligned((first + h) * d.stride, 8)
                dst[pl.ds(at, d.tokens), :] = out[:, h * d.head_dim:(h + 1) * d.head_dim]

        many = self.group

        @pl.loop(0, d.n_q // many)
        def _(j):
            def body(refs):
                outs = [product(ref) for ref in refs]
                for u in range(many):
                    put(self.q_s, (many * j + u) * (CHUNK // d.head_dim), outs[u])

            self.with_cols(col0 + many * j, many, body)

        def body(refs):
            outs = [product(ref) for ref in refs]
            put(self.kn_s, 0, outs[0])
            put(self.vn_s, 0, outs[1])

        self.with_cols(col0 + d.n_q, 2, body)

    def insert(self, page, n, row):
        d = self.d
        val = page.astype(F32)
        for t in PAIR:
            new = jnp.broadcast_to(row(t, 0), (8, d.head_dim))
            for g in range(1, d.kv_heads):
                new = jnp.where(self.tile_head == g, row(t, g), new)
            val = jnp.where(self.page_pos == n - d.page + t, jnp.concatenate([new] * (d.page_rows // 8), axis=0), val)
        return val.astype(BF16)

    def attend(self, lens, first_page, last_page, put_page, events=(), begin=0, count=None):
        d = self.d
        count = count or d.rows
        unroll = min(self.unroll, count)

        def some(first):
            ids = [first + u for u in range(unroll)]
            scores, vals = [], []
            for i in ids:
                n = lens(i)

                def updated(p, new_ref):
                    val = self.insert(last_page(p, i), n, lambda t, g: new_ref[pl.ds(g * d.stride + t * d.rows + i, 1), :])
                    put_page(p, i, val)
                    return val

                keys = jnp.concatenate([first_page(0, i), updated(0, self.kn_s)], axis=0)
                vals.append(updated(1, self.vn_s))
                qs = jnp.concatenate([self.q_s[pl.ds(t * d.rows + i, d.heads, stride=d.stride), :] for t in PAIR], axis=0)
                score = lax.dot_general(qs.astype(BF16), keys, (((1,), (1,)), ((), ())), preferred_element_type=F32) * d.head_dim ** -0.5
                scores.append(jnp.where(self.limit <= n, score, -jnp.inf))
            tops = [jnp.max(score, axis=1, keepdims=True) for score in scores]
            probs = [jnp.exp(score - top) for score, top in zip(scores, tops)]
            totals = [jnp.sum(prob, axis=1, keepdims=True) for prob in probs]
            for u, i in enumerate(ids):
                both = jnp.concatenate([first_page(1, i), vals[u]], axis=0)
                out = dot(probs[u].astype(BF16), both) / totals[u]
                for t in PAIR:
                    self.o_s[pl.ds(t * d.rows + i, d.heads, stride=d.stride), :] = out[t * d.heads:(t + 1) * d.heads]

        @pl.loop(0, count // unroll)
        def _(block):
            for k, run in events:
                pl.when(block == k)(run)
            some(begin + block * unroll)

    def gather_heads(self):
        d = self.d
        for h in range(d.heads):
            self.att[:, h * d.head_dim:(h + 1) * d.head_dim] = self.o_s[h * d.stride:h * d.stride + d.tokens, :].astype(BF16)

    def span(self, j):
        return pl.ds(aligned(j * CHUNK, CHUNK), CHUNK)

    def out_project(self, layer, after=None):
        d, many = self.d, self.group

        @pl.loop(0, d.n_o // many)
        def _(j):
            def body(refs):
                outs = [dot(self.att[...], ref[...]) for ref in refs]
                for u in range(many):
                    at = self.span(many * j + u)
                    self.y_ref[:, at] = (self.y_ref[:, at].astype(F32) + outs[u]).astype(BF16)

            self.with_cols(layer * self.col_layer + d.n_q + len(PAIR) + many * j, many, body)
            if after:
                after(j)

    def mix(self, layer, events=()):
        d = self.d
        layer = self.zero + layer
        col0 = layer * self.col_layer + d.n_q + 2
        many = self.group
        pairs = d.n_u // many

        def between(j, first):
            for k, run in events:
                if first <= k < first + pairs:
                    pl.when(j == k - first)(run)

        self.out_project(layer)

        def up(first, count):
            def body(refs):
                ups = [dot(self.y_ref[...], ref[...]) for ref in refs]
                for u in range(count):
                    self.act[:, self.span(first + u)] = jax.nn.gelu(ups[u].astype(BF16).astype(F32), approximate=True).astype(BF16)

            self.with_cols(col0 + d.n_o + first, count, body)

        def down(first, count):
            def body(refs):
                out = self.acc[...]
                for u in range(count):
                    out += dot(self.act[:, self.span(first + u)], refs[u][...])
                self.acc[...] = out

            self.with_rows(layer * self.whole + first, count, body)

        @pl.loop(0, pairs)
        def _(j):
            between(j, 0)
            up(many * j, many)

        if d.n_u % many:
            up(d.n_u - 1, 1)

        self.acc[...] = self.y_ref[...].astype(F32)

        @pl.loop(0, pairs)
        def _(j):
            between(j, pairs)
            down(many * j, many)

        if d.n_u % many:
            down(d.n_u - 1, 1)

        self.y_ref[...] = self.acc[...].astype(BF16)


    def half_loads(self, layer):
        at = pl.ds(aligned(self.begin + self.whole * CHUNK, LANES), HALF)
        return (pltpu.make_async_copy(self.weights[4].at[layer].at[:, at], self.half_col, self.half_sem.at[0]),
                pltpu.make_async_copy(self.weights[5].at[layer].at[at], self.half_row, self.half_sem.at[1]))

    def mix_shared(self, layer, send_hidden, wait_hidden, swap_sums, events=()):
        d = self.d
        half_loads, next_loads = self.half_loads(layer), self.half_loads(layer + 1) if layer + 1 < d.layers else ()
        layer = self.zero + layer
        col0 = layer * self.col_layer + d.n_q + 2
        many = MLP_GROUP
        rows = d.tokens
        offset = d.ff // 2
        pairs = self.whole // many

        def between(j, first):
            for k, run in events:
                if first <= k < first + pairs:
                    pl.when(j == k - first)(run)

        self.out_project(layer, send_hidden)

        self.acc[...] = self.y_ref[...].astype(F32)
        self.acc_other[...] = jnp.zeros_like(self.acc_other)
        wait_hidden()

        def hidden():
            return jnp.concatenate([self.y_ref[...], self.y_other[...]], axis=0)

        def activate(up, at, size):
            val = jax.nn.gelu(up.astype(BF16).astype(F32), approximate=True).astype(BF16)
            self.act[:, pl.ds(aligned(at, LANES), size)] = val[:rows]
            self.act[:, pl.ds(aligned(at + offset, LANES), size)] = val[rows:]

        @pl.loop(0, pairs)
        def _(j):
            between(j, 0)

            def body(refs):
                ups = [dot(hidden(), ref[...]) for ref in refs]
                for u in range(many):
                    activate(ups[u], (many * j + u) * CHUNK, CHUNK)

            self.with_cols(col0 + d.n_o + many * j, many, body)

        tail = self.whole % many
        for u in range(tail):
            def body(refs, at=(self.whole - tail + u) * CHUNK):
                activate(dot(hidden(), refs[0][...]), at, CHUNK)

            self.with_cols(col0 + d.n_o + self.whole - tail + u, 1, body)
        for copy in half_loads:
            copy.wait()
        activate(dot(hidden(), self.half_col[...]), self.whole * CHUNK, HALF)

        def acts(at, size):
            return jnp.concatenate([self.act[:, pl.ds(aligned(at, LANES), size)], self.act[:, pl.ds(aligned(at + offset, LANES), size)]], axis=0)

        def add(out):
            self.acc[...] += out[:rows]
            self.acc_other[...] += out[rows:]

        @pl.loop(0, pairs)
        def _(j):
            between(j, pairs)

            def body(refs):
                add(sum(dot(acts((many * j + u) * CHUNK, CHUNK), refs[u][...]) for u in range(many)))

            self.with_rows(layer * self.whole + many * j, many, body)

        for u in range(tail):
            def body(refs, at=(self.whole - tail + u) * CHUNK):
                add(dot(acts(at, CHUNK), refs[0][...]))

            self.with_rows(layer * self.whole + self.whole - tail + u, 1, body)
        add(dot(acts(self.whole * CHUNK, HALF), self.half_row[...]))
        for copy in next_loads:
            copy.start()
        self.y_ref[...] = (self.acc[...] + swap_sums()).astype(BF16)


class Exchange:
    STEPS = 11

    def __init__(self, side, layer, work, core_buf, ring_buf, out, send_sem, recv_sem):
        self.layer = layer
        self.work, self.core_buf, self.ring_buf, self.out, self.send_sem, self.recv_sem = work, core_buf, ring_buf, out, send_sem, recv_sem
        me = lax.axis_index('kv')
        core, x, y = me % 2, me // 2 % side, me // (2 * side)

        def pairings(pos, stride):
            return (((pos + 1) // 2 % 2, me + (1 - 2 * (pos % 2)) * stride), (pos // 2, me + (side - 1 - 2 * pos) * stride))

        xs, ys = pairings(x, 2), pairings(y, 2 * side)
        self.orders = [xs + ys, xs[::-1] + ys[::-1], ys + xs, ys[::-1] + xs[::-1]]
        self.partner = me + 1 - 2 * core
        self.peers = [self.partner] + [dev for _, dev in xs + ys]
        self.half = work.shape[1] // 2
        self.stream = self.half // 4
        self.base, self.other = core * self.half, (1 - core) * self.half
        self.copies, self.done = [], 0
        self.path = [[self.base + k * self.stream for k in range(4)]]
        self.away = []
        for ring in range(4):
            size = self.stream >> (ring + 1)
            self.away.append([self.path[-1][k] + (1 - self.orders[k][ring][0]) * size for k in range(4)])
            self.path.append([self.path[-1][k] + self.orders[k][ring][0] * size for k in range(4)])

    def send(self, src, dst, step, lane, dev):
        def copy():
            return pltpu.make_async_remote_copy(src(), dst(), self.send_sem.at[self.layer, step, lane], self.recv_sem.at[self.layer, step, lane], device_id={'kv': dev})

        copy().start()
        self.copies.append(copy)

    def units(self, ref, at, count):
        return lambda: ref.at[self.layer].at[pl.ds(at, count)]

    def results(self, at, count):
        return lambda: self.out.at[pl.ds(at, count)]

    def add(self, dst_at, buf, src_at, count):
        @pl.loop(0, count)
        def _(u):
            self.work[self.layer, dst_at + u] = self.work[self.layer, dst_at + u] + buf[self.layer, src_at + u]

    def halve(self, ring, k):
        size = self.stream >> (ring + 1)
        src = self.units(self.work, self.away[ring][k], size)
        self.send(src, self.units(self.ring_buf, (k + 1) * self.stream - 2 * size, size), 1 + ring, k, self.orders[k][ring][1])

    def halved(self, ring, k):
        size = self.stream >> (ring + 1)
        self.add(self.path[ring + 1][k], self.ring_buf, (k + 1) * self.stream - 2 * size, size)

    def double(self, ring, k):
        at = self.results(self.path[ring + 1][k], self.stream >> (ring + 1))
        self.send(at, at, 8 - ring, k, self.orders[k][ring][1])

    def step(self):
        step, self.done = self.done, self.done + 1
        started, self.copies = self.copies, []
        if step in (1, 9, 10):
            for copy in started:
                copy().wait()
        if step == 0:
            self.send(self.units(self.work, self.other, self.half), self.units(self.core_buf, 0, self.half), 0, 0, self.partner)
        elif step == 1:
            self.add(self.base, self.core_buf, 0, self.half)
            for k in range(4):
                self.halve(0, k)
        elif step < 9:
            for k in range(4):
                started[k]().wait()
                if step < 6:
                    self.halved(step - 2, k)
                if step < 5:
                    self.halve(step - 1, k)
                    continue
                if step == 5:
                    for u in range(self.stream >> 4):
                        self.out[self.path[4][k] + u] = self.work[self.layer, self.path[4][k] + u]
                self.double(8 - step, k)
        elif step == 9:
            at = self.results(self.base, self.half)
            self.send(at, at, 9, 0, self.partner)


def adjacent_kernel(dims, side, group_size, entries, src_s, dst_s, table_hbm, lens_hbm, embeds_hbm, wq, wk, wv, wo, wu, wd, k_hbm, v_hbm,
                    ya_ref, yb_ref, info_s, last_out,
                    table_s, lens_s, table_v, embeds_v, y_ref, send_buf, got_buf, last_buf, new_buf, work, core_buf, ring_buf, mid_in, mid_out, x_in, plan_v, plan_s, y_other, acc_other, sums_in, half_col, half_row, *rest):
    d = dims
    migs, rest = rest[:d.layers], rest[d.layers:]
    pools, rest = [rest[2 * l:2 * l + 2] for l in range(d.layers)], rest[2 * d.layers:]
    compute, (load_sem, pool_sem, plan_sem, x_send, x_recv, page_send, page_recv, new_send, new_recv, mig_send, mig_recv, out_sem, half_sem, pair_send, pair_recv) = rest[:-15], rest[-15:]
    half = d.rows // 2
    me = lax.axis_index('kv')
    ahead, behind = lax.rem(me + 1, group_size), lax.rem(me + group_size - 1, group_size)
    dec = Decoder(d, 0, d.layers, (wq, wk, wv, wo, wu, wd), y_ref, compute, shared=True)
    dec.y_other, dec.acc_other, dec.half_col, dec.half_row, dec.half_sem = y_other, acc_other, half_col, half_row, half_sem
    exchanges = [Exchange(side, l, work, core_buf, ring_buf, migs[l], mig_send, mig_recv) for l in range(d.layers)]

    def scope(name, run, *args):
        with jax.named_scope(name):
            return run(*args)

    pool_loads = [[pltpu.make_async_copy(src.at[:, l], pools[l][p], pool_sem.at[l, p]) for p, src in enumerate((k_hbm, v_hbm))] for l in range(d.layers)]
    embeds_load, table_load, lens_load, table_load_v = [
        pltpu.make_async_copy(src, dst, load_sem.at[i]) for i, (src, dst) in enumerate(((embeds_hbm, embeds_v), (table_hbm, table_s), (lens_hbm, lens_s), (table_hbm, table_v)))]
    for load in [embeds_load] + pool_loads[0] + [table_load, table_load_v, lens_load]:
        load.start()
    barrier = pltpu.get_barrier_semaphore()

    @pl.loop(1, group_size)
    def _(r):
        pl.semaphore_signal(barrier, inc=1, device_id={'kv': lax.rem(me + r, group_size)})

    scope("barrier", lambda: pl.semaphore_wait(barrier, group_size - 1))

    groups = d.tokens // 8
    splits = group_size // groups
    cols = d.width // splits

    def piece(ref, m):
        return ref.at[m // splits, :, pl.ds(aligned(m % splits * cols, cols), cols)]

    def all_pieces(phase):
        some = mid_in.at[pl.ds(0, group_size - 1)]
        pltpu.make_async_remote_copy(some, some, x_send.at[phase], x_recv.at[phase], device_id={'kv': me}).wait()

    def send_embeddings():
        embeds_load.wait()

        @pl.loop(1, group_size)
        def _(r):
            m = lax.rem(me + r, group_size)
            pltpu.make_async_remote_copy(piece(embeds_v, m), mid_in.at[me], x_send.at[0], x_recv.at[0], device_id={'kv': m}).start()

        mid_in[me] = piece(embeds_v, me)[...]

    def load_tables():
        for load in (table_load, lens_load, table_load_v):
            load.wait()
        return lax.rem(table_s[1, 0] // d.slots + group_size, group_size)

    scope("pool_wait_0", lambda: [load.wait() for load in pool_loads[0]])

    def own(l):
        @pl.loop(0, entries)
        def _(e):
            slot = src_s[e] - me * d.slots
            mine = (slot >= 0) & (slot < d.slots)
            slot = local_slot(src_s[e], me, d.slots)
            for p in PAIR:
                page = pools[l][p][slot]
                work[l, p * entries + e] = jnp.where(mine, page, jnp.zeros_like(page))

    def step(l):
        scope(f"exchange_{l}_{exchanges[l].done}", exchanges[l].step)

    step_0, step_1 = functools.partial(step, 0), functools.partial(step, 1)

    scope("own_0", own, 0)
    step_0()
    for l in range(1, d.layers):
        for load in pool_loads[l]:
            load.start()
    scope("start_stream", dec.start_stream)
    for copy in dec.half_loads(0):
        copy.start()
    shift = scope("load_tables", load_tables)
    home_a = lax.rem(me - shift + group_size, group_size)
    home_b = lax.rem(home_a + 1, group_size)

    def clipped(slot):
        return local_slot(slot, me, d.slots)

    def first_here(l, p, i):
        return pools[l][p][clipped(table_s[0, home_b * d.rows + i])]

    def last_here(l, p, i):
        return pools[l][p][clipped(table_s[1, home_a * d.rows + i])]

    def migrated(l, p, home, i, page):
        entry = plan_s[0, home * d.rows + i]
        return jnp.where(entry >= 0, migs[l][p * entries + jnp.maximum(entry, 0)], page)

    def pack(l):
        @pl.loop(0, half)
        def _(i):
            for p in PAIR:
                send_buf[l, 0, p, i] = first_here(l, p, i)
                send_buf[l, 1, p, i] = last_here(l, p, half + i)

    parts = 4
    size = half // parts

    def page_copy(l, way, p, rows):
        return pltpu.make_async_remote_copy(
            send_buf.at[l, way, p, rows], got_buf.at[l, way, p, rows], page_send.at[l, way, p], page_recv.at[l, way, p], device_id={'kv': (ahead, behind)[way]})

    pieces = [iter([(p, part) for part in range(parts) for p in PAIR]) for _ in range(d.layers)]

    def pages_start(l):
        p, part = next(pieces[l])
        for way in PAIR:
            page_copy(l, way, p, pl.ds(part * size, size)).start()

    pages_0, pages_1 = functools.partial(pages_start, 0), functools.partial(pages_start, 1)

    def pages_wait(l):
        for way in PAIR:
            for p in PAIR:
                page_copy(l, way, p, pl.ds(0, half)).wait()

    def pass_on():
        all_pieces(0)
        later = me // splits * 8 % d.rows // half

        @pl.loop(0, group_size)
        def _(m):
            mid_out[m] = mid_in[lax.rem(m - shift + later + group_size, group_size)]

        @pl.loop(1, group_size)
        def _(r):
            m = lax.rem(me + r, group_size)
            pltpu.make_async_remote_copy(mid_out.at[m], piece(x_in, me), x_send.at[1], x_recv.at[1], device_id={'kv': m}).start()

        piece(x_in, me)[...] = mid_out[me]

    def take_embeddings():
        all_pieces(1)
        y_ref[...] = x_in[...].reshape(d.tokens, d.width)

    plan_copy = pltpu.make_async_copy(plan_v, plan_s, plan_sem)

    def plan():
        seq = iota((1, table_v.shape[1]), 1)
        worker = lax.rem(seq // d.rows + shift, group_size)
        before = lax.rem(worker + group_size - 1, group_size)
        first, last = table_v[0:1, :], table_v[1:2, :]
        bad = (last < worker * d.slots) | (last >= worker * d.slots + d.slots) | (first < before * d.slots) | (first >= before * d.slots + d.slots)

        def entry(e, state):
            plan, bad = state
            return jnp.where(last == dst_s[e], e, plan), bad | (first == dst_s[e]).astype(jnp.int32)

        plan, bad = lax.fori_loop(0, entries, entry, (jnp.full_like(last, -1), bad.astype(jnp.int32)))
        plan_v[...] = plan
        plan_copy.start()
        info_s[0] = shift
        info_s[1] = 1 - jnp.max(bad)

    def new_copies(l):
        return [pltpu.make_async_remote_copy(
            ref.at[pl.ds(g * d.stride + t * d.rows + half, half)], new_buf.at[l, p, g, t], new_send.at[l, p, g, t], new_recv.at[l, p, g, t], device_id={'kv': ahead})
            for p, ref in enumerate((dec.kn_s, dec.vn_s)) for g in range(d.kv_heads) for t in PAIR]

    def project(l):
        dec.project(l)
        for copy in new_copies(l):
            copy.start()

    scope("pack_0", pack, 0)
    step_0()
    scope("send_embeddings", send_embeddings)
    pages_0()
    scope("plan", plan)
    step_0()
    pages_0()
    for l in range(1, d.layers):
        for load in pool_loads[l]:
            load.wait()
    scope("own_1", own, 1)

    def both():
        step_0()
        pages_0()
        step_1()

    both()
    scope("pass_on", pass_on)
    both()
    both()
    scope("pack_1", pack, 1)
    both()
    scope("take_embeddings", take_embeddings)
    both()
    scope("project_0", project, 0)
    both()
    plan_copy.wait()
    step_0()
    step_1()
    step_0()
    scope("pages_wait_0", pages_wait, 0)

    def attend(l, events_a, events_b):
        def put_page(p, i, val):
            last_buf[p, i] = val

        dec.attend(lambda i: lens_s[home_a * d.rows + i], lambda p, i: got_buf[l, 0, p, i],
                   lambda p, i: migrated(l, p, home_a, i, last_here(l, p, i)), put_page, events_a, 0, half)
        dec.attend(lambda i: lens_s[home_b * d.rows + i], lambda p, i: first_here(l, p, i),
                   lambda p, i: migrated(l, p, home_b, i, got_buf[l, 1, p, i - half]), lambda p, i, val: None, events_b, half, half)
        dec.gather_heads()

    def finish_pages(l):
        for copy in new_copies(l):
            copy.wait()

        @pl.loop(0, half)
        def _(i):
            row = half + i
            for p in PAIR:
                page = migrated(l, p, home_a, row, last_here(l, p, row))
                last_buf[p, row] = dec.insert(page, lens_s[home_a * d.rows + row], lambda t, g: new_buf[l, p, g, t, pl.ds(i, 1), :])

        pltpu.make_async_copy(last_buf, last_out.at[l], out_sem).start()

    def last_wait(l):
        pltpu.make_async_copy(last_buf, last_out.at[l], out_sem).wait()

    def event(run):
        return lambda: run()

    def hidden_copy(at):
        return pltpu.make_async_remote_copy(y_ref.at[:, at], y_other.at[:, at], pair_send.at[0], pair_recv.at[0], device_id={'kv': exchanges[0].partner})

    def send_hidden(j):
        hidden_copy(pl.ds(aligned(j * dec.group * CHUNK, CHUNK), dec.group * CHUNK)).start()

    def wait_hidden():
        hidden_copy(pl.ds(0, d.width)).wait()

    def swap_sums():
        copy = pltpu.make_async_remote_copy(acc_other, sums_in, pair_send.at[1], pair_recv.at[1], device_id={'kv': exchanges[0].partner})
        copy.start()
        copy.wait()
        return sums_in[...]

    blocks = half // min(UNROLL, half)
    last_pair = 2 * (dec.whole // MLP_GROUP) - 1
    for l in range(d.layers):
        between_a, between_b, events = (), (), []
        if l:
            scope(f"project_{l}", project, l)
            scope(f"pages_wait_{l}", pages_wait, l)
            last_wait(l - 1)
        else:
            between_a, between_b = [(blocks // 2, event(step_1))], [(0, event(pages_1)), (blocks // 2, event(pages_1))]
            events = [(k * last_pair // 7, event(pages_1)) for k in range(2 * parts - 2)]
            events += [(k * last_pair // 3, event(step_1)) for k in PAIR] + [(last_pair - parts, event(step_1))]
        with jax.named_scope(f"attend_{l}"):
            attend(l, between_a, between_b)
        events += [(last_pair, functools.partial(scope, f"finish_{l}", finish_pages, l))]
        with jax.named_scope(f"mix_{l}"):
            dec.mix_shared(l, send_hidden, wait_hidden, swap_sums, sorted(events, key=lambda event: event[0]))
    for t in PAIR:
        ya_ref[t] = y_ref[pl.ds(t * d.rows, half), :]
        yb_ref[t] = y_ref[pl.ds(t * d.rows + half, half), :]
    last_wait(d.layers - 1)


def decode_adjacent(side, group_size, d, table, seq_lens, mig_src, mig_dst, embeds, weights, k_pool, v_pool):
    entries = mig_src.shape[0]
    half = d.rows // 2
    page = (d.page_rows, d.head_dim)
    struct = lambda *shape: jax.ShapeDtypeStruct(shape, BF16)
    groups = d.tokens // 8
    mid = pltpu.VMEM((group_size, 8, d.width * groups // group_size), BF16)
    return pl.pallas_call(
        functools.partial(adjacent_kernel, d, side, group_size, entries),
        out_shape=[struct(2, half, d.width), struct(2, half, d.width), jax.ShapeDtypeStruct((2,), jnp.int32), struct(d.layers, 2, d.rows, *page)],
        in_specs=[SMEM] * 2 + [ANY] * 11,
        out_specs=[VMEM, VMEM, SMEM, ANY],
        scratch_shapes=[
            pltpu.SMEM(table.shape, jnp.int32),
            pltpu.SMEM(seq_lens.shape, jnp.int32),
            pltpu.VMEM(table.shape, jnp.int32),
            pltpu.VMEM((groups, 8, d.width), BF16),
            pltpu.VMEM((d.tokens, d.width), BF16),
        ] + [pltpu.VMEM((d.layers, 2, 2, half) + page, BF16)] * len(PAIR) + [
            pltpu.VMEM((2, d.rows) + page, BF16),
            pltpu.VMEM((d.layers, 2, d.kv_heads, 2, half, d.head_dim), F32),
            pltpu.VMEM((d.layers, 2 * entries) + page, BF16),
        ] + [pltpu.VMEM((d.layers, entries) + page, BF16)] * len(PAIR) + [
            mid,
            mid,
            pltpu.VMEM((groups, 8, d.width), BF16),
            pltpu.VMEM((1, table.shape[1]), jnp.int32),
            pltpu.SMEM((1, table.shape[1]), jnp.int32),
            pltpu.VMEM((d.tokens, d.width), BF16),
            pltpu.VMEM((d.tokens, d.width), F32),
            pltpu.VMEM((d.tokens, d.width), F32),
            pltpu.VMEM((d.width, HALF), BF16),
            pltpu.VMEM((HALF, d.width), BF16),
        ] + [pltpu.VMEM((2 * entries,) + page, BF16)] * d.layers + [pltpu.VMEM((d.slots,) + page, BF16)] * (2 * d.layers) + d.compute_scratch(8, 6) + [
            DMA((4,)),
            DMA((d.layers, 2)),
            DMA,
        ] + [DMA(shape) for shape in ((2,), (d.layers, 2, 2), (d.layers, 2, d.kv_heads, 2), (d.layers, 10, 4)) for _ in PAIR] + [DMA] + [DMA((2,))] * 3,
        compiler_params=pltpu.CompilerParams(collective_id=1, has_side_effects=True, skip_device_barrier=True, vmem_limit_bytes=LIMIT),
        cost_estimate=d.cost(d.layers),
        name="decode_adjacent",
    )(mig_src, mig_dst, table, seq_lens, embeds.reshape(groups, 8, d.width), *weights, k_pool, v_pool)


def fill_pools_kernel(dims, group_size, info_s, table_s, src_s, k_hbm, v_hbm, last_hbm, k_out, v_out, k_buf, v_buf, sem, put_sem):
    d = dims
    me = lax.axis_index('kv')
    home = lax.rem(me - info_s[0] + group_size, group_size)
    pools = ((k_hbm, k_buf, k_out), (v_hbm, v_buf, v_out))
    parts = sem.shape[1]
    size = d.slots // parts

    def moves(part, out):
        at = pl.ds(part * size, size)
        return [pltpu.make_async_copy(*((buf.at[at], dst.at[at]) if out else (src.at[at], buf.at[at])), sem.at[p, part]) for p, (src, buf, dst) in enumerate(pools)]

    def all_parts(out, run):
        @pl.loop(0, parts)
        def _(part):
            for copy in moves(part, out):
                run(copy)

    start, wait = lambda copy: copy.start(), lambda copy: copy.wait()
    all_parts(False, start)
    all_parts(False, wait)

    @pl.loop(0, d.rows)
    def _(i):
        slot = local_slot(table_s[1, home * d.rows + i], me, d.slots)
        for p, (_, buf, _) in enumerate(pools):
            pltpu.make_async_copy(last_hbm.at[:, p, i], buf.at[slot], put_sem).start()

    @pl.loop(0, src_s.shape[0])
    def _(e):
        slot = src_s[e] - me * d.slots

        @pl.when((slot >= 0) & (slot < d.slots))
        def _():
            for _, buf, _ in pools:
                buf[local_slot(src_s[e], me, d.slots)] = jnp.zeros(buf.shape[1:], buf.dtype)

    for src, buf, _ in pools:
        pltpu.make_async_copy(src.at[pl.ds(0, d.rows)], buf.at[pl.ds(0, d.rows)], put_sem).wait()
    all_parts(True, start)
    all_parts(True, wait)


def fill_pools(group_size, d, info, table, mig_src, k_pool, v_pool, last):
    return pl.pallas_call(
        functools.partial(fill_pools_kernel, d, group_size),
        out_shape=[jax.ShapeDtypeStruct(k_pool.shape, k_pool.dtype)] * 2,
        in_specs=[SMEM] * 3 + [ANY] * 3,
        out_specs=[ANY, ANY],
        scratch_shapes=[pltpu.VMEM(k_pool.shape, k_pool.dtype), pltpu.VMEM(k_pool.shape, k_pool.dtype), DMA((2, 4)), DMA],
        compiler_params=pltpu.CompilerParams(vmem_limit_bytes=LIMIT),
        cost_estimate=d.cost(1),
        name="fill_pools",
    )(info, table, mig_src, k_pool, v_pool, last)


def gather_pages_kernel(idx_ref, k_hbm, v_hbm, k_out, v_out, sem):
    rows = k_out.shape[0]

    def copies(i):
        slot = jnp.maximum(idx_ref[i], 0)
        return (pltpu.make_async_copy(k_hbm.at[slot], k_out.at[i], sem), pltpu.make_async_copy(v_hbm.at[slot], v_out.at[i], sem))

    @pl.loop(0, rows)
    def _(i):
        @pl.when(idx_ref[i] >= 0)
        def _():
            for copy in copies(i):
                copy.start()

        @pl.when(idx_ref[i] < 0)
        def _():
            k_out[i] = jnp.zeros(k_out.shape[1:], k_out.dtype)
            v_out[i] = jnp.zeros(v_out.shape[1:], v_out.dtype)

    @pl.loop(0, rows)
    def _(i):
        @pl.when(idx_ref[i] >= 0)
        def _():
            for copy in copies(i):
                copy.wait()


def gather_pages(idx, k_pool, v_pool):
    shape = jax.ShapeDtypeStruct((idx.shape[0],) + k_pool.shape[1:], k_pool.dtype)
    return pl.pallas_call(
        gather_pages_kernel,
        out_shape=[shape, shape],
        in_specs=[SMEM, ANY, ANY],
        out_specs=[VMEM, VMEM],
        scratch_shapes=[DMA],
        compiler_params=pltpu.CompilerParams(vmem_limit_bytes=LIMIT),
        name="gather_pages",
    )(idx, k_pool, v_pool)


def share_kernel(side, k_hbm, v_hbm, k_out, v_out, work, core_buf, ring_buf, load_sem, send_sem, recv_sem, result):
    entries = k_hbm.shape[0]
    exchange = Exchange(side, 0, work, core_buf, ring_buf, result, send_sem, recv_sem)
    units = [pl.ds(p * entries, entries) for p in PAIR]
    for p, src in enumerate((k_hbm, v_hbm)):
        pltpu.make_async_copy(src, work.at[0].at[units[p]], load_sem.at[p]).start()
    for p, src in enumerate((k_hbm, v_hbm)):
        pltpu.make_async_copy(src, work.at[0].at[units[p]], load_sem.at[p]).wait()
    for _ in range(Exchange.STEPS):
        exchange.step()
    for p, dst in enumerate((k_out, v_out)):
        pltpu.make_async_copy(result.at[units[p]], dst, load_sem.at[p]).start()
    for p, dst in enumerate((k_out, v_out)):
        pltpu.make_async_copy(result.at[units[p]], dst, load_sem.at[p]).wait()


def share(side, mig_k, mig_v):
    entries = mig_k.shape[0]
    page = mig_k.shape[1:]
    return pl.pallas_call(
        functools.partial(share_kernel, side),
        out_shape=[jax.ShapeDtypeStruct(mig_k.shape, BF16)] * 2,
        in_specs=[ANY, ANY],
        out_specs=[ANY, ANY],
        scratch_shapes=[pltpu.VMEM((1, n * entries) + page, BF16) for n in (2, 1, 1)] + [DMA((2,)), DMA((1, 10, 4)), DMA((1, 10, 4)), pltpu.VMEM((2 * entries,) + page, BF16)],
        compiler_params=pltpu.CompilerParams(has_side_effects=True, vmem_limit_bytes=LIMIT),
        name="share",
    )(mig_k, mig_v)


def migrate_kernel(dst_ref, src_ref, k_hbm, v_hbm, mk_hbm, mv_hbm, k_out, v_out, k_buf, v_buf, sem, fix_sem):
    entries = dst_ref.shape[0]
    pairs = ((k_hbm, mk_hbm, k_buf, k_out), (v_hbm, mv_hbm, v_buf, v_out))
    for p, (src, _, buf, _) in enumerate(pairs):
        pltpu.make_async_copy(src, buf, sem.at[p]).start()
    for p, (src, _, buf, _) in enumerate(pairs):
        pltpu.make_async_copy(src, buf, sem.at[p]).wait()

    @pl.loop(0, entries)
    def _(e):
        @pl.when(dst_ref[e] >= 0)
        def _():
            for _, mig, buf, _ in pairs:
                copy = pltpu.make_async_copy(mig.at[e], buf.at[jnp.maximum(dst_ref[e], 0)], fix_sem)
                copy.start()
                copy.wait()

        @pl.when(src_ref[e] >= 0)
        def _():
            for _, _, buf, _ in pairs:
                buf[jnp.maximum(src_ref[e], 0)] = jnp.zeros(buf.shape[1:], buf.dtype)

    for p, (_, _, buf, dst) in enumerate(pairs):
        pltpu.make_async_copy(buf, dst, sem.at[p]).start()
    for p, (_, _, buf, dst) in enumerate(pairs):
        pltpu.make_async_copy(buf, dst, sem.at[p]).wait()


def migrate(dst_local, src_local, k_pool, v_pool, mig_k, mig_v):
    shape = jax.ShapeDtypeStruct(k_pool.shape, k_pool.dtype)
    return pl.pallas_call(
        migrate_kernel,
        out_shape=[shape, shape],
        in_specs=[SMEM, SMEM, ANY, ANY, ANY, ANY],
        out_specs=[ANY, ANY],
        scratch_shapes=[pltpu.VMEM(k_pool.shape, k_pool.dtype), pltpu.VMEM(k_pool.shape, k_pool.dtype), DMA((2,)), DMA],
        compiler_params=pltpu.CompilerParams(vmem_limit_bytes=LIMIT),
        name="migrate",
    )(dst_local, src_local, k_pool, v_pool, mig_k, mig_v)


def decode_kernel(dims, sc_ref, x_ref, p0k_hbm, p0v_hbm, wq, wk, wv, wo, wu, wd, k_in, v_in, y_ref, k_out, v_out,
                  first_buf, last_buf, *rest):
    compute, (page_sem, put_sem) = rest[:-2], rest[-2:]
    d = dims
    dec = Decoder(d, 0, d.layers, (wq, wk, wv, wo, wu, wd), y_ref, compute, 1, 2)
    dec.start_stream()
    y_ref[...] = x_ref[...]
    loads = [pltpu.make_async_copy(src, first_buf.at[p], page_sem.at[p]) for p, src in enumerate((p0k_hbm, p0v_hbm))]
    for load in loads:
        load.start()

    def last_loads(run):
        @pl.loop(0, d.rows)
        def _(i):
            for p, src in enumerate((k_in, v_in)):
                run(pltpu.make_async_copy(src.at[sc_ref[0, i]], last_buf.at[p, i], page_sem.at[2]))

    def puts(run):
        @pl.loop(0, d.rows)
        def _(i):
            @pl.when(sc_ref[2, i] > 0)
            def _():
                for p, dst in enumerate((k_out, v_out)):
                    run(pltpu.make_async_copy(last_buf.at[p, i], dst.at[sc_ref[0, i]], put_sem))

    last_loads(lambda copy: copy.start())
    for load in loads:
        load.wait()
    last_loads(lambda copy: copy.wait())

    @pl.loop(0, d.layers)
    def _(layer):
        def put_page(p, i, val):
            last_buf[p, i, layer] = val

        dec.project(layer)
        dec.attend(lambda i: sc_ref[1, i], lambda p, i: first_buf[p, i, layer], lambda p, i: last_buf[p, i, layer], put_page)
        dec.gather_heads()
        dec.mix(layer)

    puts(lambda copy: copy.start())
    puts(lambda copy: copy.wait())


def decode(d, scalars, x, p0k, p0v, weights, k_pool, v_pool):
    pool = jax.ShapeDtypeStruct(k_pool.shape, k_pool.dtype)
    pages = pltpu.VMEM((2, d.rows, d.layers, d.page_rows, d.head_dim), BF16)
    return pl.pallas_call(
        functools.partial(decode_kernel, d),
        out_shape=[jax.ShapeDtypeStruct(x.shape, x.dtype), pool, pool],
        in_specs=[SMEM, VMEM] + [ANY] * 10,
        out_specs=[VMEM, ANY, ANY],
        input_output_aliases={10: 1, 11: 2},
        scratch_shapes=[pages, pages] + d.compute_scratch(16, 16) + [DMA((3,)), DMA],
        compiler_params=pltpu.CompilerParams(vmem_limit_bytes=LIMIT),
        cost_estimate=d.cost(d.layers),
        name="decode",
    )(scalars, x, p0k, p0v, *weights, k_pool, v_pool)


def permute(arrays, shift, group_size):
    if shift == group_size // 2:
        return permute(permute(arrays, shift // 2, group_size), shift // 2, group_size)
    perm = [(i, (i + shift) % group_size) for i in range(group_size)]
    return jax.tree.map(lambda a: lax.ppermute(a, 'kv', perm), arrays) if shift else arrays


def rotate_back(first, second, shift, group_size, beside):
    def branch(r):
        def run(args):
            parts = permute(args[0], -r % group_size, group_size), permute(args[1], (1 - r) % group_size, group_size)
            return jnp.concatenate(parts, axis=1), beside()

        return run

    return lax.switch(shift, [branch(r) for r in range(group_size)], (first, second))


def rotate(arrays, shift, group_size):
    stride = math.isqrt(2 * group_size)
    for count, move in ((shift // stride, stride), (shift % stride, 1)):
        arrays = lax.fori_loop(0, count, lambda _, a: permute(a, move, group_size), arrays)
    return arrays


def solution(mesh):
    group_size = mesh.shape['kv']
    side = math.isqrt(group_size // 2)
    pool_spec = P(('rep', 'kv'))
    tok_spec = P(None, ('rep', 'kv'), None)

    def device_fn(embeds, w_query, w_key, w_value, w_out, w_up, w_down, k_pool5, v_pool5, new_table, seq_lens, mig_src, mig_dst):
        me = lax.axis_index('kv')
        slots, layers, page, kv_heads, head_dim = k_pool5.shape
        rows, width = embeds.shape[1:]
        weights = (w_query, w_key, w_value, w_out, w_up, w_down)
        k_pool = k_pool5.reshape(slots, layers, page * kv_heads, head_dim)
        v_pool = v_pool5.reshape(slots, layers, page * kv_heads, head_dim)
        d = Dims(rows, weights, k_pool, page)
        ints = jnp.int32

        def local(ids):
            loc = ids - me * slots
            return jnp.where((loc >= 0) & (loc < slots), loc, -1)

        def take(vec, dev):
            return lax.dynamic_slice(vec, (dev * rows,), (rows,))

        def inside(ids):
            return local_slot(ids, me, slots)

        def general_path():
            first_new, last_new = new_table[:, 0], new_table[:, 1]
            moved = first_new[None, :] == mig_dst[:, None]
            first_old = jnp.where(jnp.any(moved, axis=0), jnp.sum(jnp.where(moved, mig_src[:, None], 0), axis=0), first_new)
            home = jnp.arange(first_new.shape[0], dtype=ints) // rows
            worker = last_new // slots
            shift_of = (worker - home + group_size) % group_size
            first_shift = (worker - first_old // slots + group_size) % group_size
            shift_ids = jnp.arange(group_size, dtype=ints)
            wanted = jnp.any(shift_of[None, :] == shift_ids[:, None], axis=1)
            mig_k, mig_v = gather_pages(local(mig_src), k_pool, v_pool)
            by_layer = tuple(m.swapaxes(0, 1) for m in (mig_k, mig_v))
            mig_k, mig_v = (m.swapaxes(0, 1) for m in lax.map(lambda pages: tuple(share(side, *pages)), by_layer))
            k_new, v_new = migrate(local(mig_dst), local(mig_src), k_pool, v_pool, mig_k, mig_v)

            def one_round(shift, y, k_new, v_new):
                src_home = (me - shift + group_size) % group_size
                x = rotate(embeds.reshape(2 * rows, width), shift, group_size)
                in_round = shift_of == shift
                wanted2 = jnp.any(in_round[None, :] & (first_shift[None, :] == shift_ids[:, None]), axis=1)

                def more(state):
                    left, pk, pv = state
                    shift2 = jnp.argmax(left).astype(ints)
                    dest_home = (me + shift2 - shift + group_size) % group_size
                    got = gather_pages(inside(take(first_old, dest_home)), k_pool, v_pool)
                    got_k, got_v = rotate(tuple(got), shift2, group_size)
                    mine = (take(first_shift, src_home) == shift2)[:, None, None, None]
                    return left & (shift_ids != shift2), jnp.where(mine, got_k, pk), jnp.where(mine, got_v, pv)

                zeros = jnp.zeros((rows,) + k_pool.shape[1:], k_pool.dtype)
                _, pk, pv = lax.while_loop(lambda state: jnp.any(state[0]), more, (wanted2, zeros, zeros))
                valid = take(shift_of, src_home) == shift
                scalars = jnp.stack([inside(take(last_new, src_home)), take(seq_lens, src_home), valid.astype(ints)])
                out, k_new, v_new = decode(d, scalars, x, pk, pv, weights, k_new, v_new)
                back = rotate(out, (group_size - shift) % group_size, group_size)
                mine = (take(shift_of, me) == shift)[None, :, None]
                return jnp.where(mine, back.reshape(embeds.shape), y), k_new, v_new

            def next_round(state):
                left, y, k_new, v_new = state
                shift = jnp.argmax(left).astype(ints)
                y, k_new, v_new = one_round(shift, y, k_new, v_new)
                return left & (shift_ids != shift), y, k_new, v_new

            _, y, k_new, v_new = lax.while_loop(lambda state: jnp.any(state[0]), next_round, (wanted, jnp.zeros_like(embeds), k_new, v_new))
            return y, k_new, v_new

        table = new_table.T
        ya, yb, info, last = decode_adjacent(side, group_size, d, table, seq_lens, mig_src, mig_dst, embeds, weights, k_pool, v_pool)
        y, (k_new, v_new) = rotate_back(ya, yb, info[0], group_size, lambda: fill_pools(group_size, d, info, table, mig_src, k_pool, v_pool, last))
        _, y, k_new, v_new = lax.while_loop(lambda state: state[0] == 0, lambda state: (jnp.ones_like(state[0]),) + general_path(), (info[1], y, k_new, v_new))
        return y, k_new.reshape(k_pool5.shape), v_new.reshape(v_pool5.shape)

    return jax.shard_map(device_fn, mesh=mesh, in_specs=(tok_spec, P(), P(), P(), P(), P(), P(), pool_spec, pool_spec, P('rep', None), P('rep'), P('rep'), P('rep')), out_specs=(tok_spec, pool_spec, pool_spec), check_vma=False)
```

```python
import functools
import math

import jax
import jax.numpy as jnp
from jax import lax
from jax.experimental import pallas as pl
from jax.experimental.pallas import tpu as pltpu
from jax.sharding import PartitionSpec as P

ANY = pl.BlockSpec(memory_space=pl.ANY)
SMEM = pl.BlockSpec(memory_space=pltpu.SMEM)
VMEM = pl.BlockSpec(memory_space=pltpu.VMEM)
DMA = pltpu.SemaphoreType.DMA
CHUNK = 256
UNROLL = 8
MLP_GROUP = 3
LANES = 128
HALF = CHUNK // 2
PAIR = (0, 1)
LIMIT = 1023 << 16
F32, BF16 = jnp.float32, jnp.bfloat16


def iota(shape, axis):
    return lax.broadcasted_iota(jnp.int32, shape, axis)


def dot(a, b):
    return jnp.dot(a, b, preferred_element_type=F32)


def local_slot(ids, me, slots):
    return jnp.clip(ids - me * slots, 0, slots - 1)


def aligned(x, multiple):
    return x if isinstance(x, int) else pl.multiple_of(x, multiple)


class Dims:
    def __init__(self, rows, weights, k_pool, page):
        w_query, w_key, _, _, w_up, _ = weights
        self.layers, self.width, self.q_width = w_query.shape
        self.ff = w_up.shape[2]
        self.slots, _, self.page_rows, self.head_dim = k_pool.shape
        self.kv_heads = w_key.shape[2] // self.head_dim
        self.heads = self.q_width // self.head_dim
        self.page, self.rows = page, rows
        self.tokens = 2 * rows
        self.stride = self.tokens + 8
        self.n_q, self.n_o, self.n_u = self.q_width // CHUNK, self.width // CHUNK, self.ff // CHUNK

    def compute_scratch(self, n_col, n_row):
        return [
            pltpu.VMEM((n_col, self.width, CHUNK), BF16),
            pltpu.VMEM((n_row, CHUNK, self.width), BF16),
            pltpu.VMEM((self.heads * self.stride, self.head_dim), F32),
            pltpu.VMEM((self.kv_heads * self.stride, self.head_dim), F32),
            pltpu.VMEM((self.kv_heads * self.stride, self.head_dim), F32),
            pltpu.VMEM((self.heads * self.stride, self.head_dim), F32),
            pltpu.VMEM((self.tokens, self.q_width), BF16),
            pltpu.VMEM((self.tokens, self.ff), BF16),
            pltpu.VMEM((self.tokens, self.width), F32),
            DMA((n_col,)),
            DMA((n_row,)),
        ]

    def cost(self, layers):
        size = layers * self.width * (2 * self.q_width + 2 * self.kv_heads * self.head_dim + 2 * self.ff)
        return pl.CostEstimate(flops=2 * size * self.tokens, bytes_accessed=2 * size, transcendentals=0)


class Decoder:
    def __init__(self, dims, first, layers, weights, y_ref, scratch, group=2, unroll=UNROLL, shared=False):
        self.group, self.unroll, self.shared = group, unroll, shared
        self.d, self.first, self.layers, self.weights, self.y_ref = dims, first, layers, weights, y_ref
        (self.col_buf, self.row_buf, self.q_s, self.kn_s, self.vn_s, self.o_s, self.att, self.act, self.acc, self.col_sem, self.row_sem) = scratch
        self.n_col, self.n_row = self.col_buf.shape[0], self.row_buf.shape[0]
        self.zero = lax.axis_index('kv') * 0
        d = dims
        self.whole = d.ff // 2 // CHUNK if shared else d.n_u
        self.begin = lax.axis_index('kv') % 2 * (d.ff // 2) if shared else 0
        self.col_layer = d.n_q + 2 + d.n_o + self.whole
        cols = 2 * d.page * d.kv_heads
        col_pos = iota((2 * d.heads, cols), 1)
        row_pos = iota((2 * d.heads, cols), 0)
        same_head = (col_pos % d.kv_heads) == (row_pos % d.heads) // (d.heads // d.kv_heads)
        self.limit = jnp.where(same_head, col_pos // d.kv_heads - row_pos // d.heads, 4 * d.page)
        self.page_pos = iota((d.page_rows, d.head_dim), 0) // d.kv_heads
        self.tile_head = iota((8, d.head_dim), 0) % d.kv_heads

    def layer_of(self, g, per_layer):
        return sum((g >= per_layer * l).astype(jnp.int32) for l in range(1, self.layers))

    def col_start(self, g):
        d = self.d
        wq, wk, wv, wo, wu, _ = self.weights

        @pl.when(g < self.layers * self.col_layer)
        def _():
            layer = self.layer_of(g, self.col_layer)
            pos = g - layer * self.col_layer
            slot = g % self.n_col

            def go(src, c, begin=0):
                start = aligned(c * CHUNK + begin, LANES)
                pltpu.make_async_copy(src.at[self.first + layer].at[:, pl.ds(start, CHUNK)], self.col_buf.at[slot], self.col_sem.at[slot]).start()

            @pl.when(pos < d.n_q)
            def _():
                go(wq, pos)

            @pl.when(pos == d.n_q)
            def _():
                go(wk, 0)

            @pl.when(pos == d.n_q + 1)
            def _():
                go(wv, 0)

            @pl.when((pos >= d.n_q + 2) & (pos < d.n_q + 2 + d.n_o))
            def _():
                go(wo, pos - (d.n_q + 2))

            @pl.when(pos >= d.n_q + 2 + d.n_o)
            def _():
                go(wu, pos - (d.n_q + 2 + d.n_o), self.begin)

    def row_start(self, g):
        d = self.d
        wd = self.weights[5]

        @pl.when(g < self.layers * self.whole)
        def _():
            layer = self.layer_of(g, self.whole)
            slot = g % self.n_row
            start = aligned((g - layer * self.whole) * CHUNK + self.begin, LANES)
            pltpu.make_async_copy(wd.at[self.first + layer].at[pl.ds(start, CHUNK)], self.row_buf.at[slot], self.row_sem.at[slot]).start()

    def start_stream(self):
        @pl.loop(0, self.n_col)
        def _(g):
            self.col_start(g)

        @pl.loop(0, self.n_row)
        def _(g):
            self.row_start(g)

    def with_cols(self, g, count, body):
        slots = [(g + u) % self.n_col for u in range(count)]
        for slot in slots:
            pltpu.make_async_copy(self.weights[1].at[0], self.col_buf.at[slot], self.col_sem.at[slot]).wait()
        body([self.col_buf.at[slot] for slot in slots])
        for u in range(count):
            self.col_start(g + u + self.n_col)

    def with_rows(self, g, count, body):
        slots = [(g + u) % self.n_row for u in range(count)]
        for slot in slots:
            pltpu.make_async_copy(self.weights[5].at[0, pl.ds(0, CHUNK), :], self.row_buf.at[slot], self.row_sem.at[slot]).wait()
        body([self.row_buf.at[slot] for slot in slots])
        for u in range(count):
            self.row_start(g + u + self.n_row)

    def project(self, layer):
        d = self.d
        col0 = (self.zero + layer) * self.col_layer

        def product(ref):
            return dot(self.y_ref[...], ref[...]).astype(BF16).astype(F32)

        def put(dst, first, out):
            for h in range(CHUNK // d.head_dim):
                at = aligned((first + h) * d.stride, 8)
                dst[pl.ds(at, d.tokens), :] = out[:, h * d.head_dim:(h + 1) * d.head_dim]

        many = self.group

        @pl.loop(0, d.n_q // many)
        def _(j):
            def body(refs):
                outs = [product(ref) for ref in refs]
                for u in range(many):
                    put(self.q_s, (many * j + u) * (CHUNK // d.head_dim), outs[u])

            self.with_cols(col0 + many * j, many, body)

        def body(refs):
            outs = [product(ref) for ref in refs]
            put(self.kn_s, 0, outs[0])
            put(self.vn_s, 0, outs[1])

        self.with_cols(col0 + d.n_q, 2, body)

    def insert(self, page, n, row):
        d = self.d
        val = page.astype(F32)
        for t in PAIR:
            new = jnp.broadcast_to(row(t, 0), (8, d.head_dim))
            for g in range(1, d.kv_heads):
                new = jnp.where(self.tile_head == g, row(t, g), new)
            val = jnp.where(self.page_pos == n - d.page + t, jnp.concatenate([new] * (d.page_rows // 8), axis=0), val)
        return val.astype(BF16)

    def attend(self, lens, first_page, last_page, put_page, events=(), begin=0, count=None):
        d = self.d
        count = count or d.rows
        unroll = min(self.unroll, count)

        def some(first):
            ids = [first + u for u in range(unroll)]
            scores, vals = [], []
            for i in ids:
                n = lens(i)

                def updated(p, new_ref):
                    val = self.insert(last_page(p, i), n, lambda t, g: new_ref[pl.ds(g * d.stride + t * d.rows + i, 1), :])
                    put_page(p, i, val)
                    return val

                keys = jnp.concatenate([first_page(0, i), updated(0, self.kn_s)], axis=0)
                vals.append(updated(1, self.vn_s))
                qs = jnp.concatenate([self.q_s[pl.ds(t * d.rows + i, d.heads, stride=d.stride), :] for t in PAIR], axis=0)
                score = lax.dot_general(qs.astype(BF16), keys, (((1,), (1,)), ((), ())), preferred_element_type=F32) * d.head_dim ** -0.5
                scores.append(jnp.where(self.limit <= n, score, -jnp.inf))
            tops = [jnp.max(score, axis=1, keepdims=True) for score in scores]
            probs = [jnp.exp(score - top) for score, top in zip(scores, tops)]
            totals = [jnp.sum(prob, axis=1, keepdims=True) for prob in probs]
            for u, i in enumerate(ids):
                both = jnp.concatenate([first_page(1, i), vals[u]], axis=0)
                out = dot(probs[u].astype(BF16), both) / totals[u]
                for t in PAIR:
                    self.o_s[pl.ds(t * d.rows + i, d.heads, stride=d.stride), :] = out[t * d.heads:(t + 1) * d.heads]

        @pl.loop(0, count // unroll)
        def _(block):
            for k, run in events:
                pl.when(block == k)(run)
            some(begin + block * unroll)

    def gather_heads(self):
        d = self.d
        for h in range(d.heads):
            self.att[:, h * d.head_dim:(h + 1) * d.head_dim] = self.o_s[h * d.stride:h * d.stride + d.tokens, :].astype(BF16)

    def span(self, j):
        return pl.ds(aligned(j * CHUNK, CHUNK), CHUNK)

    def out_project(self, layer, after=None):
        d, many = self.d, self.group

        @pl.loop(0, d.n_o // many)
        def _(j):
            def body(refs):
                outs = [dot(self.att[...], ref[...]) for ref in refs]
                for u in range(many):
                    at = self.span(many * j + u)
                    self.y_ref[:, at] = (self.y_ref[:, at].astype(F32) + outs[u]).astype(BF16)

            self.with_cols(layer * self.col_layer + d.n_q + len(PAIR) + many * j, many, body)
            if after:
                after(j)

    def mix(self, layer, events=()):
        d = self.d
        layer = self.zero + layer
        col0 = layer * self.col_layer + d.n_q + 2
        many = self.group
        pairs = d.n_u // many

        def between(j, first):
            for k, run in events:
                if first <= k < first + pairs:
                    pl.when(j == k - first)(run)

        self.out_project(layer)

        def up(first, count):
            def body(refs):
                ups = [dot(self.y_ref[...], ref[...]) for ref in refs]
                for u in range(count):
                    self.act[:, self.span(first + u)] = jax.nn.gelu(ups[u].astype(BF16).astype(F32), approximate=True).astype(BF16)

            self.with_cols(col0 + d.n_o + first, count, body)

        def down(first, count):
            def body(refs):
                out = self.acc[...]
                for u in range(count):
                    out += dot(self.act[:, self.span(first + u)], refs[u][...])
                self.acc[...] = out

            self.with_rows(layer * self.whole + first, count, body)

        @pl.loop(0, pairs)
        def _(j):
            between(j, 0)
            up(many * j, many)

        if d.n_u % many:
            up(d.n_u - 1, 1)

        self.acc[...] = self.y_ref[...].astype(F32)

        @pl.loop(0, pairs)
        def _(j):
            between(j, pairs)
            down(many * j, many)

        if d.n_u % many:
            down(d.n_u - 1, 1)

        self.y_ref[...] = self.acc[...].astype(BF16)


    def half_loads(self, layer):
        at = pl.ds(aligned(self.begin + self.whole * CHUNK, LANES), HALF)
        return (pltpu.make_async_copy(self.weights[4].at[layer].at[:, at], self.half_col, self.half_sem.at[0]),
                pltpu.make_async_copy(self.weights[5].at[layer].at[at], self.half_row, self.half_sem.at[1]))

    def mix_shared(self, layer, send_hidden, wait_hidden, swap_sums, events=()):
        d = self.d
        half_loads, next_loads = self.half_loads(layer), self.half_loads(layer + 1) if layer + 1 < d.layers else ()
        layer = self.zero + layer
        col0 = layer * self.col_layer + d.n_q + 2
        many = MLP_GROUP
        rows = d.tokens
        offset = d.ff // 2
        pairs = self.whole // many

        def between(j, first):
            for k, run in events:
                if first <= k < first + pairs:
                    pl.when(j == k - first)(run)

        self.out_project(layer, send_hidden)

        self.acc[...] = self.y_ref[...].astype(F32)
        self.acc_other[...] = jnp.zeros_like(self.acc_other)
        wait_hidden()

        def hidden():
            return jnp.concatenate([self.y_ref[...], self.y_other[...]], axis=0)

        def activate(up, at, size):
            val = jax.nn.gelu(up.astype(BF16).astype(F32), approximate=True).astype(BF16)
            self.act[:, pl.ds(aligned(at, LANES), size)] = val[:rows]
            self.act[:, pl.ds(aligned(at + offset, LANES), size)] = val[rows:]

        @pl.loop(0, pairs)
        def _(j):
            between(j, 0)

            def body(refs):
                ups = [dot(hidden(), ref[...]) for ref in refs]
                for u in range(many):
                    activate(ups[u], (many * j + u) * CHUNK, CHUNK)

            self.with_cols(col0 + d.n_o + many * j, many, body)

        tail = self.whole % many
        for u in range(tail):
            def body(refs, at=(self.whole - tail + u) * CHUNK):
                activate(dot(hidden(), refs[0][...]), at, CHUNK)

            self.with_cols(col0 + d.n_o + self.whole - tail + u, 1, body)
        for copy in half_loads:
            copy.wait()
        activate(dot(hidden(), self.half_col[...]), self.whole * CHUNK, HALF)

        def acts(at, size):
            return jnp.concatenate([self.act[:, pl.ds(aligned(at, LANES), size)], self.act[:, pl.ds(aligned(at + offset, LANES), size)]], axis=0)

        def add(out):
            self.acc[...] += out[:rows]
            self.acc_other[...] += out[rows:]

        @pl.loop(0, pairs)
        def _(j):
            between(j, pairs)

            def body(refs):
                add(sum(dot(acts((many * j + u) * CHUNK, CHUNK), refs[u][...]) for u in range(many)))

            self.with_rows(layer * self.whole + many * j, many, body)

        for u in range(tail):
            def body(refs, at=(self.whole - tail + u) * CHUNK):
                add(dot(acts(at, CHUNK), refs[0][...]))

            self.with_rows(layer * self.whole + self.whole - tail + u, 1, body)
        add(dot(acts(self.whole * CHUNK, HALF), self.half_row[...]))
        for copy in next_loads:
            copy.start()
        self.y_ref[...] = (self.acc[...] + swap_sums()).astype(BF16)


class Exchange:
    STEPS = 11

    def __init__(self, side, layer, work, core_buf, ring_buf, out, send_sem, recv_sem):
        self.layer = layer
        self.work, self.core_buf, self.ring_buf, self.out, self.send_sem, self.recv_sem = work, core_buf, ring_buf, out, send_sem, recv_sem
        me = lax.axis_index('kv')
        core, x, y = me % 2, me // 2 % side, me // (2 * side)

        def pairings(pos, stride):
            return (((pos + 1) // 2 % 2, me + (1 - 2 * (pos % 2)) * stride), (pos // 2, me + (side - 1 - 2 * pos) * stride))

        xs, ys = pairings(x, 2), pairings(y, 2 * side)
        self.orders = [xs + ys, xs[::-1] + ys[::-1], ys + xs, ys[::-1] + xs[::-1]]
        self.partner = me + 1 - 2 * core
        self.peers = [self.partner] + [dev for _, dev in xs + ys]
        self.half = work.shape[1] // 2
        self.stream = self.half // 4
        self.base, self.other = core * self.half, (1 - core) * self.half
        self.copies, self.done = [], 0
        self.path = [[self.base + k * self.stream for k in range(4)]]
        self.away = []
        for ring in range(4):
            size = self.stream >> (ring + 1)
            self.away.append([self.path[-1][k] + (1 - self.orders[k][ring][0]) * size for k in range(4)])
            self.path.append([self.path[-1][k] + self.orders[k][ring][0] * size for k in range(4)])

    def send(self, src, dst, step, lane, dev):
        def copy():
            return pltpu.make_async_remote_copy(src(), dst(), self.send_sem.at[self.layer, step, lane], self.recv_sem.at[self.layer, step, lane], device_id={'kv': dev})

        copy().start()
        self.copies.append(copy)

    def units(self, ref, at, count):
        return lambda: ref.at[self.layer].at[pl.ds(at, count)]

    def results(self, at, count):
        return lambda: self.out.at[pl.ds(at, count)]

    def add(self, dst_at, buf, src_at, count):
        @pl.loop(0, count)
        def _(u):
            self.work[self.layer, dst_at + u] = self.work[self.layer, dst_at + u] + buf[self.layer, src_at + u]

    def halve(self, ring, k):
        size = self.stream >> (ring + 1)
        src = self.units(self.work, self.away[ring][k], size)
        self.send(src, self.units(self.ring_buf, (k + 1) * self.stream - 2 * size, size), 1 + ring, k, self.orders[k][ring][1])

    def halved(self, ring, k):
        size = self.stream >> (ring + 1)
        self.add(self.path[ring + 1][k], self.ring_buf, (k + 1) * self.stream - 2 * size, size)

    def double(self, ring, k):
        at = self.results(self.path[ring + 1][k], self.stream >> (ring + 1))
        self.send(at, at, 8 - ring, k, self.orders[k][ring][1])

    def step(self):
        step, self.done = self.done, self.done + 1
        started, self.copies = self.copies, []
        if step in (1, 9, 10):
            for copy in started:
                copy().wait()
        if step == 0:
            self.send(self.units(self.work, self.other, self.half), self.units(self.core_buf, 0, self.half), 0, 0, self.partner)
        elif step == 1:
            self.add(self.base, self.core_buf, 0, self.half)
            for k in range(4):
                self.halve(0, k)
        elif step < 9:
            for k in range(4):
                started[k]().wait()
                if step < 6:
                    self.halved(step - 2, k)
                if step < 5:
                    self.halve(step - 1, k)
                    continue
                if step == 5:
                    for u in range(self.stream >> 4):
                        self.out[self.path[4][k] + u] = self.work[self.layer, self.path[4][k] + u]
                self.double(8 - step, k)
        elif step == 9:
            at = self.results(self.base, self.half)
            self.send(at, at, 9, 0, self.partner)


def adjacent_kernel(dims, side, group_size, entries, src_s, dst_s, table_hbm, lens_hbm, embeds_hbm, wq, wk, wv, wo, wu, wd, k_hbm, v_hbm,
                    ya_ref, yb_ref, info_s, last_out,
                    table_s, lens_s, table_v, embeds_v, y_ref, send_buf, got_buf, last_buf, new_buf, work, core_buf, ring_buf, mid_in, mid_out, x_in, plan_v, plan_s, y_other, acc_other, sums_in, half_col, half_row, *rest):
    d = dims
    migs, rest = rest[:d.layers], rest[d.layers:]
    pools, rest = [rest[2 * l:2 * l + 2] for l in range(d.layers)], rest[2 * d.layers:]
    compute, (load_sem, pool_sem, plan_sem, x_send, x_recv, page_send, page_recv, new_send, new_recv, mig_send, mig_recv, out_sem, half_sem, pair_send, pair_recv) = rest[:-15], rest[-15:]
    half = d.rows // 2
    me = lax.axis_index('kv')
    ahead, behind = lax.rem(me + 1, group_size), lax.rem(me + group_size - 1, group_size)
    dec = Decoder(d, 0, d.layers, (wq, wk, wv, wo, wu, wd), y_ref, compute, shared=True)
    dec.y_other, dec.acc_other, dec.half_col, dec.half_row, dec.half_sem = y_other, acc_other, half_col, half_row, half_sem
    exchanges = [Exchange(side, l, work, core_buf, ring_buf, migs[l], mig_send, mig_recv) for l in range(d.layers)]

    def scope(name, run, *args):
        with jax.named_scope(name):
            return run(*args)

    pool_loads = [[pltpu.make_async_copy(src.at[:, l], pools[l][p], pool_sem.at[l, p]) for p, src in enumerate((k_hbm, v_hbm))] for l in range(d.layers)]
    embeds_load, table_load, lens_load, table_load_v = [
        pltpu.make_async_copy(src, dst, load_sem.at[i]) for i, (src, dst) in enumerate(((embeds_hbm, embeds_v), (table_hbm, table_s), (lens_hbm, lens_s), (table_hbm, table_v)))]
    for load in [embeds_load] + pool_loads[0] + [table_load, table_load_v, lens_load]:
        load.start()
    barrier = pltpu.get_barrier_semaphore()

    @pl.loop(1, group_size)
    def _(r):
        pl.semaphore_signal(barrier, inc=1, device_id={'kv': lax.rem(me + r, group_size)})

    scope("barrier", lambda: pl.semaphore_wait(barrier, group_size - 1))

    groups = d.tokens // 8
    splits = group_size // groups
    cols = d.width // splits

    def piece(ref, m):
        return ref.at[m // splits, :, pl.ds(aligned(m % splits * cols, cols), cols)]

    def all_pieces(phase):
        some = mid_in.at[pl.ds(0, group_size - 1)]
        pltpu.make_async_remote_copy(some, some, x_send.at[phase], x_recv.at[phase], device_id={'kv': me}).wait()

    def send_embeddings():
        embeds_load.wait()

        @pl.loop(1, group_size)
        def _(r):
            m = lax.rem(me + r, group_size)
            pltpu.make_async_remote_copy(piece(embeds_v, m), mid_in.at[me], x_send.at[0], x_recv.at[0], device_id={'kv': m}).start()

        mid_in[me] = piece(embeds_v, me)[...]

    def load_tables():
        for load in (table_load, lens_load, table_load_v):
            load.wait()
        return lax.rem(table_s[1, 0] // d.slots + group_size, group_size)

    scope("pool_wait_0", lambda: [load.wait() for load in pool_loads[0]])

    def own(l):
        @pl.loop(0, entries)
        def _(e):
            slot = src_s[e] - me * d.slots
            mine = (slot >= 0) & (slot < d.slots)
            slot = local_slot(src_s[e], me, d.slots)
            for p in PAIR:
                page = pools[l][p][slot]
                work[l, p * entries + e] = jnp.where(mine, page, jnp.zeros_like(page))

    def step(l):
        scope(f"exchange_{l}_{exchanges[l].done}", exchanges[l].step)

    step_0, step_1 = functools.partial(step, 0), functools.partial(step, 1)

    scope("own_0", own, 0)
    step_0()
    for l in range(1, d.layers):
        for load in pool_loads[l]:
            load.start()
    scope("start_stream", dec.start_stream)
    for copy in dec.half_loads(0):
        copy.start()
    shift = scope("load_tables", load_tables)
    home_a = lax.rem(me - shift + group_size, group_size)
    home_b = lax.rem(home_a + 1, group_size)

    def clipped(slot):
        return local_slot(slot, me, d.slots)

    def first_here(l, p, i):
        return pools[l][p][clipped(table_s[0, home_b * d.rows + i])]

    def last_here(l, p, i):
        return pools[l][p][clipped(table_s[1, home_a * d.rows + i])]

    def migrated(l, p, home, i, page):
        entry = plan_s[0, home * d.rows + i]
        return jnp.where(entry >= 0, migs[l][p * entries + jnp.maximum(entry, 0)], page)

    def pack(l):
        @pl.loop(0, half)
        def _(i):
            for p in PAIR:
                send_buf[l, 0, p, i] = first_here(l, p, i)
                send_buf[l, 1, p, i] = last_here(l, p, half + i)

    parts = 4
    size = half // parts

    def page_copy(l, way, p, rows):
        return pltpu.make_async_remote_copy(
            send_buf.at[l, way, p, rows], got_buf.at[l, way, p, rows], page_send.at[l, way, p], page_recv.at[l, way, p], device_id={'kv': (ahead, behind)[way]})

    pieces = [iter([(p, part) for part in range(parts) for p in PAIR]) for _ in range(d.layers)]

    def pages_start(l):
        p, part = next(pieces[l])
        for way in PAIR:
            page_copy(l, way, p, pl.ds(part * size, size)).start()

    pages_0, pages_1 = functools.partial(pages_start, 0), functools.partial(pages_start, 1)

    def pages_wait(l):
        for way in PAIR:
            for p in PAIR:
                page_copy(l, way, p, pl.ds(0, half)).wait()

    def pass_on():
        all_pieces(0)
        later = me // splits * 8 % d.rows // half

        @pl.loop(0, group_size)
        def _(m):
            mid_out[m] = mid_in[lax.rem(m - shift + later + group_size, group_size)]

        @pl.loop(1, group_size)
        def _(r):
            m = lax.rem(me + r, group_size)
            pltpu.make_async_remote_copy(mid_out.at[m], piece(x_in, me), x_send.at[1], x_recv.at[1], device_id={'kv': m}).start()

        piece(x_in, me)[...] = mid_out[me]

    def take_embeddings():
        all_pieces(1)
        y_ref[...] = x_in[...].reshape(d.tokens, d.width)

    plan_copy = pltpu.make_async_copy(plan_v, plan_s, plan_sem)

    def plan():
        seq = iota((1, table_v.shape[1]), 1)
        worker = lax.rem(seq // d.rows + shift, group_size)
        before = lax.rem(worker + group_size - 1, group_size)
        first, last = table_v[0:1, :], table_v[1:2, :]
        bad = (last < worker * d.slots) | (last >= worker * d.slots + d.slots) | (first < before * d.slots) | (first >= before * d.slots + d.slots)

        def entry(e, state):
            plan, bad = state
            return jnp.where(last == dst_s[e], e, plan), bad | (first == dst_s[e]).astype(jnp.int32)

        plan, bad = lax.fori_loop(0, entries, entry, (jnp.full_like(last, -1), bad.astype(jnp.int32)))
        plan_v[...] = plan
        plan_copy.start()
        info_s[0] = shift
        info_s[1] = 1 - jnp.max(bad)

    def new_copies(l):
        return [pltpu.make_async_remote_copy(
            ref.at[pl.ds(g * d.stride + t * d.rows + half, half)], new_buf.at[l, p, g, t], new_send.at[l, p, g, t], new_recv.at[l, p, g, t], device_id={'kv': ahead})
            for p, ref in enumerate((dec.kn_s, dec.vn_s)) for g in range(d.kv_heads) for t in PAIR]

    def project(l):
        dec.project(l)
        for copy in new_copies(l):
            copy.start()

    scope("pack_0", pack, 0)
    step_0()
    scope("send_embeddings", send_embeddings)
    pages_0()
    scope("plan", plan)
    step_0()
    pages_0()
    for l in range(1, d.layers):
        for load in pool_loads[l]:
            load.wait()
    scope("own_1", own, 1)

    def both():
        step_0()
        pages_0()
        step_1()

    both()
    scope("pass_on", pass_on)
    both()
    both()
    scope("pack_1", pack, 1)
    both()
    scope("take_embeddings", take_embeddings)
    both()
    scope("project_0", project, 0)
    both()
    plan_copy.wait()
    step_0()
    step_1()
    step_0()
    scope("pages_wait_0", pages_wait, 0)

    def attend(l, events_a, events_b):
        def put_page(p, i, val):
            last_buf[p, i] = val

        dec.attend(lambda i: lens_s[home_a * d.rows + i], lambda p, i: got_buf[l, 0, p, i],
                   lambda p, i: migrated(l, p, home_a, i, last_here(l, p, i)), put_page, events_a, 0, half)
        dec.attend(lambda i: lens_s[home_b * d.rows + i], lambda p, i: first_here(l, p, i),
                   lambda p, i: migrated(l, p, home_b, i, got_buf[l, 1, p, i - half]), lambda p, i, val: None, events_b, half, half)
        dec.gather_heads()

    def finish_pages(l):
        for copy in new_copies(l):
            copy.wait()

        @pl.loop(0, half)
        def _(i):
            row = half + i
            for p in PAIR:
                page = migrated(l, p, home_a, row, last_here(l, p, row))
                last_buf[p, row] = dec.insert(page, lens_s[home_a * d.rows + row], lambda t, g: new_buf[l, p, g, t, pl.ds(i, 1), :])

        pltpu.make_async_copy(last_buf, last_out.at[l], out_sem).start()

    def last_wait(l):
        pltpu.make_async_copy(last_buf, last_out.at[l], out_sem).wait()

    def event(run):
        return lambda: run()

    def hidden_copy(at):
        return pltpu.make_async_remote_copy(y_ref.at[:, at], y_other.at[:, at], pair_send.at[0], pair_recv.at[0], device_id={'kv': exchanges[0].partner})

    def send_hidden(j):
        hidden_copy(pl.ds(aligned(j * dec.group * CHUNK, CHUNK), dec.group * CHUNK)).start()

    def wait_hidden():
        hidden_copy(pl.ds(0, d.width)).wait()

    def swap_sums():
        copy = pltpu.make_async_remote_copy(acc_other, sums_in, pair_send.at[1], pair_recv.at[1], device_id={'kv': exchanges[0].partner})
        copy.start()
        copy.wait()
        return sums_in[...]

    blocks = half // min(UNROLL, half)
    last_pair = 2 * (dec.whole // MLP_GROUP) - 1
    for l in range(d.layers):
        between_a, between_b, events = (), (), []
        if l:
            scope(f"project_{l}", project, l)
            scope(f"pages_wait_{l}", pages_wait, l)
            last_wait(l - 1)
        else:
            between_a, between_b = [(blocks // 2, event(step_1))], [(0, event(pages_1)), (blocks // 2, event(pages_1))]
            events = [(k * last_pair // 7, event(pages_1)) for k in range(2 * parts - 2)]
            events += [(k * last_pair // 3, event(step_1)) for k in PAIR] + [(last_pair - parts, event(step_1))]
        with jax.named_scope(f"attend_{l}"):
            attend(l, between_a, between_b)
        events += [(last_pair, functools.partial(scope, f"finish_{l}", finish_pages, l))]
        with jax.named_scope(f"mix_{l}"):
            dec.mix_shared(l, send_hidden, wait_hidden, swap_sums, sorted(events, key=lambda event: event[0]))
    for t in PAIR:
        ya_ref[t] = y_ref[pl.ds(t * d.rows, half), :]
        yb_ref[t] = y_ref[pl.ds(t * d.rows + half, half), :]
    last_wait(d.layers - 1)


def decode_adjacent(side, group_size, d, table, seq_lens, mig_src, mig_dst, embeds, weights, k_pool, v_pool):
    entries = mig_src.shape[0]
    half = d.rows // 2
    page = (d.page_rows, d.head_dim)
    struct = lambda *shape: jax.ShapeDtypeStruct(shape, BF16)
    groups = d.tokens // 8
    mid = pltpu.VMEM((group_size, 8, d.width * groups // group_size), BF16)
    return pl.pallas_call(
        functools.partial(adjacent_kernel, d, side, group_size, entries),
        out_shape=[struct(2, half, d.width), struct(2, half, d.width), jax.ShapeDtypeStruct((2,), jnp.int32), struct(d.layers, 2, d.rows, *page)],
        in_specs=[SMEM] * 2 + [ANY] * 11,
        out_specs=[VMEM, VMEM, SMEM, ANY],
        scratch_shapes=[
            pltpu.SMEM(table.shape, jnp.int32),
            pltpu.SMEM(seq_lens.shape, jnp.int32),
            pltpu.VMEM(table.shape, jnp.int32),
            pltpu.VMEM((groups, 8, d.width), BF16),
            pltpu.VMEM((d.tokens, d.width), BF16),
        ] + [pltpu.VMEM((d.layers, 2, 2, half) + page, BF16)] * len(PAIR) + [
            pltpu.VMEM((2, d.rows) + page, BF16),
            pltpu.VMEM((d.layers, 2, d.kv_heads, 2, half, d.head_dim), F32),
            pltpu.VMEM((d.layers, 2 * entries) + page, BF16),
        ] + [pltpu.VMEM((d.layers, entries) + page, BF16)] * len(PAIR) + [
            mid,
            mid,
            pltpu.VMEM((groups, 8, d.width), BF16),
            pltpu.VMEM((1, table.shape[1]), jnp.int32),
            pltpu.SMEM((1, table.shape[1]), jnp.int32),
            pltpu.VMEM((d.tokens, d.width), BF16),
            pltpu.VMEM((d.tokens, d.width), F32),
            pltpu.VMEM((d.tokens, d.width), F32),
            pltpu.VMEM((d.width, HALF), BF16),
            pltpu.VMEM((HALF, d.width), BF16),
        ] + [pltpu.VMEM((2 * entries,) + page, BF16)] * d.layers + [pltpu.VMEM((d.slots,) + page, BF16)] * (2 * d.layers) + d.compute_scratch(8, 6) + [
            DMA((4,)),
            DMA((d.layers, 2)),
            DMA,
        ] + [DMA(shape) for shape in ((2,), (d.layers, 2, 2), (d.layers, 2, d.kv_heads, 2), (d.layers, 10, 4)) for _ in PAIR] + [DMA] + [DMA((2,))] * 3,
        compiler_params=pltpu.CompilerParams(collective_id=1, has_side_effects=True, skip_device_barrier=True, vmem_limit_bytes=LIMIT),
        cost_estimate=d.cost(d.layers),
        name="decode_adjacent",
    )(mig_src, mig_dst, table, seq_lens, embeds.reshape(groups, 8, d.width), *weights, k_pool, v_pool)


def fill_pools_kernel(dims, group_size, info_s, table_s, src_s, k_hbm, v_hbm, last_hbm, k_out, v_out, k_buf, v_buf, sem, put_sem):
    d = dims
    me = lax.axis_index('kv')
    home = lax.rem(me - info_s[0] + group_size, group_size)
    pools = ((k_hbm, k_buf, k_out), (v_hbm, v_buf, v_out))
    parts = sem.shape[1]
    size = d.slots // parts

    def moves(part, out):
        at = pl.ds(part * size, size)
        return [pltpu.make_async_copy(*((buf.at[at], dst.at[at]) if out else (src.at[at], buf.at[at])), sem.at[p, part]) for p, (src, buf, dst) in enumerate(pools)]

    def all_parts(out, run):
        @pl.loop(0, parts)
        def _(part):
            for copy in moves(part, out):
                run(copy)

    start, wait = lambda copy: copy.start(), lambda copy: copy.wait()
    all_parts(False, start)
    all_parts(False, wait)

    @pl.loop(0, d.rows)
    def _(i):
        slot = local_slot(table_s[1, home * d.rows + i], me, d.slots)
        for p, (_, buf, _) in enumerate(pools):
            pltpu.make_async_copy(last_hbm.at[:, p, i], buf.at[slot], put_sem).start()

    @pl.loop(0, src_s.shape[0])
    def _(e):
        slot = src_s[e] - me * d.slots

        @pl.when((slot >= 0) & (slot < d.slots))
        def _():
            for _, buf, _ in pools:
                buf[local_slot(src_s[e], me, d.slots)] = jnp.zeros(buf.shape[1:], buf.dtype)

    for src, buf, _ in pools:
        pltpu.make_async_copy(src.at[pl.ds(0, d.rows)], buf.at[pl.ds(0, d.rows)], put_sem).wait()
    all_parts(True, start)
    all_parts(True, wait)


def fill_pools(group_size, d, info, table, mig_src, k_pool, v_pool, last):
    return pl.pallas_call(
        functools.partial(fill_pools_kernel, d, group_size),
        out_shape=[jax.ShapeDtypeStruct(k_pool.shape, k_pool.dtype)] * 2,
        in_specs=[SMEM] * 3 + [ANY] * 3,
        out_specs=[ANY, ANY],
        scratch_shapes=[pltpu.VMEM(k_pool.shape, k_pool.dtype), pltpu.VMEM(k_pool.shape, k_pool.dtype), DMA((2, 4)), DMA],
        compiler_params=pltpu.CompilerParams(vmem_limit_bytes=LIMIT),
        cost_estimate=d.cost(1),
        name="fill_pools",
    )(info, table, mig_src, k_pool, v_pool, last)


def gather_pages_kernel(idx_ref, k_hbm, v_hbm, k_out, v_out, sem):
    rows = k_out.shape[0]

    def copies(i):
        slot = jnp.maximum(idx_ref[i], 0)
        return (pltpu.make_async_copy(k_hbm.at[slot], k_out.at[i], sem), pltpu.make_async_copy(v_hbm.at[slot], v_out.at[i], sem))

    @pl.loop(0, rows)
    def _(i):
        @pl.when(idx_ref[i] >= 0)
        def _():
            for copy in copies(i):
                copy.start()

        @pl.when(idx_ref[i] < 0)
        def _():
            k_out[i] = jnp.zeros(k_out.shape[1:], k_out.dtype)
            v_out[i] = jnp.zeros(v_out.shape[1:], v_out.dtype)

    @pl.loop(0, rows)
    def _(i):
        @pl.when(idx_ref[i] >= 0)
        def _():
            for copy in copies(i):
                copy.wait()


def gather_pages(idx, k_pool, v_pool):
    shape = jax.ShapeDtypeStruct((idx.shape[0],) + k_pool.shape[1:], k_pool.dtype)
    return pl.pallas_call(
        gather_pages_kernel,
        out_shape=[shape, shape],
        in_specs=[SMEM, ANY, ANY],
        out_specs=[VMEM, VMEM],
        scratch_shapes=[DMA],
        compiler_params=pltpu.CompilerParams(vmem_limit_bytes=LIMIT),
        name="gather_pages",
    )(idx, k_pool, v_pool)


def share_kernel(side, k_hbm, v_hbm, k_out, v_out, work, core_buf, ring_buf, load_sem, send_sem, recv_sem, result):
    entries = k_hbm.shape[0]
    exchange = Exchange(side, 0, work, core_buf, ring_buf, result, send_sem, recv_sem)
    units = [pl.ds(p * entries, entries) for p in PAIR]
    for p, src in enumerate((k_hbm, v_hbm)):
        pltpu.make_async_copy(src, work.at[0].at[units[p]], load_sem.at[p]).start()
    for p, src in enumerate((k_hbm, v_hbm)):
        pltpu.make_async_copy(src, work.at[0].at[units[p]], load_sem.at[p]).wait()
    for _ in range(Exchange.STEPS):
        exchange.step()
    for p, dst in enumerate((k_out, v_out)):
        pltpu.make_async_copy(result.at[units[p]], dst, load_sem.at[p]).start()
    for p, dst in enumerate((k_out, v_out)):
        pltpu.make_async_copy(result.at[units[p]], dst, load_sem.at[p]).wait()


def share(side, mig_k, mig_v):
    entries = mig_k.shape[0]
    page = mig_k.shape[1:]
    return pl.pallas_call(
        functools.partial(share_kernel, side),
        out_shape=[jax.ShapeDtypeStruct(mig_k.shape, BF16)] * 2,
        in_specs=[ANY, ANY],
        out_specs=[ANY, ANY],
        scratch_shapes=[pltpu.VMEM((1, n * entries) + page, BF16) for n in (2, 1, 1)] + [DMA((2,)), DMA((1, 10, 4)), DMA((1, 10, 4)), pltpu.VMEM((2 * entries,) + page, BF16)],
        compiler_params=pltpu.CompilerParams(has_side_effects=True, vmem_limit_bytes=LIMIT),
        name="share",
    )(mig_k, mig_v)


def migrate_kernel(dst_ref, src_ref, k_hbm, v_hbm, mk_hbm, mv_hbm, k_out, v_out, k_buf, v_buf, sem, fix_sem):
    entries = dst_ref.shape[0]
    pairs = ((k_hbm, mk_hbm, k_buf, k_out), (v_hbm, mv_hbm, v_buf, v_out))
    for p, (src, _, buf, _) in enumerate(pairs):
        pltpu.make_async_copy(src, buf, sem.at[p]).start()
    for p, (src, _, buf, _) in enumerate(pairs):
        pltpu.make_async_copy(src, buf, sem.at[p]).wait()

    @pl.loop(0, entries)
    def _(e):
        @pl.when(dst_ref[e] >= 0)
        def _():
            for _, mig, buf, _ in pairs:
                copy = pltpu.make_async_copy(mig.at[e], buf.at[jnp.maximum(dst_ref[e], 0)], fix_sem)
                copy.start()
                copy.wait()

        @pl.when(src_ref[e] >= 0)
        def _():
            for _, _, buf, _ in pairs:
                buf[jnp.maximum(src_ref[e], 0)] = jnp.zeros(buf.shape[1:], buf.dtype)

    for p, (_, _, buf, dst) in enumerate(pairs):
        pltpu.make_async_copy(buf, dst, sem.at[p]).start()
    for p, (_, _, buf, dst) in enumerate(pairs):
        pltpu.make_async_copy(buf, dst, sem.at[p]).wait()


def migrate(dst_local, src_local, k_pool, v_pool, mig_k, mig_v):
    shape = jax.ShapeDtypeStruct(k_pool.shape, k_pool.dtype)
    return pl.pallas_call(
        migrate_kernel,
        out_shape=[shape, shape],
        in_specs=[SMEM, SMEM, ANY, ANY, ANY, ANY],
        out_specs=[ANY, ANY],
        scratch_shapes=[pltpu.VMEM(k_pool.shape, k_pool.dtype), pltpu.VMEM(k_pool.shape, k_pool.dtype), DMA((2,)), DMA],
        compiler_params=pltpu.CompilerParams(vmem_limit_bytes=LIMIT),
        name="migrate",
    )(dst_local, src_local, k_pool, v_pool, mig_k, mig_v)


def decode_kernel(dims, sc_ref, x_ref, p0k_hbm, p0v_hbm, wq, wk, wv, wo, wu, wd, k_in, v_in, y_ref, k_out, v_out,
                  first_buf, last_buf, *rest):
    compute, (page_sem, put_sem) = rest[:-2], rest[-2:]
    d = dims
    dec = Decoder(d, 0, d.layers, (wq, wk, wv, wo, wu, wd), y_ref, compute, 1, 2)
    dec.start_stream()
    y_ref[...] = x_ref[...]
    loads = [pltpu.make_async_copy(src, first_buf.at[p], page_sem.at[p]) for p, src in enumerate((p0k_hbm, p0v_hbm))]
    for load in loads:
        load.start()

    def last_loads(run):
        @pl.loop(0, d.rows)
        def _(i):
            for p, src in enumerate((k_in, v_in)):
                run(pltpu.make_async_copy(src.at[sc_ref[0, i]], last_buf.at[p, i], page_sem.at[2]))

    def puts(run):
        @pl.loop(0, d.rows)
        def _(i):
            @pl.when(sc_ref[2, i] > 0)
            def _():
                for p, dst in enumerate((k_out, v_out)):
                    run(pltpu.make_async_copy(last_buf.at[p, i], dst.at[sc_ref[0, i]], put_sem))

    last_loads(lambda copy: copy.start())
    for load in loads:
        load.wait()
    last_loads(lambda copy: copy.wait())

    @pl.loop(0, d.layers)
    def _(layer):
        def put_page(p, i, val):
            last_buf[p, i, layer] = val

        dec.project(layer)
        dec.attend(lambda i: sc_ref[1, i], lambda p, i: first_buf[p, i, layer], lambda p, i: last_buf[p, i, layer], put_page)
        dec.gather_heads()
        dec.mix(layer)

    puts(lambda copy: copy.start())
    puts(lambda copy: copy.wait())


def decode(d, scalars, x, p0k, p0v, weights, k_pool, v_pool):
    pool = jax.ShapeDtypeStruct(k_pool.shape, k_pool.dtype)
    pages = pltpu.VMEM((2, d.rows, d.layers, d.page_rows, d.head_dim), BF16)
    return pl.pallas_call(
        functools.partial(decode_kernel, d),
        out_shape=[jax.ShapeDtypeStruct(x.shape, x.dtype), pool, pool],
        in_specs=[SMEM, VMEM] + [ANY] * 10,
        out_specs=[VMEM, ANY, ANY],
        input_output_aliases={10: 1, 11: 2},
        scratch_shapes=[pages, pages] + d.compute_scratch(16, 16) + [DMA((3,)), DMA],
        compiler_params=pltpu.CompilerParams(vmem_limit_bytes=LIMIT),
        cost_estimate=d.cost(d.layers),
        name="decode",
    )(scalars, x, p0k, p0v, *weights, k_pool, v_pool)


def permute(arrays, shift, group_size):
    perm = [(i, (i + shift) % group_size) for i in range(group_size)]
    return jax.tree.map(lambda a: lax.ppermute(a, 'kv', perm), arrays) if shift else arrays


def rotate_back(first, second, shift, group_size, beside):
    def branch(r):
        def run(args):
            parts = permute(args[0], -r % group_size, group_size), permute(args[1], (1 - r) % group_size, group_size)
            return jnp.concatenate(parts, axis=1), beside()

        return run

    return lax.switch(shift, [branch(r) for r in range(group_size)], (first, second))


def rotate(arrays, shift, group_size):
    stride = math.isqrt(2 * group_size)
    for count, move in ((shift // stride, stride), (shift % stride, 1)):
        arrays = lax.fori_loop(0, count, lambda _, a: permute(a, move, group_size), arrays)
    return arrays


def solution(mesh):
    group_size = mesh.shape['kv']
    side = math.isqrt(group_size // 2)
    pool_spec = P(('rep', 'kv'))
    tok_spec = P(None, ('rep', 'kv'), None)

    def device_fn(embeds, w_query, w_key, w_value, w_out, w_up, w_down, k_pool5, v_pool5, new_table, seq_lens, mig_src, mig_dst):
        me = lax.axis_index('kv')
        slots, layers, page, kv_heads, head_dim = k_pool5.shape
        rows, width = embeds.shape[1:]
        weights = (w_query, w_key, w_value, w_out, w_up, w_down)
        k_pool = k_pool5.reshape(slots, layers, page * kv_heads, head_dim)
        v_pool = v_pool5.reshape(slots, layers, page * kv_heads, head_dim)
        d = Dims(rows, weights, k_pool, page)
        ints = jnp.int32

        def local(ids):
            loc = ids - me * slots
            return jnp.where((loc >= 0) & (loc < slots), loc, -1)

        def take(vec, dev):
            return lax.dynamic_slice(vec, (dev * rows,), (rows,))

        def inside(ids):
            return local_slot(ids, me, slots)

        def general_path():
            first_new, last_new = new_table[:, 0], new_table[:, 1]
            moved = first_new[None, :] == mig_dst[:, None]
            first_old = jnp.where(jnp.any(moved, axis=0), jnp.sum(jnp.where(moved, mig_src[:, None], 0), axis=0), first_new)
            home = jnp.arange(first_new.shape[0], dtype=ints) // rows
            worker = last_new // slots
            shift_of = (worker - home + group_size) % group_size
            first_shift = (worker - first_old // slots + group_size) % group_size
            shift_ids = jnp.arange(group_size, dtype=ints)
            wanted = jnp.any(shift_of[None, :] == shift_ids[:, None], axis=1)
            mig_k, mig_v = gather_pages(local(mig_src), k_pool, v_pool)
            by_layer = tuple(m.swapaxes(0, 1) for m in (mig_k, mig_v))
            mig_k, mig_v = (m.swapaxes(0, 1) for m in lax.map(lambda pages: tuple(share(side, *pages)), by_layer))
            k_new, v_new = migrate(local(mig_dst), local(mig_src), k_pool, v_pool, mig_k, mig_v)

            def one_round(shift, y, k_new, v_new):
                src_home = (me - shift + group_size) % group_size
                x = rotate(embeds.reshape(2 * rows, width), shift, group_size)
                in_round = shift_of == shift
                wanted2 = jnp.any(in_round[None, :] & (first_shift[None, :] == shift_ids[:, None]), axis=1)

                def more(state):
                    left, pk, pv = state
                    shift2 = jnp.argmax(left).astype(ints)
                    dest_home = (me + shift2 - shift + group_size) % group_size
                    got = gather_pages(inside(take(first_old, dest_home)), k_pool, v_pool)
                    got_k, got_v = rotate(tuple(got), shift2, group_size)
                    mine = (take(first_shift, src_home) == shift2)[:, None, None, None]
                    return left & (shift_ids != shift2), jnp.where(mine, got_k, pk), jnp.where(mine, got_v, pv)

                zeros = jnp.zeros((rows,) + k_pool.shape[1:], k_pool.dtype)
                _, pk, pv = lax.while_loop(lambda state: jnp.any(state[0]), more, (wanted2, zeros, zeros))
                valid = take(shift_of, src_home) == shift
                scalars = jnp.stack([inside(take(last_new, src_home)), take(seq_lens, src_home), valid.astype(ints)])
                out, k_new, v_new = decode(d, scalars, x, pk, pv, weights, k_new, v_new)
                back = rotate(out, (group_size - shift) % group_size, group_size)
                mine = (take(shift_of, me) == shift)[None, :, None]
                return jnp.where(mine, back.reshape(embeds.shape), y), k_new, v_new

            def next_round(state):
                left, y, k_new, v_new = state
                shift = jnp.argmax(left).astype(ints)
                y, k_new, v_new = one_round(shift, y, k_new, v_new)
                return left & (shift_ids != shift), y, k_new, v_new

            _, y, k_new, v_new = lax.while_loop(lambda state: jnp.any(state[0]), next_round, (wanted, jnp.zeros_like(embeds), k_new, v_new))
            return y, k_new, v_new

        table = new_table.T
        ya, yb, info, last = decode_adjacent(side, group_size, d, table, seq_lens, mig_src, mig_dst, embeds, weights, k_pool, v_pool)
        y, (k_new, v_new) = rotate_back(ya, yb, info[0], group_size, lambda: fill_pools(group_size, d, info, table, mig_src, k_pool, v_pool, last))
        _, y, k_new, v_new = lax.while_loop(lambda state: state[0] == 0, lambda state: (jnp.ones_like(state[0]),) + general_path(), (info[1], y, k_new, v_new))
        return y, k_new.reshape(k_pool5.shape), v_new.reshape(v_pool5.shape)

    return jax.shard_map(device_fn, mesh=mesh, in_specs=(tok_spec, P(), P(), P(), P(), P(), P(), pool_spec, pool_spec, P('rep', None), P('rep'), P('rep'), P('rep')), out_specs=(tok_spec, pool_spec, pool_spec), check_vma=False)
```
